32 devices in a mesh: dp: 16 (over z, y, core), cp: 2 (over x).
Axes of the slice: x: 2, y: 2, z: 4, core: 2. Of those that a mesh axis runs over, the one named last changes fastest.
Arguments:
- x_source: bfloat16 [16, 1024, 768], P(None, ('cp', 'dp')), may hold values from -6 to 6
- cotangent: bfloat16 [16, 1024, 768], P('dp', 'cp'), may hold values from -6 to 6
- lengths: int32 [16], replicated, may hold values from 1 to 1024, 10240 in all
- dealing: int32 [16], replicated, may hold values from 0 to 15, each once
- qkv_weight: float32 [768, 2304], P('cp', 'dp'), may hold values from -0.21875 to 0.21875
- proj_weight: float32 [768, 768], P('cp', 'dp'), may hold values from -2 to 2
- up_weight: float32 [768, 3072], P('cp', 'dp'), may hold values from -0.21875 to 0.21875
- down_weight: float32 [3072, 768], P('cp', 'dp'), may hold values from -0.109375 to 0.109375
- first_gain: float32 [768], P('dp'), may hold values from 0.1 to 1.9
- first_shift: float32 [768], P('dp'), may hold values from -1.75 to 1.75
- proj_bias: float32 [768], P('dp'), may hold values from -1.75 to 1.75
- second_gain: float32 [768], P('dp'), may hold values from 0.1 to 1.9
- second_shift: float32 [768], P('dp'), may hold values from -1.75 to 1.75
- up_bias: float32 [3072], P('dp'), may hold values from -3 to 3
- down_bias: float32 [768], P('dp'), may hold values from -1.75 to 1.75
Outputs:
- output: bfloat16 [16, 1024, 768], P('dp', 'cp')
- input_grad: bfloat16 [16, 1024, 768], P(None, ('cp', 'dp'))
- qkv_grad: float32 [768, 2304], P('cp', 'dp')
- proj_grad: float32 [768, 768], P('cp', 'dp')
- up_grad: float32 [768, 3072], P('cp', 'dp')
- down_grad: float32 [3072, 768], P('cp', 'dp')
- first_gain_grad: float32 [768], P('dp')
- first_shift_grad: float32 [768], P('dp')
- proj_bias_grad: float32 [768], P('dp')
- second_gain_grad: float32 [768], P('dp')
- second_shift_grad: float32 [768], P('dp')
- up_bias_grad: float32 [3072], P('dp')
- down_bias_grad: float32 [768], P('dp')
The draws below stay inside these ranges and needn't reach their ends.
Inputs may be any that keep to these rules, and one draw needn't show every extreme that they name: The lengths sum to 10240 and the longest is exactly 1024. `dealing`: a permutation of the sequence numbers.
All inputs are finite; a program needn't handle non-finite values.
Results may differ from the reference program's by a relative error of at most 0.019.
Values may be sent and summed in bfloat16 or wider, within the bound.
A program may use at most 192 MiB of HBM per device.

```python
import math
import jax
import jax.numpy as jnp
import numpy as np
from jax import lax

D = 768
HEADS = 12
HEAD_DIM = 64
FF = 3072
LEN = 1024
SEQS = 16


def block_scale(rng, shape, split, low, largest):
    level, own = 1.0, jax.random.fold_in(rng, 6)
    for dim, parts in split:
        steps = jnp.exp(jax.random.uniform(jax.random.fold_in(own, dim), (parts,), jnp.float32, low / len(split), largest / len(split)))
        level = level * jnp.repeat(steps, shape[dim] // parts).reshape([-1 if axis == dim else 1 for axis in range(len(shape))])
    return level


def length_profile(count, total, limit, skew):
    weights = [(1 << 20) // math.isqrt(grade ** skew) + 1 for grade in range(2, count + 1)]
    spare, holding = total - limit - (count - 1), [1] * (count - 1)
    while spare > 0:
        free = [i for i in range(count - 1) if holding[i] < limit]
        whole, remaining = sum([weights[i] for i in free]), spare
        for i in free:
            more = min(limit - holding[i], max(1, remaining * weights[i] // whole), spare)
            holding[i] = holding[i] + more
            spare = spare - more
    return np.array([limit] + holding)


def ragged(key, count, total, bound, slope):
    if count == 2:
        one = jax.random.randint(key, (), max(1, total - bound), min(bound, total - 1) + 1)
        return jnp.stack([one, total - one])
    tallies = jnp.asarray(length_profile(count, total, bound, slope), jnp.int32)
    couples = (count - 1) // 2
    giver, receiver = tallies[1:1 + 2 * couples:2], tallies[2:2 + 2 * couples:2]
    margin = jnp.minimum(giver - 1, bound - receiver)
    moved = jax.random.randint(jax.random.fold_in(key, 1), (couples,), 0, 1 << 20) % (margin + 1)
    tallies = tallies.at[1:1 + 2 * couples:2].set(giver - moved).at[2:2 + 2 * couples:2].set(receiver + moved)
    return tallies[jax.random.permutation(jax.random.fold_in(key, 2), count)]


def bell_draw(key, extent, scale, limit, shards=(), held_as=jnp.bfloat16):
    values = jax.random.normal(key, extent, jnp.float32) * scale
    if len(shards) > 0:
        values = block_scale(key, extent, shards, -0.22, 0.18) * values
    return jnp.clip(values, min=-limit, max=limit).astype(held_as)


def setup_inputs(seed: int = 0) -> dict:
    streams_of = jax.random.split(jax.random.key(seed), 16)
    x_source = bell_draw(streams_of[0], (SEQS, LEN, D), 1.0, 6.0, ((1, 32),))
    cotangent = bell_draw(streams_of[1], (SEQS, LEN, D), 1.0, 6.0, ((0, 16), (1, 2)))
    lengths = ragged(streams_of[2], SEQS, SEQS * LEN * 5 // 8, LEN, 1).astype(jnp.int32)
    dealing = jax.random.permutation(streams_of[3], SEQS).astype(jnp.int32)
    qkv_weight = bell_draw(streams_of[4], (D, 3 * D), D ** -0.5, 0.21875, ((0, 2), (1, 16)), jnp.float32)
    proj_weight = bell_draw(streams_of[5], (D, D), (max(1, D // 100)) ** -0.5, 2.0, ((0, 2), (1, 16)), jnp.float32)
    up_weight = bell_draw(streams_of[6], (D, FF), D ** -0.5, 0.21875, ((0, 2), (1, 16)), jnp.float32)
    down_weight = bell_draw(streams_of[7], (FF, D), FF ** -0.5, 0.109375, ((0, 2), (1, 16)), jnp.float32)
    first_gain = jnp.clip(1.0 + 0.18 * jax.random.normal(streams_of[8], (D,), jnp.float32), 0.1, 1.9)
    first_shift = bell_draw(streams_of[9], (D,), 0.3, 1.75, ((0, 16),), jnp.float32)
    proj_bias = bell_draw(streams_of[10], (D,), 0.3, 1.75, ((0, 16),), jnp.float32)
    second_gain = jnp.clip(1.0 + 0.18 * jax.random.normal(streams_of[11], (D,), jnp.float32), 0.1, 1.9)
    second_shift = bell_draw(streams_of[12], (D,), 0.3, 1.75, ((0, 16),), jnp.float32)
    up_bias = bell_draw(streams_of[13], (FF,), 0.5, 3.0, ((0, 16),), jnp.float32)
    down_bias = bell_draw(streams_of[14], (D,), 0.3, 1.75, ((0, 16),), jnp.float32)
    return dict(x_source=x_source, cotangent=cotangent, lengths=lengths, dealing=dealing, qkv_weight=qkv_weight, proj_weight=proj_weight, up_weight=up_weight, down_weight=down_weight, first_gain=first_gain, first_shift=first_shift, proj_bias=proj_bias, second_gain=second_gain, second_shift=second_shift, up_bias=up_bias, down_bias=down_bias)


EPSILON = 1e-05
NEG_BIG = -1e+30
TANH_SCALE = 0.7978845608028654
CUBIC_TERM = 0.044715

@jax.custom_vjp
def low(v):
    return lax.optimization_barrier(v.astype(jnp.bfloat16)).astype(jnp.float32)

@jax.custom_vjp
def low_back(v):
    return v

def low_keep(v):
    return (low(v), None)

def low_pass(kept, grad):
    return (grad,)

def back_keep(v):
    return (v, None)

def back_low(kept, grad):
    return (low(grad),)
low.defvjp(low_keep, low_pass)
low_back.defvjp(back_keep, back_low)

def layer_norm(values, scaling, offset):
    centered = values - lax.optimization_barrier(jnp.mean(values, axis=-1, keepdims=True))
    spread = lax.optimization_barrier(jnp.mean(centered * centered, axis=-1, keepdims=True))
    return centered * lax.rsqrt(spread + EPSILON) * scaling + offset

def gelu_tanh(values):
    return 0.5 * values * (1.0 + jnp.tanh(TANH_SCALE * (values + CUBIC_TERM * values * values * values)))

def block_forward(inputs, length, qkv_weight, proj_weight, up_weight, down_weight, first_gain, first_shift, proj_bias, second_gain, second_shift, up_bias, down_bias):
    highest = lax.Precision.HIGHEST
    row_count = inputs.shape[0]
    act_one = low(layer_norm(inputs, low(first_gain), low(first_shift)))
    mixed_rows = low_back(low(jnp.dot(act_one, low(qkv_weight), precision=highest)))
    queries = mixed_rows[:, :D].reshape(row_count, HEADS, HEAD_DIM)
    key_rows = mixed_rows[:, D:2 * D].reshape(row_count, HEADS, HEAD_DIM)
    val_rows = mixed_rows[:, 2 * D:].reshape(row_count, HEADS, HEAD_DIM)
    scores = jnp.einsum('qhd,khd->hqk', queries, key_rows, precision=highest) * HEAD_DIM ** (-0.5)
    places = jnp.arange(row_count)
    scores = low_back(jnp.where(places[None, :] <= places[:, None], scores, NEG_BIG))
    row_top = lax.optimization_barrier(jnp.max(scores, axis=-1, keepdims=True))
    exponent = jnp.exp(scores - row_top)
    weights = exponent / lax.optimization_barrier(jnp.sum(exponent, axis=-1, keepdims=True))
    attended = jnp.einsum('hqk,khd->qhd', low(weights), val_rows, precision=highest).reshape(row_count, D)
    attended = low_back(low(attended))
    residual = inputs + low_back(jnp.dot(attended, low(proj_weight), precision=highest)) + low(proj_bias)
    act_two = low(layer_norm(residual, low(second_gain), low(second_shift)))
    up_raw = low_back(jnp.dot(act_two, low(up_weight), precision=highest) + low(up_bias))
    hidden = low(gelu_tanh(up_raw))
    result = residual + jnp.dot(hidden, low(down_weight), precision=highest) + low(down_bias)
    return jnp.where(places[:, None] < length, result, 0.0)

def reference(x_source, cotangent, lengths, dealing, qkv_weight, proj_weight, up_weight, down_weight, first_gain, first_shift, proj_bias, second_gain, second_shift, up_bias, down_bias):
    owners = jnp.argsort(dealing).astype(jnp.int32)
    x_slots = x_source[owners]
    len_slots = lengths[owners]
    params = (qkv_weight, proj_weight, up_weight, down_weight, first_gain, first_shift, proj_bias, second_gain, second_shift, up_bias, down_bias)

    def one_sequence(totals, item):
        x_one, length, grad_one = item
        result, back = jax.vjp(lambda inputs, *weights: block_forward(inputs, length, *weights), x_one.astype(jnp.float32), *params)
        grads = back(grad_one.astype(jnp.float32))
        totals = tuple((former + latter for former, latter in zip(totals, grads[1:])))
        return (totals, (result.astype(jnp.bfloat16), grads[0].astype(jnp.bfloat16)))
    zeros = tuple((jnp.zeros_like(param) for param in params))
    totals, (output, grad_slots) = lax.scan(one_sequence, zeros, (x_slots, len_slots, cotangent))
    input_grad = grad_slots[dealing]
    return (output, input_grad, totals[0], totals[1], totals[2], totals[3], totals[4], totals[5], totals[6], totals[7], totals[8], totals[9], totals[10])
```

```python
import functools
import math

import jax
import jax.numpy as jnp
from jax import lax
from jax.experimental import pallas as pl
from jax.experimental.pallas import tpu as pltpu
from jax.sharding import PartitionSpec as P

HEADS = 12
HEAD_DIM = 64


EPSILON = 1e-05
NEG_BIG = -1e30
TANH_SCALE = 0.7978845608028654
CUBIC_TERM = 0.044715
MESH_IDS = pl.DeviceIdType.MESH
BF = jnp.bfloat16
F32 = jnp.float32

Z, Y, C, X = 4, 2, 2, 2


def mult(value, n):
    return value if isinstance(value, int) else pl.multiple_of(value, n)


def coords():
    d = lax.axis_index("dp")
    x = lax.axis_index("cp")
    return d // (Y * C), (d // C) % Y, d % C, x, d


def dev(z, y, c, x):
    return {"dp": (z * Y + y) * C + c, "cp": x}


def rcopy(src, dst, ssem, rsem, where):
    return pltpu.make_async_remote_copy(
        src_ref=src, dst_ref=dst, send_sem=ssem, recv_sem=rsem, device_id=where, device_id_type=MESH_IDS
    )


def wait_bytes(ref, sem):
    pltpu.make_async_copy(ref, ref, sem).wait()


def enter(everyone):
    d = lax.axis_index("dp")
    x = lax.axis_index("cp")
    barrier = pltpu.get_barrier_semaphore()

    def greet(k, carry):
        kd = k // X
        kx = k % X

        @pl.when(jnp.logical_or(kd != d, kx != x))
        def _():
            pl.semaphore_signal(barrier, inc=1, device_id={"dp": kd, "cp": kx}, device_id_type=MESH_IDS)

        return carry

    lax.fori_loop(0, everyone, greet, 0)
    pl.semaphore_wait(barrier, everyone - 1)


def dot_nn(a, b):
    return lax.dot_general(a, b, (((1,), (0,)), ((), ())), preferred_element_type=F32)


def dot_nt(a, b):
    return lax.dot_general(a, b, (((1,), (1,)), ((), ())), preferred_element_type=F32)


def dot_tn(a, b):
    return lax.dot_general(a, b, (((0,), (0,)), ((), ())), preferred_element_type=F32)


def norm_parts(v):
    mean = jnp.mean(v, axis=-1, keepdims=True)
    cen = v - mean
    var = jnp.mean(cen * cen, axis=-1, keepdims=True)
    rstd = lax.rsqrt(var + EPSILON)
    return cen * rstd, rstd


def live_length(len_ref, deal_ref, slot):
    total = jnp.int32(0)
    for s in range(len_ref.shape[0]):
        total = total + jnp.where(deal_ref[s] == slot, len_ref[s], 0)
    return total


class Piece:
    def __init__(self, full, shard, R, r0, rn, step, c0, cn):
        self.full, self.shard = full, shard
        self.R, self.r0, self.rn, self.step, self.c0, self.cn = R, r0, rn, step, c0, cn

    def at(self, z, y, c, x):
        d = (z * Y + y) * C + c
        return self.full.at[
            pl.ds(mult(d * self.R + self.r0, 16), self.rn), pl.ds(mult(x * self.step + self.c0, 128), self.cn)
        ]

    def own(self):
        return self.shard.at[pl.ds(self.r0, self.rn), pl.ds(self.c0, self.cn)]


class Gather:
    LOC, ZS, ZR, S2, R2, S3, R3, S4, R4 = range(9)

    def __init__(self, piece, sems, k, dummy, where):
        self.p, self.sems, self.k, self.dummy = piece, sems, k, dummy
        z, y, c, x, _ = where
        self.z, self.y, self.c, self.x = z, y, c, x
        self.y2, self.x2 = (y + 1 - c) % 2, (x + c) % 2
        self.y3, self.x3 = (y + c) % 2, (x + 1 - c) % 2

    def sem(self, which):
        return self.sems.at[self.k, which]

    def wait(self, count, which):
        p = self.p
        wait_bytes(self.dummy.at[pl.ds(0, count * p.rn), pl.ds(0, p.cn)], self.sem(which))

    def start(self):
        p, z, y, c, x = self.p, self.z, self.y, self.c, self.x
        pltpu.make_async_copy(p.own(), p.at(z, y, c, x), self.sem(self.LOC)).start()
        for dz in range(1, Z):
            z2 = (z + dz) % Z
            rcopy(p.own(), p.at(z, y, c, x), self.sem(self.ZS), self.sem(self.ZR), dev(z2, y, c, x)).start()

    def tick2(self):
        p, z, y, c, x = self.p, self.z, self.y, self.c, self.x
        self.wait(1, self.LOC)
        self.wait(Z - 1, self.ZR)
        for zz in range(Z):
            q = p.at(zz, y, c, x)
            rcopy(q, q, self.sem(self.S2), self.sem(self.R2), dev(z, self.y2, c, self.x2)).start()
        for zz in range(Z):
            q = p.at(zz, y, c, x)
            rcopy(q, q, self.sem(self.S3), self.sem(self.R3), dev(z, self.y3, c, self.x3)).start()
            rcopy(q, q, self.sem(self.S4), self.sem(self.R4), dev(z, y, 1 - c, x)).start()

    def tick3(self):
        p, z, y, c, x = self.p, self.z, self.y, self.c, self.x
        self.wait(Z, self.R2)
        for zz in range(Z):
            q = p.at(zz, self.y2, c, self.x2)
            rcopy(q, q, self.sem(self.S3), self.sem(self.R3), dev(z, self.y3, c, self.x3)).start()
            rcopy(q, q, self.sem(self.S4), self.sem(self.R4), dev(z, y, 1 - c, x)).start()

    def tick4(self):
        p, z, y, c, x = self.p, self.z, self.y, self.c, self.x
        self.wait(2 * Z, self.R3)
        for zz in range(Z):
            for which in range(2):
                yy = which * (1 - c) + (1 - y) * c
                xx = (1 - x) * (1 - c) + which * c
                q = p.at(zz, yy, c, xx)
                rcopy(q, q, self.sem(self.S4), self.sem(self.R4), dev(z, y, 1 - c, x)).start()

    def tick5(self):
        self.wait(4 * Z, self.R4)

    def drain(self):
        self.wait(Z - 1, self.ZS)
        self.wait(Z, self.S2)
        self.wait(2 * Z, self.S3)
        self.wait(4 * Z, self.S4)


class Vectors:
    LOC, ZS, ZR, S2, R2, S4, R4 = range(7)

    def __init__(self, full, shard, sems, where):
        self.full, self.shard, self.sems, self.where = full, shard, sems, where

    def at(self, z, y, c):
        return self.full.at[(z * Y + y) * C + c]

    def start(self):
        z, y, c, x, _ = self.where
        pltpu.make_async_copy(self.shard, self.at(z, y, c), self.sems.at[self.LOC]).start()
        for dz in range(1, Z):
            z2 = (z + dz) % Z
            rcopy(self.shard, self.at(z, y, c), self.sems.at[self.ZS], self.sems.at[self.ZR], dev(z2, y, c, x)).start()

    def wait(self, count, which):
        wait_bytes(self.full.at[pl.ds(0, count)], self.sems.at[which])

    def tick2(self):
        z, y, c, x, _ = self.where
        self.wait(1, self.LOC)
        self.wait(Z - 1, self.ZR)
        for zz in range(Z):
            q = self.at(zz, y, c)
            rcopy(q, q, self.sems.at[self.S2], self.sems.at[self.R2], dev(z, 1 - y, c, x)).start()
            rcopy(q, q, self.sems.at[self.S4], self.sems.at[self.R4], dev(z, y, 1 - c, x)).start()

    def tick3(self):
        z, y, c, x, _ = self.where
        self.wait(Z, self.R2)
        for zz in range(Z):
            q = self.at(zz, 1 - y, c)
            rcopy(q, q, self.sems.at[self.S4], self.sems.at[self.R4], dev(z, y, 1 - c, x)).start()

    def tick4(self):
        self.wait(2 * Z, self.R4)

    def drain(self):
        self.wait(Z - 1, self.ZS)
        self.wait(Z, self.S2)
        self.wait(2 * Z, self.S4)


G1, C1, BP, G2, C2, BD, BU = range(7)


def gather_chunks(wq, wp, wu, wd, sq, sp, su, sd):
    rq, rp, ru, rd = sq.shape[0], sp.shape[0], su.shape[0], sd.shape[0]
    half, wide = sq.shape[1], sd.shape[1]
    out = []
    for k in range(3):
        out.append(Piece(wq, sq, rq, k * (rq // 3), rq // 3, half, 0, half))
    out.append(Piece(wp, sp, rp, 0, rp, half, 0, half))
    for k in range(4):
        out.append(Piece(wu, su, ru, k * (ru // 4), ru // 4, half, 0, half))
    for k in range(4):
        out.append(Piece(wd, sd, rd, 0, rd, wide, k * (wide // 4), wide // 4))
    return out


N_GATHER = 12


def forward_kernel(
    len_ref, deal_ref, xg, cot, sq, sp, su, sd, sv,
    wq_o, wp_o, wu_o, wd_o, xr_o, gw_o, qs_o, ka_o, va_o, at_o, lse_o, r_o, a2_o, hd_o, gp_o, vec_o, out_o,
    wq, wp, wu, wd, xr, a1, qs, ka, va, at, lse, r, a2, hd, gp, vg, vec, bu3, sc0, sc1, outw,
    gsem, vsem, msem, osem,
):
    where = coords()
    z, y, c, x, d = where
    width = xr.shape[1]
    rows = xr.shape[0]
    qrows = rows // 2
    small = xg.shape[1]
    pairs = width // 128
    tile = 256

    enter(Z * Y * C * X)

    vectors = Vectors(vg, sv, vsem, where)
    vectors.start()
    per_quarter = qrows // small
    place = mult(x * qrows + (d % per_quarter) * small, 16)
    core_to = (x + d // per_quarter) % 2
    dst = xr.at[pl.ds(place, small)]

    def deal_out(t, carry):
        td = (t // 2) * 2 + core_to
        tx = t % 2
        mine = jnp.logical_and(td == d, tx == x)

        @pl.when(mine)
        def _():
            pltpu.make_async_copy(xg.at[t], dst, msem.at[1]).start()

        @pl.when(jnp.logical_not(mine))
        def _():
            rcopy(xg.at[t], dst, msem.at[0], msem.at[1], {"dp": td, "cp": tx}).start()

        return carry

    lax.fori_loop(0, xg.shape[0], deal_out, 0)
    chunks = [
        Gather(p, gsem, k, wu, where) for k, p in enumerate(gather_chunks(wq, wp, wu, wd, sq, sp, su, sd))
    ]
    for ch in chunks:
        ch.start()

    vectors.tick2()
    vectors.tick3()

    order = []
    for s in range(len(chunks) + 2):
        for back, name in ((0, "tick2"), (1, "tick3"), (2, "tick4")):
            if 0 <= s - back < len(chunks):
                order.append((s - back, name))
    pending = [getattr(chunks[k], name) for k, name in order]

    def run(n):
        for _ in range(n):
            if pending:
                pending.pop(0)()

    vectors.tick4()

    def add_table(k, acc):
        return acc + vg[k].astype(F32)

    vec[...] = lax.fori_loop(1, Z * Y * C, add_table, vg[0].astype(F32))
    for k in range(bu3.shape[0]):
        per = width // tile
        bu3[k] = vec[BU + k // per:BU + k // per + 1, (k % per) * tile:(k % per + 1) * tile]

    wait_bytes(xr, msem.at[1])
    lrows = 128

    def first_norm(k, carry):
        at_rows = pl.ds(mult(k * lrows, lrows), lrows)
        n1, _ = norm_parts(xr[at_rows, :].astype(F32))
        a1[at_rows, :] = (n1 * vec[G1:G1 + 1, :] + vec[C1:C1 + 1, :]).astype(BF)
        return carry

    lax.fori_loop(0, rows // lrows, first_norm, 0)

    run(13)
    for k in range(3):
        chunks[k].tick5()
    keep = [pltpu.make_async_copy(wq, wq_o, osem.at[0])]
    keep[-1].start()

    def cot_copy(b):
        return (x + b) % 2, cot.at[pl.ds(b * qrows, qrows)], gw_o.at[pl.ds(mult(x * qrows, qrows), qrows)]

    for b in range(2):
        core_b, src_b, dst_b = cot_copy(b)
        same = jnp.logical_and(core_b == c, c == x)

        @pl.when(same)
        def _(src_b=src_b, dst_b=dst_b):
            pltpu.make_async_copy(src_b, dst_b, msem.at[3]).start()

        @pl.when(jnp.logical_not(same))
        def _(src_b=src_b, dst_b=dst_b, core_b=core_b):
            rcopy(src_b, dst_b, msem.at[2], msem.at[3], dev(z, y, core_b, c)).start()

    quarters = (c, 3 - c)

    def q_at(i):
        return pl.ds(mult(quarters[i] * qrows, qrows), qrows)

    steps = width // tile
    for part in range(3):
        def project(n, carry, part=part):
            lanes = pl.ds(mult(n * tile, tile), tile)
            res = dot_nt(a1[...], wq[pl.ds(mult(part * width + n * tile, tile), tile), :]).astype(BF)
            if part == 0:
                qs[:, lanes] = res * jnp.asarray(HEAD_DIM ** -0.5, BF)
            else:
                to = ka if part == 1 else va
                for i in range(2):
                    to[q_at(i), lanes] = res[i * qrows:(i + 1) * qrows]
            return carry

        lax.fori_loop(0, steps, project, 0)
        if part > 0:
            to = ka if part == 1 else va
            for i in range(2):
                rcopy(to.at[q_at(i)], to.at[q_at(i)], msem.at[4 + 2 * (part - 1)], msem.at[5 + 2 * (part - 1)], dev(z, y, 1 - c, x)).start()
        run(1)
    wait_bytes(ka.at[pl.ds(0, rows)], msem.at[5])
    wait_bytes(va.at[pl.ds(0, rows)], msem.at[7])
    for src, out, s in ((qs, qs_o, 1), (ka, ka_o, 2), (va, va_o, 3), (xr, xr_o, 4), (vec, vec_o, 5)):
        keep.append(pltpu.make_async_copy(src, out, osem.at[s]))
        keep[-1].start()

    lane = lax.broadcasted_iota(jnp.int32, (qrows, 128), 1)
    kpos = lax.broadcasted_iota(jnp.int32, (qrows, qrows), 0)
    qpos = lax.broadcasted_iota(jnp.int32, (qrows, qrows), 1)
    groups = qrows // 8

    def pair_body(p, carry):
        lanes = pl.ds(mult(p * 128, 128), 128)
        for i in range(2):
            quarter = quarters[i]
            qp = qs[i * qrows:(i + 1) * qrows, lanes]
            zero = jnp.zeros_like(qp)
            qh = (jnp.where(lane < HEAD_DIM, qp, zero), jnp.where(lane >= HEAD_DIM, qp, zero))

            def scores(j, tops):
                at_keys = pl.ds(mult(j * qrows, qrows), qrows)
                kj = ka[at_keys, lanes]
                keep_it = jnp.logical_or(kpos <= qpos, j < quarter)
                new = []
                for h, sc in enumerate((sc0, sc1)):
                    s = jnp.where(keep_it, dot_nt(kj, qh[h]), NEG_BIG)
                    sc[at_keys, :] = s
                    new.append(jnp.maximum(tops[h], jnp.max(s.reshape(groups, 8, qrows), axis=0)))
                return tuple(new)

            low = jnp.full((8, qrows), NEG_BIG, F32)
            tops = lax.fori_loop(0, quarter + 1, scores, (low, low))
            tops = tuple(jnp.max(t, axis=0, keepdims=True) for t in tops)

            def values(j, state):
                at_keys = pl.ds(mult(j * qrows, qrows), qrows)
                vt = va[at_keys, lanes].T
                new = []
                for h, sc in enumerate((sc0, sc1)):
                    total, acc = state[h]
                    e = jnp.exp(sc[at_keys, :] - tops[h])
                    total = total + jnp.sum(e.reshape(groups, 8, qrows), axis=0)
                    acc = acc + dot_nn(vt[h * HEAD_DIM:(h + 1) * HEAD_DIM], e.astype(BF))
                    new.append((total, acc))
                return tuple(new)

            blank = (jnp.zeros((8, qrows), F32), jnp.zeros((HEAD_DIM, qrows), F32))
            state = lax.fori_loop(0, quarter + 1, values, (blank, blank))
            parts = []
            for h in range(2):
                total = jnp.sum(state[h][0], axis=0, keepdims=True)
                parts.append(state[h][1] / total)
                lse[p, i * 2 + h:i * 2 + h + 1, :] = tops[h] + jnp.log(total)
            at[i * qrows:(i + 1) * qrows, lanes] = jnp.concatenate(parts, axis=0).T.astype(BF)
        return carry

    per = 2
    for k in range(0, pairs, per):
        lax.fori_loop(k, k + per, pair_body, 0)
        run(5)

    chunks[3].tick5()
    for src, out, s in ((wp, wp_o, 6), (at, at_o, 7), (lse, lse_o, 8)):
        keep.append(pltpu.make_async_copy(src, out, osem.at[s]))
        keep[-1].start()

    def attend_out(n, carry):
        lanes = pl.ds(mult(n * tile, tile), tile)
        res = dot_nt(at[...], wp[pl.ds(mult(n * tile, tile), tile), :])
        r[:, lanes] = xr[:, lanes].astype(F32) + res + vec[BP:BP + 1, lanes]
        return carry

    lax.fori_loop(0, steps, attend_out, 0)

    def second_norm(k, carry):
        at_rows = pl.ds(mult(k * lrows, lrows), lrows)
        n2, _ = norm_parts(r[at_rows, :])
        a2[at_rows, :] = (n2 * vec[G2:G2 + 1, :] + vec[C2:C2 + 1, :]).astype(BF)
        return carry

    lax.fori_loop(0, rows // lrows, second_norm, 0)
    run(2)
    for k in range(4, 8):
        chunks[k].tick5()
    for src, out, s in ((wu, wu_o, 9), (r, r_o, 10), (a2, a2_o, 11)):
        keep.append(pltpu.make_async_copy(src, out, osem.at[s]))
        keep[-1].start()

    def up(n, carry):
        lanes = pl.ds(mult(n * tile, tile), tile)
        u = dot_nt(a2[...], wu[lanes, :]) + bu3[n]
        sq_u = u * u
        t = jnp.tanh(TANH_SCALE * (u + CUBIC_TERM * sq_u * u))
        half_up = 0.5 * (1.0 + t)
        hd[:, lanes] = (u * half_up).astype(BF)
        slope = TANH_SCALE * (1.0 + 3.0 * CUBIC_TERM * sq_u)
        gp[:, lanes] = (half_up + 0.5 * u * (1.0 - t * t) * slope).astype(BF)
        return carry

    blocks = hd.shape[1] // tile
    for k in range(0, blocks, 4):
        lax.fori_loop(k, k + 4, up, 0)
        run(2)
    for src, out, s in ((hd, hd_o, 12), (gp, gp_o, 13)):
        keep.append(pltpu.make_async_copy(src, out, osem.at[s]))
        keep[-1].start()
    run(len(pending))
    for k in range(8, len(chunks)):
        chunks[k].tick5()
    keep.append(pltpu.make_async_copy(wd, wd_o, osem.at[14]))
    keep[-1].start()
    my_len = live_length(len_ref, deal_ref, (z * Y + y) * C + x)
    rowpos = lax.broadcasted_iota(jnp.int32, (qrows, 1), 0)

    def down(n, carry):
        lanes = pl.ds(mult(n * tile, tile), tile)
        res = dot_nt(hd[...], wd[pl.ds(mult(n * tile, tile), tile), :])
        res = r[:, lanes] + res + vec[BD:BD + 1, lanes]
        for i in range(2):
            live = quarters[i] * qrows + rowpos < my_len
            outw[i * qrows:(i + 1) * qrows, lanes] = jnp.where(live, res[i * qrows:(i + 1) * qrows], 0.0).astype(BF)
        return carry

    lax.fori_loop(0, steps, down, 0)
    keep.append(pltpu.make_async_copy(outw, out_o, osem.at[15]))
    keep[-1].start()

    for ch in chunks:
        ch.drain()
    vectors.drain()

    @pl.when(core_to == c)
    def _():
        wait_bytes(xr.at[pl.ds(0, rows - small)], msem.at[0])

    @pl.when(core_to != c)
    def _():
        wait_bytes(xr, msem.at[0])

    @pl.when(c == x)
    def _():
        wait_bytes(xr.at[pl.ds(0, qrows)], msem.at[2])

    @pl.when(c != x)
    def _():
        wait_bytes(xr, msem.at[2])

    wait_bytes(xr, msem.at[3])
    wait_bytes(ka.at[pl.ds(0, rows)], msem.at[4])
    wait_bytes(va.at[pl.ds(0, rows)], msem.at[6])
    for cp in keep:
        cp.wait()


def forward(lengths, dealing, xg, cot, sq, sp, su, sd, sv):
    width = xg.shape[2]
    rows = cot.shape[0]
    ff = su.shape[0] * Z * Y * C
    keys = rows * 2
    pairs = width // 128

    def arr(shape, dtype=BF):
        return jax.ShapeDtypeStruct(shape, dtype)

    outs = [
        arr((3 * width, width)), arr((width, width)), arr((ff, width)), arr((width, ff)),
        arr((rows, width)), arr((rows, width)), arr((rows, width)), arr((keys, width)), arr((keys, width)),
        arr((rows, width)), arr((pairs, 8, rows // 2), F32), arr((rows, width), F32), arr((rows, width)),
        arr((rows, ff)), arr((rows, ff)), arr((16, width), F32), arr((rows, width)),
    ]
    vm = pltpu.VMEM
    scratch = [
        vm((3 * width, width), BF), vm((width, width), BF), vm((ff, width), BF), vm((width, ff), BF),
        vm((rows, width), BF), vm((rows, width), BF), vm((rows, width), BF), vm((keys, width), BF),
        vm((keys, width), BF), vm((rows, width), BF), vm((pairs, 8, rows // 2), F32), vm((rows, width), F32),
        vm((rows, width), BF), vm((rows, ff), BF), vm((rows, ff), BF), vm((Z * Y * C, 16, width), BF),
        vm((16, width), F32), vm((ff // 256, 1, 256), F32), vm((keys, rows // 2), F32), vm((keys, rows // 2), F32),
        vm((rows, width), BF),
        pltpu.SemaphoreType.DMA((N_GATHER, 9)), pltpu.SemaphoreType.DMA((7,)), pltpu.SemaphoreType.DMA((8,)),
        pltpu.SemaphoreType.DMA((16,)),
    ]
    anyspec = pl.BlockSpec(memory_space=pl.ANY)
    smem = pl.BlockSpec(memory_space=pltpu.SMEM)
    return pl.pallas_call(
        forward_kernel,
        out_shape=outs,
        in_specs=[smem, smem] + [anyspec] * 7,
        out_specs=[anyspec] * len(outs),
        scratch_shapes=scratch,
        compiler_params=pltpu.CompilerParams(
            collective_id=0, has_side_effects=True, vmem_limit_bytes=60 * 1024 * 1024
        ),
        name="forward",
    )(lengths, dealing, xg, cot, sq, sp, su, sd, sv)


class Reduce:
    S1, R1, S2, R2, S3, R3, S4, R4 = range(8)

    def __init__(self, grad, R, step, c0, C, zlist, bufs, out, out_c0, sems, k, where):
        self.grad, self.R, self.step, self.c0, self.cn, self.zlist = grad, R, step, c0, C, zlist
        self.r1, self.r2, self.r3, self.r4 = bufs
        self.out, self.out_c0, self.sems, self.k = out, out_c0, sems, k
        self.z, self.y, self.c, self.x, _ = where
        c, y, x = self.c, self.y, self.x
        self.y2, self.x2 = (y + c) % 2, (x + 1 - c) % 2
        self.y3, self.x3 = (y + 1 - c) % 2, (x + c) % 2

    def sem(self, which):
        return self.sems.at[self.k, which]

    def rows(self, z, y, c):
        return pl.ds(mult(((z * Y + y) * C + c) * self.R, 16), self.R)

    def cols(self, x):
        return pl.ds(mult(x * self.step + self.c0, 128), self.cn)

    def at(self, z, y, c, x):
        return self.grad.at[self.rows(z, y, c), self.cols(x)]

    def add(self, rows, cols, got):
        self.grad[rows, cols] = (self.grad[rows, cols].astype(F32) + got.astype(F32)).astype(BF)

    def zidx(self, zi):
        return self.zlist[0] if len(self.zlist) == 1 else zi

    def start(self):
        z, y, c, x = self.z, self.y, self.c, self.x
        to = dev(z, y, 1 - c, x)
        for zi, zz in enumerate(self.zlist):
            for yy in range(Y):
                for xx in range(X):
                    rcopy(
                        self.at(zz, yy, 1 - c, xx), self.r1.at[zi * Y + yy, xx],
                        self.sem(self.S1), self.sem(self.R1), to,
                    ).start()

    def tick2(self):
        z, y, c, x = self.z, self.y, self.c, self.x
        wait_bytes(self.r1, self.sem(self.R1))

        def body(e, carry):
            rows = self.rows(self.zidx(e // Y), e % Y, c)
            for xx in range(X):
                self.add(rows, self.cols(xx), self.r1[e, xx])
            return carry

        lax.fori_loop(0, len(self.zlist) * Y, body, 0)
        to = dev(z, self.y2, c, self.x2)
        for zi, zz in enumerate(self.zlist):
            for w in range(2):
                yy = w * (1 - c) + (1 - y) * c
                xx = (1 - x) * (1 - c) + w * c
                rcopy(self.at(zz, yy, c, xx), self.r2.at[zi * 2 + w], self.sem(self.S2), self.sem(self.R2), to).start()

    def tick3(self):
        z, y, c, x = self.z, self.y, self.c, self.x
        wait_bytes(self.r2, self.sem(self.R2))

        def body(e, carry):
            w = e % 2
            yy = w * (1 - c) + y * c
            xx = x * (1 - c) + w * c
            self.add(self.rows(self.zidx(e // 2), yy, c), self.cols(xx), self.r2[e])
            return carry

        lax.fori_loop(0, len(self.zlist) * 2, body, 0)
        to = dev(z, self.y3, c, self.x3)
        for zi, zz in enumerate(self.zlist):
            rcopy(self.at(zz, self.y3, c, self.x3), self.r3.at[zi], self.sem(self.S3), self.sem(self.R3), to).start()

    def tick4(self):
        z, y, c, x = self.z, self.y, self.c, self.x
        wait_bytes(self.r3, self.sem(self.R3))

        def body(zi, carry):
            self.add(self.rows(self.zidx(zi), y, c), self.cols(x), self.r3[zi])
            return carry

        lax.fori_loop(0, len(self.zlist), body, 0)
        for zz in self.zlist:
            @pl.when(z != zz)
            def _(zz=zz):
                rcopy(
                    self.at(zz, y, c, x), self.r4.at[z], self.sem(self.S4), self.sem(self.R4), dev(zz, y, c, x)
                ).start()

    def tick5(self):
        z, y, c, x = self.z, self.y, self.c, self.x

        def last():
            wait_bytes(self.r4.at[pl.ds(0, Z - 1)], self.sem(self.R4))
            total = self.grad[self.rows(z, y, c), self.cols(x)].astype(F32)
            for dz in range(1, Z):
                total = total + self.r4[(z + dz) % Z].astype(F32)
            self.out[:, self.out_c0:self.out_c0 + self.cn] = total

        if len(self.zlist) == Z:
            last()
        else:
            pl.when(z == self.zlist[0])(last)

    def drain(self):
        wait_bytes(self.r1, self.sem(self.S1))
        wait_bytes(self.r2, self.sem(self.S2))
        wait_bytes(self.r3, self.sem(self.S3))
        if len(self.zlist) == Z:
            wait_bytes(self.r4.at[pl.ds(0, Z - 1)], self.sem(self.S4))
        else:
            @pl.when(self.z != self.zlist[0])
            def _():
                wait_bytes(self.r4.at[0], self.sem(self.S4))


def reduce_shapes(width, ff):
    n = Z * Y * C
    every = list(range(Z))
    half = width // X
    wide = ff // X
    shapes = [("d", width // n, wide, k * (wide // 2), wide // 2, every, k * (wide // 2)) for k in range(2)]
    shapes += [("u", ff // n, half, 0, half, [k], 0) for k in range(Z)]
    shapes += [("p", width // n, half, 0, half, every, 0)]
    shapes += [("q", 3 * width // n, half, 0, half, [k], 0) for k in range(Z)]
    return shapes


def backward_kernel(*refs):
    names = (
        "len_ref", "deal_ref", "wq_i", "wp_i", "wu_i", "wd_i", "xr_i", "gw_i", "qs_i", "ka_i", "va_i", "at_i",
        "lse_i", "r_i", "a2_i", "hd_i", "gp_i", "vec_i", "out_i", "og_q", "og_p", "og_u", "og_d", "osum", "ret",
        "out_n", "wq", "wp", "xr", "g", "qs", "ka", "va", "at", "lse", "r", "a2", "vec", "gt", "d2", "dr", "drl",
        "do", "gq", "gp_", "gu", "gd", "wd_t", "wu_t", "hd_t", "gp_t", "dka", "dva", "own_v", "sv", "rk", "rv", "dm",
        "vs", "vr", "bub", "lsem", "tsem", "rsem", "msem", "vsem",
    )
    env = dict(zip(names, refs[: len(names)]))
    env.update(a1=env["a2"], own_k=env["d2"], sk=env["drl"], dx=env["do"])
    bufs = refs[len(names):]
    e = type("Refs", (), env)
    where = coords()
    z, y, c, x, d = where
    rows, width = e.g.shape
    ff = e.hd_i.shape[1]
    qrows = rows // 2
    pairs = width // 128
    tile = 256
    lrows = 128
    steps = width // tile
    quarters = (c, 3 - c)
    theirs = (1 - c, 2 + c)

    def at_quarter(k):
        return pl.ds(mult(k * qrows, qrows), qrows)

    enter(Z * Y * C * X)

    loads = {}
    for k, (src, dst) in enumerate(
        (
            ("gw_i", "g"), ("a2_i", "a2"), ("r_i", "r"), ("vec_i", "vec"), ("wp_i", "wp"), ("at_i", "at"),
            ("qs_i", "qs"), ("ka_i", "ka"), ("va_i", "va"), ("lse_i", "lse"), ("xr_i", "xr"), ("wq_i", "wq"),
        )
    ):
        loads[dst] = pltpu.make_async_copy(env[src], env[dst], e.lsem.at[k])

    def tile_of(idx):
        block = idx // 3
        return (block % 2) * 2 * 3 + (block // 2) * 3 + idx % 3

    def tile_copies(idx):
        n = tile_of(idx)
        slot = idx % 2
        cut = pl.ds(mult(n * tile, tile), tile)
        return (
            pltpu.make_async_copy(e.wd_i.at[:, cut], e.wd_t.at[slot], e.tsem.at[0, slot]),
            pltpu.make_async_copy(e.gp_i.at[:, cut], e.gp_t.at[slot], e.tsem.at[1, slot]),
            pltpu.make_async_copy(e.hd_i.at[:, cut], e.hd_t.at[slot], e.tsem.at[2, slot]),
            pltpu.make_async_copy(e.wu_i.at[cut, :], e.wu_t.at[slot], e.tsem.at[3, slot]),
        )

    loads["g"].start()
    for cp in tile_copies(0):
        cp.start()
    loads["a2"].start()
    for name in ("r", "vec", "wp", "at", "qs", "ka", "va", "lse", "xr", "wq"):
        loads[name].start()

    for i in range(2):
        same = jnp.logical_and(x == c, x == i)
        src = e.out_i.at[pl.ds(i * qrows, qrows)]
        dst = e.out_n.at[pl.ds(mult(((i + c) % 2) * qrows, qrows), qrows)]

        @pl.when(same)
        def _(src=src, dst=dst):
            pltpu.make_async_copy(src, dst, e.msem.at[1]).start()

        @pl.when(jnp.logical_not(same))
        def _(src=src, dst=dst, i=i):
            rcopy(src, dst, e.msem.at[0], e.msem.at[1], dev(z, y, x, i)).start()

    grads = {"q": (e.gq, e.og_q), "p": (e.gp_, e.og_p), "u": (e.gu, e.og_u), "d": (e.gd, e.og_d)}
    chunks = []
    for k, (name, R, step, c0, cn, zlist, oc) in enumerate(reduce_shapes(width, ff)):
        grad, out = grads[name]
        chunks.append(Reduce(grad, R, step, c0, cn, zlist, bufs[4 * k:4 * k + 4], out, oc, e.rsem, k, where))
    dA, dB, u0, u1, u2, u3, pj, q0, q1, q2, q3 = chunks

    my_len = live_length(e.len_ref, e.deal_ref, (z * Y + y) * C + x)
    rowpos = lax.broadcasted_iota(jnp.int32, (lrows, 1), 0)
    loads["g"].wait()
    blank = jnp.zeros((1, width), F32)
    total_bd = blank
    for k in range(rows // lrows):
        base = quarters[k * lrows // qrows] * qrows + (k * lrows) % qrows
        live = base + rowpos < my_len
        part = jnp.where(live, e.g[k * lrows:(k + 1) * lrows, :], jnp.zeros((), BF))
        e.g[k * lrows:(k + 1) * lrows, :] = part
        e.gt[:, k * lrows:(k + 1) * lrows] = part.T
        total_bd = total_bd + jnp.sum(part.astype(F32), axis=0, keepdims=True)
    e.d2[...] = jnp.zeros_like(e.d2)
    loads["a2"].wait()

    ff_tiles = ff // tile
    plan = {
        2: [u0.start], 3: [u0.tick2], 5: [u2.start, dA.start, u0.tick3], 7: [u0.tick4, u2.tick2],
        8: [u1.start, dA.tick2], 9: [u2.tick3], 10: [dA.tick3], 11: [u3.start, dB.start, u2.tick4],
    }

    def ffn(idx, carry):
        slot = idx % 2
        n = tile_of(idx)
        cut = pl.ds(mult(n * tile, tile), tile)

        @pl.when(idx + 1 < ff_tiles)
        def _():
            for cp in tile_copies(idx + 1):
                cp.start()

        for cp in tile_copies(idx):
            cp.wait()
        du = (e.gp_t[slot].astype(F32) * dot_nn(e.g[...], e.wd_t[slot])).astype(BF)
        e.bub[n] = jnp.sum(du.astype(F32), axis=0, keepdims=True)
        e.gd[:, cut] = dot_nn(e.gt[...], e.hd_t[slot]).astype(BF)
        e.gu[cut, :] = dot_tn(du, e.a2[...]).astype(BF)
        e.d2[...] += dot_nn(du, e.wu_t[slot])
        for at_idx, acts in plan.items():
            @pl.when(idx == at_idx)
            def _(acts=acts):
                for act in acts:
                    act()
        return carry

    lax.fori_loop(0, ff_tiles, ffn, 0)

    loads["r"].wait()
    loads["vec"].wait()

    def norm_two(k, sums):
        at_rows = pl.ds(mult(k * lrows, lrows), lrows)
        n2, rstd = norm_parts(e.r[at_rows, :])
        da = e.d2[at_rows, :]
        ee = da * e.vec[G2:G2 + 1, :]
        gg = e.g[at_rows, :].astype(F32)
        m1 = jnp.mean(ee, axis=-1, keepdims=True)
        m2 = jnp.mean(ee * n2, axis=-1, keepdims=True)
        dr = gg + (ee - m1 - n2 * m2) * rstd
        e.dr[at_rows, :] = dr
        e.drl[at_rows, :] = dr.astype(BF)
        return (
            sums[0] + jnp.sum(da * n2, axis=0, keepdims=True),
            sums[1] + jnp.sum(da, axis=0, keepdims=True),
            sums[2] + jnp.sum(dr, axis=0, keepdims=True),
        )

    sum_g2, sum_c2, sum_bp = lax.fori_loop(0, rows // lrows, norm_two, (blank, blank, blank))
    u1.tick2()
    dA.tick4()

    loads["wp"].wait()
    loads["at"].wait()

    def proj_back(n, carry):
        cut = pl.ds(mult(n * tile, tile), tile)
        e.do[:, cut] = dot_nn(e.drl[...], e.wp[:, cut]).astype(BF)
        e.gp_[cut, :] = dot_tn(e.drl[:, cut], e.at[...]).astype(BF)
        return carry

    lax.fori_loop(0, steps, proj_back, 0)
    pj.start()
    u1.tick3()
    u3.tick2()

    for name in ("qs", "ka", "va", "lse"):
        loads[name].wait()
    lane = lax.broadcasted_iota(jnp.int32, (qrows, 128), 1)
    kpos = lax.broadcasted_iota(jnp.int32, (qrows, qrows), 0)
    qpos = lax.broadcasted_iota(jnp.int32, (qrows, qrows), 1)

    def split(v):
        zero = jnp.zeros_like(v)
        return jnp.where(lane < HEAD_DIM, v, zero), jnp.where(lane >= HEAD_DIM, v, zero)

    def pair_body(p, carry):
        lanes = pl.ds(mult(p * 128, 128), 128)
        e.dka[...] = jnp.zeros_like(e.dka)
        e.dva[...] = jnp.zeros_like(e.dva)
        for i in range(2):
            quarter = quarters[i]
            own = slice(i * qrows, (i + 1) * qrows)
            qp, dop = e.qs[own, lanes], e.do[own, lanes]
            qh, doh = split(qp), split(dop)
            qq, dd = jnp.concatenate(qh, axis=0), jnp.concatenate(doh, axis=0)
            prod = (dop.astype(F32) * e.at[own, lanes].astype(F32)).T
            delta = [jnp.sum(prod[h * HEAD_DIM:(h + 1) * HEAD_DIM], axis=0, keepdims=True) for h in range(2)]
            logs = [e.lse[p, i * 2 + h:i * 2 + h + 1, :] for h in range(2)]

            def keys(j, dq):
                at_keys = pl.ds(mult(j * qrows, qrows), qrows)
                kj, vj = e.ka[at_keys, lanes], e.va[at_keys, lanes]
                kt = kj.T
                keep_it = jnp.logical_or(kpos <= qpos, j < quarter)
                probs, grads_s, new = [], [], []
                for h in range(2):
                    s = jnp.where(keep_it, dot_nt(kj, qh[h]), NEG_BIG)
                    pt = jnp.exp(s - logs[h])
                    ds = (pt * (dot_nt(vj, doh[h]) - delta[h])).astype(BF)
                    probs.append(pt.astype(BF))
                    grads_s.append(ds)
                    new.append(dq[h] + dot_nn(kt[h * HEAD_DIM:(h + 1) * HEAD_DIM], ds))
                e.dva[at_keys, :] += dot_nn(jnp.concatenate(probs, axis=1), dd)
                e.dka[at_keys, :] += dot_nn(jnp.concatenate(grads_s, axis=1), qq)
                return tuple(new)

            none = jnp.zeros((HEAD_DIM, qrows), F32)
            dq = lax.fori_loop(0, quarter + 1, keys, (none, none))
            e.dm[own, lanes] = (jnp.concatenate(dq, axis=0).T * HEAD_DIM ** -0.5).astype(BF)
        for i in range(2):
            own = slice(i * qrows, (i + 1) * qrows)
            e.own_k[own, lanes] = e.dka[at_quarter(quarters[i]), :]
            e.own_v[own, lanes] = e.dva[at_quarter(quarters[i]), :]
            e.sk[own, lanes] = e.dka[at_quarter(theirs[i]), :].astype(BF)
            e.sv[own, lanes] = e.dva[at_quarter(theirs[i]), :].astype(BF)
        return carry

    between = [[dB.tick2, u1.tick4, u3.tick3, pj.tick2], [dB.tick3, u3.tick4, pj.tick3], [dB.tick4, pj.tick4]]
    for k in range(3):
        lax.fori_loop(2 * k, 2 * k + 2, pair_body, 0)
        for act in between[k]:
            act()
        cut = slice(2 * k * 128, (2 * k + 2) * 128)
        for src, dst, s in ((e.sk, e.rk, 2), (e.sv, e.rv, 4)):
            rcopy(src.at[:, cut], dst.at[:, cut], e.msem.at[s], e.msem.at[s + 1], dev(z, y, 1 - c, x)).start()

    loads["xr"].wait()

    def norm_one(k, carry):
        at_rows = pl.ds(mult(k * lrows, lrows), lrows)
        n1, _ = norm_parts(e.xr[at_rows, :].astype(F32))
        e.a1[at_rows, :] = (n1 * e.vec[G1:G1 + 1, :] + e.vec[C1:C1 + 1, :]).astype(BF)
        return carry

    lax.fori_loop(0, rows // lrows, norm_one, 0)

    def qkv_grad(n, carry):
        cut = pl.ds(mult(n * tile, tile), tile)
        e.gq[cut, :] = dot_tn(e.dm[:, cut], e.a1[...]).astype(BF)
        return carry

    lax.fori_loop(0, 3, qkv_grad, 0)
    q0.start()
    wait_bytes(e.rk, e.msem.at[3])
    wait_bytes(e.rv, e.msem.at[5])
    for part, (mine, got) in enumerate(((e.own_k, e.rk), (e.own_v, e.rv))):
        def merge(k, carry, part=part, mine=mine, got=got):
            at_rows = pl.ds(mult(k * lrows, lrows), lrows)
            e.dm[at_rows, (part + 1) * width:(part + 2) * width] = (
                mine[at_rows, :] + got[at_rows, :].astype(F32)
            ).astype(BF)
            return carry

        lax.fori_loop(0, rows // lrows, merge, 0)
    lax.fori_loop(3, 5, qkv_grad, 0)
    q1.start()
    q0.tick2()
    lax.fori_loop(5, 7, qkv_grad, 0)
    q2.start()
    q1.tick2()
    lax.fori_loop(7, 9, qkv_grad, 0)
    q3.start()
    q0.tick3()
    q2.tick2()

    loads["wq"].wait()

    def input_back(n, carry):
        cut = pl.ds(mult(n * tile, tile), tile)
        e.d2[:, cut] = dot_nn(e.dm[...], e.wq[:, cut])
        return carry

    lax.fori_loop(0, steps, input_back, 0)
    q1.tick3()
    q3.tick2()

    def norm_one_back(k, sums):
        at_rows = pl.ds(mult(k * lrows, lrows), lrows)
        n1, rstd = norm_parts(e.xr[at_rows, :].astype(F32))
        da = e.d2[at_rows, :]
        ee = da * e.vec[G1:G1 + 1, :]
        m1 = jnp.mean(ee, axis=-1, keepdims=True)
        m2 = jnp.mean(ee * n1, axis=-1, keepdims=True)
        e.dx[at_rows, :] = (e.dr[at_rows, :] + (ee - m1 - n1 * m2) * rstd).astype(BF)
        return sums[0] + jnp.sum(da * n1, axis=0, keepdims=True), sums[1] + jnp.sum(da, axis=0, keepdims=True)

    sum_g1, sum_c1 = lax.fori_loop(0, rows // lrows, norm_one_back, (blank, blank))

    e.vs[0] = jnp.zeros_like(e.vs[0])
    for row, value in ((G1, sum_g1), (C1, sum_c1), (BP, sum_bp), (G2, sum_g2), (C2, sum_c2), (BD, total_bd)):
        e.vs[0, row:row + 1, :] = value
    per = width // tile
    for k in range(ff_tiles):
        e.vs[0, BU + k // per:BU + k // per + 1, (k % per) * tile:(k % per + 1) * tile] = e.bub[k]
    hops = (
        dev(z, y, 1 - c, x), dev(z, y, c, 1 - x), dev(z, 1 - y, c, x),
        dev(z + 1 - 2 * (z % 2), y, c, x), dev((z + 2) % 4, y, c, x),
    )

    def hop(k):
        rcopy(e.vs.at[k], e.vr.at[k], e.vsem.at[0, k], e.vsem.at[1, k], hops[k]).start()

    def land(k):
        wait_bytes(e.vr.at[k], e.vsem.at[1, k])
        e.vs[k + 1] = e.vs[k] + e.vr[k]

    hop(0)

    small = e.ret.shape[1]
    per_quarter = qrows // small
    slot = (z * Y + y) * C + x
    for i in range(2):
        def give_back(b, carry, i=i):
            td = ((i + c) % 2) * per_quarter + b
            src = e.dx.at[pl.ds(mult(i * qrows + b * small, small), small)]
            mine = jnp.logical_and(td == d, x == i)

            @pl.when(mine)
            def _():
                pltpu.make_async_copy(src, e.ret.at[slot], e.msem.at[7]).start()

            @pl.when(jnp.logical_not(mine))
            def _():
                rcopy(src, e.ret.at[slot], e.msem.at[6], e.msem.at[7], {"dp": td, "cp": i}).start()

            return carry

        lax.fori_loop(0, per_quarter, give_back, 0)

    q2.tick3()
    land(0)
    hop(1)
    q0.tick4()
    q3.tick3()
    land(1)
    hop(2)
    q1.tick4()
    q2.tick4()
    for ch in (u0, u1, u2, u3, dA, dB, pj):
        ch.tick5()
    land(2)
    hop(3)
    q3.tick4()
    land(3)
    hop(4)
    for ch in (q0, q1, q2, q3):
        ch.tick5()
    land(4)
    e.osum[...] = e.vs[5]

    for ch in chunks:
        ch.drain()
    for k in range(5):
        wait_bytes(e.vr.at[k], e.vsem.at[0, k])
    wait_bytes(e.rk, e.msem.at[2])
    wait_bytes(e.rv, e.msem.at[4])

    @pl.when((x + c) % 2 == d // per_quarter)
    def _():
        wait_bytes(e.dx.at[pl.ds(0, rows - small)], e.msem.at[6])

    @pl.when((x + c) % 2 != d // per_quarter)
    def _():
        wait_bytes(e.dx, e.msem.at[6])

    wait_bytes(e.dx, e.msem.at[7])

    @pl.when(c == x)
    def _():
        wait_bytes(e.dx.at[pl.ds(0, qrows)], e.msem.at[0])

    @pl.when(c != x)
    def _():
        wait_bytes(e.dx, e.msem.at[0])

    wait_bytes(e.dx, e.msem.at[1])


def backward(lengths, dealing, saved, shards):
    wq, wp, wu, wd, xr, gw, qs, ka, va, at, lse, r, a2, hd, gp, vec, outw = saved
    rows, width = xr.shape
    ff = hd.shape[1]
    n = Z * Y * C
    keys = ka.shape[0]
    small = rows // n
    pairs = width // 128

    def arr(shape, dtype=BF):
        return jax.ShapeDtypeStruct(shape, dtype)

    outs = [arr(s.shape, F32) for s in shards] + [
        arr((16, width), F32), arr((n, small, width)), arr((rows, width)),
    ]
    vm = pltpu.VMEM
    acts = vm((rows, width), BF)
    acts32 = vm((rows, width), F32)
    scratch = [
        vm(wq.shape, BF), vm(wp.shape, BF), acts, acts, acts, vm(ka.shape, BF), vm(va.shape, BF), acts,
        vm(lse.shape, F32), acts32, acts, vm(vec.shape, F32), vm((width, rows), BF), acts32, acts32, acts, acts,
        vm(wq.shape, BF), vm(wp.shape, BF), vm(wu.shape, BF), vm(wd.shape, BF),
        vm((2, width, 256), BF), vm((2, 256, width), BF), vm((2, rows, 256), BF), vm((2, rows, 256), BF),
        vm((keys, 128), F32), vm((keys, 128), F32),
        acts32, acts, acts, acts, vm((rows, 3 * width), BF),
        vm((6, 16, width), F32), vm((5, 16, width), F32), vm((ff // 256, 1, 256), F32),
        pltpu.SemaphoreType.DMA((12,)), pltpu.SemaphoreType.DMA((4, 2)), pltpu.SemaphoreType.DMA((11, 8)),
        pltpu.SemaphoreType.DMA((8,)), pltpu.SemaphoreType.DMA((2, 5)),
    ]
    for _, R, _, _, cn, zlist, _ in reduce_shapes(width, ff):
        k = len(zlist)
        scratch += [vm((2 * k, 2, R, cn), BF), vm((2 * k, R, cn), BF), vm((k, R, cn), BF), vm((Z, R, cn), BF)]
    anyspec = pl.BlockSpec(memory_space=pl.ANY)
    smem = pl.BlockSpec(memory_space=pltpu.SMEM)
    vmem = pl.BlockSpec(memory_space=pltpu.VMEM)
    return pl.pallas_call(
        backward_kernel,
        out_shape=outs,
        in_specs=[smem, smem] + [anyspec] * len(saved),
        out_specs=[vmem] * 5 + [anyspec] * 2,
        scratch_shapes=scratch,
        compiler_params=pltpu.CompilerParams(
            collective_id=1, has_side_effects=True, vmem_limit_bytes=67043328
        ),
        name="backward",
    )(lengths, dealing, *saved)


def slice_plan(
    x_source, cotangent, lengths, dealing, qkv_weight, proj_weight, up_weight, down_weight,
    first_gain, first_shift, proj_bias, second_gain, second_shift, up_bias, down_bias,
):
    slots = dealing.shape[0]
    width = x_source.shape[2]
    n = Z * Y * C
    d = lax.axis_index("dp")
    owners = jnp.sum(
        jnp.where(dealing[None, :] == jnp.arange(slots)[:, None], jnp.arange(slots)[None, :], 0), axis=1
    )
    xg = x_source[owners]
    shards = [w.astype(BF).T for w in (qkv_weight, proj_weight, up_weight, down_weight)]
    seven = jnp.stack([first_gain, first_shift, proj_bias, second_gain, second_shift, down_bias]).astype(BF)
    own = seven.shape[1]
    place = jnp.arange(width) // own
    table = jnp.where(place == d, jnp.tile(seven, (1, n)), jnp.zeros((), BF))
    long = up_bias.astype(BF)
    wide = jnp.where(jnp.arange(long.shape[0] * n) // long.shape[0] == d, jnp.tile(long, n), jnp.zeros((), BF))
    sv = jnp.concatenate([table, wide.reshape(-1, width), jnp.zeros((16 - 6 - wide.shape[0] // width, width), BF)])
    saved = forward(lengths, dealing, xg, cotangent[0], *shards, sv)
    gq, gp, gu, gd, sums, ret, out = backward(lengths, dealing, saved, shards)
    input_grad = ret[dealing]
    picked = lax.dynamic_slice_in_dim(sums[:6].reshape(6, n, own), d, 1, axis=1)[:, 0]
    long_sum = lax.dynamic_slice_in_dim(sums[BU:BU + wide.shape[0] // width].reshape(-1), d * long.shape[0], long.shape[0])
    return (
        out[None], input_grad, gq.T, gp.T, gu.T, gd.T,
        picked[G1], picked[C1], picked[BP], picked[G2], picked[C2], long_sum, picked[BD],
    )


def layer_norm(values, scaling, offset):
    centered = values - jnp.mean(values, axis=-1, keepdims=True)
    spread = jnp.mean(centered * centered, axis=-1, keepdims=True)
    return centered * lax.rsqrt(spread + EPSILON) * scaling + offset


def gelu_tanh(values):
    return (
        0.5
        * values
        * (1.0 + jnp.tanh(TANH_SCALE * (values + CUBIC_TERM * values * values * values)))
    )


def grouped(array, block_seqs):
    return array.reshape(
        (array.shape[0] // block_seqs, block_seqs, array.shape[1], HEADS, array.shape[2] // HEADS)
    )


def grouped_stats(array, block_seqs):
    return array.reshape((array.shape[0] // block_seqs, block_seqs) + array.shape[1:])


def joined(array):
    return array.reshape(
        (array.shape[0] * array.shape[1], array.shape[2], array.shape[3] * array.shape[4])
    )


def masked_scores(queries, key_rows, query_start, score_scale):
    scores = (
        jnp.einsum("bqhd,bkhd->bhqk", queries, key_rows, preferred_element_type=jnp.float32)
        * score_scale
    )
    query_pos = query_start + jnp.arange(queries.shape[1])
    key_pos = jnp.arange(key_rows.shape[1])
    return jnp.where(key_pos[None, :] <= query_pos[:, None], scores, NEG_BIG)


def attend(inputs, query_start, score_scale):
    queries, key_rows, val_rows = inputs
    scores = masked_scores(queries, key_rows, query_start, score_scale)
    row_top = jnp.max(scores, axis=-1, keepdims=True)
    exponent = jnp.exp(scores - row_top)
    totals = jnp.sum(exponent, axis=-1, keepdims=True)
    weights = (exponent / totals).astype(jnp.bfloat16)
    attended = jnp.einsum("bhqk,bkhd->bqhd", weights, val_rows, preferred_element_type=jnp.float32)
    return (attended.astype(jnp.bfloat16), (row_top + jnp.log(totals))[..., 0])


def rows_back(inputs, query_start, score_scale):
    queries, key_rows, val_rows, grad_rows, log_total = inputs
    scores = masked_scores(queries, key_rows, query_start, score_scale)
    weights = jnp.exp(scores - log_total[..., None])
    grad_weights = jnp.einsum(
        "bqhd,bkhd->bhqk", grad_rows, val_rows, preferred_element_type=jnp.float32
    )
    delta_rows = jnp.sum(weights * grad_weights, axis=-1)
    grad_scores = (weights * (grad_weights - delta_rows[..., None])).astype(jnp.bfloat16)
    grad_query = (
        jnp.einsum("bhqk,bkhd->bqhd", grad_scores, key_rows, preferred_element_type=jnp.float32)
        * score_scale
    )
    grad_keys = (
        jnp.einsum("bhqk,bqhd->bkhd", grad_scores, queries, preferred_element_type=jnp.float32)
        * score_scale
    )
    grad_vals = jnp.einsum(
        "bhqk,bqhd->bkhd",
        weights.astype(jnp.bfloat16),
        grad_rows,
        preferred_element_type=jnp.float32,
    )
    return (grad_query, grad_keys, grad_vals)


def fetch_weights(
    qkv_weight,
    proj_weight,
    up_weight,
    down_weight,
    first_gain,
    first_shift,
    proj_bias,
    second_gain,
    second_shift,
    up_bias,
    down_bias,
):
    qkv_part, proj_part, up_part, down_part = (
        lax.all_gather(qkv_weight.astype(jnp.bfloat16), "cp", axis=0, tiled=True),
        lax.all_gather(proj_weight.astype(jnp.bfloat16), "cp", axis=0, tiled=True),
        lax.all_gather(up_weight.astype(jnp.bfloat16), "cp", axis=0, tiled=True),
        lax.all_gather(down_weight.astype(jnp.bfloat16), "cp", axis=0, tiled=True),
    )
    return (
        lax.all_gather(qkv_part, "dp", axis=1, tiled=True),
        lax.all_gather(proj_part, "dp", axis=1, tiled=True),
        lax.all_gather(up_part, "dp", axis=1, tiled=True),
        lax.all_gather(down_part, "dp", axis=1, tiled=True),
        lax.all_gather(first_gain.astype(jnp.bfloat16), "dp", axis=0, tiled=True),
        lax.all_gather(first_shift.astype(jnp.bfloat16), "dp", axis=0, tiled=True),
        lax.all_gather(proj_bias.astype(jnp.bfloat16), "dp", axis=0, tiled=True),
        lax.all_gather(second_gain.astype(jnp.bfloat16), "dp", axis=0, tiled=True),
        lax.all_gather(second_shift.astype(jnp.bfloat16), "dp", axis=0, tiled=True),
        lax.all_gather(up_bias.astype(jnp.bfloat16), "dp", axis=0, tiled=True),
        lax.all_gather(down_bias.astype(jnp.bfloat16), "dp", axis=0, tiled=True),
    )


def mat_rows(left, right):
    return jnp.einsum("sqd,de->sqe", left, right, preferred_element_type=jnp.float32)


def mat_back(left, right):
    return jnp.einsum("sqe,de->sqd", left, right, preferred_element_type=jnp.float32)


def mat_grad(left, right):
    return jnp.einsum("sqd,sqe->de", left, right, preferred_element_type=jnp.float32)


def general(
    x_source,
    cotangent,
    lengths,
    dealing,
    qkv_weight,
    proj_weight,
    up_weight,
    down_weight,
    first_gain,
    first_shift,
    proj_bias,
    second_gain,
    second_shift,
    up_bias,
    down_bias,
):
    groups = lax.axis_size("dp")
    seqs_all, piece_rows, features = x_source.shape
    seq_group = seqs_all // groups
    span_rows = groups * piece_rows
    score_scale = HEAD_DIM ** (-0.5)
    block_seqs = math.gcd(seq_group, max(1, 512 // span_rows))
    owners = jnp.argsort(dealing)
    send_order = owners.reshape(groups, seq_group).T.reshape(-1)
    outgoing = x_source[send_order].reshape(seq_group, span_rows, features)
    arrived = lax.all_to_all(outgoing, "dp", split_axis=1, concat_axis=1, tiled=True)
    first_slot = lax.axis_index("dp") * seq_group
    my_lengths = lax.dynamic_slice_in_dim(lengths[owners], first_slot, seq_group)
    query_start = lax.axis_index("cp") * span_rows
    positions = query_start + jnp.arange(span_rows)
    live_rows = positions[None, :] < my_lengths[:, None]
    fetched = fetch_weights(
        qkv_weight,
        proj_weight,
        up_weight,
        down_weight,
        first_gain,
        first_shift,
        proj_bias,
        second_gain,
        second_shift,
        up_bias,
        down_bias,
    )
    qkv_full, proj_full, up_full, down_full = (fetched[0], fetched[1], fetched[2], fetched[3])
    gain_one, shift_one, bias_proj, gain_two, shift_two, bias_up, bias_down = [
        vector.astype(jnp.float32) for vector in fetched[4:]
    ]
    inputs_f = arrived.astype(jnp.float32)
    norm_one, back_one = jax.vjp(layer_norm, inputs_f, gain_one, shift_one)
    act_one = norm_one.astype(jnp.bfloat16)
    mixed_rows = mat_rows(act_one, qkv_full).astype(jnp.bfloat16)
    queries = mixed_rows[..., :features]
    kv_local = mixed_rows[..., features:]
    kv_all = lax.all_gather(kv_local, "cp", axis=1, tiled=True)
    attended, log_total = lax.map(
        lambda inputs: attend(inputs, query_start, score_scale),
        (
            grouped(queries, block_seqs),
            grouped(kv_all[..., :features], block_seqs),
            grouped(kv_all[..., features:], block_seqs),
        ),
    )
    attended = joined(attended)
    log_total = log_total.reshape((seq_group,) + log_total.shape[2:])
    residual = inputs_f + mat_rows(attended, proj_full) + bias_proj
    norm_two, back_two = jax.vjp(layer_norm, residual, gain_two, shift_two)
    act_two = norm_two.astype(jnp.bfloat16)
    up_raw = mat_rows(act_two, up_full) + bias_up
    hidden, back_gelu = jax.vjp(gelu_tanh, up_raw)
    hid_low = hidden.astype(jnp.bfloat16)
    result = residual + mat_rows(hid_low, down_full) + bias_down
    output = jnp.where(live_rows[..., None], result, 0.0).astype(jnp.bfloat16)
    fetched = fetch_weights(
        qkv_weight,
        proj_weight,
        up_weight,
        down_weight,
        first_gain,
        first_shift,
        proj_bias,
        second_gain,
        second_shift,
        up_bias,
        down_bias,
    )
    qkv_full, proj_full, up_full, down_full = (fetched[0], fetched[1], fetched[2], fetched[3])
    gain_one, gain_two = (fetched[4].astype(jnp.float32), fetched[7].astype(jnp.float32))
    grad_out = jnp.where(live_rows[..., None], cotangent.astype(jnp.float32), 0.0)
    grad_low = grad_out.astype(jnp.bfloat16)
    grad_down = mat_grad(hid_low, grad_low)
    grad_bias_down = jnp.sum(grad_out, axis=(0, 1))
    grad_hidden = mat_back(grad_low, down_full)
    grad_up_raw = back_gelu(grad_hidden)[0].astype(jnp.bfloat16)
    grad_up = mat_grad(act_two, grad_up_raw)
    grad_bias_up = jnp.sum(grad_up_raw.astype(jnp.float32), axis=(0, 1))
    grad_act_two = mat_back(grad_up_raw, up_full)
    grad_resid, grad_gain_two, grad_shift_two = back_two(grad_act_two)
    grad_resid = grad_resid + grad_out
    grad_bias_proj = jnp.sum(grad_resid, axis=(0, 1))
    resid_low = grad_resid.astype(jnp.bfloat16)
    grad_proj = mat_grad(attended, resid_low)
    grad_attended = mat_back(resid_low, proj_full).astype(jnp.bfloat16)
    kv_back = lax.all_gather(kv_local, "cp", axis=1, tiled=True)
    key_rows = kv_back[..., :features]
    val_rows = kv_back[..., features:]
    grad_query, grad_keys, grad_vals = lax.map(
        lambda inputs: rows_back(inputs, query_start, score_scale),
        (
            grouped(queries, block_seqs),
            grouped(key_rows, block_seqs),
            grouped(val_rows, block_seqs),
            grouped(grad_attended, block_seqs),
            grouped_stats(log_total, block_seqs),
        ),
    )
    grad_keys, grad_vals = (
        lax.psum_scatter(
            joined(grad_keys).astype(jnp.bfloat16), "cp", scatter_dimension=1, tiled=True
        ).astype(jnp.float32),
        lax.psum_scatter(
            joined(grad_vals).astype(jnp.bfloat16), "cp", scatter_dimension=1, tiled=True
        ).astype(jnp.float32),
    )
    grad_mixed = jnp.concatenate([joined(grad_query), grad_keys, grad_vals], axis=-1).astype(
        jnp.bfloat16
    )
    grad_qkv = mat_grad(act_one, grad_mixed)
    grad_act_one = mat_back(grad_mixed, qkv_full)
    grad_input, grad_gain_one, grad_shift_one = back_one(grad_act_one)
    grad_input = (grad_input + grad_resid).astype(jnp.bfloat16)
    returned = lax.all_to_all(grad_input, "dp", split_axis=1, concat_axis=0, tiled=True)
    input_grad = returned[dealing]
    (
        grad_qkv,
        grad_proj,
        grad_up,
        grad_down,
        grad_gain_one,
        grad_shift_one,
        grad_bias_proj,
        grad_gain_two,
        grad_shift_two,
        grad_bias_up,
        grad_bias_down,
    ) = (
        lax.psum_scatter(
            grad_qkv.astype(jnp.bfloat16), "dp", scatter_dimension=1, tiled=True
        ).astype(jnp.float32),
        lax.psum_scatter(
            grad_proj.astype(jnp.bfloat16), "dp", scatter_dimension=1, tiled=True
        ).astype(jnp.float32),
        lax.psum_scatter(
            grad_up.astype(jnp.bfloat16), "dp", scatter_dimension=1, tiled=True
        ).astype(jnp.float32),
        lax.psum_scatter(
            grad_down.astype(jnp.bfloat16), "dp", scatter_dimension=1, tiled=True
        ).astype(jnp.float32),
        lax.psum_scatter(
            grad_gain_one.astype(jnp.bfloat16), "dp", scatter_dimension=0, tiled=True
        ).astype(jnp.float32),
        lax.psum_scatter(
            grad_shift_one.astype(jnp.bfloat16), "dp", scatter_dimension=0, tiled=True
        ).astype(jnp.float32),
        lax.psum_scatter(
            grad_bias_proj.astype(jnp.bfloat16), "dp", scatter_dimension=0, tiled=True
        ).astype(jnp.float32),
        lax.psum_scatter(
            grad_gain_two.astype(jnp.bfloat16), "dp", scatter_dimension=0, tiled=True
        ).astype(jnp.float32),
        lax.psum_scatter(
            grad_shift_two.astype(jnp.bfloat16), "dp", scatter_dimension=0, tiled=True
        ).astype(jnp.float32),
        lax.psum_scatter(
            grad_bias_up.astype(jnp.bfloat16), "dp", scatter_dimension=0, tiled=True
        ).astype(jnp.float32),
        lax.psum_scatter(
            grad_bias_down.astype(jnp.bfloat16), "dp", scatter_dimension=0, tiled=True
        ).astype(jnp.float32),
    )
    grad_qkv, grad_proj, grad_up, grad_down = (
        lax.psum_scatter(
            grad_qkv.astype(jnp.bfloat16), "cp", scatter_dimension=0, tiled=True
        ).astype(jnp.float32),
        lax.psum_scatter(
            grad_proj.astype(jnp.bfloat16), "cp", scatter_dimension=0, tiled=True
        ).astype(jnp.float32),
        lax.psum_scatter(
            grad_up.astype(jnp.bfloat16), "cp", scatter_dimension=0, tiled=True
        ).astype(jnp.float32),
        lax.psum_scatter(
            grad_down.astype(jnp.bfloat16), "cp", scatter_dimension=0, tiled=True
        ).astype(jnp.float32),
    )
    (
        grad_gain_one,
        grad_shift_one,
        grad_bias_proj,
        grad_gain_two,
        grad_shift_two,
        grad_bias_up,
        grad_bias_down,
    ) = lax.psum(
        (
            grad_gain_one,
            grad_shift_one,
            grad_bias_proj,
            grad_gain_two,
            grad_shift_two,
            grad_bias_up,
            grad_bias_down,
        ),
        "cp",
    )
    return (
        output,
        input_grad,
        grad_qkv,
        grad_proj,
        grad_up,
        grad_down,
        grad_gain_one,
        grad_shift_one,
        grad_bias_proj,
        grad_gain_two,
        grad_shift_two,
        grad_bias_up,
        grad_bias_down,
    )


def solution(mesh):
    in_specs = (
        P(None, ("cp", "dp"), None),
        P("dp", "cp", None),
        P(),
        P(),
        P("cp", "dp"),
        P("cp", "dp"),
        P("cp", "dp"),
        P("cp", "dp"),
        P("dp"),
        P("dp"),
        P("dp"),
        P("dp"),
        P("dp"),
        P("dp"),
        P("dp"),
    )
    out_specs = (
        P("dp", "cp", None),
        P(None, ("cp", "dp"), None),
        P("cp", "dp"),
        P("cp", "dp"),
        P("cp", "dp"),
        P("cp", "dp"),
        P("dp"),
        P("dp"),
        P("dp"),
        P("dp"),
        P("dp"),
        P("dp"),
        P("dp"),
    )
    planned = tuple(mesh.shape.items()) == (("dp", Z * Y * C), ("cp", X))
    local = slice_plan if planned else general
    return jax.shard_map(local, mesh=mesh, in_specs=in_specs, out_specs=out_specs, check_vma=False)
```

```python
import functools
import math

import jax
import jax.numpy as jnp
from jax import lax
from jax.experimental import pallas as pl
from jax.experimental.pallas import tpu as pltpu
from jax.sharding import PartitionSpec as P

HEADS = 12
HEAD_DIM = 64


EPSILON = 1e-05
NEG_BIG = -1e30
TANH_SCALE = 0.7978845608028654
CUBIC_TERM = 0.044715
MESH_IDS = pl.DeviceIdType.MESH
BF = jnp.bfloat16
F32 = jnp.float32

Z, Y, C, X = 4, 2, 2, 2


def mult(value, n):
    return value if isinstance(value, int) else pl.multiple_of(value, n)


def coords():
    d = lax.axis_index("dp")
    x = lax.axis_index("cp")
    return d // (Y * C), (d // C) % Y, d % C, x, d


def dev(z, y, c, x):
    return {"dp": (z * Y + y) * C + c, "cp": x}


def rcopy(src, dst, ssem, rsem, where):
    return pltpu.make_async_remote_copy(
        src_ref=src, dst_ref=dst, send_sem=ssem, recv_sem=rsem, device_id=where, device_id_type=MESH_IDS
    )


def lcopy(src, dst, sem):
    return pltpu.make_async_copy(src, dst, sem)


def wait_bytes(ref, sem):
    pltpu.make_async_copy(ref, ref, sem).wait()


def enter(everyone):
    d = lax.axis_index("dp")
    x = lax.axis_index("cp")
    barrier = pltpu.get_barrier_semaphore()

    def greet(k, carry):
        kd = k // X
        kx = k % X

        @pl.when(jnp.logical_or(kd != d, kx != x))
        def _():
            pl.semaphore_signal(barrier, inc=1, device_id={"dp": kd, "cp": kx}, device_id_type=MESH_IDS)

        return carry

    lax.fori_loop(0, everyone, greet, 0)

    def entered():
        pl.semaphore_wait(barrier, everyone - 1)

    return entered


def dot_nn(a, b):
    return lax.dot_general(a, b, (((1,), (0,)), ((), ())), preferred_element_type=F32)


def dot_nt(a, b):
    return lax.dot_general(a, b, (((1,), (1,)), ((), ())), preferred_element_type=F32)


def dot_tn(a, b):
    return lax.dot_general(a, b, (((0,), (0,)), ((), ())), preferred_element_type=F32)


def norm_parts(v):
    mean = jnp.mean(v, axis=-1, keepdims=True)
    cen = v - mean
    var = jnp.mean(cen * cen, axis=-1, keepdims=True)
    rstd = lax.rsqrt(var + EPSILON)
    return cen * rstd, rstd


def live_length(len_ref, deal_ref, slot):
    total = jnp.int32(0)
    for s in range(len_ref.shape[0]):
        total = total + jnp.where(deal_ref[s] == slot, len_ref[s], 0)
    return total


class Piece:
    def __init__(self, full, R, r0, rn, step, c0, cn):
        self.full = full
        self.R, self.r0, self.rn, self.step, self.c0, self.cn = R, r0, rn, step, c0, cn

    def at(self, z, y, c, x):
        d = (z * Y + y) * C + c
        return self.full.at[
            pl.ds(mult(d * self.R + self.r0, 16), self.rn), pl.ds(mult(x * self.step + self.c0, 128), self.cn)
        ]


class Gather:
    ZS, ZR, S2, R2, S3, R3, S4, R4 = range(8)

    def __init__(self, piece, sems, k, dummy, where, turned):
        self.p, self.sems, self.k, self.dummy = piece, sems, k, dummy
        z, y, c, x, _ = where
        self.z, self.y, self.c, self.x = z, y, c, x
        self.o = o = 1 if turned else c
        self.y2, self.x2 = (y + 1 - o) % 2, (x + o) % 2
        self.y3, self.x3 = (y + o) % 2, (x + 1 - o) % 2

    def sem(self, which):
        return self.sems.at[self.k, which]

    def wait(self, count, which):
        p = self.p
        wait_bytes(self.dummy.at[pl.ds(0, count * p.rn), pl.ds(0, p.cn)], self.sem(which))

    def start(self):
        p, z, y, c, x = self.p, self.z, self.y, self.c, self.x
        own = p.at(z, y, c, x)
        for dz in range(1, Z):
            z2 = (z + dz) % Z
            rcopy(own, own, self.sem(self.ZS), self.sem(self.ZR), dev(z2, y, c, x)).start()

    def tick2(self):
        p, z, y, c, x = self.p, self.z, self.y, self.c, self.x
        self.wait(Z - 1, self.ZR)
        for zz in range(Z):
            q = p.at(zz, y, c, x)
            rcopy(q, q, self.sem(self.S2), self.sem(self.R2), dev(z, self.y2, c, self.x2)).start()
        for zz in range(Z):
            q = p.at(zz, y, c, x)
            rcopy(q, q, self.sem(self.S3), self.sem(self.R3), dev(z, self.y3, c, self.x3)).start()
            rcopy(q, q, self.sem(self.S4), self.sem(self.R4), dev(z, y, 1 - c, x)).start()

    def tick3(self):
        p, z, y, c, x = self.p, self.z, self.y, self.c, self.x
        self.wait(Z, self.R2)
        for zz in range(Z):
            q = p.at(zz, self.y2, c, self.x2)
            rcopy(q, q, self.sem(self.S3), self.sem(self.R3), dev(z, self.y3, c, self.x3)).start()
            rcopy(q, q, self.sem(self.S4), self.sem(self.R4), dev(z, y, 1 - c, x)).start()

    def tick4(self):
        p, z, y, c, x = self.p, self.z, self.y, self.c, self.x
        self.wait(2 * Z, self.R3)
        for zz in range(Z):
            for which in range(2):
                yy = which * (1 - self.o) + (1 - y) * self.o
                xx = (1 - x) * (1 - self.o) + which * self.o
                q = p.at(zz, yy, c, xx)
                rcopy(q, q, self.sem(self.S4), self.sem(self.R4), dev(z, y, 1 - c, x)).start()

    def tick5(self):
        self.wait(4 * Z, self.R4)

    def drain(self):
        self.wait(Z - 1, self.ZS)
        self.wait(Z, self.S2)
        self.wait(2 * Z, self.S3)
        self.wait(4 * Z, self.S4)


class Vectors:
    ZS, ZR, S2, R2, S4, R4 = range(6)

    def __init__(self, full, sems, where):
        self.full, self.sems, self.where = full, sems, where

    def at(self, z, y, c):
        return self.full.at[(z * Y + y) * C + c]

    def start(self):
        z, y, c, x, _ = self.where
        own = self.at(z, y, c)
        for dz in range(1, Z):
            z2 = (z + dz) % Z
            rcopy(own, own, self.sems.at[self.ZS], self.sems.at[self.ZR], dev(z2, y, c, x)).start()

    def wait(self, count, which):
        wait_bytes(self.full.at[pl.ds(0, count)], self.sems.at[which])

    def tick2(self):
        z, y, c, x, _ = self.where
        self.wait(Z - 1, self.ZR)
        for zz in range(Z):
            q = self.at(zz, y, c)
            rcopy(q, q, self.sems.at[self.S2], self.sems.at[self.R2], dev(z, 1 - y, c, x)).start()
            rcopy(q, q, self.sems.at[self.S4], self.sems.at[self.R4], dev(z, y, 1 - c, x)).start()

    def tick3(self):
        z, y, c, x, _ = self.where
        self.wait(Z, self.R2)
        for zz in range(Z):
            q = self.at(zz, 1 - y, c)
            rcopy(q, q, self.sems.at[self.S4], self.sems.at[self.R4], dev(z, y, 1 - c, x)).start()

    def tick4(self):
        self.wait(2 * Z, self.R4)

    def drain(self):
        self.wait(Z - 1, self.ZS)
        self.wait(Z, self.S2)
        self.wait(2 * Z, self.S4)


G1, C1, BP, G2, C2, BD, BU = range(7)


def gather_chunks(wq, wp, wu, wd):
    rq, rp, ru, rd = (w.shape[0] // (Z * Y * C) for w in (wq, wp, wu, wd))
    half, wide = wq.shape[1] // X, wd.shape[1] // X
    out = []
    for k in range(3):
        out.append(Piece(wq, rq, k * (rq // 3), rq // 3, half, 0, half))
    out.append(Piece(wp, rp, 0, rp, half, 0, half))
    for k in range(4):
        out.append(Piece(wu, ru, k * (ru // 4), ru // 4, half, 0, half))
    for k in range(4):
        out.append(Piece(wd, rd, 0, rd, wide, k * (wide // 4), wide // 4))
    return out


def one_hot(count, width, first):
    at_row = lax.broadcasted_iota(jnp.int32, (count, width), 0)
    at_col = lax.broadcasted_iota(jnp.int32, (count, width), 1)
    return (at_col == at_row + first).astype(BF)


N_GATHER = 12
TURNED = (7, 9, 11)
COT_STEPS = (5, 7)


def forward_kernel(
    len_ref, deal_ref, cot, x_in, sq, sp, su, sd, v_g1, v_c1, v_bp, v_g2, v_c2, v_bd, v_bu,
    wq_o, wp_o, wu_o, wd_o, xr_o, gw_o, qs_o, ka_o, va_o, at_o, lse_o, r_o, a2_o, hd_o, gp_o, vec_o, out_o,
    wq, wp, wu, wd, xr, a1, qs, ka, va, at, lse, r, a2, hd, gp, vg, vec, bu3, sc0, sc1, outw, xg, acc,
    gsem, vsem, msem, osem,
):
    where = coords()
    z, y, c, x, d = where
    width = xr.shape[1]
    rows = xr.shape[0]
    qrows = rows // 2
    small = x_in.shape[1]
    pairs = width // 128
    tile = 256

    entered = enter(Z * Y * C * X)

    n = Z * Y * C
    for shard, full in ((sq, wq), (sp, wp), (su, wu), (sd, wd)):
        own, long = shard.shape
        full[pl.ds(mult(d * own, 16), own), pl.ds(mult(x * long, 128), long)] = shard[...].astype(BF)
    vg[d] = jnp.zeros(vg.shape[1:], BF)
    own = v_g1.shape[1]
    seven = jnp.concatenate([v[...] for v in (v_g1, v_c1, v_bp, v_g2, v_c2, v_bd)], axis=0).astype(BF)
    placed = dot_nn(seven, one_hot(own, width, d * own))
    long = v_bu.shape[1]
    per_row = width // long
    placed_long = dot_nn(v_bu[...].astype(BF), one_hot(long, width, (d % per_row) * long))
    rows_long = [jnp.where(d // per_row == k, placed_long, 0.0) for k in range(n // per_row)]
    rest = jnp.zeros((16 - 6 - n // per_row, width), F32)
    vg[d] = jnp.concatenate([placed] + rows_long + [rest], axis=0).astype(BF)
    slots = x_in.shape[0]
    for t in range(slots):
        owner = jnp.int32(0)
        for s in range(slots):
            owner = jnp.where(deal_ref[s] == t, s, owner)
        xg[t] = x_in[owner]

    entered()

    vectors = Vectors(vg, vsem, where)
    vectors.start()
    chunks = [
        Gather(p, gsem, k, wu, where, k in TURNED) for k, p in enumerate(gather_chunks(wq, wp, wu, wd))
    ]

    def send_cot(b):
        core_b = (x + b) % 2
        src_b = cot.at[pl.ds(b * qrows, qrows)]
        dst_b = gw_o.at[pl.ds(mult(x * qrows, qrows), qrows)]
        same = jnp.logical_and(core_b == c, c == x)

        @pl.when(same)
        def _():
            lcopy(src_b, dst_b, msem.at[3]).start()

        @pl.when(jnp.logical_not(same))
        def _():
            rcopy(src_b, dst_b, msem.at[2], msem.at[3], dev(z, y, core_b, c)).start()

    per_quarter = qrows // small
    place = mult(x * qrows + (d % per_quarter) * small, 16)
    core_to = (x + d // per_quarter) % 2
    dst = xr.at[pl.ds(place, small)]

    def deal_out(k, carry):
        t = (d + k + x * (slots // 2)) % slots
        td = (t // 2) * 2 + core_to
        tx = t % 2
        mine = jnp.logical_and(td == d, tx == x)

        @pl.when(mine)
        def _():
            lcopy(xg.at[t], dst, msem.at[1]).start()

        @pl.when(jnp.logical_not(mine))
        def _():
            rcopy(xg.at[t], dst, msem.at[0], msem.at[1], {"dp": td, "cp": tx}).start()

        return carry

    ahead = 2
    for ch in chunks[:ahead]:
        ch.start()

    def step(s):
        if s + ahead < len(chunks):
            chunks[s + ahead].start()
        if s < 4:
            lax.fori_loop(s * slots // 4, (s + 1) * slots // 4, deal_out, 0)
        if s in COT_STEPS:
            send_cot(COT_STEPS.index(s))
        for back, name in ((0, "tick2"), (1, "tick3"), (2, "tick4")):
            if 0 <= s - back < len(chunks):
                getattr(chunks[s - back], name)()

    step(0)
    vectors.tick2()
    step(1)
    vectors.tick3()
    step(2)
    step(3)
    vectors.tick4()

    def add_table(k, acc):
        return acc + vg[k].astype(F32)

    vec[...] = lax.fori_loop(1, Z * Y * C, add_table, vg[0].astype(F32))
    for k in range(bu3.shape[0]):
        per = width // tile
        bu3[k] = vec[BU + k // per:BU + k // per + 1, (k % per) * tile:(k % per + 1) * tile]

    wait_bytes(xr, msem.at[1])
    lrows = 128

    def first_norm(k, carry):
        at_rows = pl.ds(mult(k * lrows, lrows), lrows)
        n1, _ = norm_parts(xr[at_rows, :].astype(F32))
        a1[at_rows, :] = (n1 * vec[G1:G1 + 1, :] + vec[C1:C1 + 1, :]).astype(BF)
        return carry

    lax.fori_loop(0, rows // lrows, first_norm, 0)

    step(4)
    for k in range(3):
        chunks[k].tick5()
    keep = [pltpu.make_async_copy(wq, wq_o, osem.at[0])]
    keep[-1].start()

    quarters = (c, 3 - c)

    def q_at(i):
        return pl.ds(mult(quarters[i] * qrows, qrows), qrows)

    steps = width // tile
    for part in range(3):
        def project(n, carry, part=part):
            lanes = pl.ds(mult(n * tile, tile), tile)
            res = dot_nt(a1[...], wq[pl.ds(mult(part * width + n * tile, tile), tile), :]).astype(BF)
            if part == 0:
                qs[:, lanes] = res * jnp.asarray(HEAD_DIM ** -0.5, BF)
            else:
                to = ka if part == 1 else va
                for i in range(2):
                    to[q_at(i), lanes] = res[i * qrows:(i + 1) * qrows]
            return carry

        lax.fori_loop(0, steps, project, 0)
        if part > 0:
            to = ka if part == 1 else va
            for i in range(2):
                rcopy(to.at[q_at(i)], to.at[q_at(i)], msem.at[4 + 2 * (part - 1)], msem.at[5 + 2 * (part - 1)], dev(z, y, 1 - c, x)).start()
    step(5)
    wait_bytes(ka.at[pl.ds(0, rows)], msem.at[5])
    wait_bytes(va.at[pl.ds(0, rows)], msem.at[7])
    for src, out, s in ((qs, qs_o, 1), (ka, ka_o, 2), (va, va_o, 3), (xr, xr_o, 4), (vec, vec_o, 5)):
        keep.append(pltpu.make_async_copy(src, out, osem.at[s]))
        keep[-1].start()

    lane = lax.broadcasted_iota(jnp.int32, (qrows, 128), 1)
    kpos = lax.broadcasted_iota(jnp.int32, (qrows, qrows), 0)
    qpos = lax.broadcasted_iota(jnp.int32, (qrows, qrows), 1)
    groups = qrows // 8

    def pair_body(p, carry):
        lanes = pl.ds(mult(p * 128, 128), 128)
        for i in range(2):
            quarter = quarters[i]
            qp = qs[i * qrows:(i + 1) * qrows, lanes]
            zero = jnp.zeros_like(qp)
            qh = (jnp.where(lane < HEAD_DIM, qp, zero), jnp.where(lane >= HEAD_DIM, qp, zero))

            def scores(j, tops):
                at_keys = pl.ds(mult(j * qrows, qrows), qrows)
                kj = ka[at_keys, lanes]
                keep_it = jnp.logical_or(kpos <= qpos, j < quarter)
                new = []
                for h, sc in enumerate((sc0, sc1)):
                    s = jnp.where(keep_it, dot_nt(kj, qh[h]), NEG_BIG)
                    sc[at_keys, :] = s
                    new.append(jnp.maximum(tops[h], jnp.max(s.reshape(groups, 8, qrows), axis=0)))
                return tuple(new)

            low = jnp.full((8, qrows), NEG_BIG, F32)
            tops = lax.fori_loop(0, quarter + 1, scores, (low, low))
            tops = tuple(jnp.max(t, axis=0, keepdims=True) for t in tops)

            def values(j, state):
                at_keys = pl.ds(mult(j * qrows, qrows), qrows)
                vt = va[at_keys, lanes].T
                new = []
                for h, sc in enumerate((sc0, sc1)):
                    total, acc = state[h]
                    e = jnp.exp(sc[at_keys, :] - tops[h])
                    total = total + jnp.sum(e.reshape(groups, 8, qrows), axis=0)
                    acc = acc + dot_nn(vt[h * HEAD_DIM:(h + 1) * HEAD_DIM], e.astype(BF))
                    new.append((total, acc))
                return tuple(new)

            blank = (jnp.zeros((8, qrows), F32), jnp.zeros((HEAD_DIM, qrows), F32))
            state = lax.fori_loop(0, quarter + 1, values, (blank, blank))
            parts = []
            for h in range(2):
                total = jnp.sum(state[h][0], axis=0, keepdims=True)
                parts.append(state[h][1] / total)
                lse[p, i * 2 + h:i * 2 + h + 1, :] = tops[h] + jnp.log(total)
            at[i * qrows:(i + 1) * qrows, lanes] = jnp.concatenate(parts, axis=0).T.astype(BF)
        return carry

    per = 2
    for k in range(0, pairs, per):
        lax.fori_loop(k, k + per, pair_body, 0)
        step(6 + k // per)

    chunks[3].tick5()
    for src, out, s in ((wp, wp_o, 6), (at, at_o, 7), (lse, lse_o, 8)):
        keep.append(pltpu.make_async_copy(src, out, osem.at[s]))
        keep[-1].start()

    def attend_out(n, carry):
        lanes = pl.ds(mult(n * tile, tile), tile)
        res = dot_nt(at[...], wp[pl.ds(mult(n * tile, tile), tile), :])
        r[:, lanes] = xr[:, lanes].astype(F32) + res + vec[BP:BP + 1, lanes]
        return carry

    lax.fori_loop(0, steps, attend_out, 0)

    def second_norm(k, carry):
        at_rows = pl.ds(mult(k * lrows, lrows), lrows)
        n2, _ = norm_parts(r[at_rows, :])
        a2[at_rows, :] = (n2 * vec[G2:G2 + 1, :] + vec[C2:C2 + 1, :]).astype(BF)
        return carry

    lax.fori_loop(0, rows // lrows, second_norm, 0)
    step(9)
    for k in range(4, 8):
        chunks[k].tick5()
    for src, out, s in ((wu, wu_o, 9), (r, r_o, 10), (a2, a2_o, 11)):
        keep.append(pltpu.make_async_copy(src, out, osem.at[s]))
        keep[-1].start()

    def up(n, carry):
        lanes = pl.ds(mult(n * tile, tile), tile)
        u = dot_nt(a2[...], wu[lanes, :]) + bu3[n]
        sq_u = u * u
        t = jnp.tanh(TANH_SCALE * (u + CUBIC_TERM * sq_u * u))
        half_up = 0.5 * (1.0 + t)
        hd[:, lanes] = (u * half_up).astype(BF)
        slope = TANH_SCALE * (1.0 + 3.0 * CUBIC_TERM * sq_u)
        gp[:, lanes] = (half_up + 0.5 * u * (1.0 - t * t) * slope).astype(BF)
        return carry

    blocks = hd.shape[1] // tile
    for k in range(0, blocks, 4):
        lax.fori_loop(k, k + 4, up, 0)
        step(10 + k // 4)
    for src, out, s in ((hd, hd_o, 12), (gp, gp_o, 13)):
        keep.append(pltpu.make_async_copy(src, out, osem.at[s]))
        keep[-1].start()
    my_len = live_length(len_ref, deal_ref, (z * Y + y) * C + x)
    rowpos = lax.broadcasted_iota(jnp.int32, (qrows, 1), 0)
    parts = len(chunks) - 8
    wide = wd.shape[1] // X
    for k in range(parts):
        if k == 1:
            step(13)
        chunks[8 + k].tick5()
        cuts = [slice(h * wide + k * (wide // parts), h * wide + (k + 1) * (wide // parts)) for h in range(X)]
        for h, cut in enumerate(cuts):
            keep.append(pltpu.make_async_copy(wd.at[:, cut], wd_o.at[:, cut], osem.at[16 + X * k + h]))
            keep[-1].start()

        def down(n, carry, k=k, cuts=cuts):
            lanes = pl.ds(mult(n * tile, tile), tile)
            res = dot_nt(hd[:, cuts[0]], wd[lanes, cuts[0]])
            for cut in cuts[1:]:
                res = res + dot_nt(hd[:, cut], wd[lanes, cut])
            res = res + (r[:, lanes] + vec[BD:BD + 1, lanes] if k == 0 else acc[:, lanes])
            if k < parts - 1:
                acc[:, lanes] = res
            else:
                for i in range(2):
                    live = quarters[i] * qrows + rowpos < my_len
                    outw[i * qrows:(i + 1) * qrows, lanes] = jnp.where(live, res[i * qrows:(i + 1) * qrows], 0.0).astype(BF)
            return carry

        lax.fori_loop(0, steps, down, 0)
    keep.append(pltpu.make_async_copy(outw, out_o, osem.at[15]))
    keep[-1].start()

    for ch in chunks:
        ch.drain()
    vectors.drain()

    @pl.when(core_to == c)
    def _():
        wait_bytes(xr.at[pl.ds(0, rows - small)], msem.at[0])

    @pl.when(core_to != c)
    def _():
        wait_bytes(xr, msem.at[0])

    @pl.when(c == x)
    def _():
        wait_bytes(xr.at[pl.ds(0, qrows)], msem.at[2])

    @pl.when(c != x)
    def _():
        wait_bytes(xr, msem.at[2])

    wait_bytes(xr, msem.at[3])
    wait_bytes(ka.at[pl.ds(0, rows)], msem.at[4])
    wait_bytes(va.at[pl.ds(0, rows)], msem.at[6])
    for cp in keep:
        cp.wait()


def forward(lengths, dealing, cot, x_source, shards, vectors):
    slots, small, width = x_source.shape
    rows = cot.shape[0]
    ff = shards[2].shape[0] * Z * Y * C
    keys = rows * 2
    pairs = width // 128

    def arr(shape, dtype=BF):
        return jax.ShapeDtypeStruct(shape, dtype)

    outs = [
        arr((3 * width, width)), arr((width, width)), arr((ff, width)), arr((width, ff)),
        arr((rows, width)), arr((rows, width)), arr((rows, width)), arr((keys, width)), arr((keys, width)),
        arr((rows, width)), arr((pairs, 8, rows // 2), F32), arr((rows, width), F32), arr((rows, width)),
        arr((rows, ff)), arr((rows, ff)), arr((16, width), F32), arr((rows, width)),
    ]
    vm = pltpu.VMEM
    scratch = [
        vm((3 * width, width), BF), vm((width, width), BF), vm((ff, width), BF), vm((width, ff), BF),
        vm((rows, width), BF), vm((rows, width), BF), vm((rows, width), BF), vm((keys, width), BF),
        vm((keys, width), BF), vm((rows, width), BF), vm((pairs, 8, rows // 2), F32), vm((rows, width), F32),
        vm((rows, width), BF), vm((rows, ff), BF), vm((rows, ff), BF), vm((Z * Y * C, 16, width), BF),
        vm((16, width), F32), vm((ff // 256, 1, 256), F32), vm((keys, rows // 2), F32), vm((keys, rows // 2), F32),
        vm((rows, width), BF), vm(x_source.shape, BF), vm((rows, width), F32),
        pltpu.SemaphoreType.DMA((N_GATHER, 8)), pltpu.SemaphoreType.DMA((6,)), pltpu.SemaphoreType.DMA((8,)),
        pltpu.SemaphoreType.DMA((24,)),
    ]
    anyspec = pl.BlockSpec(memory_space=pl.ANY)
    smem = pl.BlockSpec(memory_space=pltpu.SMEM)
    vmem = pl.BlockSpec(memory_space=pltpu.VMEM)
    return pl.pallas_call(
        forward_kernel,
        out_shape=outs,
        in_specs=[smem, smem, anyspec] + [vmem] * 12,
        out_specs=[anyspec] * len(outs),
        scratch_shapes=scratch,
        compiler_params=pltpu.CompilerParams(
            collective_id=0, has_side_effects=True, vmem_limit_bytes=60 * 1024 * 1024
        ),
        name="forward",
    )(lengths, dealing, cot, x_source, *shards, *vectors)


def when(cond):
    if isinstance(cond, bool):
        return (lambda f: f()) if cond else (lambda f: None)
    return pl.when(cond)


class Reduce:
    S1, R1, S2, R2, S3, R3, S4, R4, S5, R5 = range(10)

    def __init__(self, grad, R, step, c0, C, zlist, bufs, out, out_c0, sems, k, where, turned):
        self.grad, self.R, self.step, self.c0, self.cn, self.zlist = grad, R, step, c0, C, zlist
        self.r1, self.r2, self.r3, self.r4, self.r5 = bufs
        self.out, self.out_c0, self.sems, self.k = out, out_c0, sems, k
        self.z, self.y, self.c, self.x, _ = where
        y, x = self.y, self.x
        self.o = o = 1 if turned else self.c
        self.y2, self.x2 = (y + o) % 2, (x + 1 - o) % 2
        self.y3, self.x3 = (y + 1 - o) % 2, (x + o) % 2
        self.every = len(zlist) == Z

    def sem(self, which):
        return self.sems.at[self.k, which]

    def rows(self, z, y, c):
        return pl.ds(mult(((z * Y + y) * C + c) * self.R, 16), self.R)

    def cols(self, x):
        return pl.ds(mult(x * self.step + self.c0, 128), self.cn)

    def at(self, z, y, c, x):
        return self.grad.at[self.rows(z, y, c), self.cols(x)]

    def add(self, rows, cols, got):
        self.grad[rows, cols] = (self.grad[rows, cols].astype(F32) + got.astype(F32)).astype(BF)

    def zidx(self, zi):
        return zi if self.every else self.zlist[0]

    def start(self):
        z, y, c, x = self.z, self.y, self.c, self.x
        to = dev(z, y, 1 - c, x)
        for zi, zz in enumerate(self.zlist):
            for yy in range(Y):
                for xx in range(X):
                    rcopy(
                        self.at(zz, yy, 1 - c, xx), self.r1.at[zi * Y + yy, xx],
                        self.sem(self.S1), self.sem(self.R1), to,
                    ).start()

    def tick2(self):
        z, y, c, x, o = self.z, self.y, self.c, self.x, self.o
        wait_bytes(self.r1, self.sem(self.R1))

        def body(e, carry):
            rows = self.rows(self.zidx(e // Y), e % Y, c)
            for xx in range(X):
                self.add(rows, self.cols(xx), self.r1[e, xx])
            return carry

        lax.fori_loop(0, len(self.zlist) * Y, body, 0)
        to = dev(z, self.y2, c, self.x2)
        for zi, zz in enumerate(self.zlist):
            for w in range(2):
                yy = w * (1 - o) + (1 - y) * o
                xx = (1 - x) * (1 - o) + w * o
                rcopy(self.at(zz, yy, c, xx), self.r2.at[zi * 2 + w], self.sem(self.S2), self.sem(self.R2), to).start()

    def tick3(self):
        z, y, c, x, o = self.z, self.y, self.c, self.x, self.o
        wait_bytes(self.r2, self.sem(self.R2))

        def body(e, carry):
            w = e % 2
            yy = w * (1 - o) + y * o
            xx = x * (1 - o) + w * o
            self.add(self.rows(self.zidx(e // 2), yy, c), self.cols(xx), self.r2[e])
            return carry

        lax.fori_loop(0, len(self.zlist) * 2, body, 0)
        to = dev(z, self.y3, c, self.x3)
        for zi, zz in enumerate(self.zlist):
            rcopy(self.at(zz, self.y3, c, self.x3), self.r3.at[zi], self.sem(self.S3), self.sem(self.R3), to).start()

    def first_hop(self, k):
        return [(k ^ 1, k, 0), ((3 - k) ^ 1, 3 - k, 1)]

    def tick4(self):
        z, y, c, x = self.z, self.y, self.c, self.x
        wait_bytes(self.r3, self.sem(self.R3))

        def body(zi, carry):
            self.add(self.rows(self.zidx(zi), y, c), self.cols(x), self.r3[zi])
            return carry

        lax.fori_loop(0, len(self.zlist), body, 0)
        if self.every:
            mate = z + 1 - 2 * (z % 2)
            for slot, zz in enumerate((mate, 3 - mate)):
                rcopy(
                    self.at(zz, y, c, x), self.r4.at[slot], self.sem(self.S4), self.sem(self.R4), dev(mate, y, c, x)
                ).start()
        else:
            k = self.zlist[0]
            for sender, taker, slot in self.first_hop(k):
                @pl.when(z == sender)
                def _(taker=taker, slot=slot):
                    rcopy(
                        self.at(k, y, c, x), self.r4.at[slot], self.sem(self.S4), self.sem(self.R4),
                        dev(taker, y, c, x),
                    ).start()

    def tick5(self):
        z, y, c, x = self.z, self.y, self.c, self.x
        k = self.zlist[0]

        def take(zz, slot):
            self.add(self.rows(zz, y, c), self.cols(x), self.r4[slot])

        def pass_on(zz):
            rcopy(self.at(zz, y, c, x), self.r5, self.sem(self.S5), self.sem(self.R5), dev(zz, y, c, x)).start()

        if self.every:
            wait_bytes(self.r4, self.sem(self.R4))
            take(3 - z, 1)
            pass_on(3 - z)
            take(z, 0)
        else:
            @pl.when(z == 3 - k)
            def _():
                wait_bytes(self.r4.at[1], self.sem(self.R4))
                take(k, 1)
                pass_on(k)

            @pl.when(z == k)
            def _():
                wait_bytes(self.r4.at[0], self.sem(self.R4))
                take(k, 0)

    def tick6(self):
        z, y, c, x = self.z, self.y, self.c, self.x

        @when(True if self.every else z == self.zlist[0])
        def _():
            wait_bytes(self.r5, self.sem(self.R5))
            own = self.grad[self.rows(z, y, c), self.cols(x)].astype(F32)
            self.out[:, self.out_c0:self.out_c0 + self.cn] = own + self.r5[...].astype(F32)

    def drain(self):
        z = self.z
        wait_bytes(self.r1, self.sem(self.S1))
        wait_bytes(self.r2, self.sem(self.S2))
        wait_bytes(self.r3, self.sem(self.S3))
        if self.every:
            wait_bytes(self.r4, self.sem(self.S4))
            wait_bytes(self.r5, self.sem(self.S5))
        else:
            k = self.zlist[0]
            for sender, _, slot in self.first_hop(k):
                @pl.when(z == sender)
                def _():
                    wait_bytes(self.r4.at[0], self.sem(self.S4))

            @pl.when(z == 3 - k)
            def _():
                wait_bytes(self.r5, self.sem(self.S5))


TURNED_BACK = (3, 6)


def reduce_shapes(width, ff):
    n = Z * Y * C
    every = list(range(Z))
    half = width // X
    wide = ff // X
    shapes = [("d", width // n, wide, k * (wide // 2), wide // 2, every, k * (wide // 2)) for k in range(2)]
    shapes += [("u", ff // n, half, 0, half, [k], 0) for k in range(Z)]
    shapes += [("p", width // n, half, 0, half, every, 0)]
    shapes += [("q", 3 * width // n, half, 0, half, [k], 0) for k in range(Z)]
    return shapes


def backward_kernel(*refs):
    names = (
        "len_ref", "deal_ref", "wq_i", "wp_i", "wu_i", "wd_i", "xr_i", "gw_i", "qs_i", "ka_i", "va_i", "at_i",
        "lse_i", "r_i", "a2_i", "hd_i", "gp_i", "vec_i", "out_i", "og_q", "og_p", "og_u", "og_d", "osum", "ret",
        "out_n", "wq", "wp", "xr", "g", "qs", "ka", "va", "at", "lse", "r", "a2", "vec", "gt", "d2", "dr", "drl",
        "do", "gq", "gp_", "gu", "gd", "wd_t", "wu_t", "hd_t", "gp_t", "dka", "dva", "own_v", "sv", "rk", "rv", "dm",
        "vs", "vr", "bub", "ret_v", "lsem", "tsem", "rsem", "msem", "vsem",
    )
    env = dict(zip(names, refs[: len(names)]))
    env.update(a1=env["a2"], own_k=env["d2"], sk=env["drl"], dx=env["do"])
    bufs = refs[len(names):]
    e = type("Refs", (), env)
    where = coords()
    z, y, c, x, d = where
    rows, width = e.g.shape
    ff = e.hd_i.shape[1]
    qrows = rows // 2
    pairs = width // 128
    tile = 256
    lrows = 128
    steps = width // tile
    quarters = (c, 3 - c)
    theirs = (1 - c, 2 + c)

    def at_quarter(k):
        return pl.ds(mult(k * qrows, qrows), qrows)

    entered = enter(Z * Y * C * X)

    loads = {}
    for k, (src, dst) in enumerate(
        (
            ("gw_i", "g"), ("a2_i", "a2"), ("r_i", "r"), ("vec_i", "vec"), ("wp_i", "wp"), ("at_i", "at"),
            ("qs_i", "qs"), ("ka_i", "ka"), ("va_i", "va"), ("lse_i", "lse"), ("xr_i", "xr"), ("wq_i", "wq"),
        )
    ):
        loads[dst] = pltpu.make_async_copy(env[src], env[dst], e.lsem.at[k])

    def tile_of(idx):
        block = idx // 3
        return (block % 2) * 2 * 3 + (block // 2) * 3 + idx % 3

    def tile_copies(idx):
        n = tile_of(idx)
        slot = idx % 2
        cut = pl.ds(mult(n * tile, tile), tile)
        return (
            pltpu.make_async_copy(e.wd_i.at[:, cut], e.wd_t.at[slot], e.tsem.at[0, slot]),
            pltpu.make_async_copy(e.gp_i.at[:, cut], e.gp_t.at[slot], e.tsem.at[1, slot]),
            pltpu.make_async_copy(e.hd_i.at[:, cut], e.hd_t.at[slot], e.tsem.at[2, slot]),
            pltpu.make_async_copy(e.wu_i.at[cut, :], e.wu_t.at[slot], e.tsem.at[3, slot]),
        )

    loads["g"].start()
    for cp in tile_copies(0):
        cp.start()
    loads["a2"].start()
    for name in ("r", "vec", "wp", "at", "qs", "ka", "va", "lse", "xr", "wq"):
        loads[name].start()

    entered()

    for i in range(2):
        same = jnp.logical_and(x == c, x == i)
        src = e.out_i.at[pl.ds(i * qrows, qrows)]
        dst = e.out_n.at[pl.ds(mult(((i + c) % 2) * qrows, qrows), qrows)]

        @pl.when(same)
        def _(src=src, dst=dst):
            lcopy(src, dst, e.msem.at[1]).start()

        @pl.when(jnp.logical_not(same))
        def _(src=src, dst=dst, i=i):
            rcopy(src, dst, e.msem.at[0], e.msem.at[1], dev(z, y, x, i)).start()

    grads = {"q": (e.gq, e.og_q), "p": (e.gp_, e.og_p), "u": (e.gu, e.og_u), "d": (e.gd, e.og_d)}
    chunks = []
    for k, (name, R, step, c0, cn, zlist, oc) in enumerate(reduce_shapes(width, ff)):
        grad, out = grads[name]
        chunks.append(Reduce(grad, R, step, c0, cn, zlist, bufs[5 * k:5 * k + 5], out, oc, e.rsem, k, where, k in TURNED_BACK))
    dA, dB, u0, u1, u2, u3, pj, q0, q1, q2, q3 = chunks

    my_len = live_length(e.len_ref, e.deal_ref, (z * Y + y) * C + x)
    rowpos = lax.broadcasted_iota(jnp.int32, (lrows, 1), 0)
    loads["g"].wait()
    blank = jnp.zeros((1, width), F32)
    total_bd = blank
    for k in range(rows // lrows):
        base = quarters[k * lrows // qrows] * qrows + (k * lrows) % qrows
        live = base + rowpos < my_len
        part = jnp.where(live, e.g[k * lrows:(k + 1) * lrows, :], jnp.zeros((), BF))
        e.g[k * lrows:(k + 1) * lrows, :] = part
        e.gt[:, k * lrows:(k + 1) * lrows] = part.T
        total_bd = total_bd + jnp.sum(part.astype(F32), axis=0, keepdims=True)
    e.d2[...] = jnp.zeros_like(e.d2)
    loads["a2"].wait()

    ff_tiles = ff // tile
    plan = {
        2: [u0.start], 4: [u0.tick2], 5: [u2.start, dA.start], 7: [u2.tick2], 8: [u1.start, u0.tick3],
        9: [dA.tick2], 10: [u1.tick2, u2.tick3], 11: [u3.start, dB.start, u0.tick4],
    }

    def ffn(idx, carry):
        slot = idx % 2
        n = tile_of(idx)
        cut = pl.ds(mult(n * tile, tile), tile)

        @pl.when(idx + 1 < ff_tiles)
        def _():
            for cp in tile_copies(idx + 1):
                cp.start()

        for cp in tile_copies(idx):
            cp.wait()
        du = (e.gp_t[slot].astype(F32) * dot_nn(e.g[...], e.wd_t[slot])).astype(BF)
        e.bub[n] = jnp.sum(du.astype(F32), axis=0, keepdims=True)
        e.gd[:, cut] = dot_nn(e.gt[...], e.hd_t[slot]).astype(BF)
        e.gu[cut, :] = dot_tn(du, e.a2[...]).astype(BF)
        e.d2[...] += dot_nn(du, e.wu_t[slot])
        for at_idx, acts in plan.items():
            @pl.when(idx == at_idx)
            def _(acts=acts):
                for act in acts:
                    act()
        return carry

    lax.fori_loop(0, ff_tiles, ffn, 0)

    loads["r"].wait()
    loads["vec"].wait()

    def norm_two(k, sums):
        at_rows = pl.ds(mult(k * lrows, lrows), lrows)
        n2, rstd = norm_parts(e.r[at_rows, :])
        da = e.d2[at_rows, :]
        ee = da * e.vec[G2:G2 + 1, :]
        gg = e.g[at_rows, :].astype(F32)
        m1 = jnp.mean(ee, axis=-1, keepdims=True)
        m2 = jnp.mean(ee * n2, axis=-1, keepdims=True)
        dr = gg + (ee - m1 - n2 * m2) * rstd
        e.dr[at_rows, :] = dr
        e.drl[at_rows, :] = dr.astype(BF)
        return (
            sums[0] + jnp.sum(da * n2, axis=0, keepdims=True),
            sums[1] + jnp.sum(da, axis=0, keepdims=True),
            sums[2] + jnp.sum(dr, axis=0, keepdims=True),
        )

    sum_g2, sum_c2, sum_bp = lax.fori_loop(0, rows // lrows, norm_two, (blank, blank, blank))

    loads["wp"].wait()
    loads["at"].wait()

    def proj_back(n, carry):
        cut = pl.ds(mult(n * tile, tile), tile)
        e.do[:, cut] = dot_nn(e.drl[...], e.wp[:, cut]).astype(BF)
        e.gp_[cut, :] = dot_tn(e.drl[:, cut], e.at[...]).astype(BF)
        return carry

    lax.fori_loop(0, steps, proj_back, 0)
    pj.start()
    u3.tick2()
    u0.tick5()

    for name in ("qs", "ka", "va", "lse"):
        loads[name].wait()
    lane = lax.broadcasted_iota(jnp.int32, (qrows, 128), 1)
    kpos = lax.broadcasted_iota(jnp.int32, (qrows, qrows), 0)
    qpos = lax.broadcasted_iota(jnp.int32, (qrows, qrows), 1)

    def split(v):
        zero = jnp.zeros_like(v)
        return jnp.where(lane < HEAD_DIM, v, zero), jnp.where(lane >= HEAD_DIM, v, zero)

    between = {
        (0, 0): [dB.tick2, pj.tick2, dA.tick3], (1, 1): [u1.tick3], (2, 0): [u2.tick4], (2, 1): [u3.tick3],
        (3, 0): [u2.tick5], (4, 0): [dB.tick3, u1.tick4], (5, 0): [u1.tick5], (5, 1): [pj.tick3],
    }

    def pair_body(p, carry):
        lanes = pl.ds(mult(p * 128, 128), 128)
        e.dka[...] = jnp.zeros_like(e.dka)
        e.dva[...] = jnp.zeros_like(e.dva)
        for i in range(2):
            quarter = quarters[i]
            own = slice(i * qrows, (i + 1) * qrows)
            qp, dop = e.qs[own, lanes], e.do[own, lanes]
            qh, doh = split(qp), split(dop)
            qq, dd = jnp.concatenate(qh, axis=0), jnp.concatenate(doh, axis=0)
            prod = (dop.astype(F32) * e.at[own, lanes].astype(F32)).T
            delta = [jnp.sum(prod[h * HEAD_DIM:(h + 1) * HEAD_DIM], axis=0, keepdims=True) for h in range(2)]
            logs = [e.lse[p, i * 2 + h:i * 2 + h + 1, :] for h in range(2)]

            def keys(j, dq):
                at_keys = pl.ds(mult(j * qrows, qrows), qrows)
                kj, vj = e.ka[at_keys, lanes], e.va[at_keys, lanes]
                kt = kj.T
                keep_it = jnp.logical_or(kpos <= qpos, j < quarter)
                probs, grads_s, new = [], [], []
                for h in range(2):
                    s = jnp.where(keep_it, dot_nt(kj, qh[h]), NEG_BIG)
                    pt = jnp.exp(s - logs[h])
                    ds = (pt * (dot_nt(vj, doh[h]) - delta[h])).astype(BF)
                    probs.append(pt.astype(BF))
                    grads_s.append(ds)
                    new.append(dq[h] + dot_nn(kt[h * HEAD_DIM:(h + 1) * HEAD_DIM], ds))
                e.dva[at_keys, :] += dot_nn(jnp.concatenate(probs, axis=1), dd)
                e.dka[at_keys, :] += dot_nn(jnp.concatenate(grads_s, axis=1), qq)
                return tuple(new)

            none = jnp.zeros((HEAD_DIM, qrows), F32)
            dq = lax.fori_loop(0, quarter + 1, keys, (none, none))
            e.dm[own, lanes] = (jnp.concatenate(dq, axis=0).T * HEAD_DIM ** -0.5).astype(BF)
            for (at_p, at_i), acts in between.items():
                if at_i == i:
                    @pl.when(p == at_p)
                    def _(acts=acts):
                        for act in acts:
                            act()
        for i in range(2):
            own = slice(i * qrows, (i + 1) * qrows)
            e.own_k[own, lanes] = e.dka[at_quarter(quarters[i]), :]
            e.own_v[own, lanes] = e.dva[at_quarter(quarters[i]), :]
            e.sk[own, lanes] = e.dka[at_quarter(theirs[i]), :].astype(BF)
            e.sv[own, lanes] = e.dva[at_quarter(theirs[i]), :].astype(BF)
        for k in range(pairs // 2):
            @pl.when(p == 2 * k + 1)
            def _(k=k):
                cut = slice(2 * k * 128, (2 * k + 2) * 128)
                for src, dst, s in ((e.sk, e.rk, 2), (e.sv, e.rv, 4)):
                    rcopy(
                        src.at[:, cut], dst.at[:, cut], e.msem.at[s], e.msem.at[s + 1], dev(z, y, 1 - c, x)
                    ).start()
        return carry

    lax.fori_loop(0, pairs, pair_body, 0)

    loads["xr"].wait()

    def norm_one(k, carry):
        at_rows = pl.ds(mult(k * lrows, lrows), lrows)
        n1, _ = norm_parts(e.xr[at_rows, :].astype(F32))
        e.a1[at_rows, :] = (n1 * e.vec[G1:G1 + 1, :] + e.vec[C1:C1 + 1, :]).astype(BF)
        return carry

    lax.fori_loop(0, rows // lrows, norm_one, 0)

    def qkv_grad(n, carry):
        cut = pl.ds(mult(n * tile, tile), tile)
        e.gq[cut, :] = dot_tn(e.dm[:, cut], e.a1[...]).astype(BF)
        return carry

    lax.fori_loop(0, 3, qkv_grad, 0)
    q0.start()
    dA.tick4()
    wait_bytes(e.rk, e.msem.at[3])
    wait_bytes(e.rv, e.msem.at[5])
    for part, (mine, got) in enumerate(((e.own_k, e.rk), (e.own_v, e.rv))):
        def merge(k, carry, part=part, mine=mine, got=got):
            at_rows = pl.ds(mult(k * lrows, lrows), lrows)
            e.dm[at_rows, (part + 1) * width:(part + 2) * width] = (
                mine[at_rows, :] + got[at_rows, :].astype(F32)
            ).astype(BF)
            return carry

        lax.fori_loop(0, rows // lrows, merge, 0)
    u3.tick4()
    loads["wq"].wait()

    def input_back(n, carry):
        cut = pl.ds(mult(n * tile, tile), tile)
        e.d2[:, cut] = dot_nn(e.dm[...], e.wq[:, cut])
        return carry

    lax.fori_loop(0, steps, input_back, 0)
    q0.tick2()
    pj.tick4()

    def norm_one_back(k, sums):
        at_rows = pl.ds(mult(k * lrows, lrows), lrows)
        n1, rstd = norm_parts(e.xr[at_rows, :].astype(F32))
        da = e.d2[at_rows, :]
        ee = da * e.vec[G1:G1 + 1, :]
        m1 = jnp.mean(ee, axis=-1, keepdims=True)
        m2 = jnp.mean(ee * n1, axis=-1, keepdims=True)
        e.dx[at_rows, :] = (e.dr[at_rows, :] + (ee - m1 - n1 * m2) * rstd).astype(BF)
        return sums[0] + jnp.sum(da * n1, axis=0, keepdims=True), sums[1] + jnp.sum(da, axis=0, keepdims=True)

    sum_g1, sum_c1 = lax.fori_loop(0, rows // lrows, norm_one_back, (blank, blank))
    dB.tick4()
    dA.tick5()

    e.vs[0] = jnp.zeros_like(e.vs[0])
    for row, value in ((G1, sum_g1), (C1, sum_c1), (BP, sum_bp), (G2, sum_g2), (C2, sum_c2), (BD, total_bd)):
        e.vs[0, row:row + 1, :] = value
    per = width // tile
    for k in range(ff_tiles):
        e.vs[0, BU + k // per:BU + k // per + 1, (k % per) * tile:(k % per + 1) * tile] = e.bub[k]
    hops = (
        dev(z, y, 1 - c, x), dev(z, y, c, 1 - x), dev(z, 1 - y, c, x),
        dev(z + 1 - 2 * (z % 2), y, c, x), dev((z + 2) % 4, y, c, x),
    )

    def hop(k):
        rcopy(e.vs.at[k], e.vr.at[k], e.vsem.at[0, k], e.vsem.at[1, k], hops[k]).start()

    def land(k):
        wait_bytes(e.vr.at[k], e.vsem.at[1, k])
        e.vs[k + 1] = e.vs[k] + e.vr[k]

    hop(0)

    small = e.ret.shape[1]
    per_quarter = qrows // small
    slot = (z * Y + y) * C + x

    def give_back(k, carry):
        i = (k + x) % 2
        e8 = (k // 2 + d) % per_quarter
        td = ((i + c) % 2) * per_quarter + e8
        src = e.dx.at[pl.ds(mult(i * qrows + e8 * small, small), small)]
        mine = jnp.logical_and(td == d, x == i)

        @pl.when(mine)
        def _():
            lcopy(src, e.ret_v.at[slot], e.msem.at[7]).start()

        @pl.when(jnp.logical_not(mine))
        def _():
            rcopy(src, e.ret_v.at[slot], e.msem.at[6], e.msem.at[7], {"dp": td, "cp": i}).start()

        return carry

    share = per_quarter // 2
    lax.fori_loop(0, share, give_back, 0)
    lax.fori_loop(3, 5, qkv_grad, 0)
    q1.start()
    lax.fori_loop(share, 2 * share, give_back, 0)
    lax.fori_loop(5, 7, qkv_grad, 0)
    q2.start()
    lax.fori_loop(2 * share, 3 * share, give_back, 0)
    u3.tick5()
    lax.fori_loop(7, 9, qkv_grad, 0)
    q3.start()
    lax.fori_loop(3 * share, 4 * share, give_back, 0)
    q0.tick3()
    q1.tick2()
    pj.tick5()
    land(0)
    hop(1)
    for ch in (u0, u2, u1):
        ch.tick6()
    q2.tick2()
    q3.tick2()
    land(1)
    hop(2)
    dB.tick5()
    dA.tick6()
    q0.tick4()
    q1.tick3()
    land(2)
    hop(3)
    q2.tick3()
    q3.tick3()
    q1.tick4()
    land(3)
    hop(4)
    q2.tick4()
    q3.tick4()
    u3.tick6()
    q0.tick5()
    pj.tick6()
    q1.tick5()
    land(4)
    own = width // (Z * Y * C)
    e.osum[0:6, :] = pltpu.roll(e.vs[5, 0:6, :], (width - d * own) % width, 1)[:, :tile]
    long = ff // (Z * Y * C)
    per_row = width // long
    e.osum[6:7, :] = pltpu.roll(
        e.vs[5, pl.ds(BU + d // per_row, 1), :], (width - (d % per_row) * long) % width, 1
    )[:, :tile]
    e.osum[7:8, :] = jnp.zeros((1, tile), F32)
    q2.tick5()
    q3.tick5()
    dB.tick6()
    wait_bytes(e.dx, e.msem.at[7])
    for s in range(e.ret.shape[0]):
        e.ret[s] = e.ret_v[jnp.clip(e.deal_ref[s], 0, e.ret.shape[0] - 1)]
    for ch in (q0, q1, q2, q3):
        ch.tick6()

    for ch in chunks:
        ch.drain()
    for k in range(5):
        wait_bytes(e.vr.at[k], e.vsem.at[0, k])
    wait_bytes(e.rk, e.msem.at[2])
    wait_bytes(e.rv, e.msem.at[4])

    @pl.when((x + c) % 2 == d // per_quarter)
    def _():
        wait_bytes(e.dx.at[pl.ds(0, rows - small)], e.msem.at[6])

    @pl.when((x + c) % 2 != d // per_quarter)
    def _():
        wait_bytes(e.dx, e.msem.at[6])

    @pl.when(c == x)
    def _():
        wait_bytes(e.dx.at[pl.ds(0, qrows)], e.msem.at[0])

    @pl.when(c != x)
    def _():
        wait_bytes(e.dx, e.msem.at[0])

    wait_bytes(e.dx, e.msem.at[1])


def backward(lengths, dealing, saved, shards):
    wq, wp, wu, wd, xr, gw, qs, ka, va, at, lse, r, a2, hd, gp, vec, outw = saved
    rows, width = xr.shape
    ff = hd.shape[1]
    n = Z * Y * C
    keys = ka.shape[0]
    small = rows // n
    pairs = width // 128

    def arr(shape, dtype=BF):
        return jax.ShapeDtypeStruct(shape, dtype)

    outs = [arr(s.shape, F32) for s in shards] + [
        arr((8, 256), F32), arr((n, small, width)), arr((rows, width)),
    ]
    vm = pltpu.VMEM
    acts = vm((rows, width), BF)
    acts32 = vm((rows, width), F32)
    scratch = [
        vm(wq.shape, BF), vm(wp.shape, BF), acts, acts, acts, vm(ka.shape, BF), vm(va.shape, BF), acts,
        vm(lse.shape, F32), acts32, acts, vm(vec.shape, F32), vm((width, rows), BF), acts32, acts32, acts, acts,
        vm(wq.shape, BF), vm(wp.shape, BF), vm(wu.shape, BF), vm(wd.shape, BF),
        vm((2, width, 256), BF), vm((2, 256, width), BF), vm((2, rows, 256), BF), vm((2, rows, 256), BF),
        vm((keys, 128), F32), vm((keys, 128), F32),
        acts32, acts, acts, acts, vm((rows, 3 * width), BF),
        vm((6, 16, width), F32), vm((5, 16, width), F32), vm((ff // 256, 1, 256), F32), vm((n, small, width), BF),
        pltpu.SemaphoreType.DMA((12,)), pltpu.SemaphoreType.DMA((4, 2)), pltpu.SemaphoreType.DMA((11, 10)),
        pltpu.SemaphoreType.DMA((8,)), pltpu.SemaphoreType.DMA((2, 5)),
    ]
    for _, R, _, _, cn, zlist, _ in reduce_shapes(width, ff):
        k = len(zlist)
        scratch += [vm((2 * k, 2, R, cn), BF), vm((2 * k, R, cn), BF), vm((k, R, cn), BF), vm((2, R, cn), BF), vm((R, cn), BF)]
    anyspec = pl.BlockSpec(memory_space=pl.ANY)
    smem = pl.BlockSpec(memory_space=pltpu.SMEM)
    vmem = pl.BlockSpec(memory_space=pltpu.VMEM)
    return pl.pallas_call(
        backward_kernel,
        out_shape=outs,
        in_specs=[smem, smem] + [anyspec] * len(saved),
        out_specs=[vmem] * 6 + [anyspec],
        scratch_shapes=scratch,
        compiler_params=pltpu.CompilerParams(
            collective_id=1, has_side_effects=True, vmem_limit_bytes=67043328
        ),
        name="backward",
    )(lengths, dealing, *saved)


def slice_plan(
    x_source, cotangent, lengths, dealing, qkv_weight, proj_weight, up_weight, down_weight,
    first_gain, first_shift, proj_bias, second_gain, second_shift, up_bias, down_bias,
):
    shards = [w.T for w in (qkv_weight, proj_weight, up_weight, down_weight)]
    vectors = [
        v[None] for v in (first_gain, first_shift, proj_bias, second_gain, second_shift, down_bias, up_bias)
    ]
    saved = forward(lengths, dealing, cotangent[0], x_source, shards, vectors)
    gq, gp, gu, gd, sums, input_grad, out = backward(lengths, dealing, saved, shards)
    own, long = first_gain.shape[0], up_bias.shape[0]
    return (
        out[None], input_grad, gq.T, gp.T, gu.T, gd.T,
        sums[G1, :own], sums[C1, :own], sums[BP, :own], sums[G2, :own], sums[C2, :own], sums[6, :long], sums[BD, :own],
    )


def layer_norm(values, scaling, offset):
    centered = values - jnp.mean(values, axis=-1, keepdims=True)
    spread = jnp.mean(centered * centered, axis=-1, keepdims=True)
    return centered * lax.rsqrt(spread + EPSILON) * scaling + offset


def gelu_tanh(values):
    return (
        0.5
        * values
        * (1.0 + jnp.tanh(TANH_SCALE * (values + CUBIC_TERM * values * values * values)))
    )


def grouped(array, block_seqs):
    return array.reshape(
        (array.shape[0] // block_seqs, block_seqs, array.shape[1], HEADS, array.shape[2] // HEADS)
    )


def grouped_stats(array, block_seqs):
    return array.reshape((array.shape[0] // block_seqs, block_seqs) + array.shape[1:])


def joined(array):
    return array.reshape(
        (array.shape[0] * array.shape[1], array.shape[2], array.shape[3] * array.shape[4])
    )


def masked_scores(queries, key_rows, query_start, score_scale):
    scores = (
        jnp.einsum("bqhd,bkhd->bhqk", queries, key_rows, preferred_element_type=jnp.float32)
        * score_scale
    )
    query_pos = query_start + jnp.arange(queries.shape[1])
    key_pos = jnp.arange(key_rows.shape[1])
    return jnp.where(key_pos[None, :] <= query_pos[:, None], scores, NEG_BIG)


def attend(inputs, query_start, score_scale):
    queries, key_rows, val_rows = inputs
    scores = masked_scores(queries, key_rows, query_start, score_scale)
    row_top = jnp.max(scores, axis=-1, keepdims=True)
    exponent = jnp.exp(scores - row_top)
    totals = jnp.sum(exponent, axis=-1, keepdims=True)
    weights = (exponent / totals).astype(jnp.bfloat16)
    attended = jnp.einsum("bhqk,bkhd->bqhd", weights, val_rows, preferred_element_type=jnp.float32)
    return (attended.astype(jnp.bfloat16), (row_top + jnp.log(totals))[..., 0])


def rows_back(inputs, query_start, score_scale):
    queries, key_rows, val_rows, grad_rows, log_total = inputs
    scores = masked_scores(queries, key_rows, query_start, score_scale)
    weights = jnp.exp(scores - log_total[..., None])
    grad_weights = jnp.einsum(
        "bqhd,bkhd->bhqk", grad_rows, val_rows, preferred_element_type=jnp.float32
    )
    delta_rows = jnp.sum(weights * grad_weights, axis=-1)
    grad_scores = (weights * (grad_weights - delta_rows[..., None])).astype(jnp.bfloat16)
    grad_query = (
        jnp.einsum("bhqk,bkhd->bqhd", grad_scores, key_rows, preferred_element_type=jnp.float32)
        * score_scale
    )
    grad_keys = (
        jnp.einsum("bhqk,bqhd->bkhd", grad_scores, queries, preferred_element_type=jnp.float32)
        * score_scale
    )
    grad_vals = jnp.einsum(
        "bhqk,bqhd->bkhd",
        weights.astype(jnp.bfloat16),
        grad_rows,
        preferred_element_type=jnp.float32,
    )
    return (grad_query, grad_keys, grad_vals)


def fetch_weights(
    qkv_weight,
    proj_weight,
    up_weight,
    down_weight,
    first_gain,
    first_shift,
    proj_bias,
    second_gain,
    second_shift,
    up_bias,
    down_bias,
):
    qkv_part, proj_part, up_part, down_part = (
        lax.all_gather(qkv_weight.astype(jnp.bfloat16), "cp", axis=0, tiled=True),
        lax.all_gather(proj_weight.astype(jnp.bfloat16), "cp", axis=0, tiled=True),
        lax.all_gather(up_weight.astype(jnp.bfloat16), "cp", axis=0, tiled=True),
        lax.all_gather(down_weight.astype(jnp.bfloat16), "cp", axis=0, tiled=True),
    )
    return (
        lax.all_gather(qkv_part, "dp", axis=1, tiled=True),
        lax.all_gather(proj_part, "dp", axis=1, tiled=True),
        lax.all_gather(up_part, "dp", axis=1, tiled=True),
        lax.all_gather(down_part, "dp", axis=1, tiled=True),
        lax.all_gather(first_gain.astype(jnp.bfloat16), "dp", axis=0, tiled=True),
        lax.all_gather(first_shift.astype(jnp.bfloat16), "dp", axis=0, tiled=True),
        lax.all_gather(proj_bias.astype(jnp.bfloat16), "dp", axis=0, tiled=True),
        lax.all_gather(second_gain.astype(jnp.bfloat16), "dp", axis=0, tiled=True),
        lax.all_gather(second_shift.astype(jnp.bfloat16), "dp", axis=0, tiled=True),
        lax.all_gather(up_bias.astype(jnp.bfloat16), "dp", axis=0, tiled=True),
        lax.all_gather(down_bias.astype(jnp.bfloat16), "dp", axis=0, tiled=True),
    )


def mat_rows(left, right):
    return jnp.einsum("sqd,de->sqe", left, right, preferred_element_type=jnp.float32)


def mat_back(left, right):
    return jnp.einsum("sqe,de->sqd", left, right, preferred_element_type=jnp.float32)


def mat_grad(left, right):
    return jnp.einsum("sqd,sqe->de", left, right, preferred_element_type=jnp.float32)


def general(
    x_source,
    cotangent,
    lengths,
    dealing,
    qkv_weight,
    proj_weight,
    up_weight,
    down_weight,
    first_gain,
    first_shift,
    proj_bias,
    second_gain,
    second_shift,
    up_bias,
    down_bias,
):
    groups = lax.axis_size("dp")
    seqs_all, piece_rows, features = x_source.shape
    seq_group = seqs_all // groups
    span_rows = groups * piece_rows
    score_scale = HEAD_DIM ** (-0.5)
    block_seqs = math.gcd(seq_group, max(1, 512 // span_rows))
    owners = jnp.argsort(dealing)
    send_order = owners.reshape(groups, seq_group).T.reshape(-1)
    outgoing = x_source[send_order].reshape(seq_group, span_rows, features)
    arrived = lax.all_to_all(outgoing, "dp", split_axis=1, concat_axis=1, tiled=True)
    first_slot = lax.axis_index("dp") * seq_group
    my_lengths = lax.dynamic_slice_in_dim(lengths[owners], first_slot, seq_group)
    query_start = lax.axis_index("cp") * span_rows
    positions = query_start + jnp.arange(span_rows)
    live_rows = positions[None, :] < my_lengths[:, None]
    fetched = fetch_weights(
        qkv_weight,
        proj_weight,
        up_weight,
        down_weight,
        first_gain,
        first_shift,
        proj_bias,
        second_gain,
        second_shift,
        up_bias,
        down_bias,
    )
    qkv_full, proj_full, up_full, down_full = (fetched[0], fetched[1], fetched[2], fetched[3])
    gain_one, shift_one, bias_proj, gain_two, shift_two, bias_up, bias_down = [
        vector.astype(jnp.float32) for vector in fetched[4:]
    ]
    inputs_f = arrived.astype(jnp.float32)
    norm_one, back_one = jax.vjp(layer_norm, inputs_f, gain_one, shift_one)
    act_one = norm_one.astype(jnp.bfloat16)
    mixed_rows = mat_rows(act_one, qkv_full).astype(jnp.bfloat16)
    queries = mixed_rows[..., :features]
    kv_local = mixed_rows[..., features:]
    kv_all = lax.all_gather(kv_local, "cp", axis=1, tiled=True)
    attended, log_total = lax.map(
        lambda inputs: attend(inputs, query_start, score_scale),
        (
            grouped(queries, block_seqs),
            grouped(kv_all[..., :features], block_seqs),
            grouped(kv_all[..., features:], block_seqs),
        ),
    )
    attended = joined(attended)
    log_total = log_total.reshape((seq_group,) + log_total.shape[2:])
    residual = inputs_f + mat_rows(attended, proj_full) + bias_proj
    norm_two, back_two = jax.vjp(layer_norm, residual, gain_two, shift_two)
    act_two = norm_two.astype(jnp.bfloat16)
    up_raw = mat_rows(act_two, up_full) + bias_up
    hidden, back_gelu = jax.vjp(gelu_tanh, up_raw)
    hid_low = hidden.astype(jnp.bfloat16)
    result = residual + mat_rows(hid_low, down_full) + bias_down
    output = jnp.where(live_rows[..., None], result, 0.0).astype(jnp.bfloat16)
    fetched = fetch_weights(
        qkv_weight,
        proj_weight,
        up_weight,
        down_weight,
        first_gain,
        first_shift,
        proj_bias,
        second_gain,
        second_shift,
        up_bias,
        down_bias,
    )
    qkv_full, proj_full, up_full, down_full = (fetched[0], fetched[1], fetched[2], fetched[3])
    gain_one, gain_two = (fetched[4].astype(jnp.float32), fetched[7].astype(jnp.float32))
    grad_out = jnp.where(live_rows[..., None], cotangent.astype(jnp.float32), 0.0)
    grad_low = grad_out.astype(jnp.bfloat16)
    grad_down = mat_grad(hid_low, grad_low)
    grad_bias_down = jnp.sum(grad_out, axis=(0, 1))
    grad_hidden = mat_back(grad_low, down_full)
    grad_up_raw = back_gelu(grad_hidden)[0].astype(jnp.bfloat16)
    grad_up = mat_grad(act_two, grad_up_raw)
    grad_bias_up = jnp.sum(grad_up_raw.astype(jnp.float32), axis=(0, 1))
    grad_act_two = mat_back(grad_up_raw, up_full)
    grad_resid, grad_gain_two, grad_shift_two = back_two(grad_act_two)
    grad_resid = grad_resid + grad_out
    grad_bias_proj = jnp.sum(grad_resid, axis=(0, 1))
    resid_low = grad_resid.astype(jnp.bfloat16)
    grad_proj = mat_grad(attended, resid_low)
    grad_attended = mat_back(resid_low, proj_full).astype(jnp.bfloat16)
    kv_back = lax.all_gather(kv_local, "cp", axis=1, tiled=True)
    key_rows = kv_back[..., :features]
    val_rows = kv_back[..., features:]
    grad_query, grad_keys, grad_vals = lax.map(
        lambda inputs: rows_back(inputs, query_start, score_scale),
        (
            grouped(queries, block_seqs),
            grouped(key_rows, block_seqs),
            grouped(val_rows, block_seqs),
            grouped(grad_attended, block_seqs),
            grouped_stats(log_total, block_seqs),
        ),
    )
    grad_keys, grad_vals = (
        lax.psum_scatter(
            joined(grad_keys).astype(jnp.bfloat16), "cp", scatter_dimension=1, tiled=True
        ).astype(jnp.float32),
        lax.psum_scatter(
            joined(grad_vals).astype(jnp.bfloat16), "cp", scatter_dimension=1, tiled=True
        ).astype(jnp.float32),
    )
    grad_mixed = jnp.concatenate([joined(grad_query), grad_keys, grad_vals], axis=-1).astype(
        jnp.bfloat16
    )
    grad_qkv = mat_grad(act_one, grad_mixed)
    grad_act_one = mat_back(grad_mixed, qkv_full)
    grad_input, grad_gain_one, grad_shift_one = back_one(grad_act_one)
    grad_input = (grad_input + grad_resid).astype(jnp.bfloat16)
    returned = lax.all_to_all(grad_input, "dp", split_axis=1, concat_axis=0, tiled=True)
    input_grad = returned[dealing]
    (
        grad_qkv,
        grad_proj,
        grad_up,
        grad_down,
        grad_gain_one,
        grad_shift_one,
        grad_bias_proj,
        grad_gain_two,
        grad_shift_two,
        grad_bias_up,
        grad_bias_down,
    ) = (
        lax.psum_scatter(
            grad_qkv.astype(jnp.bfloat16), "dp", scatter_dimension=1, tiled=True
        ).astype(jnp.float32),
        lax.psum_scatter(
            grad_proj.astype(jnp.bfloat16), "dp", scatter_dimension=1, tiled=True
        ).astype(jnp.float32),
        lax.psum_scatter(
            grad_up.astype(jnp.bfloat16), "dp", scatter_dimension=1, tiled=True
        ).astype(jnp.float32),
        lax.psum_scatter(
            grad_down.astype(jnp.bfloat16), "dp", scatter_dimension=1, tiled=True
        ).astype(jnp.float32),
        lax.psum_scatter(
            grad_gain_one.astype(jnp.bfloat16), "dp", scatter_dimension=0, tiled=True
        ).astype(jnp.float32),
        lax.psum_scatter(
            grad_shift_one.astype(jnp.bfloat16), "dp", scatter_dimension=0, tiled=True
        ).astype(jnp.float32),
        lax.psum_scatter(
            grad_bias_proj.astype(jnp.bfloat16), "dp", scatter_dimension=0, tiled=True
        ).astype(jnp.float32),
        lax.psum_scatter(
            grad_gain_two.astype(jnp.bfloat16), "dp", scatter_dimension=0, tiled=True
        ).astype(jnp.float32),
        lax.psum_scatter(
            grad_shift_two.astype(jnp.bfloat16), "dp", scatter_dimension=0, tiled=True
        ).astype(jnp.float32),
        lax.psum_scatter(
            grad_bias_up.astype(jnp.bfloat16), "dp", scatter_dimension=0, tiled=True
        ).astype(jnp.float32),
        lax.psum_scatter(
            grad_bias_down.astype(jnp.bfloat16), "dp", scatter_dimension=0, tiled=True
        ).astype(jnp.float32),
    )
    grad_qkv, grad_proj, grad_up, grad_down = (
        lax.psum_scatter(
            grad_qkv.astype(jnp.bfloat16), "cp", scatter_dimension=0, tiled=True
        ).astype(jnp.float32),
        lax.psum_scatter(
            grad_proj.astype(jnp.bfloat16), "cp", scatter_dimension=0, tiled=True
        ).astype(jnp.float32),
        lax.psum_scatter(
            grad_up.astype(jnp.bfloat16), "cp", scatter_dimension=0, tiled=True
        ).astype(jnp.float32),
        lax.psum_scatter(
            grad_down.astype(jnp.bfloat16), "cp", scatter_dimension=0, tiled=True
        ).astype(jnp.float32),
    )
    (
        grad_gain_one,
        grad_shift_one,
        grad_bias_proj,
        grad_gain_two,
        grad_shift_two,
        grad_bias_up,
        grad_bias_down,
    ) = lax.psum(
        (
            grad_gain_one,
            grad_shift_one,
            grad_bias_proj,
            grad_gain_two,
            grad_shift_two,
            grad_bias_up,
            grad_bias_down,
        ),
        "cp",
    )
    return (
        output,
        input_grad,
        grad_qkv,
        grad_proj,
        grad_up,
        grad_down,
        grad_gain_one,
        grad_shift_one,
        grad_bias_proj,
        grad_gain_two,
        grad_shift_two,
        grad_bias_up,
        grad_bias_down,
    )


def solution(mesh):
    in_specs = (
        P(None, ("cp", "dp"), None),
        P("dp", "cp", None),
        P(),
        P(),
        P("cp", "dp"),
        P("cp", "dp"),
        P("cp", "dp"),
        P("cp", "dp"),
        P("dp"),
        P("dp"),
        P("dp"),
        P("dp"),
        P("dp"),
        P("dp"),
        P("dp"),
    )
    out_specs = (
        P("dp", "cp", None),
        P(None, ("cp", "dp"), None),
        P("cp", "dp"),
        P("cp", "dp"),
        P("cp", "dp"),
        P("cp", "dp"),
        P("dp"),
        P("dp"),
        P("dp"),
        P("dp"),
        P("dp"),
        P("dp"),
        P("dp"),
    )
    planned = tuple(mesh.shape.items()) == (("dp", Z * Y * C), ("cp", X))
    local = slice_plan if planned else general
    return jax.shard_map(local, mesh=mesh, in_specs=in_specs, out_specs=out_specs, check_vma=False)
```

```python
import functools
import math

import jax
import jax.numpy as jnp
from jax import lax
from jax.experimental import pallas as pl
from jax.experimental.pallas import tpu as pltpu
from jax.sharding import PartitionSpec as P

HEADS = 12
HEAD_DIM = 64


EPSILON = 1e-05
NEG_BIG = -1e30
TANH_SCALE = 0.7978845608028654
CUBIC_TERM = 0.044715
MESH_IDS = pl.DeviceIdType.MESH
BF = jnp.bfloat16
F32 = jnp.float32

Z, Y, C, X = 4, 2, 2, 2


def mult(value, n):
    return value if isinstance(value, int) else pl.multiple_of(value, n)


def coords():
    d = lax.axis_index("dp")
    x = lax.axis_index("cp")
    return d // (Y * C), (d // C) % Y, d % C, x, d


def dev(z, y, c, x):
    return {"dp": (z * Y + y) * C + c, "cp": x}


def rcopy(src, dst, ssem, rsem, where):
    return pltpu.make_async_remote_copy(
        src_ref=src, dst_ref=dst, send_sem=ssem, recv_sem=rsem, device_id=where, device_id_type=MESH_IDS
    )


def lcopy(src, dst, sem):
    return pltpu.make_async_copy(src, dst, sem)


def wait_bytes(ref, sem):
    pltpu.make_async_copy(ref, ref, sem).wait()


def enter(everyone):
    d = lax.axis_index("dp")
    x = lax.axis_index("cp")
    barrier = pltpu.get_barrier_semaphore()

    def greet(k, carry):
        kd = k // X
        kx = k % X

        @pl.when(jnp.logical_or(kd != d, kx != x))
        def _():
            pl.semaphore_signal(barrier, inc=1, device_id={"dp": kd, "cp": kx}, device_id_type=MESH_IDS)

        return carry

    lax.fori_loop(0, everyone, greet, 0)

    def entered():
        pl.semaphore_wait(barrier, everyone - 1)

    return entered


def dot_nn(a, b):
    return lax.dot_general(a, b, (((1,), (0,)), ((), ())), preferred_element_type=F32)


def dot_nt(a, b):
    return lax.dot_general(a, b, (((1,), (1,)), ((), ())), preferred_element_type=F32)


def dot_tn(a, b):
    return lax.dot_general(a, b, (((0,), (0,)), ((), ())), preferred_element_type=F32)


def norm_parts(v):
    mean = jnp.mean(v, axis=-1, keepdims=True)
    cen = v - mean
    var = jnp.mean(cen * cen, axis=-1, keepdims=True)
    rstd = lax.rsqrt(var + EPSILON)
    return cen * rstd, rstd


def live_length(len_ref, deal_ref, slot):
    total = jnp.int32(0)
    for s in range(len_ref.shape[0]):
        total = total + jnp.where(deal_ref[s] == slot, len_ref[s], 0)
    return total


class Piece:
    def __init__(self, full, R, r0, rn, step, c0, cn):
        self.full = full
        self.R, self.r0, self.rn, self.step, self.c0, self.cn = R, r0, rn, step, c0, cn

    def at(self, z, y, c, x):
        d = (z * Y + y) * C + c
        return self.full.at[
            pl.ds(mult(d * self.R + self.r0, 16), self.rn), pl.ds(mult(x * self.step + self.c0, 128), self.cn)
        ]


class Gather:
    FAR, MATE, A, B, CORE = range(5)

    def __init__(self, piece, sems, k, dummy, where, kind, turned):
        self.p, self.sems, self.k, self.dummy, self.kind = piece, sems, k, dummy, kind
        z, y, c, x, _ = where
        self.z, self.y, self.c, self.x = z, y, c, x
        o = 1 if turned else c
        self.far, self.mate = 3 - z, z + 1 - 2 * (z % 2)
        self.ya, self.xa = (y + 1 - o) % 2, (x + o) % 2
        self.yb, self.xb = (y + o) % 2, (x + 1 - o) % 2
        self.to = {
            self.FAR: dev(self.far, y, c, x), self.MATE: dev(self.mate, y, c, x), self.A: dev(z, self.ya, c, self.xa),
            self.B: dev(z, self.yb, c, self.xb), self.CORE: dev(z, y, 1 - c, x),
        }
        self.counts = {self.FAR: 1, self.MATE: 2, self.A: 4} if kind == 1 else {self.FAR: 2, self.MATE: 4, self.A: 1}
        self.counts.update({self.B: 8, self.CORE: 16})

    def send(self, pieces, *ways):
        for way in ways:
            for z, y, x in pieces:
                q = self.p.at(z, y, self.c, x)
                rcopy(q, q, self.sems.at[self.k, 0, way], self.sems.at[self.k, 1, way], self.to[way]).start()

    def wait(self, way, side=1):
        p = self.p
        wait_bytes(self.dummy.at[pl.ds(0, self.counts[way] * p.rn), pl.ds(0, p.cn)], self.sems.at[self.k, side, way])

    def start(self):
        own = [(self.z, self.y, self.x)]
        if self.kind == 1:
            self.send(own, self.FAR, self.MATE, self.A, self.B, self.CORE)
        else:
            self.send(own, self.A, self.FAR, self.MATE, self.B, self.CORE)

    def tick1(self):
        if self.kind == 1:
            self.wait(self.FAR)
            self.send([(self.far, self.y, self.x)], self.MATE, self.A, self.B, self.CORE)
        else:
            self.wait(self.A)
            self.send([(self.z, self.ya, self.xa)], self.FAR, self.MATE, self.B, self.CORE)

    def tick2(self):
        if self.kind == 1:
            self.wait(self.MATE)
            self.send([(self.mate, self.y, self.x), (3 - self.mate, self.y, self.x)], self.A, self.B, self.CORE)
        else:
            self.wait(self.FAR)
            self.send([(self.far, self.y, self.x), (self.far, self.ya, self.xa)], self.MATE, self.B, self.CORE)

    def tick3(self):
        if self.kind == 1:
            self.wait(self.A)
            self.send([(k, self.ya, self.xa) for k in range(Z)], self.B, self.CORE)
        else:
            self.wait(self.MATE)
            self.send(
                [(k, y, x) for k in (self.mate, 3 - self.mate) for y, x in ((self.y, self.x), (self.ya, self.xa))],
                self.B, self.CORE,
            )

    def tick4(self):
        self.wait(self.B)
        self.send(
            [(k, y, x) for k in range(Z) for y, x in ((self.yb, self.xb), (1 - self.y, 1 - self.x))], self.CORE
        )

    def tick5(self):
        self.wait(self.CORE)

    def drain(self):
        for way in range(5):
            self.wait(way, 0)


class Vectors:
    FAR, MATE, A, CORE = range(4)

    def __init__(self, full, sems, where):
        self.full, self.sems = full, sems
        z, y, c, x, _ = where
        self.z, self.y, self.c = z, y, c
        self.far, self.mate = 3 - z, z + 1 - 2 * (z % 2)
        self.to = (dev(self.far, y, c, x), dev(self.mate, y, c, x), dev(z, 1 - y, c, x), dev(z, y, 1 - c, x))
        self.counts = (1, 2, 4, 8)

    def send(self, pieces, *ways):
        for way in ways:
            for z, y in pieces:
                q = self.full.at[(z * Y + y) * C + self.c]
                rcopy(q, q, self.sems.at[0, way], self.sems.at[1, way], self.to[way]).start()

    def wait(self, way, side=1):
        wait_bytes(self.full.at[pl.ds(0, self.counts[way])], self.sems.at[side, way])

    def start(self):
        self.send([(self.z, self.y)], self.FAR, self.MATE, self.A, self.CORE)

    def tick1(self):
        self.wait(self.FAR)
        self.send([(self.far, self.y)], self.MATE, self.A, self.CORE)

    def tick2(self):
        self.wait(self.MATE)
        self.send([(self.mate, self.y), (3 - self.mate, self.y)], self.A, self.CORE)

    def tick3(self):
        self.wait(self.A)
        self.send([(k, 1 - self.y) for k in range(Z)], self.CORE)

    def tick4(self):
        self.wait(self.CORE)

    def drain(self):
        for way in range(4):
            self.wait(way, 0)


G1, C1, BP, G2, C2, BD, BU = range(7)


def gather_chunks(wq, wp, wu, wd):
    rq, rp, ru, rd = (w.shape[0] // (Z * Y * C) for w in (wq, wp, wu, wd))
    half, wide = wq.shape[1] // X, wd.shape[1] // X
    out = []
    for k in range(3):
        out.append(Piece(wq, rq, k * (rq // 3), rq // 3, half, 0, half))
    out.append(Piece(wp, rp, 0, rp, half, 0, half))
    for k in range(4):
        out.append(Piece(wu, ru, k * (ru // 4), ru // 4, half, 0, half))
    for k in range(4):
        out.append(Piece(wd, rd, 0, rd, wide, k * (wide // 4), wide // 4))
    return out


def one_hot(count, width, first):
    at_row = lax.broadcasted_iota(jnp.int32, (count, width), 0)
    at_col = lax.broadcasted_iota(jnp.int32, (count, width), 1)
    return (at_col == at_row + first).astype(BF)


N_GATHER = 12
TICKS = ("tick1", "tick2", "tick3", "tick4")
KINDS = (1, 1, 1, 1, 2, 2, 1, 2, 2, 1, 2, 2)
TURNED = (7,)
COT_STEPS = (6, 8)
LAGS = ((0, 1, 2, 3),) * 4 + ((0, 1, 2, 4),) * 8


def forward_kernel(
    len_ref, deal_ref, cot, x_in, sq, sp, su, sd, v_g1, v_c1, v_bp, v_g2, v_c2, v_bd, v_bu,
    wq_o, wp_o, wu_o, wd_o, xr_o, gw_o, qs_o, ka_o, va_o, at_o, lse_o, r_o, a2_o, hd_o, gp_o, vec_o, out_o,
    wq, wp, wu, wd, xr, a1, qs, ka, va, at, lse, r, a2, hd, gp, vg, vec, bu3, sc0, sc1, outw, xg, acc,
    gsem, vsem, msem, osem,
):
    where = coords()
    z, y, c, x, d = where
    width = xr.shape[1]
    rows = xr.shape[0]
    qrows = rows // 2
    small = x_in.shape[1]
    pairs = width // 128
    tile = 256

    entered = enter(Z * Y * C * X)

    n = Z * Y * C
    for shard, full in ((sq, wq), (sp, wp), (su, wu), (sd, wd)):
        own, long = shard.shape
        full[pl.ds(mult(d * own, 16), own), pl.ds(mult(x * long, 128), long)] = shard[...].astype(BF)
    vg[d] = jnp.zeros(vg.shape[1:], BF)
    own = v_g1.shape[1]
    seven = jnp.concatenate([v[...] for v in (v_g1, v_c1, v_bp, v_g2, v_c2, v_bd)], axis=0).astype(BF)
    placed = dot_nn(seven, one_hot(own, width, d * own))
    long = v_bu.shape[1]
    per_row = width // long
    placed_long = dot_nn(v_bu[...].astype(BF), one_hot(long, width, (d % per_row) * long))
    rows_long = [jnp.where(d // per_row == k, placed_long, 0.0) for k in range(n // per_row)]
    rest = jnp.zeros((16 - 6 - n // per_row, width), F32)
    vg[d] = jnp.concatenate([placed] + rows_long + [rest], axis=0).astype(BF)
    slots = x_in.shape[0]
    for t in range(slots):
        owner = jnp.int32(0)
        for s in range(slots):
            owner = jnp.where(deal_ref[s] == t, s, owner)
        xg[t] = x_in[owner]

    entered()

    vectors = Vectors(vg, vsem, where)
    vectors.start()
    chunks = [
        Gather(p, gsem, k, wu, where, KINDS[k], k in TURNED) for k, p in enumerate(gather_chunks(wq, wp, wu, wd))
    ]

    def send_cot(b):
        core_b = (x + b) % 2
        src_b = cot.at[pl.ds(b * qrows, qrows)]
        dst_b = gw_o.at[pl.ds(mult(x * qrows, qrows), qrows)]
        same = jnp.logical_and(core_b == c, c == x)

        @pl.when(same)
        def _():
            lcopy(src_b, dst_b, msem.at[3]).start()

        @pl.when(jnp.logical_not(same))
        def _():
            rcopy(src_b, dst_b, msem.at[2], msem.at[3], dev(z, y, core_b, c)).start()

    per_quarter = qrows // small
    place = mult(x * qrows + (d % per_quarter) * small, 16)
    core_to = (x + d // per_quarter) % 2
    dst = xr.at[pl.ds(place, small)]

    def deal_out(k, carry):
        t = (d + k + x * (slots // 2)) % slots
        td = (t // 2) * 2 + core_to
        tx = t % 2
        mine = jnp.logical_and(td == d, tx == x)

        @pl.when(mine)
        def _():
            lcopy(xg.at[t], dst, msem.at[1]).start()

        @pl.when(jnp.logical_not(mine))
        def _():
            rcopy(xg.at[t], dst, msem.at[0], msem.at[1], {"dp": td, "cp": tx}).start()

        return carry

    ahead = 2
    for ch in chunks[:ahead]:
        ch.start()

    def step(s):
        if s + ahead < len(chunks):
            chunks[s + ahead].start()
        if s < 4:
            lax.fori_loop(s * slots // 4, (s + 1) * slots // 4, deal_out, 0)
        if s in COT_STEPS:
            send_cot(COT_STEPS.index(s))
        for n in range(4):
            for k in range(len(chunks)):
                if k + LAGS[k][n] == s:
                    getattr(chunks[k], TICKS[n])()

    step(0)
    vectors.tick1()
    step(1)
    vectors.tick2()
    step(2)
    vectors.tick3()
    step(3)
    vectors.tick4()

    def add_table(k, acc):
        return acc + vg[k].astype(F32)

    vec[...] = lax.fori_loop(1, Z * Y * C, add_table, vg[0].astype(F32))
    for k in range(bu3.shape[0]):
        per = width // tile
        bu3[k] = vec[BU + k // per:BU + k // per + 1, (k % per) * tile:(k % per + 1) * tile]

    wait_bytes(xr, msem.at[1])
    lrows = 128

    def first_norm(k, carry):
        at_rows = pl.ds(mult(k * lrows, lrows), lrows)
        n1, _ = norm_parts(xr[at_rows, :].astype(F32))
        a1[at_rows, :] = (n1 * vec[G1:G1 + 1, :] + vec[C1:C1 + 1, :]).astype(BF)
        return carry

    lax.fori_loop(0, rows // lrows, first_norm, 0)

    step(4)
    step(5)
    for k in range(3):
        chunks[k].tick5()
    keep = [pltpu.make_async_copy(wq, wq_o, osem.at[0])]
    keep[-1].start()

    quarters = (c, 3 - c)

    def q_at(i):
        return pl.ds(mult(quarters[i] * qrows, qrows), qrows)

    steps = width // tile
    for part in range(3):
        def project(n, carry, part=part):
            lanes = pl.ds(mult(n * tile, tile), tile)
            res = dot_nt(a1[...], wq[pl.ds(mult(part * width + n * tile, tile), tile), :]).astype(BF)
            if part == 0:
                qs[:, lanes] = res * jnp.asarray(HEAD_DIM ** -0.5, BF)
            else:
                to = ka if part == 1 else va
                for i in range(2):
                    to[q_at(i), lanes] = res[i * qrows:(i + 1) * qrows]
            return carry

        lax.fori_loop(0, steps, project, 0)
        if part > 0:
            to = ka if part == 1 else va
            for i in range(2):
                rcopy(to.at[q_at(i)], to.at[q_at(i)], msem.at[4 + 2 * (part - 1)], msem.at[5 + 2 * (part - 1)], dev(z, y, 1 - c, x)).start()
    step(6)
    wait_bytes(ka.at[pl.ds(0, rows)], msem.at[5])
    wait_bytes(va.at[pl.ds(0, rows)], msem.at[7])
    for src, out, s in ((qs, qs_o, 1), (ka, ka_o, 2), (va, va_o, 3), (xr, xr_o, 4), (vec, vec_o, 5)):
        keep.append(pltpu.make_async_copy(src, out, osem.at[s]))
        keep[-1].start()

    lane = lax.broadcasted_iota(jnp.int32, (qrows, 128), 1)
    kpos = lax.broadcasted_iota(jnp.int32, (qrows, qrows), 0)
    qpos = lax.broadcasted_iota(jnp.int32, (qrows, qrows), 1)
    groups = qrows // 8

    def pair_body(p, carry):
        lanes = pl.ds(mult(p * 128, 128), 128)
        for i in range(2):
            quarter = quarters[i]
            qp = qs[i * qrows:(i + 1) * qrows, lanes]
            zero = jnp.zeros_like(qp)
            qh = (jnp.where(lane < HEAD_DIM, qp, zero), jnp.where(lane >= HEAD_DIM, qp, zero))

            def scores(j, tops):
                at_keys = pl.ds(mult(j * qrows, qrows), qrows)
                kj = ka[at_keys, lanes]
                keep_it = jnp.logical_or(kpos <= qpos, j < quarter)
                new = []
                for h, sc in enumerate((sc0, sc1)):
                    s = jnp.where(keep_it, dot_nt(kj, qh[h]), NEG_BIG)
                    sc[at_keys, :] = s
                    new.append(jnp.maximum(tops[h], jnp.max(s.reshape(groups, 8, qrows), axis=0)))
                return tuple(new)

            low = jnp.full((8, qrows), NEG_BIG, F32)
            tops = lax.fori_loop(0, quarter + 1, scores, (low, low))
            tops = tuple(jnp.max(t, axis=0, keepdims=True) for t in tops)

            def values(j, state):
                at_keys = pl.ds(mult(j * qrows, qrows), qrows)
                vt = va[at_keys, lanes].T
                new = []
                for h, sc in enumerate((sc0, sc1)):
                    total, acc = state[h]
                    e = jnp.exp(sc[at_keys, :] - tops[h])
                    total = total + jnp.sum(e.reshape(groups, 8, qrows), axis=0)
                    acc = acc + dot_nn(vt[h * HEAD_DIM:(h + 1) * HEAD_DIM], e.astype(BF))
                    new.append((total, acc))
                return tuple(new)

            blank = (jnp.zeros((8, qrows), F32), jnp.zeros((HEAD_DIM, qrows), F32))
            state = lax.fori_loop(0, quarter + 1, values, (blank, blank))
            parts = []
            for h in range(2):
                total = jnp.sum(state[h][0], axis=0, keepdims=True)
                parts.append(state[h][1] / total)
                lse[p, i * 2 + h:i * 2 + h + 1, :] = tops[h] + jnp.log(total)
            at[i * qrows:(i + 1) * qrows, lanes] = jnp.concatenate(parts, axis=0).T.astype(BF)
        return carry

    per = 2
    for k in range(0, pairs, per):
        lax.fori_loop(k, k + per, pair_body, 0)
        step(7 + k // per)

    chunks[3].tick5()
    for src, out, s in ((wp, wp_o, 6), (at, at_o, 7), (lse, lse_o, 8)):
        keep.append(pltpu.make_async_copy(src, out, osem.at[s]))
        keep[-1].start()

    def attend_out(n, carry):
        lanes = pl.ds(mult(n * tile, tile), tile)
        res = dot_nt(at[...], wp[pl.ds(mult(n * tile, tile), tile), :])
        r[:, lanes] = xr[:, lanes].astype(F32) + res + vec[BP:BP + 1, lanes]
        return carry

    lax.fori_loop(0, steps, attend_out, 0)

    def second_norm(k, carry):
        at_rows = pl.ds(mult(k * lrows, lrows), lrows)
        n2, _ = norm_parts(r[at_rows, :])
        a2[at_rows, :] = (n2 * vec[G2:G2 + 1, :] + vec[C2:C2 + 1, :]).astype(BF)
        return carry

    lax.fori_loop(0, rows // lrows, second_norm, 0)
    step(10)
    step(11)
    for k in range(4, 8):
        chunks[k].tick5()
    for src, out, s in ((wu, wu_o, 9), (r, r_o, 10), (a2, a2_o, 11)):
        keep.append(pltpu.make_async_copy(src, out, osem.at[s]))
        keep[-1].start()

    def up(n, carry):
        lanes = pl.ds(mult(n * tile, tile), tile)
        u = dot_nt(a2[...], wu[lanes, :]) + bu3[n]
        sq_u = u * u
        t = jnp.tanh(TANH_SCALE * (u + CUBIC_TERM * sq_u * u))
        half_up = 0.5 * (1.0 + t)
        hd[:, lanes] = (u * half_up).astype(BF)
        slope = TANH_SCALE * (1.0 + 3.0 * CUBIC_TERM * sq_u)
        gp[:, lanes] = (half_up + 0.5 * u * (1.0 - t * t) * slope).astype(BF)
        return carry

    blocks = hd.shape[1] // tile
    for k in range(0, blocks, 4):
        lax.fori_loop(k, k + 4, up, 0)
        step(12 + k // 4)
    for src, out, s in ((hd, hd_o, 12), (gp, gp_o, 13)):
        keep.append(pltpu.make_async_copy(src, out, osem.at[s]))
        keep[-1].start()
    my_len = live_length(len_ref, deal_ref, (z * Y + y) * C + x)
    rowpos = lax.broadcasted_iota(jnp.int32, (qrows, 1), 0)
    parts = len(chunks) - 8
    wide = wd.shape[1] // X
    for k in range(parts):
        if k == 1:
            step(15)
        chunks[8 + k].tick5()
        cuts = [slice(h * wide + k * (wide // parts), h * wide + (k + 1) * (wide // parts)) for h in range(X)]
        for h, cut in enumerate(cuts):
            keep.append(pltpu.make_async_copy(wd.at[:, cut], wd_o.at[:, cut], osem.at[16 + X * k + h]))
            keep[-1].start()

        def down(n, carry, k=k, cuts=cuts):
            lanes = pl.ds(mult(n * tile, tile), tile)
            res = dot_nt(hd[:, cuts[0]], wd[lanes, cuts[0]])
            for cut in cuts[1:]:
                res = res + dot_nt(hd[:, cut], wd[lanes, cut])
            res = res + (r[:, lanes] + vec[BD:BD + 1, lanes] if k == 0 else acc[:, lanes])
            if k < parts - 1:
                acc[:, lanes] = res
            else:
                for i in range(2):
                    live = quarters[i] * qrows + rowpos < my_len
                    outw[i * qrows:(i + 1) * qrows, lanes] = jnp.where(live, res[i * qrows:(i + 1) * qrows], 0.0).astype(BF)
            return carry

        lax.fori_loop(0, steps, down, 0)
    keep.append(pltpu.make_async_copy(outw, out_o, osem.at[15]))
    keep[-1].start()

    for ch in chunks:
        ch.drain()
    vectors.drain()

    @pl.when(core_to == c)
    def _():
        wait_bytes(xr.at[pl.ds(0, rows - small)], msem.at[0])

    @pl.when(core_to != c)
    def _():
        wait_bytes(xr, msem.at[0])

    @pl.when(c == x)
    def _():
        wait_bytes(xr.at[pl.ds(0, qrows)], msem.at[2])

    @pl.when(c != x)
    def _():
        wait_bytes(xr, msem.at[2])

    wait_bytes(xr, msem.at[3])
    wait_bytes(ka.at[pl.ds(0, rows)], msem.at[4])
    wait_bytes(va.at[pl.ds(0, rows)], msem.at[6])
    for cp in keep:
        cp.wait()


def forward(lengths, dealing, cot, x_source, shards, vectors):
    slots, small, width = x_source.shape
    rows = cot.shape[0]
    ff = shards[2].shape[0] * Z * Y * C
    keys = rows * 2
    pairs = width // 128

    def arr(shape, dtype=BF):
        return jax.ShapeDtypeStruct(shape, dtype)

    outs = [
        arr((3 * width, width)), arr((width, width)), arr((ff, width)), arr((width, ff)),
        arr((rows, width)), arr((rows, width)), arr((rows, width)), arr((keys, width)), arr((keys, width)),
        arr((rows, width)), arr((pairs, 8, rows // 2), F32), arr((rows, width), F32), arr((rows, width)),
        arr((rows, ff)), arr((rows, ff)), arr((16, width), F32), arr((rows, width)),
    ]
    vm = pltpu.VMEM
    scratch = [
        vm((3 * width, width), BF), vm((width, width), BF), vm((ff, width), BF), vm((width, ff), BF),
        vm((rows, width), BF), vm((rows, width), BF), vm((rows, width), BF), vm((keys, width), BF),
        vm((keys, width), BF), vm((rows, width), BF), vm((pairs, 8, rows // 2), F32), vm((rows, width), F32),
        vm((rows, width), BF), vm((rows, ff), BF), vm((rows, ff), BF), vm((Z * Y * C, 16, width), BF),
        vm((16, width), F32), vm((ff // 256, 1, 256), F32), vm((keys, rows // 2), F32), vm((keys, rows // 2), F32),
        vm((rows, width), BF), vm(x_source.shape, BF), vm((rows, width), F32),
        pltpu.SemaphoreType.DMA((N_GATHER, 2, 5)), pltpu.SemaphoreType.DMA((2, 4)), pltpu.SemaphoreType.DMA((8,)),
        pltpu.SemaphoreType.DMA((24,)),
    ]
    anyspec = pl.BlockSpec(memory_space=pl.ANY)
    smem = pl.BlockSpec(memory_space=pltpu.SMEM)
    vmem = pl.BlockSpec(memory_space=pltpu.VMEM)
    return pl.pallas_call(
        forward_kernel,
        out_shape=outs,
        in_specs=[smem, smem, anyspec] + [vmem] * 12,
        out_specs=[anyspec] * len(outs),
        scratch_shapes=scratch,
        compiler_params=pltpu.CompilerParams(
            collective_id=0, has_side_effects=True, vmem_limit_bytes=60 * 1024 * 1024
        ),
        name="forward",
    )(lengths, dealing, cot, x_source, *shards, *vectors)


def when(cond):
    if isinstance(cond, bool):
        return (lambda f: f()) if cond else (lambda f: None)
    return pl.when(cond)


class Reduce:
    S1, R1, S2, R2, S3, R3, S4, R4, S5, R5 = range(10)

    def __init__(self, grad, R, step, c0, C, zlist, bufs, out, out_c0, sems, k, where, turned):
        self.grad, self.R, self.step, self.c0, self.cn, self.zlist = grad, R, step, c0, C, zlist
        self.r1, self.r2, self.r3, self.r4, self.r5 = bufs
        self.out, self.out_c0, self.sems, self.k = out, out_c0, sems, k
        self.z, self.y, self.c, self.x, _ = where
        y, x = self.y, self.x
        self.o = o = 1 if turned else self.c
        self.y2, self.x2 = (y + o) % 2, (x + 1 - o) % 2
        self.y3, self.x3 = (y + 1 - o) % 2, (x + o) % 2
        self.every = len(zlist) == Z

    def sem(self, which):
        return self.sems.at[self.k, which]

    def rows(self, z, y, c):
        return pl.ds(mult(((z * Y + y) * C + c) * self.R, 16), self.R)

    def cols(self, x):
        return pl.ds(mult(x * self.step + self.c0, 128), self.cn)

    def at(self, z, y, c, x):
        return self.grad.at[self.rows(z, y, c), self.cols(x)]

    def add(self, rows, cols, got):
        self.grad[rows, cols] = (self.grad[rows, cols].astype(F32) + got.astype(F32)).astype(BF)

    def zidx(self, zi):
        return zi if self.every else self.zlist[0]

    def start(self):
        z, y, c, x = self.z, self.y, self.c, self.x
        to = dev(z, y, 1 - c, x)
        for zi, zz in enumerate(self.zlist):
            for yy in range(Y):
                for xx in range(X):
                    rcopy(
                        self.at(zz, yy, 1 - c, xx), self.r1.at[zi * Y + yy, xx],
                        self.sem(self.S1), self.sem(self.R1), to,
                    ).start()

    def tick2(self):
        z, y, c, x, o = self.z, self.y, self.c, self.x, self.o
        wait_bytes(self.r1, self.sem(self.R1))

        def body(e, carry):
            rows = self.rows(self.zidx(e // Y), e % Y, c)
            for xx in range(X):
                self.add(rows, self.cols(xx), self.r1[e, xx])
            return carry

        lax.fori_loop(0, len(self.zlist) * Y, body, 0)
        to = dev(z, self.y2, c, self.x2)
        for zi, zz in enumerate(self.zlist):
            for w in range(2):
                yy = w * (1 - o) + (1 - y) * o
                xx = (1 - x) * (1 - o) + w * o
                rcopy(self.at(zz, yy, c, xx), self.r2.at[zi * 2 + w], self.sem(self.S2), self.sem(self.R2), to).start()

    def tick3(self):
        z, y, c, x, o = self.z, self.y, self.c, self.x, self.o
        wait_bytes(self.r2, self.sem(self.R2))

        def body(e, carry):
            w = e % 2
            yy = w * (1 - o) + y * o
            xx = x * (1 - o) + w * o
            self.add(self.rows(self.zidx(e // 2), yy, c), self.cols(xx), self.r2[e])
            return carry

        lax.fori_loop(0, len(self.zlist) * 2, body, 0)
        to = dev(z, self.y3, c, self.x3)
        for zi, zz in enumerate(self.zlist):
            rcopy(self.at(zz, self.y3, c, self.x3), self.r3.at[zi], self.sem(self.S3), self.sem(self.R3), to).start()

    def first_hop(self, k):
        return [(k ^ 1, k, 0), ((3 - k) ^ 1, 3 - k, 1)]

    def tick4(self):
        z, y, c, x = self.z, self.y, self.c, self.x
        wait_bytes(self.r3, self.sem(self.R3))

        def body(zi, carry):
            self.add(self.rows(self.zidx(zi), y, c), self.cols(x), self.r3[zi])
            return carry

        lax.fori_loop(0, len(self.zlist), body, 0)
        if self.every:
            mate = z + 1 - 2 * (z % 2)
            for slot, zz in enumerate((mate, 3 - mate)):
                rcopy(
                    self.at(zz, y, c, x), self.r4.at[slot], self.sem(self.S4), self.sem(self.R4), dev(mate, y, c, x)
                ).start()
        else:
            k = self.zlist[0]
            for sender, taker, slot in self.first_hop(k):
                @pl.when(z == sender)
                def _(taker=taker, slot=slot):
                    rcopy(
                        self.at(k, y, c, x), self.r4.at[slot], self.sem(self.S4), self.sem(self.R4),
                        dev(taker, y, c, x),
                    ).start()

    def tick5(self):
        z, y, c, x = self.z, self.y, self.c, self.x
        k = self.zlist[0]

        def take(zz, slot):
            self.add(self.rows(zz, y, c), self.cols(x), self.r4[slot])

        def pass_on(zz):
            rcopy(self.at(zz, y, c, x), self.r5, self.sem(self.S5), self.sem(self.R5), dev(zz, y, c, x)).start()

        if self.every:
            wait_bytes(self.r4, self.sem(self.R4))
            take(3 - z, 1)
            pass_on(3 - z)
            take(z, 0)
        else:
            @pl.when(z == 3 - k)
            def _():
                wait_bytes(self.r4.at[1], self.sem(self.R4))
                take(k, 1)
                pass_on(k)

            @pl.when(z == k)
            def _():
                wait_bytes(self.r4.at[0], self.sem(self.R4))
                take(k, 0)

    def tick6(self):
        z, y, c, x = self.z, self.y, self.c, self.x

        @when(True if self.every else z == self.zlist[0])
        def _():
            wait_bytes(self.r5, self.sem(self.R5))
            own = self.grad[self.rows(z, y, c), self.cols(x)].astype(F32)
            self.out[:, self.out_c0:self.out_c0 + self.cn] = own + self.r5[...].astype(F32)

    def drain(self):
        z = self.z
        wait_bytes(self.r1, self.sem(self.S1))
        wait_bytes(self.r2, self.sem(self.S2))
        wait_bytes(self.r3, self.sem(self.S3))
        if self.every:
            wait_bytes(self.r4, self.sem(self.S4))
            wait_bytes(self.r5, self.sem(self.S5))
        else:
            k = self.zlist[0]
            for sender, _, slot in self.first_hop(k):
                @pl.when(z == sender)
                def _():
                    wait_bytes(self.r4.at[0], self.sem(self.S4))

            @pl.when(z == 3 - k)
            def _():
                wait_bytes(self.r5, self.sem(self.S5))


TURNED_BACK = (3, 6)


def reduce_shapes(width, ff):
    n = Z * Y * C
    every = list(range(Z))
    half = width // X
    wide = ff // X
    shapes = [("d", width // n, wide, k * (wide // 2), wide // 2, every, k * (wide // 2)) for k in range(2)]
    shapes += [("u", ff // n, half, 0, half, [k], 0) for k in range(Z)]
    shapes += [("p", width // n, half, 0, half, every, 0)]
    shapes += [("q", 3 * width // n, half, 0, half, [k], 0) for k in range(Z)]
    return shapes


def backward_kernel(*refs):
    names = (
        "len_ref", "deal_ref", "wq_i", "wp_i", "wu_i", "wd_i", "xr_i", "gw_i", "qs_i", "ka_i", "va_i", "at_i",
        "lse_i", "r_i", "a2_i", "hd_i", "gp_i", "vec_i", "out_i", "og_q", "og_p", "og_u", "og_d", "osum", "ret",
        "out_n", "wq", "wp", "xr", "g", "qs", "ka", "va", "at", "lse", "r", "a2", "vec", "gt", "d2", "dr", "drl",
        "do", "gq", "gp_", "gu", "gd", "wd_t", "wu_t", "hd_t", "gp_t", "dka", "dva", "own_v", "sv", "rk", "rv", "dm",
        "vs", "vr", "bub", "ret_v", "lsem", "tsem", "rsem", "msem", "vsem",
    )
    env = dict(zip(names, refs[: len(names)]))
    env.update(a1=env["a2"], own_k=env["d2"], sk=env["drl"], dx=env["do"])
    bufs = refs[len(names):]
    e = type("Refs", (), env)
    where = coords()
    z, y, c, x, d = where
    rows, width = e.g.shape
    ff = e.hd_i.shape[1]
    qrows = rows // 2
    pairs = width // 128
    tile = 256
    lrows = 128
    steps = width // tile
    quarters = (c, 3 - c)
    theirs = (1 - c, 2 + c)

    def at_quarter(k):
        return pl.ds(mult(k * qrows, qrows), qrows)

    entered = enter(Z * Y * C * X)

    loads = {}
    for k, (src, dst) in enumerate(
        (
            ("gw_i", "g"), ("a2_i", "a2"), ("r_i", "r"), ("vec_i", "vec"), ("wp_i", "wp"), ("at_i", "at"),
            ("qs_i", "qs"), ("ka_i", "ka"), ("va_i", "va"), ("lse_i", "lse"), ("xr_i", "xr"), ("wq_i", "wq"),
        )
    ):
        loads[dst] = pltpu.make_async_copy(env[src], env[dst], e.lsem.at[k])

    def tile_of(idx):
        block = idx // 3
        return (block % 2) * 2 * 3 + (block // 2) * 3 + idx % 3

    def tile_copies(idx):
        n = tile_of(idx)
        slot = idx % 2
        cut = pl.ds(mult(n * tile, tile), tile)
        return (
            pltpu.make_async_copy(e.wd_i.at[:, cut], e.wd_t.at[slot], e.tsem.at[0, slot]),
            pltpu.make_async_copy(e.gp_i.at[:, cut], e.gp_t.at[slot], e.tsem.at[1, slot]),
            pltpu.make_async_copy(e.hd_i.at[:, cut], e.hd_t.at[slot], e.tsem.at[2, slot]),
            pltpu.make_async_copy(e.wu_i.at[cut, :], e.wu_t.at[slot], e.tsem.at[3, slot]),
        )

    loads["g"].start()
    for cp in tile_copies(0):
        cp.start()
    loads["a2"].start()
    for name in ("r", "vec", "wp", "at", "qs", "ka", "va", "lse", "xr", "wq"):
        loads[name].start()

    entered()

    for i in range(2):
        same = jnp.logical_and(x == c, x == i)
        src = e.out_i.at[pl.ds(i * qrows, qrows)]
        dst = e.out_n.at[pl.ds(mult(((i + c) % 2) * qrows, qrows), qrows)]

        @pl.when(same)
        def _(src=src, dst=dst):
            lcopy(src, dst, e.msem.at[1]).start()

        @pl.when(jnp.logical_not(same))
        def _(src=src, dst=dst, i=i):
            rcopy(src, dst, e.msem.at[0], e.msem.at[1], dev(z, y, x, i)).start()

    grads = {"q": (e.gq, e.og_q), "p": (e.gp_, e.og_p), "u": (e.gu, e.og_u), "d": (e.gd, e.og_d)}
    chunks = []
    for k, (name, R, step, c0, cn, zlist, oc) in enumerate(reduce_shapes(width, ff)):
        grad, out = grads[name]
        chunks.append(Reduce(grad, R, step, c0, cn, zlist, bufs[5 * k:5 * k + 5], out, oc, e.rsem, k, where, k in TURNED_BACK))
    dA, dB, u0, u1, u2, u3, pj, q0, q1, q2, q3 = chunks

    my_len = live_length(e.len_ref, e.deal_ref, (z * Y + y) * C + x)
    rowpos = lax.broadcasted_iota(jnp.int32, (lrows, 1), 0)
    loads["g"].wait()
    blank = jnp.zeros((1, width), F32)
    total_bd = blank
    for k in range(rows // lrows):
        base = quarters[k * lrows // qrows] * qrows + (k * lrows) % qrows
        live = base + rowpos < my_len
        part = jnp.where(live, e.g[k * lrows:(k + 1) * lrows, :], jnp.zeros((), BF))
        e.g[k * lrows:(k + 1) * lrows, :] = part
        e.gt[:, k * lrows:(k + 1) * lrows] = part.T
        total_bd = total_bd + jnp.sum(part.astype(F32), axis=0, keepdims=True)
    e.d2[...] = jnp.zeros_like(e.d2)
    loads["a2"].wait()

    ff_tiles = ff // tile
    plan = {
        2: [u0.start], 4: [u0.tick2], 5: [u2.start, dA.start], 7: [u2.tick2], 8: [u1.start, u0.tick3],
        9: [dA.tick2], 10: [u1.tick2, u2.tick3], 11: [u3.start, dB.start, u0.tick4],
    }

    def ffn(idx, carry):
        slot = idx % 2
        n = tile_of(idx)
        cut = pl.ds(mult(n * tile, tile), tile)

        @pl.when(idx + 1 < ff_tiles)
        def _():
            for cp in tile_copies(idx + 1):
                cp.start()

        for cp in tile_copies(idx):
            cp.wait()
        du = (e.gp_t[slot].astype(F32) * dot_nn(e.g[...], e.wd_t[slot])).astype(BF)
        e.bub[n] = jnp.sum(du.astype(F32), axis=0, keepdims=True)
        e.gd[:, cut] = dot_nn(e.gt[...], e.hd_t[slot]).astype(BF)
        e.gu[cut, :] = dot_tn(du, e.a2[...]).astype(BF)
        e.d2[...] += dot_nn(du, e.wu_t[slot])
        for at_idx, acts in plan.items():
            @pl.when(idx == at_idx)
            def _(acts=acts):
                for act in acts:
                    act()
        return carry

    lax.fori_loop(0, ff_tiles, ffn, 0)

    loads["r"].wait()
    loads["vec"].wait()

    def norm_two(k, sums):
        at_rows = pl.ds(mult(k * lrows, lrows), lrows)
        n2, rstd = norm_parts(e.r[at_rows, :])
        da = e.d2[at_rows, :]
        ee = da * e.vec[G2:G2 + 1, :]
        gg = e.g[at_rows, :].astype(F32)
        m1 = jnp.mean(ee, axis=-1, keepdims=True)
        m2 = jnp.mean(ee * n2, axis=-1, keepdims=True)
        dr = gg + (ee - m1 - n2 * m2) * rstd
        e.dr[at_rows, :] = dr
        e.drl[at_rows, :] = dr.astype(BF)
        return (
            sums[0] + jnp.sum(da * n2, axis=0, keepdims=True),
            sums[1] + jnp.sum(da, axis=0, keepdims=True),
            sums[2] + jnp.sum(dr, axis=0, keepdims=True),
        )

    sum_g2, sum_c2, sum_bp = lax.fori_loop(0, rows // lrows, norm_two, (blank, blank, blank))

    loads["wp"].wait()
    loads["at"].wait()

    def proj_back(n, carry):
        cut = pl.ds(mult(n * tile, tile), tile)
        e.do[:, cut] = dot_nn(e.drl[...], e.wp[:, cut]).astype(BF)
        e.gp_[cut, :] = dot_tn(e.drl[:, cut], e.at[...]).astype(BF)
        return carry

    lax.fori_loop(0, steps, proj_back, 0)
    pj.start()
    u3.tick2()
    u0.tick5()

    for name in ("qs", "ka", "va", "lse"):
        loads[name].wait()
    lane = lax.broadcasted_iota(jnp.int32, (qrows, 128), 1)
    kpos = lax.broadcasted_iota(jnp.int32, (qrows, qrows), 0)
    qpos = lax.broadcasted_iota(jnp.int32, (qrows, qrows), 1)

    def split(v):
        zero = jnp.zeros_like(v)
        return jnp.where(lane < HEAD_DIM, v, zero), jnp.where(lane >= HEAD_DIM, v, zero)

    between = {
        (0, 0): [dB.tick2, pj.tick2, dA.tick3], (1, 1): [u1.tick3], (2, 0): [u2.tick4], (2, 1): [u3.tick3],
        (3, 0): [u2.tick5], (4, 0): [dB.tick3, u1.tick4], (5, 0): [u1.tick5], (5, 1): [pj.tick3],
    }

    def pair_body(p, carry):
        lanes = pl.ds(mult(p * 128, 128), 128)
        e.dka[...] = jnp.zeros_like(e.dka)
        e.dva[...] = jnp.zeros_like(e.dva)
        for i in range(2):
            quarter = quarters[i]
            own = slice(i * qrows, (i + 1) * qrows)
            qp, dop = e.qs[own, lanes], e.do[own, lanes]
            qh, doh = split(qp), split(dop)
            qq, dd = jnp.concatenate(qh, axis=0), jnp.concatenate(doh, axis=0)
            prod = (dop.astype(F32) * e.at[own, lanes].astype(F32)).T
            delta = [jnp.sum(prod[h * HEAD_DIM:(h + 1) * HEAD_DIM], axis=0, keepdims=True) for h in range(2)]
            logs = [e.lse[p, i * 2 + h:i * 2 + h + 1, :] for h in range(2)]

            def keys(j, dq):
                at_keys = pl.ds(mult(j * qrows, qrows), qrows)
                kj, vj = e.ka[at_keys, lanes], e.va[at_keys, lanes]
                kt = kj.T
                keep_it = jnp.logical_or(kpos <= qpos, j < quarter)
                probs, grads_s, new = [], [], []
                for h in range(2):
                    s = jnp.where(keep_it, dot_nt(kj, qh[h]), NEG_BIG)
                    pt = jnp.exp(s - logs[h])
                    ds = (pt * (dot_nt(vj, doh[h]) - delta[h])).astype(BF)
                    probs.append(pt.astype(BF))
                    grads_s.append(ds)
                    new.append(dq[h] + dot_nn(kt[h * HEAD_DIM:(h + 1) * HEAD_DIM], ds))
                e.dva[at_keys, :] += dot_nn(jnp.concatenate(probs, axis=1), dd)
                e.dka[at_keys, :] += dot_nn(jnp.concatenate(grads_s, axis=1), qq)
                return tuple(new)

            none = jnp.zeros((HEAD_DIM, qrows), F32)
            dq = lax.fori_loop(0, quarter + 1, keys, (none, none))
            e.dm[own, lanes] = (jnp.concatenate(dq, axis=0).T * HEAD_DIM ** -0.5).astype(BF)
            for (at_p, at_i), acts in between.items():
                if at_i == i:
                    @pl.when(p == at_p)
                    def _(acts=acts):
                        for act in acts:
                            act()
        for i in range(2):
            own = slice(i * qrows, (i + 1) * qrows)
            e.own_k[own, lanes] = e.dka[at_quarter(quarters[i]), :]
            e.own_v[own, lanes] = e.dva[at_quarter(quarters[i]), :]
            e.sk[own, lanes] = e.dka[at_quarter(theirs[i]), :].astype(BF)
            e.sv[own, lanes] = e.dva[at_quarter(theirs[i]), :].astype(BF)
        for k in range(pairs // 2):
            @pl.when(p == 2 * k + 1)
            def _(k=k):
                cut = slice(2 * k * 128, (2 * k + 2) * 128)
                for src, dst, s in ((e.sk, e.rk, 2), (e.sv, e.rv, 4)):
                    rcopy(
                        src.at[:, cut], dst.at[:, cut], e.msem.at[s], e.msem.at[s + 1], dev(z, y, 1 - c, x)
                    ).start()
        return carry

    lax.fori_loop(0, pairs, pair_body, 0)

    loads["xr"].wait()

    def norm_one(k, carry):
        at_rows = pl.ds(mult(k * lrows, lrows), lrows)
        n1, _ = norm_parts(e.xr[at_rows, :].astype(F32))
        e.a1[at_rows, :] = (n1 * e.vec[G1:G1 + 1, :] + e.vec[C1:C1 + 1, :]).astype(BF)
        return carry

    lax.fori_loop(0, rows // lrows, norm_one, 0)

    def qkv_grad(n, carry):
        cut = pl.ds(mult(n * tile, tile), tile)
        e.gq[cut, :] = dot_tn(e.dm[:, cut], e.a1[...]).astype(BF)
        return carry

    lax.fori_loop(0, 3, qkv_grad, 0)
    q0.start()
    dA.tick4()
    wait_bytes(e.rk, e.msem.at[3])
    wait_bytes(e.rv, e.msem.at[5])
    for part, (mine, got) in enumerate(((e.own_k, e.rk), (e.own_v, e.rv))):
        def merge(k, carry, part=part, mine=mine, got=got):
            at_rows = pl.ds(mult(k * lrows, lrows), lrows)
            e.dm[at_rows, (part + 1) * width:(part + 2) * width] = (
                mine[at_rows, :] + got[at_rows, :].astype(F32)
            ).astype(BF)
            return carry

        lax.fori_loop(0, rows // lrows, merge, 0)
    u3.tick4()
    loads["wq"].wait()

    def input_back(n, carry):
        cut = pl.ds(mult(n * tile, tile), tile)
        e.d2[:, cut] = dot_nn(e.dm[...], e.wq[:, cut])
        return carry

    lax.fori_loop(0, steps, input_back, 0)
    q0.tick2()
    pj.tick4()

    def norm_one_back(k, sums):
        at_rows = pl.ds(mult(k * lrows, lrows), lrows)
        n1, rstd = norm_parts(e.xr[at_rows, :].astype(F32))
        da = e.d2[at_rows, :]
        ee = da * e.vec[G1:G1 + 1, :]
        m1 = jnp.mean(ee, axis=-1, keepdims=True)
        m2 = jnp.mean(ee * n1, axis=-1, keepdims=True)
        e.dx[at_rows, :] = (e.dr[at_rows, :] + (ee - m1 - n1 * m2) * rstd).astype(BF)
        return sums[0] + jnp.sum(da * n1, axis=0, keepdims=True), sums[1] + jnp.sum(da, axis=0, keepdims=True)

    sum_g1, sum_c1 = lax.fori_loop(0, rows // lrows, norm_one_back, (blank, blank))
    dB.tick4()
    dA.tick5()

    e.vs[0] = jnp.zeros_like(e.vs[0])
    for row, value in ((G1, sum_g1), (C1, sum_c1), (BP, sum_bp), (G2, sum_g2), (C2, sum_c2), (BD, total_bd)):
        e.vs[0, row:row + 1, :] = value
    per = width // tile
    for k in range(ff_tiles):
        e.vs[0, BU + k // per:BU + k // per + 1, (k % per) * tile:(k % per + 1) * tile] = e.bub[k]
    hops = (
        dev(z, y, 1 - c, x), dev(z, y, c, 1 - x), dev(z, 1 - y, c, x),
        dev(z + 1 - 2 * (z % 2), y, c, x), dev((z + 2) % 4, y, c, x),
    )

    def hop(k):
        rcopy(e.vs.at[k], e.vr.at[k], e.vsem.at[0, k], e.vsem.at[1, k], hops[k]).start()

    def land(k):
        wait_bytes(e.vr.at[k], e.vsem.at[1, k])
        e.vs[k + 1] = e.vs[k] + e.vr[k]

    hop(0)

    small = e.ret.shape[1]
    per_quarter = qrows // small
    slot = (z * Y + y) * C + x

    def give_back(k, carry):
        i = (k + x) % 2
        e8 = (k // 2 + d) % per_quarter
        td = ((i + c) % 2) * per_quarter + e8
        src = e.dx.at[pl.ds(mult(i * qrows + e8 * small, small), small)]
        mine = jnp.logical_and(td == d, x == i)

        @pl.when(mine)
        def _():
            lcopy(src, e.ret_v.at[slot], e.msem.at[7]).start()

        @pl.when(jnp.logical_not(mine))
        def _():
            rcopy(src, e.ret_v.at[slot], e.msem.at[6], e.msem.at[7], {"dp": td, "cp": i}).start()

        return carry

    share = per_quarter // 2
    lax.fori_loop(0, share, give_back, 0)
    lax.fori_loop(3, 5, qkv_grad, 0)
    q1.start()
    lax.fori_loop(share, 2 * share, give_back, 0)
    lax.fori_loop(5, 7, qkv_grad, 0)
    q2.start()
    lax.fori_loop(2 * share, 3 * share, give_back, 0)
    u3.tick5()
    lax.fori_loop(7, 9, qkv_grad, 0)
    q3.start()
    lax.fori_loop(3 * share, 4 * share, give_back, 0)
    q0.tick3()
    q1.tick2()
    pj.tick5()
    land(0)
    hop(1)
    for ch in (u0, u2, u1):
        ch.tick6()
    q2.tick2()
    q3.tick2()
    land(1)
    hop(2)
    dB.tick5()
    dA.tick6()
    q0.tick4()
    q1.tick3()
    land(2)
    hop(3)
    q2.tick3()
    q3.tick3()
    q1.tick4()
    land(3)
    hop(4)
    q2.tick4()
    q3.tick4()
    u3.tick6()
    q0.tick5()
    pj.tick6()
    q1.tick5()
    land(4)
    own = width // (Z * Y * C)
    e.osum[0:6, :] = pltpu.roll(e.vs[5, 0:6, :], (width - d * own) % width, 1)[:, :tile]
    long = ff // (Z * Y * C)
    per_row = width // long
    e.osum[6:7, :] = pltpu.roll(
        e.vs[5, pl.ds(BU + d // per_row, 1), :], (width - (d % per_row) * long) % width, 1
    )[:, :tile]
    e.osum[7:8, :] = jnp.zeros((1, tile), F32)
    q2.tick5()
    q3.tick5()
    dB.tick6()
    wait_bytes(e.dx, e.msem.at[7])
    for s in range(e.ret.shape[0]):
        e.ret[s] = e.ret_v[jnp.clip(e.deal_ref[s], 0, e.ret.shape[0] - 1)]
    for ch in (q0, q1, q2, q3):
        ch.tick6()

    for ch in chunks:
        ch.drain()
    for k in range(5):
        wait_bytes(e.vr.at[k], e.vsem.at[0, k])
    wait_bytes(e.rk, e.msem.at[2])
    wait_bytes(e.rv, e.msem.at[4])

    @pl.when((x + c) % 2 == d // per_quarter)
    def _():
        wait_bytes(e.dx.at[pl.ds(0, rows - small)], e.msem.at[6])

    @pl.when((x + c) % 2 != d // per_quarter)
    def _():
        wait_bytes(e.dx, e.msem.at[6])

    @pl.when(c == x)
    def _():
        wait_bytes(e.dx.at[pl.ds(0, qrows)], e.msem.at[0])

    @pl.when(c != x)
    def _():
        wait_bytes(e.dx, e.msem.at[0])

    wait_bytes(e.dx, e.msem.at[1])


def backward(lengths, dealing, saved, shards):
    wq, wp, wu, wd, xr, gw, qs, ka, va, at, lse, r, a2, hd, gp, vec, outw = saved
    rows, width = xr.shape
    ff = hd.shape[1]
    n = Z * Y * C
    keys = ka.shape[0]
    small = rows // n
    pairs = width // 128

    def arr(shape, dtype=BF):
        return jax.ShapeDtypeStruct(shape, dtype)

    outs = [arr(s.shape, F32) for s in shards] + [
        arr((8, 256), F32), arr((n, small, width)), arr((rows, width)),
    ]
    vm = pltpu.VMEM
    acts = vm((rows, width), BF)
    acts32 = vm((rows, width), F32)
    scratch = [
        vm(wq.shape, BF), vm(wp.shape, BF), acts, acts, acts, vm(ka.shape, BF), vm(va.shape, BF), acts,
        vm(lse.shape, F32), acts32, acts, vm(vec.shape, F32), vm((width, rows), BF), acts32, acts32, acts, acts,
        vm(wq.shape, BF), vm(wp.shape, BF), vm(wu.shape, BF), vm(wd.shape, BF),
        vm((2, width, 256), BF), vm((2, 256, width), BF), vm((2, rows, 256), BF), vm((2, rows, 256), BF),
        vm((keys, 128), F32), vm((keys, 128), F32),
        acts32, acts, acts, acts, vm((rows, 3 * width), BF),
        vm((6, 16, width), F32), vm((5, 16, width), F32), vm((ff // 256, 1, 256), F32), vm((n, small, width), BF),
        pltpu.SemaphoreType.DMA((12,)), pltpu.SemaphoreType.DMA((4, 2)), pltpu.SemaphoreType.DMA((11, 10)),
        pltpu.SemaphoreType.DMA((8,)), pltpu.SemaphoreType.DMA((2, 5)),
    ]
    for _, R, _, _, cn, zlist, _ in reduce_shapes(width, ff):
        k = len(zlist)
        scratch += [vm((2 * k, 2, R, cn), BF), vm((2 * k, R, cn), BF), vm((k, R, cn), BF), vm((2, R, cn), BF), vm((R, cn), BF)]
    anyspec = pl.BlockSpec(memory_space=pl.ANY)
    smem = pl.BlockSpec(memory_space=pltpu.SMEM)
    vmem = pl.BlockSpec(memory_space=pltpu.VMEM)
    return pl.pallas_call(
        backward_kernel,
        out_shape=outs,
        in_specs=[smem, smem] + [anyspec] * len(saved),
        out_specs=[vmem] * 6 + [anyspec],
        scratch_shapes=scratch,
        compiler_params=pltpu.CompilerParams(
            collective_id=1, has_side_effects=True, vmem_limit_bytes=67043328
        ),
        name="backward",
    )(lengths, dealing, *saved)


def slice_plan(
    x_source, cotangent, lengths, dealing, qkv_weight, proj_weight, up_weight, down_weight,
    first_gain, first_shift, proj_bias, second_gain, second_shift, up_bias, down_bias,
):
    shards = [w.T for w in (qkv_weight, proj_weight, up_weight, down_weight)]
    vectors = [
        v[None] for v in (first_gain, first_shift, proj_bias, second_gain, second_shift, down_bias, up_bias)
    ]
    saved = forward(lengths, dealing, cotangent[0], x_source, shards, vectors)
    gq, gp, gu, gd, sums, input_grad, out = backward(lengths, dealing, saved, shards)
    own, long = first_gain.shape[0], up_bias.shape[0]
    return (
        out[None], input_grad, gq.T, gp.T, gu.T, gd.T,
        sums[G1, :own], sums[C1, :own], sums[BP, :own], sums[G2, :own], sums[C2, :own], sums[6, :long], sums[BD, :own],
    )


def layer_norm(values, scaling, offset):
    centered = values - jnp.mean(values, axis=-1, keepdims=True)
    spread = jnp.mean(centered * centered, axis=-1, keepdims=True)
    return centered * lax.rsqrt(spread + EPSILON) * scaling + offset


def gelu_tanh(values):
    return (
        0.5
        * values
        * (1.0 + jnp.tanh(TANH_SCALE * (values + CUBIC_TERM * values * values * values)))
    )


def grouped(array, block_seqs):
    return array.reshape(
        (array.shape[0] // block_seqs, block_seqs, array.shape[1], HEADS, array.shape[2] // HEADS)
    )


def grouped_stats(array, block_seqs):
    return array.reshape((array.shape[0] // block_seqs, block_seqs) + array.shape[1:])


def joined(array):
    return array.reshape(
        (array.shape[0] * array.shape[1], array.shape[2], array.shape[3] * array.shape[4])
    )


def masked_scores(queries, key_rows, query_start, score_scale):
    scores = (
        jnp.einsum("bqhd,bkhd->bhqk", queries, key_rows, preferred_element_type=jnp.float32)
        * score_scale
    )
    query_pos = query_start + jnp.arange(queries.shape[1])
    key_pos = jnp.arange(key_rows.shape[1])
    return jnp.where(key_pos[None, :] <= query_pos[:, None], scores, NEG_BIG)


def attend(inputs, query_start, score_scale):
    queries, key_rows, val_rows = inputs
    scores = masked_scores(queries, key_rows, query_start, score_scale)
    row_top = jnp.max(scores, axis=-1, keepdims=True)
    exponent = jnp.exp(scores - row_top)
    totals = jnp.sum(exponent, axis=-1, keepdims=True)
    weights = (exponent / totals).astype(jnp.bfloat16)
    attended = jnp.einsum("bhqk,bkhd->bqhd", weights, val_rows, preferred_element_type=jnp.float32)
    return (attended.astype(jnp.bfloat16), (row_top + jnp.log(totals))[..., 0])


def rows_back(inputs, query_start, score_scale):
    queries, key_rows, val_rows, grad_rows, log_total = inputs
    scores = masked_scores(queries, key_rows, query_start, score_scale)
    weights = jnp.exp(scores - log_total[..., None])
    grad_weights = jnp.einsum(
        "bqhd,bkhd->bhqk", grad_rows, val_rows, preferred_element_type=jnp.float32
    )
    delta_rows = jnp.sum(weights * grad_weights, axis=-1)
    grad_scores = (weights * (grad_weights - delta_rows[..., None])).astype(jnp.bfloat16)
    grad_query = (
        jnp.einsum("bhqk,bkhd->bqhd", grad_scores, key_rows, preferred_element_type=jnp.float32)
        * score_scale
    )
    grad_keys = (
        jnp.einsum("bhqk,bqhd->bkhd", grad_scores, queries, preferred_element_type=jnp.float32)
        * score_scale
    )
    grad_vals = jnp.einsum(
        "bhqk,bqhd->bkhd",
        weights.astype(jnp.bfloat16),
        grad_rows,
        preferred_element_type=jnp.float32,
    )
    return (grad_query, grad_keys, grad_vals)


def fetch_weights(
    qkv_weight,
    proj_weight,
    up_weight,
    down_weight,
    first_gain,
    first_shift,
    proj_bias,
    second_gain,
    second_shift,
    up_bias,
    down_bias,
):
    qkv_part, proj_part, up_part, down_part = (
        lax.all_gather(qkv_weight.astype(jnp.bfloat16), "cp", axis=0, tiled=True),
        lax.all_gather(proj_weight.astype(jnp.bfloat16), "cp", axis=0, tiled=True),
        lax.all_gather(up_weight.astype(jnp.bfloat16), "cp", axis=0, tiled=True),
        lax.all_gather(down_weight.astype(jnp.bfloat16), "cp", axis=0, tiled=True),
    )
    return (
        lax.all_gather(qkv_part, "dp", axis=1, tiled=True),
        lax.all_gather(proj_part, "dp", axis=1, tiled=True),
        lax.all_gather(up_part, "dp", axis=1, tiled=True),
        lax.all_gather(down_part, "dp", axis=1, tiled=True),
        lax.all_gather(first_gain.astype(jnp.bfloat16), "dp", axis=0, tiled=True),
        lax.all_gather(first_shift.astype(jnp.bfloat16), "dp", axis=0, tiled=True),
        lax.all_gather(proj_bias.astype(jnp.bfloat16), "dp", axis=0, tiled=True),
        lax.all_gather(second_gain.astype(jnp.bfloat16), "dp", axis=0, tiled=True),
        lax.all_gather(second_shift.astype(jnp.bfloat16), "dp", axis=0, tiled=True),
        lax.all_gather(up_bias.astype(jnp.bfloat16), "dp", axis=0, tiled=True),
        lax.all_gather(down_bias.astype(jnp.bfloat16), "dp", axis=0, tiled=True),
    )


def mat_rows(left, right):
    return jnp.einsum("sqd,de->sqe", left, right, preferred_element_type=jnp.float32)


def mat_back(left, right):
    return jnp.einsum("sqe,de->sqd", left, right, preferred_element_type=jnp.float32)


def mat_grad(left, right):
    return jnp.einsum("sqd,sqe->de", left, right, preferred_element_type=jnp.float32)


def general(
    x_source,
    cotangent,
    lengths,
    dealing,
    qkv_weight,
    proj_weight,
    up_weight,
    down_weight,
    first_gain,
    first_shift,
    proj_bias,
    second_gain,
    second_shift,
    up_bias,
    down_bias,
):
    groups = lax.axis_size("dp")
    seqs_all, piece_rows, features = x_source.shape
    seq_group = seqs_all // groups
    span_rows = groups * piece_rows
    score_scale = HEAD_DIM ** (-0.5)
    block_seqs = math.gcd(seq_group, max(1, 512 // span_rows))
    owners = jnp.argsort(dealing)
    send_order = owners.reshape(groups, seq_group).T.reshape(-1)
    outgoing = x_source[send_order].reshape(seq_group, span_rows, features)
    arrived = lax.all_to_all(outgoing, "dp", split_axis=1, concat_axis=1, tiled=True)
    first_slot = lax.axis_index("dp") * seq_group
    my_lengths = lax.dynamic_slice_in_dim(lengths[owners], first_slot, seq_group)
    query_start = lax.axis_index("cp") * span_rows
    positions = query_start + jnp.arange(span_rows)
    live_rows = positions[None, :] < my_lengths[:, None]
    fetched = fetch_weights(
        qkv_weight,
        proj_weight,
        up_weight,
        down_weight,
        first_gain,
        first_shift,
        proj_bias,
        second_gain,
        second_shift,
        up_bias,
        down_bias,
    )
    qkv_full, proj_full, up_full, down_full = (fetched[0], fetched[1], fetched[2], fetched[3])
    gain_one, shift_one, bias_proj, gain_two, shift_two, bias_up, bias_down = [
        vector.astype(jnp.float32) for vector in fetched[4:]
    ]
    inputs_f = arrived.astype(jnp.float32)
    norm_one, back_one = jax.vjp(layer_norm, inputs_f, gain_one, shift_one)
    act_one = norm_one.astype(jnp.bfloat16)
    mixed_rows = mat_rows(act_one, qkv_full).astype(jnp.bfloat16)
    queries = mixed_rows[..., :features]
    kv_local = mixed_rows[..., features:]
    kv_all = lax.all_gather(kv_local, "cp", axis=1, tiled=True)
    attended, log_total = lax.map(
        lambda inputs: attend(inputs, query_start, score_scale),
        (
            grouped(queries, block_seqs),
            grouped(kv_all[..., :features], block_seqs),
            grouped(kv_all[..., features:], block_seqs),
        ),
    )
    attended = joined(attended)
    log_total = log_total.reshape((seq_group,) + log_total.shape[2:])
    residual = inputs_f + mat_rows(attended, proj_full) + bias_proj
    norm_two, back_two = jax.vjp(layer_norm, residual, gain_two, shift_two)
    act_two = norm_two.astype(jnp.bfloat16)
    up_raw = mat_rows(act_two, up_full) + bias_up
    hidden, back_gelu = jax.vjp(gelu_tanh, up_raw)
    hid_low = hidden.astype(jnp.bfloat16)
    result = residual + mat_rows(hid_low, down_full) + bias_down
    output = jnp.where(live_rows[..., None], result, 0.0).astype(jnp.bfloat16)
    fetched = fetch_weights(
        qkv_weight,
        proj_weight,
        up_weight,
        down_weight,
        first_gain,
        first_shift,
        proj_bias,
        second_gain,
        second_shift,
        up_bias,
        down_bias,
    )
    qkv_full, proj_full, up_full, down_full = (fetched[0], fetched[1], fetched[2], fetched[3])
    gain_one, gain_two = (fetched[4].astype(jnp.float32), fetched[7].astype(jnp.float32))
    grad_out = jnp.where(live_rows[..., None], cotangent.astype(jnp.float32), 0.0)
    grad_low = grad_out.astype(jnp.bfloat16)
    grad_down = mat_grad(hid_low, grad_low)
    grad_bias_down = jnp.sum(grad_out, axis=(0, 1))
    grad_hidden = mat_back(grad_low, down_full)
    grad_up_raw = back_gelu(grad_hidden)[0].astype(jnp.bfloat16)
    grad_up = mat_grad(act_two, grad_up_raw)
    grad_bias_up = jnp.sum(grad_up_raw.astype(jnp.float32), axis=(0, 1))
    grad_act_two = mat_back(grad_up_raw, up_full)
    grad_resid, grad_gain_two, grad_shift_two = back_two(grad_act_two)
    grad_resid = grad_resid + grad_out
    grad_bias_proj = jnp.sum(grad_resid, axis=(0, 1))
    resid_low = grad_resid.astype(jnp.bfloat16)
    grad_proj = mat_grad(attended, resid_low)
    grad_attended = mat_back(resid_low, proj_full).astype(jnp.bfloat16)
    kv_back = lax.all_gather(kv_local, "cp", axis=1, tiled=True)
    key_rows = kv_back[..., :features]
    val_rows = kv_back[..., features:]
    grad_query, grad_keys, grad_vals = lax.map(
        lambda inputs: rows_back(inputs, query_start, score_scale),
        (
            grouped(queries, block_seqs),
            grouped(key_rows, block_seqs),
            grouped(val_rows, block_seqs),
            grouped(grad_attended, block_seqs),
            grouped_stats(log_total, block_seqs),
        ),
    )
    grad_keys, grad_vals = (
        lax.psum_scatter(
            joined(grad_keys).astype(jnp.bfloat16), "cp", scatter_dimension=1, tiled=True
        ).astype(jnp.float32),
        lax.psum_scatter(
            joined(grad_vals).astype(jnp.bfloat16), "cp", scatter_dimension=1, tiled=True
        ).astype(jnp.float32),
    )
    grad_mixed = jnp.concatenate([joined(grad_query), grad_keys, grad_vals], axis=-1).astype(
        jnp.bfloat16
    )
    grad_qkv = mat_grad(act_one, grad_mixed)
    grad_act_one = mat_back(grad_mixed, qkv_full)
    grad_input, grad_gain_one, grad_shift_one = back_one(grad_act_one)
    grad_input = (grad_input + grad_resid).astype(jnp.bfloat16)
    returned = lax.all_to_all(grad_input, "dp", split_axis=1, concat_axis=0, tiled=True)
    input_grad = returned[dealing]
    (
        grad_qkv,
        grad_proj,
        grad_up,
        grad_down,
        grad_gain_one,
        grad_shift_one,
        grad_bias_proj,
        grad_gain_two,
        grad_shift_two,
        grad_bias_up,
        grad_bias_down,
    ) = (
        lax.psum_scatter(
            grad_qkv.astype(jnp.bfloat16), "dp", scatter_dimension=1, tiled=True
        ).astype(jnp.float32),
        lax.psum_scatter(
            grad_proj.astype(jnp.bfloat16), "dp", scatter_dimension=1, tiled=True
        ).astype(jnp.float32),
        lax.psum_scatter(
            grad_up.astype(jnp.bfloat16), "dp", scatter_dimension=1, tiled=True
        ).astype(jnp.float32),
        lax.psum_scatter(
            grad_down.astype(jnp.bfloat16), "dp", scatter_dimension=1, tiled=True
        ).astype(jnp.float32),
        lax.psum_scatter(
            grad_gain_one.astype(jnp.bfloat16), "dp", scatter_dimension=0, tiled=True
        ).astype(jnp.float32),
        lax.psum_scatter(
            grad_shift_one.astype(jnp.bfloat16), "dp", scatter_dimension=0, tiled=True
        ).astype(jnp.float32),
        lax.psum_scatter(
            grad_bias_proj.astype(jnp.bfloat16), "dp", scatter_dimension=0, tiled=True
        ).astype(jnp.float32),
        lax.psum_scatter(
            grad_gain_two.astype(jnp.bfloat16), "dp", scatter_dimension=0, tiled=True
        ).astype(jnp.float32),
        lax.psum_scatter(
            grad_shift_two.astype(jnp.bfloat16), "dp", scatter_dimension=0, tiled=True
        ).astype(jnp.float32),
        lax.psum_scatter(
            grad_bias_up.astype(jnp.bfloat16), "dp", scatter_dimension=0, tiled=True
        ).astype(jnp.float32),
        lax.psum_scatter(
            grad_bias_down.astype(jnp.bfloat16), "dp", scatter_dimension=0, tiled=True
        ).astype(jnp.float32),
    )
    grad_qkv, grad_proj, grad_up, grad_down = (
        lax.psum_scatter(
            grad_qkv.astype(jnp.bfloat16), "cp", scatter_dimension=0, tiled=True
        ).astype(jnp.float32),
        lax.psum_scatter(
            grad_proj.astype(jnp.bfloat16), "cp", scatter_dimension=0, tiled=True
        ).astype(jnp.float32),
        lax.psum_scatter(
            grad_up.astype(jnp.bfloat16), "cp", scatter_dimension=0, tiled=True
        ).astype(jnp.float32),
        lax.psum_scatter(
            grad_down.astype(jnp.bfloat16), "cp", scatter_dimension=0, tiled=True
        ).astype(jnp.float32),
    )
    (
        grad_gain_one,
        grad_shift_one,
        grad_bias_proj,
        grad_gain_two,
        grad_shift_two,
        grad_bias_up,
        grad_bias_down,
    ) = lax.psum(
        (
            grad_gain_one,
            grad_shift_one,
            grad_bias_proj,
            grad_gain_two,
            grad_shift_two,
            grad_bias_up,
            grad_bias_down,
        ),
        "cp",
    )
    return (
        output,
        input_grad,
        grad_qkv,
        grad_proj,
        grad_up,
        grad_down,
        grad_gain_one,
        grad_shift_one,
        grad_bias_proj,
        grad_gain_two,
        grad_shift_two,
        grad_bias_up,
        grad_bias_down,
    )


def solution(mesh):
    in_specs = (
        P(None, ("cp", "dp"), None),
        P("dp", "cp", None),
        P(),
        P(),
        P("cp", "dp"),
        P("cp", "dp"),
        P("cp", "dp"),
        P("cp", "dp"),
        P("dp"),
        P("dp"),
        P("dp"),
        P("dp"),
        P("dp"),
        P("dp"),
        P("dp"),
    )
    out_specs = (
        P("dp", "cp", None),
        P(None, ("cp", "dp"), None),
        P("cp", "dp"),
        P("cp", "dp"),
        P("cp", "dp"),
        P("cp", "dp"),
        P("dp"),
        P("dp"),
        P("dp"),
        P("dp"),
        P("dp"),
        P("dp"),
        P("dp"),
    )
    planned = tuple(mesh.shape.items()) == (("dp", Z * Y * C), ("cp", X))
    local = slice_plan if planned else general
    return jax.shard_map(local, mesh=mesh, in_specs=in_specs, out_specs=out_specs, check_vma=False)
```

```python
import functools
import math

import jax
import jax.numpy as jnp
from jax import lax
from jax.experimental import pallas as pl
from jax.experimental.pallas import tpu as pltpu
from jax.sharding import PartitionSpec as P

HEADS = 12
HEAD_DIM = 64


EPSILON = 1e-05
NEG_BIG = -1e30
TANH_SCALE = 0.7978845608028654
CUBIC_TERM = 0.044715
MESH_IDS = pl.DeviceIdType.MESH
BF = jnp.bfloat16
F32 = jnp.float32

Z, Y, C, X = 4, 2, 2, 2


def mult(value, n):
    return value if isinstance(value, int) else pl.multiple_of(value, n)


def coords():
    d = lax.axis_index("dp")
    x = lax.axis_index("cp")
    return d // (Y * C), (d // C) % Y, d % C, x, d


def dev(z, y, c, x):
    return {"dp": (z * Y + y) * C + c, "cp": x}


def rcopy(src, dst, ssem, rsem, where):
    return pltpu.make_async_remote_copy(
        src_ref=src, dst_ref=dst, send_sem=ssem, recv_sem=rsem, device_id=where, device_id_type=MESH_IDS
    )


def lcopy(src, dst, sem):
    return pltpu.make_async_copy(src, dst, sem)


def wait_bytes(ref, sem):
    pltpu.make_async_copy(ref, ref, sem).wait()


def enter(everyone):
    d = lax.axis_index("dp")
    x = lax.axis_index("cp")
    barrier = pltpu.get_barrier_semaphore()

    def greet(k, carry):
        kd = k // X
        kx = k % X

        @pl.when(jnp.logical_or(kd != d, kx != x))
        def _():
            pl.semaphore_signal(barrier, inc=1, device_id={"dp": kd, "cp": kx}, device_id_type=MESH_IDS)

        return carry

    lax.fori_loop(0, everyone, greet, 0)

    def entered():
        pl.semaphore_wait(barrier, everyone - 1)

    return entered


def dot_nn(a, b):
    return lax.dot_general(a, b, (((1,), (0,)), ((), ())), preferred_element_type=F32)


def dot_nt(a, b):
    return lax.dot_general(a, b, (((1,), (1,)), ((), ())), preferred_element_type=F32)


def dot_tn(a, b):
    return lax.dot_general(a, b, (((0,), (0,)), ((), ())), preferred_element_type=F32)


def norm_parts(v):
    mean = jnp.mean(v, axis=-1, keepdims=True)
    cen = v - mean
    var = jnp.mean(cen * cen, axis=-1, keepdims=True)
    rstd = lax.rsqrt(var + EPSILON)
    return cen * rstd, rstd


def live_length(len_ref, deal_ref, slot):
    total = jnp.int32(0)
    for s in range(len_ref.shape[0]):
        total = total + jnp.where(deal_ref[s] == slot, len_ref[s], 0)
    return total


class Piece:
    def __init__(self, full, R, r0, rn, step, c0, cn):
        self.full = full
        self.R, self.r0, self.rn, self.step, self.c0, self.cn = R, r0, rn, step, c0, cn

    def at(self, z, y, c, x):
        d = (z * Y + y) * C + c
        return self.full.at[
            pl.ds(mult(d * self.R + self.r0, 16), self.rn), pl.ds(mult(x * self.step + self.c0, 128), self.cn)
        ]


class Gather:
    FAR, MATE, A, B, CORE = range(5)

    def __init__(self, piece, sems, k, dummy, where, kind, turned):
        self.p, self.sems, self.k, self.dummy, self.kind = piece, sems, k, dummy, kind
        z, y, c, x, _ = where
        self.z, self.y, self.c, self.x = z, y, c, x
        o = 1 if turned else c
        self.far, self.mate = 3 - z, z + 1 - 2 * (z % 2)
        self.ya, self.xa = (y + 1 - o) % 2, (x + o) % 2
        self.yb, self.xb = (y + o) % 2, (x + 1 - o) % 2
        self.to = {
            self.FAR: dev(self.far, y, c, x), self.MATE: dev(self.mate, y, c, x), self.A: dev(z, self.ya, c, self.xa),
            self.B: dev(z, self.yb, c, self.xb), self.CORE: dev(z, y, 1 - c, x),
        }
        self.counts = {self.FAR: 1, self.MATE: 2, self.A: 4} if kind == 1 else {self.FAR: 2, self.MATE: 4, self.A: 1}
        self.counts.update({self.B: 8, self.CORE: 16})

    def send(self, pieces, *ways):
        for way in ways:
            for z, y, x in pieces:
                q = self.p.at(z, y, self.c, x)
                rcopy(q, q, self.sems.at[self.k, 0, way], self.sems.at[self.k, 1, way], self.to[way]).start()

    def wait(self, way, side=1):
        p = self.p
        wait_bytes(self.dummy.at[pl.ds(0, self.counts[way] * p.rn), pl.ds(0, p.cn)], self.sems.at[self.k, side, way])

    def start(self):
        own = [(self.z, self.y, self.x)]
        if self.kind == 1:
            self.send(own, self.FAR, self.MATE, self.A, self.B, self.CORE)
        else:
            self.send(own, self.A, self.FAR, self.MATE, self.B, self.CORE)

    def tick1(self):
        if self.kind == 1:
            self.wait(self.FAR)
            self.send([(self.far, self.y, self.x)], self.MATE, self.A, self.B, self.CORE)
        else:
            self.wait(self.A)
            self.send([(self.z, self.ya, self.xa)], self.FAR, self.MATE, self.B, self.CORE)

    def tick2(self):
        if self.kind == 1:
            self.wait(self.MATE)
            self.send([(self.mate, self.y, self.x), (3 - self.mate, self.y, self.x)], self.A, self.B, self.CORE)
        else:
            self.wait(self.FAR)
            self.send([(self.far, self.y, self.x), (self.far, self.ya, self.xa)], self.MATE, self.B, self.CORE)

    def tick3(self):
        if self.kind == 1:
            self.wait(self.A)
            self.send([(k, self.ya, self.xa) for k in range(Z)], self.B, self.CORE)
        else:
            self.wait(self.MATE)
            self.send(
                [(k, y, x) for k in (self.mate, 3 - self.mate) for y, x in ((self.y, self.x), (self.ya, self.xa))],
                self.B, self.CORE,
            )

    def tick4(self):
        self.wait(self.B)
        self.send(
            [(k, y, x) for k in range(Z) for y, x in ((self.yb, self.xb), (1 - self.y, 1 - self.x))], self.CORE
        )

    def tick5(self):
        self.wait(self.CORE)

    def drain(self):
        for way in range(5):
            self.wait(way, 0)


class Vectors:
    FAR, MATE, A, CORE = range(4)

    def __init__(self, full, sems, where):
        self.full, self.sems = full, sems
        z, y, c, x, _ = where
        self.z, self.y, self.c = z, y, c
        self.far, self.mate = 3 - z, z + 1 - 2 * (z % 2)
        self.to = (dev(self.far, y, c, x), dev(self.mate, y, c, x), dev(z, 1 - y, c, x), dev(z, y, 1 - c, x))
        self.counts = (1, 2, 4, 8)

    def send(self, pieces, *ways):
        for way in ways:
            for z, y in pieces:
                q = self.full.at[(z * Y + y) * C + self.c]
                rcopy(q, q, self.sems.at[0, way], self.sems.at[1, way], self.to[way]).start()

    def wait(self, way, side=1):
        wait_bytes(self.full.at[pl.ds(0, self.counts[way])], self.sems.at[side, way])

    def start(self):
        self.send([(self.z, self.y)], self.FAR, self.MATE, self.A, self.CORE)

    def tick1(self):
        self.wait(self.FAR)
        self.send([(self.far, self.y)], self.MATE, self.A, self.CORE)

    def tick2(self):
        self.wait(self.MATE)
        self.send([(self.mate, self.y), (3 - self.mate, self.y)], self.A, self.CORE)

    def tick3(self):
        self.wait(self.A)
        self.send([(k, 1 - self.y) for k in range(Z)], self.CORE)

    def tick4(self):
        self.wait(self.CORE)

    def drain(self):
        for way in range(4):
            self.wait(way, 0)


G1, C1, BP, G2, C2, BD, BU = range(7)


def gather_chunks(wq, wp, wu, wd):
    rq, rp, ru, rd = (w.shape[0] // (Z * Y * C) for w in (wq, wp, wu, wd))
    half, wide = wq.shape[1] // X, wd.shape[1] // X
    out = []
    for k in range(3):
        out.append(Piece(wq, rq, k * (rq // 3), rq // 3, half, 0, half))
    out.append(Piece(wp, rp, 0, rp, half, 0, half))
    for k in range(4):
        out.append(Piece(wu, ru, k * (ru // 4), ru // 4, half, 0, half))
    for k in range(4):
        out.append(Piece(wd, rd, 0, rd, wide, k * (wide // 4), wide // 4))
    return out


def one_hot(count, width, first):
    at_row = lax.broadcasted_iota(jnp.int32, (count, width), 0)
    at_col = lax.broadcasted_iota(jnp.int32, (count, width), 1)
    return (at_col == at_row + first).astype(BF)


N_GATHER = 12
TICKS = ("tick1", "tick2", "tick3", "tick4")
KINDS = (1, 1, 1, 1, 2, 2, 1, 2, 2, 1, 2, 2)
TURNED = (7,)
COT_STEPS = (6, 8)
LAGS = ((0, 1, 2, 3),) * 4 + ((0, 1, 2, 4),) * 8


def forward_kernel(
    len_ref, deal_ref, cot, x_in, sq, sp, su, sd, v_g1, v_c1, v_bp, v_g2, v_c2, v_bd, v_bu,
    wq_o, wp_o, wu_o, wd_o, xr_o, gw_o, qs_o, ka_o, va_o, at_o, lse_o, r_o, a2_o, hd_o, gp_o, vec_o, out_o,
    wq, wp, wu, wd, xr, a1, qs, ka, va, at, lse, r, a2, hd, gp, vg, vec, bu3, sc0, sc1, outw, xg, acc,
    gsem, vsem, msem, osem,
):
    where = coords()
    z, y, c, x, d = where
    width = xr.shape[1]
    rows = xr.shape[0]
    qrows = rows // 2
    small = x_in.shape[1]
    pairs = width // 128
    tile = 256

    entered = enter(Z * Y * C * X)

    n = Z * Y * C
    for shard, full in ((sq, wq), (sp, wp), (su, wu), (sd, wd)):
        own, long = shard.shape
        full[pl.ds(mult(d * own, 16), own), pl.ds(mult(x * long, 128), long)] = shard[...].astype(BF)
    vg[d] = jnp.zeros(vg.shape[1:], BF)
    own = v_g1.shape[1]
    seven = jnp.concatenate([v[...] for v in (v_g1, v_c1, v_bp, v_g2, v_c2, v_bd)], axis=0).astype(BF)
    placed = dot_nn(seven, one_hot(own, width, d * own))
    long = v_bu.shape[1]
    per_row = width // long
    placed_long = dot_nn(v_bu[...].astype(BF), one_hot(long, width, (d % per_row) * long))
    rows_long = [jnp.where(d // per_row == k, placed_long, 0.0) for k in range(n // per_row)]
    rest = jnp.zeros((16 - 6 - n // per_row, width), F32)
    vg[d] = jnp.concatenate([placed] + rows_long + [rest], axis=0).astype(BF)
    slots = x_in.shape[0]
    for t in range(slots):
        owner = jnp.int32(0)
        for s in range(slots):
            owner = jnp.where(deal_ref[s] == t, s, owner)
        xg[t] = x_in[owner]

    entered()

    vectors = Vectors(vg, vsem, where)
    vectors.start()
    chunks = [
        Gather(p, gsem, k, wu, where, KINDS[k], k in TURNED) for k, p in enumerate(gather_chunks(wq, wp, wu, wd))
    ]

    def send_cot(b):
        core_b = (x + b) % 2
        src_b = cot.at[pl.ds(b * qrows, qrows)]
        dst_b = gw_o.at[pl.ds(mult(x * qrows, qrows), qrows)]
        same = jnp.logical_and(core_b == c, c == x)

        @pl.when(same)
        def _():
            lcopy(src_b, dst_b, msem.at[3]).start()

        @pl.when(jnp.logical_not(same))
        def _():
            rcopy(src_b, dst_b, msem.at[2], msem.at[3], dev(z, y, core_b, c)).start()

    per_quarter = qrows // small
    place = mult(x * qrows + (d % per_quarter) * small, 16)
    core_to = (x + d // per_quarter) % 2
    dst = xr.at[pl.ds(place, small)]

    def deal_out(k, carry):
        t = (d + k + x * (slots // 2)) % slots
        td = (t // 2) * 2 + core_to
        tx = t % 2
        mine = jnp.logical_and(td == d, tx == x)

        @pl.when(mine)
        def _():
            lcopy(xg.at[t], dst, msem.at[1]).start()

        @pl.when(jnp.logical_not(mine))
        def _():
            rcopy(xg.at[t], dst, msem.at[0], msem.at[1], {"dp": td, "cp": tx}).start()

        return carry

    ahead = 2
    for ch in chunks[:ahead]:
        ch.start()

    def step(s):
        if s + ahead < len(chunks):
            chunks[s + ahead].start()
        if s < 4:
            lax.fori_loop(s * slots // 4, (s + 1) * slots // 4, deal_out, 0)
        if s in COT_STEPS:
            send_cot(COT_STEPS.index(s))
        for n in range(4):
            for k in range(len(chunks)):
                if k + LAGS[k][n] == s:
                    getattr(chunks[k], TICKS[n])()

    step(0)
    vectors.tick1()
    step(1)
    vectors.tick2()
    step(2)
    vectors.tick3()
    step(3)
    vectors.tick4()

    def add_table(k, acc):
        return acc + vg[k].astype(F32)

    vec[...] = lax.fori_loop(1, Z * Y * C, add_table, vg[0].astype(F32))
    for k in range(bu3.shape[0]):
        per = width // tile
        bu3[k] = vec[BU + k // per:BU + k // per + 1, (k % per) * tile:(k % per + 1) * tile]

    wait_bytes(xr, msem.at[1])
    lrows = 128

    def first_norm(k, carry):
        at_rows = pl.ds(mult(k * lrows, lrows), lrows)
        n1, _ = norm_parts(xr[at_rows, :].astype(F32))
        a1[at_rows, :] = (n1 * vec[G1:G1 + 1, :] + vec[C1:C1 + 1, :]).astype(BF)
        return carry

    lax.fori_loop(0, rows // lrows, first_norm, 0)

    step(4)
    step(5)
    for k in range(3):
        chunks[k].tick5()
    keep = [pltpu.make_async_copy(wq, wq_o, osem.at[0])]
    keep[-1].start()

    quarters = (c, 3 - c)

    def q_at(i):
        return pl.ds(mult(quarters[i] * qrows, qrows), qrows)

    steps = width // tile
    for part in range(3):
        def project(n, carry, part=part):
            lanes = pl.ds(mult(n * tile, tile), tile)
            res = dot_nt(a1[...], wq[pl.ds(mult(part * width + n * tile, tile), tile), :]).astype(BF)
            if part == 0:
                qs[:, lanes] = res * jnp.asarray(HEAD_DIM ** -0.5, BF)
            else:
                to = ka if part == 1 else va
                for i in range(2):
                    to[q_at(i), lanes] = res[i * qrows:(i + 1) * qrows]
            return carry

        lax.fori_loop(0, steps, project, 0)
        if part > 0:
            to = ka if part == 1 else va
            for i in range(2):
                rcopy(to.at[q_at(i)], to.at[q_at(i)], msem.at[4 + 2 * (part - 1)], msem.at[5 + 2 * (part - 1)], dev(z, y, 1 - c, x)).start()
    step(6)
    wait_bytes(ka.at[pl.ds(0, rows)], msem.at[5])
    wait_bytes(va.at[pl.ds(0, rows)], msem.at[7])
    for src, out, s in ((qs, qs_o, 1), (ka, ka_o, 2), (va, va_o, 3), (xr, xr_o, 4), (vec, vec_o, 5)):
        keep.append(pltpu.make_async_copy(src, out, osem.at[s]))
        keep[-1].start()

    lane = lax.broadcasted_iota(jnp.int32, (qrows, 128), 1)
    kpos = lax.broadcasted_iota(jnp.int32, (qrows, qrows), 0)
    qpos = lax.broadcasted_iota(jnp.int32, (qrows, qrows), 1)
    groups = qrows // 8

    def pair_body(p, carry):
        lanes = pl.ds(mult(p * 128, 128), 128)
        for i in range(2):
            quarter = quarters[i]
            qp = qs[i * qrows:(i + 1) * qrows, lanes]
            zero = jnp.zeros_like(qp)
            qh = (jnp.where(lane < HEAD_DIM, qp, zero), jnp.where(lane >= HEAD_DIM, qp, zero))

            def scores(j, tops, diagonal=False):
                at_keys = pl.ds(mult(j * qrows, qrows), qrows)
                kj = ka[at_keys, lanes]
                new = []
                for h, sc in enumerate((sc0, sc1)):
                    s = dot_nt(kj, qh[h])
                    if diagonal:
                        s = jnp.where(kpos <= qpos, s, NEG_BIG)
                    sc[at_keys, :] = s
                    new.append(jnp.maximum(tops[h], jnp.max(s.reshape(groups, 8, qrows), axis=0)))
                return tuple(new)

            low = jnp.full((8, qrows), NEG_BIG, F32)
            tops = scores(quarter, lax.fori_loop(0, quarter, scores, (low, low)), True)
            tops = tuple(jnp.max(t, axis=0, keepdims=True) for t in tops)

            def values(j, state):
                at_keys = pl.ds(mult(j * qrows, qrows), qrows)
                vt = va[at_keys, lanes].T
                new = []
                for h, sc in enumerate((sc0, sc1)):
                    total, acc = state[h]
                    e = jnp.exp(sc[at_keys, :] - tops[h])
                    total = total + jnp.sum(e.reshape(groups, 8, qrows), axis=0)
                    acc = acc + dot_nn(vt[h * HEAD_DIM:(h + 1) * HEAD_DIM], e.astype(BF))
                    new.append((total, acc))
                return tuple(new)

            blank = (jnp.zeros((8, qrows), F32), jnp.zeros((HEAD_DIM, qrows), F32))
            state = lax.fori_loop(0, quarter + 1, values, (blank, blank))
            parts = []
            for h in range(2):
                total = jnp.sum(state[h][0], axis=0, keepdims=True)
                parts.append(state[h][1] / total)
                lse[p, i * 2 + h:i * 2 + h + 1, :] = tops[h] + jnp.log(total)
            at[i * qrows:(i + 1) * qrows, lanes] = jnp.concatenate(parts, axis=0).T.astype(BF)
        return carry

    per = 2
    for k in range(0, pairs, per):
        lax.fori_loop(k, k + per, pair_body, 0)
        step(7 + k // per)

    chunks[3].tick5()
    for src, out, s in ((wp, wp_o, 6), (at, at_o, 7), (lse, lse_o, 8)):
        keep.append(pltpu.make_async_copy(src, out, osem.at[s]))
        keep[-1].start()

    def attend_out(n, carry):
        lanes = pl.ds(mult(n * tile, tile), tile)
        res = dot_nt(at[...], wp[pl.ds(mult(n * tile, tile), tile), :])
        r[:, lanes] = xr[:, lanes].astype(F32) + res + vec[BP:BP + 1, lanes]
        return carry

    lax.fori_loop(0, steps, attend_out, 0)

    def second_norm(k, carry):
        at_rows = pl.ds(mult(k * lrows, lrows), lrows)
        n2, _ = norm_parts(r[at_rows, :])
        a2[at_rows, :] = (n2 * vec[G2:G2 + 1, :] + vec[C2:C2 + 1, :]).astype(BF)
        return carry

    lax.fori_loop(0, rows // lrows, second_norm, 0)
    step(10)
    step(11)
    for k in range(4, 8):
        chunks[k].tick5()
    for src, out, s in ((wu, wu_o, 9), (r, r_o, 10), (a2, a2_o, 11)):
        keep.append(pltpu.make_async_copy(src, out, osem.at[s]))
        keep[-1].start()

    def up(n, carry):
        lanes = pl.ds(mult(n * tile, tile), tile)
        u = dot_nt(a2[...], wu[lanes, :]) + bu3[n]
        sq_u = u * u
        t = jnp.tanh(TANH_SCALE * (u + CUBIC_TERM * sq_u * u))
        half_up = 0.5 * (1.0 + t)
        hd[:, lanes] = (u * half_up).astype(BF)
        slope = TANH_SCALE * (1.0 + 3.0 * CUBIC_TERM * sq_u)
        gp[:, lanes] = (half_up + 0.5 * u * (1.0 - t * t) * slope).astype(BF)
        return carry

    blocks = hd.shape[1] // tile
    for k in range(0, blocks, 4):
        lax.fori_loop(k, k + 4, up, 0)
        step(12 + k // 4)
    for src, out, s in ((hd, hd_o, 12), (gp, gp_o, 13)):
        keep.append(pltpu.make_async_copy(src, out, osem.at[s]))
        keep[-1].start()
    my_len = live_length(len_ref, deal_ref, (z * Y + y) * C + x)
    rowpos = lax.broadcasted_iota(jnp.int32, (qrows, 1), 0)
    parts = len(chunks) - 8
    wide = wd.shape[1] // X
    for k in range(parts):
        if k == 1:
            step(15)
        chunks[8 + k].tick5()
        cuts = [slice(h * wide + k * (wide // parts), h * wide + (k + 1) * (wide // parts)) for h in range(X)]
        for h, cut in enumerate(cuts):
            keep.append(pltpu.make_async_copy(wd.at[:, cut], wd_o.at[:, cut], osem.at[16 + X * k + h]))
            keep[-1].start()

        def down(n, carry, k=k, cuts=cuts):
            lanes = pl.ds(mult(n * tile, tile), tile)
            res = dot_nt(hd[:, cuts[0]], wd[lanes, cuts[0]])
            for cut in cuts[1:]:
                res = res + dot_nt(hd[:, cut], wd[lanes, cut])
            res = res + (r[:, lanes] + vec[BD:BD + 1, lanes] if k == 0 else acc[:, lanes])
            if k < parts - 1:
                acc[:, lanes] = res
            else:
                for i in range(2):
                    live = quarters[i] * qrows + rowpos < my_len
                    outw[i * qrows:(i + 1) * qrows, lanes] = jnp.where(live, res[i * qrows:(i + 1) * qrows], 0.0).astype(BF)
            return carry

        lax.fori_loop(0, steps, down, 0)
    keep.append(pltpu.make_async_copy(outw, out_o, osem.at[15]))
    keep[-1].start()

    for ch in chunks:
        ch.drain()
    vectors.drain()

    @pl.when(core_to == c)
    def _():
        wait_bytes(xr.at[pl.ds(0, rows - small)], msem.at[0])

    @pl.when(core_to != c)
    def _():
        wait_bytes(xr, msem.at[0])

    @pl.when(c == x)
    def _():
        wait_bytes(xr.at[pl.ds(0, qrows)], msem.at[2])

    @pl.when(c != x)
    def _():
        wait_bytes(xr, msem.at[2])

    wait_bytes(xr, msem.at[3])
    wait_bytes(ka.at[pl.ds(0, rows)], msem.at[4])
    wait_bytes(va.at[pl.ds(0, rows)], msem.at[6])
    for cp in keep:
        cp.wait()


def forward(lengths, dealing, cot, x_source, shards, vectors):
    slots, small, width = x_source.shape
    rows = cot.shape[0]
    ff = shards[2].shape[0] * Z * Y * C
    keys = rows * 2
    pairs = width // 128

    def arr(shape, dtype=BF):
        return jax.ShapeDtypeStruct(shape, dtype)

    outs = [
        arr((3 * width, width)), arr((width, width)), arr((ff, width)), arr((width, ff)),
        arr((rows, width)), arr((rows, width)), arr((rows, width)), arr((keys, width)), arr((keys, width)),
        arr((rows, width)), arr((pairs, 8, rows // 2), F32), arr((rows, width), F32), arr((rows, width)),
        arr((rows, ff)), arr((rows, ff)), arr((16, width), F32), arr((rows, width)),
    ]
    vm = pltpu.VMEM
    scratch = [
        vm((3 * width, width), BF), vm((width, width), BF), vm((ff, width), BF), vm((width, ff), BF),
        vm((rows, width), BF), vm((rows, width), BF), vm((rows, width), BF), vm((keys, width), BF),
        vm((keys, width), BF), vm((rows, width), BF), vm((pairs, 8, rows // 2), F32), vm((rows, width), F32),
        vm((rows, width), BF), vm((rows, ff), BF), vm((rows, ff), BF), vm((Z * Y * C, 16, width), BF),
        vm((16, width), F32), vm((ff // 256, 1, 256), F32), vm((keys, rows // 2), F32), vm((keys, rows // 2), F32),
        vm((rows, width), BF), vm(x_source.shape, BF), vm((rows, width), F32),
        pltpu.SemaphoreType.DMA((N_GATHER, 2, 5)), pltpu.SemaphoreType.DMA((2, 4)), pltpu.SemaphoreType.DMA((8,)),
        pltpu.SemaphoreType.DMA((24,)),
    ]
    anyspec = pl.BlockSpec(memory_space=pl.ANY)
    smem = pl.BlockSpec(memory_space=pltpu.SMEM)
    vmem = pl.BlockSpec(memory_space=pltpu.VMEM)
    return pl.pallas_call(
        forward_kernel,
        out_shape=outs,
        in_specs=[smem, smem, anyspec] + [vmem] * 12,
        out_specs=[anyspec] * len(outs),
        scratch_shapes=scratch,
        compiler_params=pltpu.CompilerParams(
            collective_id=0, has_side_effects=True, vmem_limit_bytes=60 * 1024 * 1024
        ),
        name="forward",
    )(lengths, dealing, cot, x_source, *shards, *vectors)


def when(cond):
    if isinstance(cond, bool):
        return (lambda f: f()) if cond else (lambda f: None)
    return pl.when(cond)


class Reduce:
    S1, R1, S2, R2, S3, R3, S4, R4, S5, R5 = range(10)

    def __init__(self, grad, R, step, c0, C, zlist, bufs, out, out_c0, sems, k, where, kind, turned):
        self.kind = kind
        self.grad, self.R, self.step, self.c0, self.cn, self.zlist = grad, R, step, c0, C, zlist
        self.r1, self.r2, self.r3, self.r4, self.r5 = bufs
        self.out, self.out_c0, self.sems, self.k = out, out_c0, sems, k
        self.z, self.y, self.c, self.x, _ = where
        y, x = self.y, self.x
        self.o = o = 1 if turned else self.c
        self.y2, self.x2 = (y + o) % 2, (x + 1 - o) % 2
        self.y3, self.x3 = (y + 1 - o) % 2, (x + o) % 2
        self.every = len(zlist) == Z

    def sem(self, which):
        return self.sems.at[self.k, which]

    def rows(self, z, y, c):
        return pl.ds(mult(((z * Y + y) * C + c) * self.R, 16), self.R)

    def cols(self, x):
        return pl.ds(mult(x * self.step + self.c0, 128), self.cn)

    def at(self, z, y, c, x):
        return self.grad.at[self.rows(z, y, c), self.cols(x)]

    def add(self, rows, cols, got):
        self.grad[rows, cols] = (self.grad[rows, cols].astype(F32) + got.astype(F32)).astype(BF)

    def zidx(self, zi):
        return zi if self.every else self.zlist[0]

    def start(self):
        z, y, c, x = self.z, self.y, self.c, self.x
        to = dev(z, y, 1 - c, x)
        for zi, zz in enumerate(self.zlist):
            for yy in range(Y):
                for xx in range(X):
                    rcopy(
                        self.at(zz, yy, 1 - c, xx), self.r1.at[zi * Y + yy, xx],
                        self.sem(self.S1), self.sem(self.R1), to,
                    ).start()

    def tick2(self):
        z, y, c, x, o = self.z, self.y, self.c, self.x, self.o
        wait_bytes(self.r1, self.sem(self.R1))

        def body(e, carry):
            rows = self.rows(self.zidx(e // Y), e % Y, c)
            for xx in range(X):
                self.add(rows, self.cols(xx), self.r1[e, xx])
            return carry

        lax.fori_loop(0, len(self.zlist) * Y, body, 0)
        to = dev(z, self.y2, c, self.x2)
        for zi, zz in enumerate(self.zlist):
            for w in range(2):
                yy = w * (1 - o) + (1 - y) * o
                xx = (1 - x) * (1 - o) + w * o
                rcopy(self.at(zz, yy, c, xx), self.r2.at[zi * 2 + w], self.sem(self.S2), self.sem(self.R2), to).start()

    def tick3(self):
        z, y, c, x, o = self.z, self.y, self.c, self.x, self.o
        wait_bytes(self.r2, self.sem(self.R2))

        def body(e, carry):
            w = e % 2
            yy = w * (1 - o) + y * o
            xx = x * (1 - o) + w * o
            self.add(self.rows(self.zidx(e // 2), yy, c), self.cols(xx), self.r2[e])
            return carry

        lax.fori_loop(0, len(self.zlist) * 2, body, 0)
        if self.kind == 2:
            mate = z + 1 - 2 * (z % 2)
            for slot, zz in enumerate((mate, 3 - mate)):
                for w in range(2):
                    rcopy(
                        self.left(zz, w), self.r4.at[slot * 2 + w], self.sem(self.S4), self.sem(self.R4),
                        dev(mate, y, c, x),
                    ).start()
            return
        to = dev(z, self.y3, c, self.x3)
        for zi, zz in enumerate(self.zlist):
            rcopy(self.at(zz, self.y3, c, self.x3), self.r3.at[zi], self.sem(self.S3), self.sem(self.R3), to).start()

    def left_cut(self, zz, w):
        o = self.o
        return self.rows(zz, w * (1 - o) + self.y * o, self.c), self.cols(self.x * (1 - o) + w * o)

    def left(self, zz, w):
        return self.grad.at[self.left_cut(zz, w)]

    def first_hop(self, k):
        return [(k ^ 1, k, 0), ((3 - k) ^ 1, 3 - k, 1)]

    def tick4(self):
        z, y, c, x = self.z, self.y, self.c, self.x
        if self.kind == 2:
            wait_bytes(self.r4, self.sem(self.R4))
            for w in range(2):
                self.add(*self.left_cut(3 - z, w), self.r4[2 + w])
                rcopy(
                    self.left(3 - z, w), self.r5.at[w], self.sem(self.S5), self.sem(self.R5), dev(3 - z, y, c, x)
                ).start()
            for w in range(2):
                self.add(*self.left_cut(z, w), self.r4[w])
            return
        wait_bytes(self.r3, self.sem(self.R3))

        def body(zi, carry):
            self.add(self.rows(self.zidx(zi), y, c), self.cols(x), self.r3[zi])
            return carry

        lax.fori_loop(0, len(self.zlist), body, 0)
        if self.every:
            mate = z + 1 - 2 * (z % 2)
            for slot, zz in enumerate((mate, 3 - mate)):
                rcopy(
                    self.at(zz, y, c, x), self.r4.at[slot], self.sem(self.S4), self.sem(self.R4), dev(mate, y, c, x)
                ).start()
        else:
            k = self.zlist[0]
            for sender, taker, slot in self.first_hop(k):
                @pl.when(z == sender)
                def _(taker=taker, slot=slot):
                    rcopy(
                        self.at(k, y, c, x), self.r4.at[slot], self.sem(self.S4), self.sem(self.R4),
                        dev(taker, y, c, x),
                    ).start()

    def tick5(self):
        z, y, c, x = self.z, self.y, self.c, self.x
        if self.kind == 2:
            wait_bytes(self.r5, self.sem(self.R5))
            for w in range(2):
                self.add(*self.left_cut(z, w), self.r5[w])
            rcopy(
                self.at(z, self.y3, c, self.x3), self.r3.at[0], self.sem(self.S3), self.sem(self.R3),
                dev(z, self.y3, c, self.x3),
            ).start()
            return
        k = self.zlist[0]

        def take(zz, slot):
            self.add(self.rows(zz, y, c), self.cols(x), self.r4[slot])

        def pass_on(zz):
            rcopy(self.at(zz, y, c, x), self.r5.at[0], self.sem(self.S5), self.sem(self.R5), dev(zz, y, c, x)).start()

        if self.every:
            wait_bytes(self.r4, self.sem(self.R4))
            take(3 - z, 1)
            pass_on(3 - z)
            take(z, 0)
        else:
            @pl.when(z == 3 - k)
            def _():
                wait_bytes(self.r4.at[1], self.sem(self.R4))
                take(k, 1)
                pass_on(k)

            @pl.when(z == k)
            def _():
                wait_bytes(self.r4.at[0], self.sem(self.R4))
                take(k, 0)

    def tick6(self):
        z, y, c, x = self.z, self.y, self.c, self.x

        @when(True if self.every else z == self.zlist[0])
        def _():
            last, sem = (self.r3, self.R3) if self.kind == 2 else (self.r5, self.R5)
            wait_bytes(last, self.sem(sem))
            own = self.grad[self.rows(z, y, c), self.cols(x)].astype(F32)
            self.out[:, self.out_c0:self.out_c0 + self.cn] = own + last[0].astype(F32)

    def drain(self):
        z = self.z
        wait_bytes(self.r1, self.sem(self.S1))
        wait_bytes(self.r2, self.sem(self.S2))
        wait_bytes(self.r3, self.sem(self.S3))
        if self.every:
            wait_bytes(self.r4, self.sem(self.S4))
            wait_bytes(self.r5, self.sem(self.S5))
        else:
            k = self.zlist[0]
            for sender, _, slot in self.first_hop(k):
                @pl.when(z == sender)
                def _():
                    wait_bytes(self.r4.at[0], self.sem(self.S4))

            @pl.when(z == 3 - k)
            def _():
                wait_bytes(self.r5, self.sem(self.S5))


TURNED_BACK = ()
KINDS_BACK = (2,) * 4 + (1,) * 9


def reduce_shapes(width, ff):
    n = Z * Y * C
    every = list(range(Z))
    half = width // X
    wide = ff // X
    shapes = [("d", width // n, wide, k * (wide // 4), wide // 4, every, k * (wide // 4)) for k in range(4)]
    shapes += [("u", ff // n, half, 0, half, [k], 0) for k in range(Z)]
    shapes += [("p", width // n, half, 0, half, every, 0)]
    shapes += [("q", 3 * width // n, half, 0, half, [k], 0) for k in range(Z)]
    return shapes


PLAN = (
    "f2", ("u0", 1), "f4", ("u0", 2), "f5", ("u2", 1), ("d0", 1), ("d1", 1), "f7", ("u2", 2), "f8", ("u1", 1), ("d0", 2),
    "f9", ("d1", 2), "f10", ("u1", 2), ("u0", 3), "f11", ("u3", 1), ("d2", 1), ("d3", 1), "norm2", ("u2", 3),
    "proj", ("pj", 1), ("u3", 2), ("d2", 2), ("d0", 3), ("d3", 2), "a00", ("pj", 2), ("d1", 3), "a10", ("u1", 3), ("d0", 4),
    "a11", ("u0", 4), ("d1", 4), ("u2", 4), "a21", ("u3", 3), ("d0", 5), ("u0", 5), "a31", ("d2", 3), ("d1", 5), ("u2", 5),
    "a40", ("d3", 3), "a50", ("pj", 3), ("d2", 4), ("u1", 4), "a51", ("u3", 4), "norm1", ("d3", 4), "qa", ("q0", 1),
    ("pj", 4), "merge", ("d2", 5), "qb", ("q1", 1), ("u1", 5), ("q0", 2), "qc", ("q2", 1), ("u3", 5), "qd", ("q3", 1),
    ("q1", 2), ("d3", 5), "da", ("q2", 2), ("q3", 2), ("q0", 3), ("pj", 5), "ln", ("x", 0), ("u0", 6), ("u2", 6), ("d0", 6),
    ("d1", 6), ("x", 1), ("v", 0), ("q1", 3), ("d2", 6), ("u1", 6), ("u3", 6), ("x", 2), ("v", 1), ("q2", 3), ("d3", 6),
    ("x", 3), ("q3", 3), ("q0", 4), ("v", 2), ("pj", 6), ("q1", 4), ("q0", 5), ("v", 3), ("q2", 4), ("q1", 5), ("q3", 4),
    ("q2", 5), ("v", 4), ("q3", 5), ("q0", 6), ("q1", 6), ("q2", 6), ("q3", 6),
)


def part_actions(plan):
    parts, now = {}, None
    for item in plan:
        if isinstance(item, str):
            now = parts.setdefault(item, [])
        else:
            now.append(item)
    return parts


def backward_kernel(*refs):
    names = (
        "len_ref", "deal_ref", "wq_i", "wp_i", "wu_i", "wd_i", "xr_i", "gw_i", "qs_i", "ka_i", "va_i", "at_i",
        "lse_i", "r_i", "a2_i", "hd_i", "gp_i", "vec_i", "out_i", "og_q", "og_p", "og_u", "og_d", "osum", "ret",
        "out_n", "wq", "wp", "xr", "g", "qs", "ka", "va", "at", "lse", "r", "a2", "vec", "gt", "d2", "dr", "drl",
        "do", "gq", "gp_", "gu", "gd", "wd_t", "wu_t", "hd_t", "gp_t", "dka", "dva", "own_v", "sv", "rk", "rv", "dm",
        "vs", "vr", "bub", "lsem", "tsem", "rsem", "msem", "vsem",
    )
    env = dict(zip(names, refs[: len(names)]))
    env.update(a1=env["a2"], own_k=env["d2"], sk=env["drl"], dx=env["do"])
    bufs = refs[len(names):]
    e = type("Refs", (), env)
    where = coords()
    z, y, c, x, d = where
    rows, width = e.g.shape
    ff = e.hd_i.shape[1]
    qrows = rows // 2
    pairs = width // 128
    tile = 256
    lrows = 128
    steps = width // tile
    quarters = (c, 3 - c)
    theirs = (1 - c, 2 + c)

    def at_quarter(k):
        return pl.ds(mult(k * qrows, qrows), qrows)

    entered = enter(Z * Y * C * X)

    loads = {}
    for k, (src, dst) in enumerate(
        (
            ("gw_i", "g"), ("a2_i", "a2"), ("r_i", "r"), ("vec_i", "vec"), ("wp_i", "wp"), ("at_i", "at"),
            ("qs_i", "qs"), ("ka_i", "ka"), ("va_i", "va"), ("lse_i", "lse"), ("xr_i", "xr"), ("wq_i", "wq"),
        )
    ):
        loads[dst] = pltpu.make_async_copy(env[src], env[dst], e.lsem.at[k])

    def tile_of(idx):
        block = idx // 3
        return (block % 2) * 2 * 3 + (block // 2) * 3 + idx % 3

    def tile_copies(idx):
        n = tile_of(idx)
        slot = idx % 2
        cut = pl.ds(mult(n * tile, tile), tile)
        return (
            pltpu.make_async_copy(e.wd_i.at[:, cut], e.wd_t.at[slot], e.tsem.at[0, slot]),
            pltpu.make_async_copy(e.gp_i.at[:, cut], e.gp_t.at[slot], e.tsem.at[1, slot]),
            pltpu.make_async_copy(e.hd_i.at[:, cut], e.hd_t.at[slot], e.tsem.at[2, slot]),
            pltpu.make_async_copy(e.wu_i.at[cut, :], e.wu_t.at[slot], e.tsem.at[3, slot]),
        )

    loads["g"].start()
    for cp in tile_copies(0):
        cp.start()
    loads["a2"].start()
    for name in ("r", "vec", "wp", "at", "qs", "ka", "va", "lse", "xr", "wq"):
        loads[name].start()

    grads = {"q": (e.gq, e.og_q), "p": (e.gp_, e.og_p), "u": (e.gu, e.og_u), "d": (e.gd, e.og_d)}
    chunks = []
    for k, (name, R, step, c0, cn, zlist, oc) in enumerate(reduce_shapes(width, ff)):
        grad, out = grads[name]
        chunks.append(Reduce(grad, R, step, c0, cn, zlist, bufs[5 * k:5 * k + 5], out, oc, e.rsem, k, where, KINDS_BACK[k], k in TURNED_BACK))
    names_of = ("d0", "d1", "d2", "d3", "u0", "u1", "u2", "u3", "pj", "q0", "q1", "q2", "q3")
    by_name = dict(zip(names_of, chunks))
    parts = part_actions(PLAN)

    def after(part):
        for name, k in parts.get(part, ()):
            if name in by_name:
                ch = by_name[name]
                (ch.start, ch.tick2, ch.tick3, ch.tick4, ch.tick5, ch.tick6)[k - 1]()
            elif name == "x":
                give(k)
            else:
                land(k)
                if k < 4:
                    hop(k + 1)


    my_len = live_length(e.len_ref, e.deal_ref, (z * Y + y) * C + x)
    rowpos = lax.broadcasted_iota(jnp.int32, (lrows, 1), 0)
    loads["g"].wait()
    blank = jnp.zeros((1, width), F32)
    total_bd = blank
    for k in range(rows // lrows):
        base = quarters[k * lrows // qrows] * qrows + (k * lrows) % qrows
        live = base + rowpos < my_len
        part = jnp.where(live, e.g[k * lrows:(k + 1) * lrows, :], jnp.zeros((), BF))
        e.g[k * lrows:(k + 1) * lrows, :] = part
        e.gt[:, k * lrows:(k + 1) * lrows] = part.T
        total_bd = total_bd + jnp.sum(part.astype(F32), axis=0, keepdims=True)
    e.d2[...] = jnp.zeros_like(e.d2)
    loads["a2"].wait()

    ff_tiles = ff // tile
    def ffn(idx, carry, acting=True):
        slot = idx % 2
        n = tile_of(idx)
        cut = pl.ds(mult(n * tile, tile), tile)

        @pl.when(idx + 1 < ff_tiles)
        def _():
            for cp in tile_copies(idx + 1):
                cp.start()

        for cp in tile_copies(idx):
            cp.wait()
        du = (e.gp_t[slot].astype(F32) * dot_nn(e.g[...], e.wd_t[slot])).astype(BF)
        e.bub[n] = jnp.sum(du.astype(F32), axis=0, keepdims=True)
        e.gd[:, cut] = dot_nn(e.gt[...], e.hd_t[slot]).astype(BF)
        e.gu[cut, :] = dot_tn(du, e.a2[...]).astype(BF)
        e.d2[...] += dot_nn(du, e.wu_t[slot])
        for k in range(2, ff_tiles) if acting else ():
            if f"f{k}" in parts:
                @pl.when(idx == k)
                def _(k=k):
                    after(f"f{k}")

        return carry

    def ffn_first(idx, carry):
        return ffn(idx, carry, False)

    lax.fori_loop(0, 2, ffn_first, 0)

    entered()

    for i in range(2):
        same = jnp.logical_and(x == c, x == i)
        src = e.out_i.at[pl.ds(i * qrows, qrows)]
        dst = e.out_n.at[pl.ds(mult(((i + c) % 2) * qrows, qrows), qrows)]

        @pl.when(same)
        def _(src=src, dst=dst):
            lcopy(src, dst, e.msem.at[1]).start()

        @pl.when(jnp.logical_not(same))
        def _(src=src, dst=dst, i=i):
            rcopy(src, dst, e.msem.at[0], e.msem.at[1], dev(z, y, x, i)).start()

    lax.fori_loop(2, ff_tiles, ffn, 0)

    loads["r"].wait()
    loads["vec"].wait()

    def norm_two(k, sums):
        at_rows = pl.ds(mult(k * lrows, lrows), lrows)
        n2, rstd = norm_parts(e.r[at_rows, :])
        da = e.d2[at_rows, :]
        ee = da * e.vec[G2:G2 + 1, :]
        gg = e.g[at_rows, :].astype(F32)
        m1 = jnp.mean(ee, axis=-1, keepdims=True)
        m2 = jnp.mean(ee * n2, axis=-1, keepdims=True)
        dr = gg + (ee - m1 - n2 * m2) * rstd
        e.dr[at_rows, :] = dr
        e.drl[at_rows, :] = dr.astype(BF)
        return (
            sums[0] + jnp.sum(da * n2, axis=0, keepdims=True),
            sums[1] + jnp.sum(da, axis=0, keepdims=True),
            sums[2] + jnp.sum(dr, axis=0, keepdims=True),
        )

    sum_g2, sum_c2, sum_bp = lax.fori_loop(0, rows // lrows, norm_two, (blank, blank, blank))

    after("norm2")

    loads["wp"].wait()
    loads["at"].wait()

    def proj_back(n, carry):
        cut = pl.ds(mult(n * tile, tile), tile)
        e.do[:, cut] = dot_nn(e.drl[...], e.wp[:, cut]).astype(BF)
        e.gp_[cut, :] = dot_tn(e.drl[:, cut], e.at[...]).astype(BF)
        return carry

    lax.fori_loop(0, steps, proj_back, 0)
    after("proj")

    for name in ("qs", "ka", "va", "lse"):
        loads[name].wait()
    lane = lax.broadcasted_iota(jnp.int32, (qrows, 128), 1)
    kpos = lax.broadcasted_iota(jnp.int32, (qrows, qrows), 0)
    qpos = lax.broadcasted_iota(jnp.int32, (qrows, qrows), 1)

    def split(v):
        zero = jnp.zeros_like(v)
        return jnp.where(lane < HEAD_DIM, v, zero), jnp.where(lane >= HEAD_DIM, v, zero)

    def pair_body(p, carry):
        lanes = pl.ds(mult(p * 128, 128), 128)
        e.dka[...] = jnp.zeros_like(e.dka)
        e.dva[...] = jnp.zeros_like(e.dva)
        for i in range(2):
            quarter = quarters[i]
            own = slice(i * qrows, (i + 1) * qrows)
            qp, dop = e.qs[own, lanes], e.do[own, lanes]
            qh, doh = split(qp), split(dop)
            qq, dd = jnp.concatenate(qh, axis=0), jnp.concatenate(doh, axis=0)
            prod = (dop.astype(F32) * e.at[own, lanes].astype(F32)).T
            delta = [jnp.sum(prod[h * HEAD_DIM:(h + 1) * HEAD_DIM], axis=0, keepdims=True) for h in range(2)]
            logs = [e.lse[p, i * 2 + h:i * 2 + h + 1, :] for h in range(2)]

            def keys(j, dq, diagonal=False):
                at_keys = pl.ds(mult(j * qrows, qrows), qrows)
                kj, vj = e.ka[at_keys, lanes], e.va[at_keys, lanes]
                kt = kj.T
                probs, grads_s, new = [], [], []
                for h in range(2):
                    s = dot_nt(kj, qh[h])
                    if diagonal:
                        s = jnp.where(kpos <= qpos, s, NEG_BIG)
                    pt = jnp.exp(s - logs[h])
                    ds = (pt * (dot_nt(vj, doh[h]) - delta[h])).astype(BF)
                    probs.append(pt.astype(BF))
                    grads_s.append(ds)
                    new.append(dq[h] + dot_nn(kt[h * HEAD_DIM:(h + 1) * HEAD_DIM], ds))
                e.dva[at_keys, :] += dot_nn(jnp.concatenate(probs, axis=1), dd)
                e.dka[at_keys, :] += dot_nn(jnp.concatenate(grads_s, axis=1), qq)
                return tuple(new)

            none = jnp.zeros((HEAD_DIM, qrows), F32)
            dq = lax.fori_loop(0, quarter, keys, (none, none))
            dq = keys(quarter, dq, True)
            e.dm[own, lanes] = (jnp.concatenate(dq, axis=0).T * HEAD_DIM ** -0.5).astype(BF)
            for k in range(pairs):
                if f"a{k}{i}" in parts:
                    @pl.when(p == k)
                    def _(k=k, i=i):
                        after(f"a{k}{i}")

        for i in range(2):
            own = slice(i * qrows, (i + 1) * qrows)
            e.own_k[own, lanes] = e.dka[at_quarter(quarters[i]), :]
            e.own_v[own, lanes] = e.dva[at_quarter(quarters[i]), :]
            e.sk[own, lanes] = e.dka[at_quarter(theirs[i]), :].astype(BF)
            e.sv[own, lanes] = e.dva[at_quarter(theirs[i]), :].astype(BF)
        for k in range(pairs // 2):
            @pl.when(p == 2 * k + 1)
            def _(k=k):
                cut = slice(2 * k * 128, (2 * k + 2) * 128)
                for src, dst, s in ((e.sk, e.rk, 2), (e.sv, e.rv, 4)):
                    rcopy(
                        src.at[:, cut], dst.at[:, cut], e.msem.at[s], e.msem.at[s + 1], dev(z, y, 1 - c, x)
                    ).start()
        return carry

    lax.fori_loop(0, pairs, pair_body, 0)

    loads["xr"].wait()

    def norm_one(k, carry):
        at_rows = pl.ds(mult(k * lrows, lrows), lrows)
        n1, _ = norm_parts(e.xr[at_rows, :].astype(F32))
        e.a1[at_rows, :] = (n1 * e.vec[G1:G1 + 1, :] + e.vec[C1:C1 + 1, :]).astype(BF)
        return carry

    lax.fori_loop(0, rows // lrows, norm_one, 0)
    after("norm1")

    def qkv_grad(n, carry):
        cut = pl.ds(mult(n * tile, tile), tile)
        e.gq[cut, :] = dot_tn(e.dm[:, cut], e.a1[...]).astype(BF)
        return carry

    lax.fori_loop(0, 3, qkv_grad, 0)
    after("qa")
    wait_bytes(e.rk, e.msem.at[3])
    wait_bytes(e.rv, e.msem.at[5])
    for part, (mine, got) in enumerate(((e.own_k, e.rk), (e.own_v, e.rv))):
        def merge(k, carry, part=part, mine=mine, got=got):
            at_rows = pl.ds(mult(k * lrows, lrows), lrows)
            e.dm[at_rows, (part + 1) * width:(part + 2) * width] = (
                mine[at_rows, :] + got[at_rows, :].astype(F32)
            ).astype(BF)
            return carry

        lax.fori_loop(0, rows // lrows, merge, 0)
    after("merge")
    for name, first, stop in (("qb", 3, 5), ("qc", 5, 7), ("qd", 7, 9)):
        lax.fori_loop(first, stop, qkv_grad, 0)
        after(name)
    loads["wq"].wait()

    def input_back(n, carry):
        cut = pl.ds(mult(n * tile, tile), tile)
        e.d2[:, cut] = dot_nn(e.dm[...], e.wq[:, cut])
        return carry

    lax.fori_loop(0, steps, input_back, 0)
    after("da")

    def norm_one_back(k, sums):
        at_rows = pl.ds(mult(k * lrows, lrows), lrows)
        n1, rstd = norm_parts(e.xr[at_rows, :].astype(F32))
        da = e.d2[at_rows, :]
        ee = da * e.vec[G1:G1 + 1, :]
        m1 = jnp.mean(ee, axis=-1, keepdims=True)
        m2 = jnp.mean(ee * n1, axis=-1, keepdims=True)
        e.dx[at_rows, :] = (e.dr[at_rows, :] + (ee - m1 - n1 * m2) * rstd).astype(BF)
        return sums[0] + jnp.sum(da * n1, axis=0, keepdims=True), sums[1] + jnp.sum(da, axis=0, keepdims=True)

    sum_g1, sum_c1 = lax.fori_loop(0, rows // lrows, norm_one_back, (blank, blank))

    e.vs[0] = jnp.zeros_like(e.vs[0])
    for row, value in ((G1, sum_g1), (C1, sum_c1), (BP, sum_bp), (G2, sum_g2), (C2, sum_c2), (BD, total_bd)):
        e.vs[0, row:row + 1, :] = value
    per = width // tile
    for k in range(ff_tiles):
        e.vs[0, BU + k // per:BU + k // per + 1, (k % per) * tile:(k % per + 1) * tile] = e.bub[k]
    hops = (
        dev(z, y, 1 - c, x), dev(z, y, c, 1 - x), dev(z, 1 - y, c, x),
        dev(z + 1 - 2 * (z % 2), y, c, x), dev((z + 2) % 4, y, c, x),
    )

    def hop(k):
        rcopy(e.vs.at[k], e.vr.at[k], e.vsem.at[0, k], e.vsem.at[1, k], hops[k]).start()

    def land(k):
        wait_bytes(e.vr.at[k], e.vsem.at[1, k])
        e.vs[k + 1] = e.vs[k] + e.vr[k]

    hop(0)

    small = e.ret.shape[1]
    per_quarter = qrows // small
    slot = (z * Y + y) * C + x

    def give_back(k, carry):
        i = (k + x) % 2
        e8 = (k // 2 + d) % per_quarter
        td = ((i + c) % 2) * per_quarter + e8
        src = e.dx.at[pl.ds(mult(i * qrows + e8 * small, small), small)]
        mine = jnp.logical_and(td == d, x == i)

        @pl.when(mine)
        def _():
            lcopy(src, e.ret.at[slot], e.msem.at[7]).start()

        @pl.when(jnp.logical_not(mine))
        def _():
            rcopy(src, e.ret.at[slot], e.msem.at[6], e.msem.at[7], {"dp": td, "cp": i}).start()

        return carry

    share = per_quarter // 2

    def give(k):
        lax.fori_loop(k * share, (k + 1) * share, give_back, 0)

    after("ln")
    own = width // (Z * Y * C)
    e.osum[0:6, :] = pltpu.roll(e.vs[5, 0:6, :], (width - d * own) % width, 1)[:, :tile]
    long = ff // (Z * Y * C)
    per_row = width // long
    e.osum[6:7, :] = pltpu.roll(
        e.vs[5, pl.ds(BU + d // per_row, 1), :], (width - (d % per_row) * long) % width, 1
    )[:, :tile]
    e.osum[7:8, :] = jnp.zeros((1, tile), F32)
    wait_bytes(e.dx, e.msem.at[7])

    for ch in chunks:
        ch.drain()
    for k in range(5):
        wait_bytes(e.vr.at[k], e.vsem.at[0, k])
    wait_bytes(e.rk, e.msem.at[2])
    wait_bytes(e.rv, e.msem.at[4])

    @pl.when((x + c) % 2 == d // per_quarter)
    def _():
        wait_bytes(e.dx.at[pl.ds(0, rows - small)], e.msem.at[6])

    @pl.when((x + c) % 2 != d // per_quarter)
    def _():
        wait_bytes(e.dx, e.msem.at[6])

    @pl.when(c == x)
    def _():
        wait_bytes(e.dx.at[pl.ds(0, qrows)], e.msem.at[0])

    @pl.when(c != x)
    def _():
        wait_bytes(e.dx, e.msem.at[0])

    wait_bytes(e.dx, e.msem.at[1])


def backward(lengths, dealing, saved, shards):
    wq, wp, wu, wd, xr, gw, qs, ka, va, at, lse, r, a2, hd, gp, vec, outw = saved
    rows, width = xr.shape
    ff = hd.shape[1]
    n = Z * Y * C
    keys = ka.shape[0]
    small = rows // n
    pairs = width // 128

    def arr(shape, dtype=BF):
        return jax.ShapeDtypeStruct(shape, dtype)

    outs = [arr(s.shape, F32) for s in shards] + [
        arr((8, 256), F32), arr((n, small, width)), arr((rows, width)),
    ]
    vm = pltpu.VMEM
    acts = vm((rows, width), BF)
    acts32 = vm((rows, width), F32)
    scratch = [
        vm(wq.shape, BF), vm(wp.shape, BF), acts, acts, acts, vm(ka.shape, BF), vm(va.shape, BF), acts,
        vm(lse.shape, F32), acts32, acts, vm(vec.shape, F32), vm((width, rows), BF), acts32, acts32, acts, acts,
        vm(wq.shape, BF), vm(wp.shape, BF), vm(wu.shape, BF), vm(wd.shape, BF),
        vm((2, width, 256), BF), vm((2, 256, width), BF), vm((2, rows, 256), BF), vm((2, rows, 256), BF),
        vm((keys, 128), F32), vm((keys, 128), F32),
        acts32, acts, acts, acts, vm((rows, 3 * width), BF),
        vm((6, 16, width), F32), vm((5, 16, width), F32), vm((ff // 256, 1, 256), F32),
        pltpu.SemaphoreType.DMA((12,)), pltpu.SemaphoreType.DMA((4, 2)), pltpu.SemaphoreType.DMA((13, 10)),
        pltpu.SemaphoreType.DMA((8,)), pltpu.SemaphoreType.DMA((2, 5)),
    ]
    for kind, (_, R, _, _, cn, zlist, _) in zip(KINDS_BACK, reduce_shapes(width, ff)):
        k = len(zlist)
        last = (1, 4, 2) if kind == 2 else (k, 2, 1)
        scratch += [vm((2 * k, 2, R, cn), BF)] + [vm((m, R, cn), BF) for m in (2 * k,) + last]
    anyspec = pl.BlockSpec(memory_space=pl.ANY)
    smem = pl.BlockSpec(memory_space=pltpu.SMEM)
    vmem = pl.BlockSpec(memory_space=pltpu.VMEM)
    return pl.pallas_call(
        backward_kernel,
        out_shape=outs,
        in_specs=[smem, smem] + [anyspec] * len(saved),
        out_specs=[vmem] * 5 + [anyspec] * 2,
        scratch_shapes=scratch,
        compiler_params=pltpu.CompilerParams(
            collective_id=1, has_side_effects=True, vmem_limit_bytes=67043328
        ),
        name="backward",
    )(lengths, dealing, *saved)


def finish_kernel(deal_ref, gq, gp, gu, gd, sums, ret, out, grad_o, out_o, gq_o, gp_o, gu_o, gd_o, *rows_o):
    for s in range(ret.shape[0]):
        grad_o[s] = ret[deal_ref[s]]
    for src, dst in ((out, out_o), (gq, gq_o), (gp, gp_o), (gu, gu_o), (gd, gd_o)):
        dst[...] = src[...]
    for k, row in enumerate(rows_o):
        row[...] = sums[k:k + 1, :row.shape[1]]


def finish(dealing, grads, sums, ret, out, own, long):
    def like(a):
        return jax.ShapeDtypeStruct(a.shape, a.dtype)

    outs = [like(ret), like(out)] + [like(g) for g in grads]
    outs += [jax.ShapeDtypeStruct((1, own), F32)] * 6 + [jax.ShapeDtypeStruct((1, long), F32)]
    vmem = pl.BlockSpec(memory_space=pltpu.VMEM)
    return pl.pallas_call(
        finish_kernel,
        out_shape=outs,
        in_specs=[pl.BlockSpec(memory_space=pltpu.SMEM)] + [vmem] * 7,
        out_specs=[vmem] * len(outs),
        name="finish",
    )(dealing, *grads, sums, ret, out)


def slice_plan(
    x_source, cotangent, lengths, dealing, qkv_weight, proj_weight, up_weight, down_weight,
    first_gain, first_shift, proj_bias, second_gain, second_shift, up_bias, down_bias,
):
    shards = [w.T for w in (qkv_weight, proj_weight, up_weight, down_weight)]
    vectors = [
        v[None] for v in (first_gain, first_shift, proj_bias, second_gain, second_shift, down_bias, up_bias)
    ]
    saved = forward(lengths, dealing, cotangent[0], x_source, shards, vectors)
    gq, gp, gu, gd, sums, ret, out = backward(lengths, dealing, saved, shards)
    done = finish(dealing, (gq, gp, gu, gd), sums, ret, out, first_gain.shape[0], up_bias.shape[0])
    input_grad, output, gq, gp, gu, gd = done[:6]
    by_row = [v.reshape(-1) for v in done[6:]]
    return (
        output[None], input_grad, gq.T, gp.T, gu.T, gd.T,
        by_row[G1], by_row[C1], by_row[BP], by_row[G2], by_row[C2], by_row[6], by_row[BD],
    )


def layer_norm(values, scaling, offset):
    centered = values - jnp.mean(values, axis=-1, keepdims=True)
    spread = jnp.mean(centered * centered, axis=-1, keepdims=True)
    return centered * lax.rsqrt(spread + EPSILON) * scaling + offset


def gelu_tanh(values):
    return (
        0.5
        * values
        * (1.0 + jnp.tanh(TANH_SCALE * (values + CUBIC_TERM * values * values * values)))
    )


def grouped(array, block_seqs):
    return array.reshape(
        (array.shape[0] // block_seqs, block_seqs, array.shape[1], HEADS, array.shape[2] // HEADS)
    )


def grouped_stats(array, block_seqs):
    return array.reshape((array.shape[0] // block_seqs, block_seqs) + array.shape[1:])


def joined(array):
    return array.reshape(
        (array.shape[0] * array.shape[1], array.shape[2], array.shape[3] * array.shape[4])
    )


def masked_scores(queries, key_rows, query_start, score_scale):
    scores = (
        jnp.einsum("bqhd,bkhd->bhqk", queries, key_rows, preferred_element_type=jnp.float32)
        * score_scale
    )
    query_pos = query_start + jnp.arange(queries.shape[1])
    key_pos = jnp.arange(key_rows.shape[1])
    return jnp.where(key_pos[None, :] <= query_pos[:, None], scores, NEG_BIG)


def attend(inputs, query_start, score_scale):
    queries, key_rows, val_rows = inputs
    scores = masked_scores(queries, key_rows, query_start, score_scale)
    row_top = jnp.max(scores, axis=-1, keepdims=True)
    exponent = jnp.exp(scores - row_top)
    totals = jnp.sum(exponent, axis=-1, keepdims=True)
    weights = (exponent / totals).astype(jnp.bfloat16)
    attended = jnp.einsum("bhqk,bkhd->bqhd", weights, val_rows, preferred_element_type=jnp.float32)
    return (attended.astype(jnp.bfloat16), (row_top + jnp.log(totals))[..., 0])


def rows_back(inputs, query_start, score_scale):
    queries, key_rows, val_rows, grad_rows, log_total = inputs
    scores = masked_scores(queries, key_rows, query_start, score_scale)
    weights = jnp.exp(scores - log_total[..., None])
    grad_weights = jnp.einsum(
        "bqhd,bkhd->bhqk", grad_rows, val_rows, preferred_element_type=jnp.float32
    )
    delta_rows = jnp.sum(weights * grad_weights, axis=-1)
    grad_scores = (weights * (grad_weights - delta_rows[..., None])).astype(jnp.bfloat16)
    grad_query = (
        jnp.einsum("bhqk,bkhd->bqhd", grad_scores, key_rows, preferred_element_type=jnp.float32)
        * score_scale
    )
    grad_keys = (
        jnp.einsum("bhqk,bqhd->bkhd", grad_scores, queries, preferred_element_type=jnp.float32)
        * score_scale
    )
    grad_vals = jnp.einsum(
        "bhqk,bqhd->bkhd",
        weights.astype(jnp.bfloat16),
        grad_rows,
        preferred_element_type=jnp.float32,
    )
    return (grad_query, grad_keys, grad_vals)


def fetch_weights(
    qkv_weight,
    proj_weight,
    up_weight,
    down_weight,
    first_gain,
    first_shift,
    proj_bias,
    second_gain,
    second_shift,
    up_bias,
    down_bias,
):
    qkv_part, proj_part, up_part, down_part = (
        lax.all_gather(qkv_weight.astype(jnp.bfloat16), "cp", axis=0, tiled=True),
        lax.all_gather(proj_weight.astype(jnp.bfloat16), "cp", axis=0, tiled=True),
        lax.all_gather(up_weight.astype(jnp.bfloat16), "cp", axis=0, tiled=True),
        lax.all_gather(down_weight.astype(jnp.bfloat16), "cp", axis=0, tiled=True),
    )
    return (
        lax.all_gather(qkv_part, "dp", axis=1, tiled=True),
        lax.all_gather(proj_part, "dp", axis=1, tiled=True),
        lax.all_gather(up_part, "dp", axis=1, tiled=True),
        lax.all_gather(down_part, "dp", axis=1, tiled=True),
        lax.all_gather(first_gain.astype(jnp.bfloat16), "dp", axis=0, tiled=True),
        lax.all_gather(first_shift.astype(jnp.bfloat16), "dp", axis=0, tiled=True),
        lax.all_gather(proj_bias.astype(jnp.bfloat16), "dp", axis=0, tiled=True),
        lax.all_gather(second_gain.astype(jnp.bfloat16), "dp", axis=0, tiled=True),
        lax.all_gather(second_shift.astype(jnp.bfloat16), "dp", axis=0, tiled=True),
        lax.all_gather(up_bias.astype(jnp.bfloat16), "dp", axis=0, tiled=True),
        lax.all_gather(down_bias.astype(jnp.bfloat16), "dp", axis=0, tiled=True),
    )


def mat_rows(left, right):
    return jnp.einsum("sqd,de->sqe", left, right, preferred_element_type=jnp.float32)


def mat_back(left, right):
    return jnp.einsum("sqe,de->sqd", left, right, preferred_element_type=jnp.float32)


def mat_grad(left, right):
    return jnp.einsum("sqd,sqe->de", left, right, preferred_element_type=jnp.float32)


def general(
    x_source,
    cotangent,
    lengths,
    dealing,
    qkv_weight,
    proj_weight,
    up_weight,
    down_weight,
    first_gain,
    first_shift,
    proj_bias,
    second_gain,
    second_shift,
    up_bias,
    down_bias,
):
    groups = lax.axis_size("dp")
    seqs_all, piece_rows, features = x_source.shape
    seq_group = seqs_all // groups
    span_rows = groups * piece_rows
    score_scale = HEAD_DIM ** (-0.5)
    block_seqs = math.gcd(seq_group, max(1, 512 // span_rows))
    owners = jnp.argsort(dealing)
    send_order = owners.reshape(groups, seq_group).T.reshape(-1)
    outgoing = x_source[send_order].reshape(seq_group, span_rows, features)
    arrived = lax.all_to_all(outgoing, "dp", split_axis=1, concat_axis=1, tiled=True)
    first_slot = lax.axis_index("dp") * seq_group
    my_lengths = lax.dynamic_slice_in_dim(lengths[owners], first_slot, seq_group)
    query_start = lax.axis_index("cp") * span_rows
    positions = query_start + jnp.arange(span_rows)
    live_rows = positions[None, :] < my_lengths[:, None]
    fetched = fetch_weights(
        qkv_weight,
        proj_weight,
        up_weight,
        down_weight,
        first_gain,
        first_shift,
        proj_bias,
        second_gain,
        second_shift,
        up_bias,
        down_bias,
    )
    qkv_full, proj_full, up_full, down_full = (fetched[0], fetched[1], fetched[2], fetched[3])
    gain_one, shift_one, bias_proj, gain_two, shift_two, bias_up, bias_down = [
        vector.astype(jnp.float32) for vector in fetched[4:]
    ]
    inputs_f = arrived.astype(jnp.float32)
    norm_one, back_one = jax.vjp(layer_norm, inputs_f, gain_one, shift_one)
    act_one = norm_one.astype(jnp.bfloat16)
    mixed_rows = mat_rows(act_one, qkv_full).astype(jnp.bfloat16)
    queries = mixed_rows[..., :features]
    kv_local = mixed_rows[..., features:]
    kv_all = lax.all_gather(kv_local, "cp", axis=1, tiled=True)
    attended, log_total = lax.map(
        lambda inputs: attend(inputs, query_start, score_scale),
        (
            grouped(queries, block_seqs),
            grouped(kv_all[..., :features], block_seqs),
            grouped(kv_all[..., features:], block_seqs),
        ),
    )
    attended = joined(attended)
    log_total = log_total.reshape((seq_group,) + log_total.shape[2:])
    residual = inputs_f + mat_rows(attended, proj_full) + bias_proj
    norm_two, back_two = jax.vjp(layer_norm, residual, gain_two, shift_two)
    act_two = norm_two.astype(jnp.bfloat16)
    up_raw = mat_rows(act_two, up_full) + bias_up
    hidden, back_gelu = jax.vjp(gelu_tanh, up_raw)
    hid_low = hidden.astype(jnp.bfloat16)
    result = residual + mat_rows(hid_low, down_full) + bias_down
    output = jnp.where(live_rows[..., None], result, 0.0).astype(jnp.bfloat16)
    fetched = fetch_weights(
        qkv_weight,
        proj_weight,
        up_weight,
        down_weight,
        first_gain,
        first_shift,
        proj_bias,
        second_gain,
        second_shift,
        up_bias,
        down_bias,
    )
    qkv_full, proj_full, up_full, down_full = (fetched[0], fetched[1], fetched[2], fetched[3])
    gain_one, gain_two = (fetched[4].astype(jnp.float32), fetched[7].astype(jnp.float32))
    grad_out = jnp.where(live_rows[..., None], cotangent.astype(jnp.float32), 0.0)
    grad_low = grad_out.astype(jnp.bfloat16)
    grad_down = mat_grad(hid_low, grad_low)
    grad_bias_down = jnp.sum(grad_out, axis=(0, 1))
    grad_hidden = mat_back(grad_low, down_full)
    grad_up_raw = back_gelu(grad_hidden)[0].astype(jnp.bfloat16)
    grad_up = mat_grad(act_two, grad_up_raw)
    grad_bias_up = jnp.sum(grad_up_raw.astype(jnp.float32), axis=(0, 1))
    grad_act_two = mat_back(grad_up_raw, up_full)
    grad_resid, grad_gain_two, grad_shift_two = back_two(grad_act_two)
    grad_resid = grad_resid + grad_out
    grad_bias_proj = jnp.sum(grad_resid, axis=(0, 1))
    resid_low = grad_resid.astype(jnp.bfloat16)
    grad_proj = mat_grad(attended, resid_low)
    grad_attended = mat_back(resid_low, proj_full).astype(jnp.bfloat16)
    kv_back = lax.all_gather(kv_local, "cp", axis=1, tiled=True)
    key_rows = kv_back[..., :features]
    val_rows = kv_back[..., features:]
    grad_query, grad_keys, grad_vals = lax.map(
        lambda inputs: rows_back(inputs, query_start, score_scale),
        (
            grouped(queries, block_seqs),
            grouped(key_rows, block_seqs),
            grouped(val_rows, block_seqs),
            grouped(grad_attended, block_seqs),
            grouped_stats(log_total, block_seqs),
        ),
    )
    grad_keys, grad_vals = (
        lax.psum_scatter(
            joined(grad_keys).astype(jnp.bfloat16), "cp", scatter_dimension=1, tiled=True
        ).astype(jnp.float32),
        lax.psum_scatter(
            joined(grad_vals).astype(jnp.bfloat16), "cp", scatter_dimension=1, tiled=True
        ).astype(jnp.float32),
    )
    grad_mixed = jnp.concatenate([joined(grad_query), grad_keys, grad_vals], axis=-1).astype(
        jnp.bfloat16
    )
    grad_qkv = mat_grad(act_one, grad_mixed)
    grad_act_one = mat_back(grad_mixed, qkv_full)
    grad_input, grad_gain_one, grad_shift_one = back_one(grad_act_one)
    grad_input = (grad_input + grad_resid).astype(jnp.bfloat16)
    returned = lax.all_to_all(grad_input, "dp", split_axis=1, concat_axis=0, tiled=True)
    input_grad = returned[dealing]
    (
        grad_qkv,
        grad_proj,
        grad_up,
        grad_down,
        grad_gain_one,
        grad_shift_one,
        grad_bias_proj,
        grad_gain_two,
        grad_shift_two,
        grad_bias_up,
        grad_bias_down,
    ) = (
        lax.psum_scatter(
            grad_qkv.astype(jnp.bfloat16), "dp", scatter_dimension=1, tiled=True
        ).astype(jnp.float32),
        lax.psum_scatter(
            grad_proj.astype(jnp.bfloat16), "dp", scatter_dimension=1, tiled=True
        ).astype(jnp.float32),
        lax.psum_scatter(
            grad_up.astype(jnp.bfloat16), "dp", scatter_dimension=1, tiled=True
        ).astype(jnp.float32),
        lax.psum_scatter(
            grad_down.astype(jnp.bfloat16), "dp", scatter_dimension=1, tiled=True
        ).astype(jnp.float32),
        lax.psum_scatter(
            grad_gain_one.astype(jnp.bfloat16), "dp", scatter_dimension=0, tiled=True
        ).astype(jnp.float32),
        lax.psum_scatter(
            grad_shift_one.astype(jnp.bfloat16), "dp", scatter_dimension=0, tiled=True
        ).astype(jnp.float32),
        lax.psum_scatter(
            grad_bias_proj.astype(jnp.bfloat16), "dp", scatter_dimension=0, tiled=True
        ).astype(jnp.float32),
        lax.psum_scatter(
            grad_gain_two.astype(jnp.bfloat16), "dp", scatter_dimension=0, tiled=True
        ).astype(jnp.float32),
        lax.psum_scatter(
            grad_shift_two.astype(jnp.bfloat16), "dp", scatter_dimension=0, tiled=True
        ).astype(jnp.float32),
        lax.psum_scatter(
            grad_bias_up.astype(jnp.bfloat16), "dp", scatter_dimension=0, tiled=True
        ).astype(jnp.float32),
        lax.psum_scatter(
            grad_bias_down.astype(jnp.bfloat16), "dp", scatter_dimension=0, tiled=True
        ).astype(jnp.float32),
    )
    grad_qkv, grad_proj, grad_up, grad_down = (
        lax.psum_scatter(
            grad_qkv.astype(jnp.bfloat16), "cp", scatter_dimension=0, tiled=True
        ).astype(jnp.float32),
        lax.psum_scatter(
            grad_proj.astype(jnp.bfloat16), "cp", scatter_dimension=0, tiled=True
        ).astype(jnp.float32),
        lax.psum_scatter(
            grad_up.astype(jnp.bfloat16), "cp", scatter_dimension=0, tiled=True
        ).astype(jnp.float32),
        lax.psum_scatter(
            grad_down.astype(jnp.bfloat16), "cp", scatter_dimension=0, tiled=True
        ).astype(jnp.float32),
    )
    (
        grad_gain_one,
        grad_shift_one,
        grad_bias_proj,
        grad_gain_two,
        grad_shift_two,
        grad_bias_up,
        grad_bias_down,
    ) = lax.psum(
        (
            grad_gain_one,
            grad_shift_one,
            grad_bias_proj,
            grad_gain_two,
            grad_shift_two,
            grad_bias_up,
            grad_bias_down,
        ),
        "cp",
    )
    return (
        output,
        input_grad,
        grad_qkv,
        grad_proj,
        grad_up,
        grad_down,
        grad_gain_one,
        grad_shift_one,
        grad_bias_proj,
        grad_gain_two,
        grad_shift_two,
        grad_bias_up,
        grad_bias_down,
    )


def solution(mesh):
    in_specs = (
        P(None, ("cp", "dp"), None),
        P("dp", "cp", None),
        P(),
        P(),
        P("cp", "dp"),
        P("cp", "dp"),
        P("cp", "dp"),
        P("cp", "dp"),
        P("dp"),
        P("dp"),
        P("dp"),
        P("dp"),
        P("dp"),
        P("dp"),
        P("dp"),
    )
    out_specs = (
        P("dp", "cp", None),
        P(None, ("cp", "dp"), None),
        P("cp", "dp"),
        P("cp", "dp"),
        P("cp", "dp"),
        P("cp", "dp"),
        P("dp"),
        P("dp"),
        P("dp"),
        P("dp"),
        P("dp"),
        P("dp"),
        P("dp"),
    )
    planned = tuple(mesh.shape.items()) == (("dp", Z * Y * C), ("cp", X))
    local = slice_plan if planned else general
    return jax.shard_map(local, mesh=mesh, in_specs=in_specs, out_specs=out_specs, check_vma=False)
```

```python
import functools
import math

import jax
import jax.numpy as jnp
from jax import lax
from jax.experimental import pallas as pl
from jax.experimental.pallas import tpu as pltpu
from jax.sharding import PartitionSpec as P

HEADS = 12
HEAD_DIM = 64


EPSILON = 1e-05
NEG_BIG = -1e30
TANH_SCALE = 0.7978845608028654
CUBIC_TERM = 0.044715
MESH_IDS = pl.DeviceIdType.MESH
BF = jnp.bfloat16
F32 = jnp.float32

Z, Y, C, X = 4, 2, 2, 2


def mult(value, n):
    return value if isinstance(value, int) else pl.multiple_of(value, n)


def coords():
    d = lax.axis_index("dp")
    x = lax.axis_index("cp")
    return d // (Y * C), (d // C) % Y, d % C, x, d


def dev(z, y, c, x):
    return {"dp": (z * Y + y) * C + c, "cp": x}


def rcopy(src, dst, ssem, rsem, where):
    return pltpu.make_async_remote_copy(
        src_ref=src, dst_ref=dst, send_sem=ssem, recv_sem=rsem, device_id=where, device_id_type=MESH_IDS
    )


def lcopy(src, dst, sem):
    return pltpu.make_async_copy(src, dst, sem)


def wait_bytes(ref, sem):
    pltpu.make_async_copy(ref, ref, sem).wait()


def enter(everyone):
    d = lax.axis_index("dp")
    x = lax.axis_index("cp")
    barrier = pltpu.get_barrier_semaphore()

    def greet(k, carry):
        kd = k // X
        kx = k % X

        @pl.when(jnp.logical_or(kd != d, kx != x))
        def _():
            pl.semaphore_signal(barrier, inc=1, device_id={"dp": kd, "cp": kx}, device_id_type=MESH_IDS)

        return carry

    lax.fori_loop(0, everyone, greet, 0)

    def entered():
        pl.semaphore_wait(barrier, everyone - 1)

    return entered


def dot_nn(a, b):
    return lax.dot_general(a, b, (((1,), (0,)), ((), ())), preferred_element_type=F32)


def dot_nt(a, b):
    return lax.dot_general(a, b, (((1,), (1,)), ((), ())), preferred_element_type=F32)


def dot_tn(a, b):
    return lax.dot_general(a, b, (((0,), (0,)), ((), ())), preferred_element_type=F32)


def norm_parts(v):
    mean = jnp.mean(v, axis=-1, keepdims=True)
    cen = v - mean
    var = jnp.mean(cen * cen, axis=-1, keepdims=True)
    rstd = lax.rsqrt(var + EPSILON)
    return cen * rstd, rstd


def live_length(len_ref, deal_ref, slot):
    total = jnp.int32(0)
    for s in range(len_ref.shape[0]):
        total = total + jnp.where(deal_ref[s] == slot, len_ref[s], 0)
    return total


class Piece:
    def __init__(self, full, R, r0, rn, step, c0, cn):
        self.full = full
        self.R, self.r0, self.rn, self.step, self.c0, self.cn = R, r0, rn, step, c0, cn

    def at(self, z, y, c, x):
        d = (z * Y + y) * C + c
        return self.full.at[
            pl.ds(mult(d * self.R + self.r0, 16), self.rn), pl.ds(mult(x * self.step + self.c0, 128), self.cn)
        ]


class Gather:
    FAR, MATE, A, B, CORE = range(5)

    def __init__(self, piece, sems, k, dummy, where, kind, turned):
        self.p, self.sems, self.k, self.dummy, self.kind = piece, sems, k, dummy, kind
        z, y, c, x, _ = where
        self.z, self.y, self.c, self.x = z, y, c, x
        o = 1 if turned else c
        self.far, self.mate = 3 - z, z + 1 - 2 * (z % 2)
        self.ya, self.xa = (y + 1 - o) % 2, (x + o) % 2
        self.yb, self.xb = (y + o) % 2, (x + 1 - o) % 2
        self.to = {
            self.FAR: dev(self.far, y, c, x), self.MATE: dev(self.mate, y, c, x), self.A: dev(z, self.ya, c, self.xa),
            self.B: dev(z, self.yb, c, self.xb), self.CORE: dev(z, y, 1 - c, x),
        }
        self.counts = {self.FAR: 1, self.MATE: 2, self.A: 4} if kind == 1 else {self.FAR: 2, self.MATE: 4, self.A: 1}
        self.counts.update({self.B: 8, self.CORE: 16})

    def send(self, pieces, *ways):
        for way in ways:
            for z, y, x in pieces:
                q = self.p.at(z, y, self.c, x)
                rcopy(q, q, self.sems.at[self.k, 0, way], self.sems.at[self.k, 1, way], self.to[way]).start()

    def wait(self, way, side=1):
        p = self.p
        wait_bytes(self.dummy.at[pl.ds(0, self.counts[way] * p.rn), pl.ds(0, p.cn)], self.sems.at[self.k, side, way])

    def start(self):
        own = [(self.z, self.y, self.x)]
        if self.kind == 1:
            self.send(own, self.FAR, self.MATE, self.A, self.B, self.CORE)
        else:
            self.send(own, self.A, self.FAR, self.MATE, self.B, self.CORE)

    def tick1(self):
        if self.kind == 1:
            self.wait(self.FAR)
            self.send([(self.far, self.y, self.x)], self.MATE, self.A, self.B, self.CORE)
        else:
            self.wait(self.A)
            self.send([(self.z, self.ya, self.xa)], self.FAR, self.MATE, self.B, self.CORE)

    def tick2(self):
        if self.kind == 1:
            self.wait(self.MATE)
            self.send([(self.mate, self.y, self.x), (3 - self.mate, self.y, self.x)], self.A, self.B, self.CORE)
        else:
            self.wait(self.FAR)
            self.send([(self.far, self.y, self.x), (self.far, self.ya, self.xa)], self.MATE, self.B, self.CORE)

    def tick3(self):
        if self.kind == 1:
            self.wait(self.A)
            self.send([(k, self.ya, self.xa) for k in range(Z)], self.B, self.CORE)
        else:
            self.wait(self.MATE)
            self.send(
                [(k, y, x) for k in (self.mate, 3 - self.mate) for y, x in ((self.y, self.x), (self.ya, self.xa))],
                self.B, self.CORE,
            )

    def tick4(self):
        self.wait(self.B)
        self.send(
            [(k, y, x) for k in range(Z) for y, x in ((self.yb, self.xb), (1 - self.y, 1 - self.x))], self.CORE
        )

    def tick5(self):
        self.wait(self.CORE)

    def drain(self):
        for way in range(5):
            self.wait(way, 0)


class Vectors:
    FAR, MATE, A, CORE = range(4)

    def __init__(self, full, sems, where):
        self.full, self.sems = full, sems
        z, y, c, x, _ = where
        self.z, self.y, self.c = z, y, c
        self.far, self.mate = 3 - z, z + 1 - 2 * (z % 2)
        self.to = (dev(self.far, y, c, x), dev(self.mate, y, c, x), dev(z, 1 - y, c, x), dev(z, y, 1 - c, x))
        self.counts = (1, 2, 4, 8)

    def send(self, pieces, *ways):
        for way in ways:
            for z, y in pieces:
                q = self.full.at[(z * Y + y) * C + self.c]
                rcopy(q, q, self.sems.at[0, way], self.sems.at[1, way], self.to[way]).start()

    def wait(self, way, side=1):
        wait_bytes(self.full.at[pl.ds(0, self.counts[way])], self.sems.at[side, way])

    def start(self):
        self.send([(self.z, self.y)], self.FAR, self.MATE, self.A, self.CORE)

    def tick1(self):
        self.wait(self.FAR)
        self.send([(self.far, self.y)], self.MATE, self.A, self.CORE)

    def tick2(self):
        self.wait(self.MATE)
        self.send([(self.mate, self.y), (3 - self.mate, self.y)], self.A, self.CORE)

    def tick3(self):
        self.wait(self.A)
        self.send([(k, 1 - self.y) for k in range(Z)], self.CORE)

    def tick4(self):
        self.wait(self.CORE)

    def drain(self):
        for way in range(4):
            self.wait(way, 0)


G1, C1, BP, G2, C2, BD, BU = range(7)


def gather_chunks(wq, wp, wu, wd):
    rq, rp, ru, rd = (w.shape[0] // (Z * Y * C) for w in (wq, wp, wu, wd))
    half, wide = wq.shape[1] // X, wd.shape[1] // X
    out = []
    for k in range(3):
        out.append(Piece(wq, rq, k * (rq // 3), rq // 3, half, 0, half))
    out.append(Piece(wp, rp, 0, rp, half, 0, half))
    for k in range(4):
        out.append(Piece(wu, ru, k * (ru // 4), ru // 4, half, 0, half))
    for k in range(4):
        out.append(Piece(wd, rd, 0, rd, wide, k * (wide // 4), wide // 4))
    return out


def one_hot(count, width, first):
    at_row = lax.broadcasted_iota(jnp.int32, (count, width), 0)
    at_col = lax.broadcasted_iota(jnp.int32, (count, width), 1)
    return (at_col == at_row + first).astype(BF)


N_GATHER = 12
TICKS = ("tick1", "tick2", "tick3", "tick4")
KINDS = (1, 1, 1, 1, 2, 2, 1, 2, 2, 1, 2, 2)
TURNED = (7,)
COT_STEPS = (6, 6, 6, 6, 8, 8, 8, 8)
LAGS = ((0, 1, 2, 3),) * 4 + ((0, 1, 2, 4),) * 8


def forward_kernel(
    len_ref, deal_ref, cot, x_any, sq_any, sp_any, su_any, sd_any, g1_any, c1_any, bp_any, g2_any, c2_any, bd_any, bu_any,
    wq_o, wp_o, wu_o, wd_o, xr_o, gw_o, qs_o, ka_o, va_o, at_o, lse_o, r_o, a2_o, hd_o, gp_o, vec_o, out_o,
    wq, wp, wu, wd, xr, a1, qs, ka, va, at, lse, r, a2, hd, gp, vg, vec, bu3, sc0, sc1, outw, xg, acc,
    x_in, sq, sp, su, sd, v_g1, v_c1, v_bp, v_g2, v_c2, v_bd, v_bu,
    gsem, vsem, msem, osem, isem,
):
    where = coords()
    z, y, c, x, d = where
    width = xr.shape[1]
    rows = xr.shape[0]
    qrows = rows // 2
    small = x_in.shape[1]
    sources = (sq_any, sp_any, su_any, sd_any, g1_any, c1_any, bp_any, g2_any, c2_any, bd_any, bu_any, x_any)
    places = (sq, sp, su, sd, v_g1, v_c1, v_bp, v_g2, v_c2, v_bd, v_bu, x_in)
    loads = [pltpu.make_async_copy(s, t, isem.at[k]) for k, (s, t) in enumerate(zip(sources, places))]
    for load in loads:
        load.start()
    pairs = width // 128
    tile = 256

    entered = enter(Z * Y * C * X)

    n = Z * Y * C
    for load, shard, full in zip(loads, (sq, sp, su, sd), (wq, wp, wu, wd)):
        load.wait()
        own, long = shard.shape
        full[pl.ds(mult(d * own, 16), own), pl.ds(mult(x * long, 128), long)] = shard[...].astype(BF)
    for load in loads[4:]:
        load.wait()
    vg[d] = jnp.zeros(vg.shape[1:], BF)
    own = v_g1.shape[1]
    seven = jnp.concatenate([v[...] for v in (v_g1, v_c1, v_bp, v_g2, v_c2, v_bd)], axis=0).astype(BF)
    placed = dot_nn(seven, one_hot(own, width, d * own))
    long = v_bu.shape[1]
    per_row = width // long
    placed_long = dot_nn(v_bu[...].astype(BF), one_hot(long, width, (d % per_row) * long))
    rows_long = [jnp.where(d // per_row == k, placed_long, 0.0) for k in range(n // per_row)]
    rest = jnp.zeros((16 - 6 - n // per_row, width), F32)
    vg[d] = jnp.concatenate([placed] + rows_long + [rest], axis=0).astype(BF)
    slots = x_in.shape[0]
    for t in range(slots):
        owner = jnp.int32(0)
        for s in range(slots):
            owner = jnp.where(deal_ref[s] == t, s, owner)
        xg[t] = x_in[owner]

    entered()

    vectors = Vectors(vg, vsem, where)
    vectors.start()
    chunks = [
        Gather(p, gsem, k, wu, where, KINDS[k], k in TURNED) for k, p in enumerate(gather_chunks(wq, wp, wu, wd))
    ]

    def send_cot(k):
        b, part = k // 4, k % 4
        some = qrows // 4
        core_b = (x + b) % 2
        src_b = cot.at[pl.ds(b * qrows + part * some, some)]
        dst_b = gw_o.at[pl.ds(mult(x * qrows + part * some, some), some)]
        same = jnp.logical_and(core_b == c, c == x)

        @pl.when(same)
        def _():
            lcopy(src_b, dst_b, msem.at[3]).start()

        @pl.when(jnp.logical_not(same))
        def _():
            rcopy(src_b, dst_b, msem.at[2], msem.at[3], dev(z, y, core_b, c)).start()

    per_quarter = qrows // small
    place = mult(x * qrows + (d % per_quarter) * small, 16)
    core_to = (x + d // per_quarter) % 2
    dst = xr.at[pl.ds(place, small)]

    def deal_out(k, carry):
        t = (d + k + x * (slots // 2)) % slots
        td = (t // 2) * 2 + core_to
        tx = t % 2
        mine = jnp.logical_and(td == d, tx == x)

        @pl.when(mine)
        def _():
            lcopy(xg.at[t], dst, msem.at[1]).start()

        @pl.when(jnp.logical_not(mine))
        def _():
            rcopy(xg.at[t], dst, msem.at[0], msem.at[1], {"dp": td, "cp": tx}).start()

        return carry

    ahead = 2
    for ch in chunks[:ahead]:
        ch.start()

    def step(s):
        if s + ahead < len(chunks):
            chunks[s + ahead].start()
        if s < 4:
            lax.fori_loop(s * slots // 4, (s + 1) * slots // 4, deal_out, 0)
        for k, at_step in enumerate(COT_STEPS):
            if at_step == s:
                send_cot(k)
        for n in range(4):
            for k in range(len(chunks)):
                if k + LAGS[k][n] == s:
                    getattr(chunks[k], TICKS[n])()

    step(0)
    vectors.tick1()
    step(1)
    vectors.tick2()
    step(2)
    vectors.tick3()
    step(3)
    vectors.tick4()

    def add_table(k, acc):
        return acc + vg[k].astype(F32)

    vec[...] = lax.fori_loop(1, Z * Y * C, add_table, vg[0].astype(F32))
    for k in range(bu3.shape[0]):
        per = width // tile
        bu3[k] = vec[BU + k // per:BU + k // per + 1, (k % per) * tile:(k % per + 1) * tile]

    wait_bytes(xr, msem.at[1])
    lrows = 128

    def first_norm(k, carry):
        at_rows = pl.ds(mult(k * lrows, lrows), lrows)
        n1, _ = norm_parts(xr[at_rows, :].astype(F32))
        a1[at_rows, :] = (n1 * vec[G1:G1 + 1, :] + vec[C1:C1 + 1, :]).astype(BF)
        return carry

    lax.fori_loop(0, rows // lrows, first_norm, 0)

    step(4)
    step(5)
    for k in range(3):
        chunks[k].tick5()
    keep = [pltpu.make_async_copy(wq, wq_o, osem.at[0])]
    keep[-1].start()

    quarters = (c, 3 - c)

    def q_at(i):
        return pl.ds(mult(quarters[i] * qrows, qrows), qrows)

    steps = width // tile
    for part in range(3):
        def project(n, carry, part=part):
            lanes = pl.ds(mult(n * tile, tile), tile)
            res = dot_nt(a1[...], wq[pl.ds(mult(part * width + n * tile, tile), tile), :]).astype(BF)
            if part == 0:
                qs[:, lanes] = res * jnp.asarray(HEAD_DIM ** -0.5, BF)
            else:
                to = ka if part == 1 else va
                for i in range(2):
                    to[q_at(i), lanes] = res[i * qrows:(i + 1) * qrows]
            return carry

        lax.fori_loop(0, steps, project, 0)
        if part > 0:
            to = ka if part == 1 else va
            for i in range(2):
                rcopy(to.at[q_at(i)], to.at[q_at(i)], msem.at[4 + 2 * (part - 1)], msem.at[5 + 2 * (part - 1)], dev(z, y, 1 - c, x)).start()
    step(6)
    wait_bytes(ka.at[pl.ds(0, rows)], msem.at[5])
    wait_bytes(va.at[pl.ds(0, rows)], msem.at[7])
    for src, out, s in ((qs, qs_o, 1), (ka, ka_o, 2), (va, va_o, 3), (xr, xr_o, 4), (vec, vec_o, 5)):
        keep.append(pltpu.make_async_copy(src, out, osem.at[s]))
        keep[-1].start()

    lane = lax.broadcasted_iota(jnp.int32, (qrows, 128), 1)
    kpos = lax.broadcasted_iota(jnp.int32, (qrows, qrows), 0)
    qpos = lax.broadcasted_iota(jnp.int32, (qrows, qrows), 1)
    groups = qrows // 8

    def pair_body(p, carry):
        lanes = pl.ds(mult(p * 128, 128), 128)
        for i in range(2):
            quarter = quarters[i]
            qp = qs[i * qrows:(i + 1) * qrows, lanes]
            zero = jnp.zeros_like(qp)
            qh = (jnp.where(lane < HEAD_DIM, qp, zero), jnp.where(lane >= HEAD_DIM, qp, zero))

            def scores(j, tops, diagonal=False):
                at_keys = pl.ds(mult(j * qrows, qrows), qrows)
                kj = ka[at_keys, lanes]
                new = []
                for h, sc in enumerate((sc0, sc1)):
                    s = dot_nt(kj, qh[h])
                    if diagonal:
                        s = jnp.where(kpos <= qpos, s, NEG_BIG)
                    sc[at_keys, :] = s
                    new.append(jnp.maximum(tops[h], jnp.max(s.reshape(groups, 8, qrows), axis=0)))
                return tuple(new)

            low = jnp.full((8, qrows), NEG_BIG, F32)
            tops = scores(quarter, lax.fori_loop(0, quarter, scores, (low, low)), True)
            tops = tuple(jnp.max(t, axis=0, keepdims=True) for t in tops)

            def values(j, state):
                at_keys = pl.ds(mult(j * qrows, qrows), qrows)
                vt = va[at_keys, lanes].T
                new = []
                for h, sc in enumerate((sc0, sc1)):
                    total, acc = state[h]
                    e = jnp.exp(sc[at_keys, :] - tops[h])
                    total = total + jnp.sum(e.reshape(groups, 8, qrows), axis=0)
                    acc = acc + dot_nn(vt[h * HEAD_DIM:(h + 1) * HEAD_DIM], e.astype(BF))
                    new.append((total, acc))
                return tuple(new)

            blank = (jnp.zeros((8, qrows), F32), jnp.zeros((HEAD_DIM, qrows), F32))
            state = lax.fori_loop(0, quarter + 1, values, (blank, blank))
            parts = []
            for h in range(2):
                total = jnp.sum(state[h][0], axis=0, keepdims=True)
                parts.append(state[h][1] / total)
                lse[p, i * 2 + h:i * 2 + h + 1, :] = tops[h] + jnp.log(total)
            at[i * qrows:(i + 1) * qrows, lanes] = jnp.concatenate(parts, axis=0).T.astype(BF)
        return carry

    per = 2
    for k in range(0, pairs, per):
        lax.fori_loop(k, k + per, pair_body, 0)
        step(7 + k // per)

    chunks[3].tick5()
    for src, out, s in ((wp, wp_o, 6), (at, at_o, 7), (lse, lse_o, 8)):
        keep.append(pltpu.make_async_copy(src, out, osem.at[s]))
        keep[-1].start()

    def attend_out(n, carry):
        lanes = pl.ds(mult(n * tile, tile), tile)
        res = dot_nt(at[...], wp[pl.ds(mult(n * tile, tile), tile), :])
        r[:, lanes] = xr[:, lanes].astype(F32) + res + vec[BP:BP + 1, lanes]
        return carry

    lax.fori_loop(0, steps, attend_out, 0)

    def second_norm(k, carry):
        at_rows = pl.ds(mult(k * lrows, lrows), lrows)
        n2, _ = norm_parts(r[at_rows, :])
        a2[at_rows, :] = (n2 * vec[G2:G2 + 1, :] + vec[C2:C2 + 1, :]).astype(BF)
        return carry

    lax.fori_loop(0, rows // lrows, second_norm, 0)
    step(10)
    step(11)
    for k in range(4, 8):
        chunks[k].tick5()
    for src, out, s in ((wu, wu_o, 9), (r, r_o, 10), (a2, a2_o, 11)):
        keep.append(pltpu.make_async_copy(src, out, osem.at[s]))
        keep[-1].start()

    def up(n, carry):
        lanes = pl.ds(mult(n * tile, tile), tile)
        u = dot_nt(a2[...], wu[lanes, :]) + bu3[n]
        sq_u = u * u
        t = jnp.tanh(TANH_SCALE * (u + CUBIC_TERM * sq_u * u))
        half_up = 0.5 * (1.0 + t)
        hd[:, lanes] = (u * half_up).astype(BF)
        slope = TANH_SCALE * (1.0 + 3.0 * CUBIC_TERM * sq_u)
        gp[:, lanes] = (half_up + 0.5 * u * (1.0 - t * t) * slope).astype(BF)
        return carry

    blocks = hd.shape[1] // tile
    for k in range(0, blocks, 4):
        lax.fori_loop(k, k + 4, up, 0)
        step(12 + k // 4)
    for src, out, s in ((hd, hd_o, 12), (gp, gp_o, 13)):
        keep.append(pltpu.make_async_copy(src, out, osem.at[s]))
        keep[-1].start()
    my_len = live_length(len_ref, deal_ref, (z * Y + y) * C + x)
    rowpos = lax.broadcasted_iota(jnp.int32, (qrows, 1), 0)
    parts = len(chunks) - 8
    wide = wd.shape[1] // X
    for k in range(parts):
        if k == 1:
            step(15)
        chunks[8 + k].tick5()
        cuts = [slice(h * wide + k * (wide // parts), h * wide + (k + 1) * (wide // parts)) for h in range(X)]
        for h, cut in enumerate(cuts):
            keep.append(pltpu.make_async_copy(wd.at[:, cut], wd_o.at[:, cut], osem.at[16 + X * k + h]))
            keep[-1].start()

        def down(n, carry, k=k, cuts=cuts):
            lanes = pl.ds(mult(n * tile, tile), tile)
            res = dot_nt(hd[:, cuts[0]], wd[lanes, cuts[0]])
            for cut in cuts[1:]:
                res = res + dot_nt(hd[:, cut], wd[lanes, cut])
            res = res + (r[:, lanes] + vec[BD:BD + 1, lanes] if k == 0 else acc[:, lanes])
            if k < parts - 1:
                acc[:, lanes] = res
            else:
                for i in range(2):
                    live = quarters[i] * qrows + rowpos < my_len
                    outw[i * qrows:(i + 1) * qrows, lanes] = jnp.where(live, res[i * qrows:(i + 1) * qrows], 0.0).astype(BF)
            return carry

        lax.fori_loop(0, steps, down, 0)
    keep.append(pltpu.make_async_copy(outw, out_o, osem.at[15]))
    keep[-1].start()

    for ch in chunks:
        ch.drain()
    vectors.drain()

    @pl.when(core_to == c)
    def _():
        wait_bytes(xr.at[pl.ds(0, rows - small)], msem.at[0])

    @pl.when(core_to != c)
    def _():
        wait_bytes(xr, msem.at[0])

    @pl.when(c == x)
    def _():
        wait_bytes(xr.at[pl.ds(0, qrows)], msem.at[2])

    @pl.when(c != x)
    def _():
        wait_bytes(xr, msem.at[2])

    wait_bytes(xr, msem.at[3])
    wait_bytes(ka.at[pl.ds(0, rows)], msem.at[4])
    wait_bytes(va.at[pl.ds(0, rows)], msem.at[6])
    for cp in keep:
        cp.wait()


def forward(lengths, dealing, cot, x_source, shards, vectors):
    slots, small, width = x_source.shape
    rows = cot.shape[0]
    ff = shards[2].shape[0] * Z * Y * C
    keys = rows * 2
    pairs = width // 128

    def arr(shape, dtype=BF):
        return jax.ShapeDtypeStruct(shape, dtype)

    outs = [
        arr((3 * width, width)), arr((width, width)), arr((ff, width)), arr((width, ff)),
        arr((rows, width)), arr((rows, width)), arr((rows, width)), arr((keys, width)), arr((keys, width)),
        arr((rows, width)), arr((pairs, 8, rows // 2), F32), arr((rows, width), F32), arr((rows, width)),
        arr((rows, ff)), arr((rows, ff)), arr((16, width), F32), arr((rows, width)),
    ]
    vm = pltpu.VMEM
    scratch = [
        vm((3 * width, width), BF), vm((width, width), BF), vm((ff, width), BF), vm((width, ff), BF),
        vm((rows, width), BF), vm((rows, width), BF), vm((rows, width), BF), vm((keys, width), BF),
        vm((keys, width), BF), vm((rows, width), BF), vm((pairs, 8, rows // 2), F32), vm((rows, width), F32),
        vm((rows, width), BF), vm((rows, ff), BF), vm((rows, ff), BF), vm((Z * Y * C, 16, width), BF),
        vm((16, width), F32), vm((ff // 256, 1, 256), F32), vm((keys, rows // 2), F32), vm((keys, rows // 2), F32),
        vm((rows, width), BF), vm(x_source.shape, BF), vm((rows, width), F32),
        vm(x_source.shape, BF), *[vm(a.shape, F32) for a in (*shards, *vectors)],
        pltpu.SemaphoreType.DMA((N_GATHER, 2, 5)), pltpu.SemaphoreType.DMA((2, 4)), pltpu.SemaphoreType.DMA((8,)),
        pltpu.SemaphoreType.DMA((24,)), pltpu.SemaphoreType.DMA((12,)),
    ]
    anyspec = pl.BlockSpec(memory_space=pl.ANY)
    smem = pl.BlockSpec(memory_space=pltpu.SMEM)
    return pl.pallas_call(
        forward_kernel,
        out_shape=outs,
        in_specs=[smem, smem] + [anyspec] * 13,
        out_specs=[anyspec] * len(outs),
        scratch_shapes=scratch,
        compiler_params=pltpu.CompilerParams(
            collective_id=0, has_side_effects=True, vmem_limit_bytes=60 * 1024 * 1024
        ),
        name="forward",
    )(lengths, dealing, cot, x_source, *shards, *vectors)


def when(cond):
    if isinstance(cond, bool):
        return (lambda f: f()) if cond else (lambda f: None)
    return pl.when(cond)


class Reduce:
    S1, R1, S2, R2, S3, R3, S4, R4, S5, R5 = range(10)

    def __init__(self, grad, R, step, c0, C, zlist, bufs, out, out_c0, sems, k, where, kind, turned):
        self.kind = kind
        self.grad, self.R, self.step, self.c0, self.cn, self.zlist = grad, R, step, c0, C, zlist
        self.r1, self.r2, self.r3, self.r4, self.r5 = bufs
        self.out, self.out_c0, self.sems, self.k = out, out_c0, sems, k
        self.z, self.y, self.c, self.x, _ = where
        y, x = self.y, self.x
        self.o = o = 1 if turned else self.c
        self.y2, self.x2 = (y + o) % 2, (x + 1 - o) % 2
        self.y3, self.x3 = (y + 1 - o) % 2, (x + o) % 2
        self.every = len(zlist) == Z

    def sem(self, which):
        return self.sems.at[self.k, which]

    def rows(self, z, y, c):
        return pl.ds(mult(((z * Y + y) * C + c) * self.R, 16), self.R)

    def cols(self, x):
        return pl.ds(mult(x * self.step + self.c0, 128), self.cn)

    def at(self, z, y, c, x):
        return self.grad.at[self.rows(z, y, c), self.cols(x)]

    def add(self, rows, cols, got):
        self.grad[rows, cols] = (self.grad[rows, cols].astype(F32) + got.astype(F32)).astype(BF)

    def zidx(self, zi):
        return zi if self.every else self.zlist[0]

    def start(self):
        z, y, c, x = self.z, self.y, self.c, self.x
        to = dev(z, y, 1 - c, x)
        for zi, zz in enumerate(self.zlist):
            for yy in range(Y):
                for xx in range(X):
                    rcopy(
                        self.at(zz, yy, 1 - c, xx), self.r1.at[zi * Y + yy, xx],
                        self.sem(self.S1), self.sem(self.R1), to,
                    ).start()

    def tick2(self):
        z, y, c, x, o = self.z, self.y, self.c, self.x, self.o
        wait_bytes(self.r1, self.sem(self.R1))

        def body(e, carry):
            rows = self.rows(self.zidx(e // Y), e % Y, c)
            for xx in range(X):
                self.add(rows, self.cols(xx), self.r1[e, xx])
            return carry

        lax.fori_loop(0, len(self.zlist) * Y, body, 0)
        to = dev(z, self.y2, c, self.x2)
        for zi, zz in enumerate(self.zlist):
            for w in range(2):
                yy = w * (1 - o) + (1 - y) * o
                xx = (1 - x) * (1 - o) + w * o
                rcopy(self.at(zz, yy, c, xx), self.r2.at[zi * 2 + w], self.sem(self.S2), self.sem(self.R2), to).start()

    def tick3(self):
        z, y, c, x, o = self.z, self.y, self.c, self.x, self.o
        wait_bytes(self.r2, self.sem(self.R2))

        def body(e, carry):
            w = e % 2
            yy = w * (1 - o) + y * o
            xx = x * (1 - o) + w * o
            self.add(self.rows(self.zidx(e // 2), yy, c), self.cols(xx), self.r2[e])
            return carry

        lax.fori_loop(0, len(self.zlist) * 2, body, 0)
        if self.kind == 2:
            mate = z + 1 - 2 * (z % 2)
            for slot, zz in enumerate((mate, 3 - mate)):
                for w in range(2):
                    rcopy(
                        self.left(zz, w), self.r4.at[slot * 2 + w], self.sem(self.S4), self.sem(self.R4),
                        dev(mate, y, c, x),
                    ).start()
            return
        to = dev(z, self.y3, c, self.x3)
        for zi, zz in enumerate(self.zlist):
            rcopy(self.at(zz, self.y3, c, self.x3), self.r3.at[zi], self.sem(self.S3), self.sem(self.R3), to).start()

    def left_cut(self, zz, w):
        o = self.o
        return self.rows(zz, w * (1 - o) + self.y * o, self.c), self.cols(self.x * (1 - o) + w * o)

    def left(self, zz, w):
        return self.grad.at[self.left_cut(zz, w)]

    def first_hop(self, k):
        return [(k ^ 1, k, 0), ((3 - k) ^ 1, 3 - k, 1)]

    def tick4(self):
        z, y, c, x = self.z, self.y, self.c, self.x
        if self.kind == 2:
            wait_bytes(self.r4, self.sem(self.R4))
            for w in range(2):
                self.add(*self.left_cut(3 - z, w), self.r4[2 + w])
                rcopy(
                    self.left(3 - z, w), self.r5.at[w], self.sem(self.S5), self.sem(self.R5), dev(3 - z, y, c, x)
                ).start()
            for w in range(2):
                self.add(*self.left_cut(z, w), self.r4[w])
            return
        wait_bytes(self.r3, self.sem(self.R3))

        def body(zi, carry):
            self.add(self.rows(self.zidx(zi), y, c), self.cols(x), self.r3[zi])
            return carry

        lax.fori_loop(0, len(self.zlist), body, 0)
        if self.every:
            mate = z + 1 - 2 * (z % 2)
            for slot, zz in enumerate((mate, 3 - mate)):
                rcopy(
                    self.at(zz, y, c, x), self.r4.at[slot], self.sem(self.S4), self.sem(self.R4), dev(mate, y, c, x)
                ).start()
        else:
            k = self.zlist[0]
            for sender, taker, slot in self.first_hop(k):
                @pl.when(z == sender)
                def _(taker=taker, slot=slot):
                    rcopy(
                        self.at(k, y, c, x), self.r4.at[slot], self.sem(self.S4), self.sem(self.R4),
                        dev(taker, y, c, x),
                    ).start()

    def tick5(self):
        z, y, c, x = self.z, self.y, self.c, self.x
        if self.kind == 2:
            wait_bytes(self.r5, self.sem(self.R5))
            for w in range(2):
                self.add(*self.left_cut(z, w), self.r5[w])
            rcopy(
                self.at(z, self.y3, c, self.x3), self.r3.at[0], self.sem(self.S3), self.sem(self.R3),
                dev(z, self.y3, c, self.x3),
            ).start()
            return
        k = self.zlist[0]

        def take(zz, slot):
            self.add(self.rows(zz, y, c), self.cols(x), self.r4[slot])

        def pass_on(zz):
            rcopy(self.at(zz, y, c, x), self.r5.at[0], self.sem(self.S5), self.sem(self.R5), dev(zz, y, c, x)).start()

        if self.every:
            wait_bytes(self.r4, self.sem(self.R4))
            take(3 - z, 1)
            pass_on(3 - z)
            take(z, 0)
        else:
            @pl.when(z == 3 - k)
            def _():
                wait_bytes(self.r4.at[1], self.sem(self.R4))
                take(k, 1)
                pass_on(k)

            @pl.when(z == k)
            def _():
                wait_bytes(self.r4.at[0], self.sem(self.R4))
                take(k, 0)

    def tick6(self):
        z, y, c, x = self.z, self.y, self.c, self.x

        @when(True if self.every else z == self.zlist[0])
        def _():
            last, sem = (self.r3, self.R3) if self.kind == 2 else (self.r5, self.R5)
            wait_bytes(last, self.sem(sem))
            own = self.grad[self.rows(z, y, c), self.cols(x)].astype(F32)
            self.out[:, self.out_c0:self.out_c0 + self.cn] = own + last[0].astype(F32)

    def drain(self):
        z = self.z
        wait_bytes(self.r1, self.sem(self.S1))
        wait_bytes(self.r2, self.sem(self.S2))
        wait_bytes(self.r3, self.sem(self.S3))
        if self.every:
            wait_bytes(self.r4, self.sem(self.S4))
            wait_bytes(self.r5, self.sem(self.S5))
        else:
            k = self.zlist[0]
            for sender, _, slot in self.first_hop(k):
                @pl.when(z == sender)
                def _():
                    wait_bytes(self.r4.at[0], self.sem(self.S4))

            @pl.when(z == 3 - k)
            def _():
                wait_bytes(self.r5, self.sem(self.S5))


TURNED_BACK = ()
KINDS_BACK = (2,) * 4 + (1,) * 9


def reduce_shapes(width, ff):
    n = Z * Y * C
    every = list(range(Z))
    half = width // X
    wide = ff // X
    shapes = [("d", width // n, wide, k * (wide // 4), wide // 4, every, k * (wide // 4)) for k in range(4)]
    shapes += [("u", ff // n, half, 0, half, [k], 0) for k in range(Z)]
    shapes += [("p", width // n, half, 0, half, every, 0)]
    shapes += [("q", 3 * width // n, half, 0, half, [k], 0) for k in range(Z)]
    return shapes


PLAN = (
    "f2", ("u0", 1), "f4", ("u0", 2), "f5", ("u2", 1), ("d0", 1), ("d1", 1), "f7", ("u2", 2), "f8", ("u1", 1),
    ("d0", 2), "f9", ("d1", 2), "f10", ("u1", 2), ("u0", 3), "f11", ("u3", 1), ("d2", 1), ("d3", 1), "norm2",
    ("u2", 3), "proj", ("pj", 1), ("u3", 2), ("d2", 2), ("d0", 3), ("d3", 2), "a00", ("pj", 2), ("d1", 3), ("o", 0),
    "a01", ("o", 1), "a10", ("u1", 3), ("d0", 4), ("o", 2), "a11", ("u0", 4), ("d1", 4), ("u2", 4), ("o", 3), "a20",
    ("o", 4), "a21", ("u3", 3), ("d0", 5), ("u0", 5), ("o", 5), "a30", ("o", 6), "a31", ("d2", 3), ("d1", 5),
    ("u2", 5), ("o", 7), "a40", ("d3", 3), "a50", ("pj", 3), ("d2", 4), ("u1", 4), "a51", ("u3", 4), "norm1",
    ("d3", 4), "qa", ("q0", 1), ("pj", 4), "merge", ("d2", 5), "qb", ("q1", 1), ("u1", 5), ("q0", 2), "qc", ("q2", 1),
    ("u3", 5), "qd", ("q3", 1), ("q1", 2), ("d3", 5), "da", ("q3", 2), ("q0", 3), ("pj", 5), "ln", ("u2", 6),
    ("q2", 2), ("x", 0), ("u0", 6), ("d0", 6), ("d1", 6), ("x", 1), ("v", 0), ("q1", 3), ("d2", 6), ("u1", 6),
    ("u3", 6), ("x", 2), ("v", 1), ("q2", 3), ("d3", 6), ("x", 3), ("q3", 3), ("q0", 4), ("v", 2), ("pj", 6),
    ("q1", 4), ("q0", 5), ("v", 3), ("q2", 4), ("q1", 5), ("q3", 4), ("q2", 5), ("v", 4), ("q3", 5), ("q0", 6),
    ("q1", 6), ("q2", 6), ("q3", 6),
)


def part_actions(plan):
    parts, now = {}, None
    for item in plan:
        if isinstance(item, str):
            now = parts.setdefault(item, [])
        else:
            now.append(item)
    return parts


def backward_kernel(*refs):
    names = (
        "len_ref", "deal_ref", "wq_i", "wp_i", "wu_i", "wd_i", "xr_i", "gw_i", "qs_i", "ka_i", "va_i", "at_i",
        "lse_i", "r_i", "a2_i", "hd_i", "gp_i", "vec_i", "out_i", "og_q", "og_p", "og_u", "og_d", "osum", "ret",
        "out_n", "wq", "wp", "xr", "g", "qs", "ka", "va", "at", "lse", "r", "a2", "vec", "gt", "d2", "dr", "drl",
        "do", "gq", "gp_", "gu", "gd", "wd_t", "wu_t", "hd_t", "gp_t", "dka", "dva", "own_v", "sv", "rk", "rv", "dm",
        "vs", "vr", "bub", "lsem", "tsem", "rsem", "msem", "vsem",
    )
    env = dict(zip(names, refs[: len(names)]))
    env.update(a1=env["a2"], own_k=env["d2"], sk=env["drl"], dx=env["do"])
    bufs = refs[len(names):]
    e = type("Refs", (), env)
    where = coords()
    z, y, c, x, d = where
    rows, width = e.g.shape
    ff = e.hd_i.shape[1]
    qrows = rows // 2
    pairs = width // 128
    tile = 256
    lrows = 128
    steps = width // tile
    quarters = (c, 3 - c)
    theirs = (1 - c, 2 + c)

    def at_quarter(k):
        return pl.ds(mult(k * qrows, qrows), qrows)

    entered = enter(Z * Y * C * X)

    loads = {}
    for k, (src, dst) in enumerate(
        (
            ("gw_i", "g"), ("a2_i", "a2"), ("r_i", "r"), ("vec_i", "vec"), ("wp_i", "wp"), ("at_i", "at"),
            ("qs_i", "qs"), ("ka_i", "ka"), ("va_i", "va"), ("lse_i", "lse"), ("xr_i", "xr"), ("wq_i", "wq"),
        )
    ):
        loads[dst] = pltpu.make_async_copy(env[src], env[dst], e.lsem.at[k])

    def tile_of(idx):
        block = idx // 3
        return (block % 2) * 2 * 3 + (block // 2) * 3 + idx % 3

    def tile_copies(idx):
        n = tile_of(idx)
        slot = idx % 2
        cut = pl.ds(mult(n * tile, tile), tile)
        return (
            pltpu.make_async_copy(e.wd_i.at[:, cut], e.wd_t.at[slot], e.tsem.at[0, slot]),
            pltpu.make_async_copy(e.gp_i.at[:, cut], e.gp_t.at[slot], e.tsem.at[1, slot]),
            pltpu.make_async_copy(e.hd_i.at[:, cut], e.hd_t.at[slot], e.tsem.at[2, slot]),
            pltpu.make_async_copy(e.wu_i.at[cut, :], e.wu_t.at[slot], e.tsem.at[3, slot]),
        )

    loads["g"].start()
    for cp in tile_copies(0):
        cp.start()
    loads["a2"].start()
    for name in ("r", "vec", "wp", "at", "qs", "ka", "va", "lse", "xr", "wq"):
        loads[name].start()

    def send_out(k):
        i, part = k // 4, k % 4
        some = qrows // 4
        same = jnp.logical_and(x == c, x == i)
        src = e.out_i.at[pl.ds(i * qrows + part * some, some)]
        dst = e.out_n.at[pl.ds(mult(((i + c) % 2) * qrows + part * some, some), some)]

        @pl.when(same)
        def _():
            lcopy(src, dst, e.msem.at[1]).start()

        @pl.when(jnp.logical_not(same))
        def _():
            rcopy(src, dst, e.msem.at[0], e.msem.at[1], dev(z, y, x, i)).start()

    grads = {"q": (e.gq, e.og_q), "p": (e.gp_, e.og_p), "u": (e.gu, e.og_u), "d": (e.gd, e.og_d)}
    chunks = []
    for k, (name, R, step, c0, cn, zlist, oc) in enumerate(reduce_shapes(width, ff)):
        grad, out = grads[name]
        chunks.append(Reduce(grad, R, step, c0, cn, zlist, bufs[5 * k:5 * k + 5], out, oc, e.rsem, k, where, KINDS_BACK[k], k in TURNED_BACK))
    names_of = ("d0", "d1", "d2", "d3", "u0", "u1", "u2", "u3", "pj", "q0", "q1", "q2", "q3")
    by_name = dict(zip(names_of, chunks))
    parts = part_actions(PLAN)

    def after(part):
        for name, k in parts.get(part, ()):
            if name in by_name:
                ch = by_name[name]
                (ch.start, ch.tick2, ch.tick3, ch.tick4, ch.tick5, ch.tick6)[k - 1]()
            elif name == "x":
                give(k)
            elif name == "o":
                send_out(k)
            else:
                land(k)
                if k < 4:
                    hop(k + 1)


    my_len = live_length(e.len_ref, e.deal_ref, (z * Y + y) * C + x)
    rowpos = lax.broadcasted_iota(jnp.int32, (lrows, 1), 0)
    loads["g"].wait()
    blank = jnp.zeros((1, width), F32)
    total_bd = blank
    for k in range(rows // lrows):
        base = quarters[k * lrows // qrows] * qrows + (k * lrows) % qrows
        live = base + rowpos < my_len
        part = jnp.where(live, e.g[k * lrows:(k + 1) * lrows, :], jnp.zeros((), BF))
        e.g[k * lrows:(k + 1) * lrows, :] = part
        e.gt[:, k * lrows:(k + 1) * lrows] = part.T
        total_bd = total_bd + jnp.sum(part.astype(F32), axis=0, keepdims=True)
    e.d2[...] = jnp.zeros_like(e.d2)
    loads["a2"].wait()

    ff_tiles = ff // tile
    def ffn(idx, carry, acting=True):
        slot = idx % 2
        n = tile_of(idx)
        cut = pl.ds(mult(n * tile, tile), tile)

        @pl.when(idx + 1 < ff_tiles)
        def _():
            for cp in tile_copies(idx + 1):
                cp.start()

        for cp in tile_copies(idx):
            cp.wait()
        du = (e.gp_t[slot].astype(F32) * dot_nn(e.g[...], e.wd_t[slot])).astype(BF)
        e.bub[n] = jnp.sum(du.astype(F32), axis=0, keepdims=True)
        e.gd[:, cut] = dot_nn(e.gt[...], e.hd_t[slot]).astype(BF)
        e.gu[cut, :] = dot_tn(du, e.a2[...]).astype(BF)
        e.d2[...] += dot_nn(du, e.wu_t[slot])
        for k in range(2, ff_tiles) if acting else ():
            if f"f{k}" in parts:
                @pl.when(idx == k)
                def _(k=k):
                    after(f"f{k}")

        return carry

    def ffn_first(idx, carry):
        return ffn(idx, carry, False)

    lax.fori_loop(0, 2, ffn_first, 0)

    entered()

    lax.fori_loop(2, ff_tiles, ffn, 0)

    loads["r"].wait()
    loads["vec"].wait()

    def norm_two(k, sums):
        at_rows = pl.ds(mult(k * lrows, lrows), lrows)
        n2, rstd = norm_parts(e.r[at_rows, :])
        da = e.d2[at_rows, :]
        ee = da * e.vec[G2:G2 + 1, :]
        gg = e.g[at_rows, :].astype(F32)
        m1 = jnp.mean(ee, axis=-1, keepdims=True)
        m2 = jnp.mean(ee * n2, axis=-1, keepdims=True)
        dr = gg + (ee - m1 - n2 * m2) * rstd
        e.dr[at_rows, :] = dr
        e.drl[at_rows, :] = dr.astype(BF)
        return (
            sums[0] + jnp.sum(da * n2, axis=0, keepdims=True),
            sums[1] + jnp.sum(da, axis=0, keepdims=True),
            sums[2] + jnp.sum(dr, axis=0, keepdims=True),
        )

    sum_g2, sum_c2, sum_bp = lax.fori_loop(0, rows // lrows, norm_two, (blank, blank, blank))

    after("norm2")

    loads["wp"].wait()
    loads["at"].wait()

    def proj_back(n, carry):
        cut = pl.ds(mult(n * tile, tile), tile)
        e.do[:, cut] = dot_nn(e.drl[...], e.wp[:, cut]).astype(BF)
        e.gp_[cut, :] = dot_tn(e.drl[:, cut], e.at[...]).astype(BF)
        return carry

    lax.fori_loop(0, steps, proj_back, 0)
    after("proj")

    for name in ("qs", "ka", "va", "lse"):
        loads[name].wait()
    lane = lax.broadcasted_iota(jnp.int32, (qrows, 128), 1)
    kpos = lax.broadcasted_iota(jnp.int32, (qrows, qrows), 0)
    qpos = lax.broadcasted_iota(jnp.int32, (qrows, qrows), 1)

    def split(v):
        zero = jnp.zeros_like(v)
        return jnp.where(lane < HEAD_DIM, v, zero), jnp.where(lane >= HEAD_DIM, v, zero)

    def pair_body(p, carry):
        lanes = pl.ds(mult(p * 128, 128), 128)
        e.dka[...] = jnp.zeros_like(e.dka)
        e.dva[...] = jnp.zeros_like(e.dva)
        for i in range(2):
            quarter = quarters[i]
            own = slice(i * qrows, (i + 1) * qrows)
            qp, dop = e.qs[own, lanes], e.do[own, lanes]
            qh, doh = split(qp), split(dop)
            qq, dd = jnp.concatenate(qh, axis=0), jnp.concatenate(doh, axis=0)
            prod = (dop.astype(F32) * e.at[own, lanes].astype(F32)).T
            delta = [jnp.sum(prod[h * HEAD_DIM:(h + 1) * HEAD_DIM], axis=0, keepdims=True) for h in range(2)]
            logs = [e.lse[p, i * 2 + h:i * 2 + h + 1, :] for h in range(2)]

            def keys(j, dq, diagonal=False):
                at_keys = pl.ds(mult(j * qrows, qrows), qrows)
                kj, vj = e.ka[at_keys, lanes], e.va[at_keys, lanes]
                kt = kj.T
                probs, grads_s, new = [], [], []
                for h in range(2):
                    s = dot_nt(kj, qh[h])
                    if diagonal:
                        s = jnp.where(kpos <= qpos, s, NEG_BIG)
                    pt = jnp.exp(s - logs[h])
                    ds = (pt * (dot_nt(vj, doh[h]) - delta[h])).astype(BF)
                    probs.append(pt.astype(BF))
                    grads_s.append(ds)
                    new.append(dq[h] + dot_nn(kt[h * HEAD_DIM:(h + 1) * HEAD_DIM], ds))
                e.dva[at_keys, :] += dot_nn(jnp.concatenate(probs, axis=1), dd)
                e.dka[at_keys, :] += dot_nn(jnp.concatenate(grads_s, axis=1), qq)
                return tuple(new)

            none = jnp.zeros((HEAD_DIM, qrows), F32)
            dq = lax.fori_loop(0, quarter, keys, (none, none))
            dq = keys(quarter, dq, True)
            e.dm[own, lanes] = (jnp.concatenate(dq, axis=0).T * HEAD_DIM ** -0.5).astype(BF)
            for k in range(pairs):
                if f"a{k}{i}" in parts:
                    @pl.when(p == k)
                    def _(k=k, i=i):
                        after(f"a{k}{i}")

        for i in range(2):
            own = slice(i * qrows, (i + 1) * qrows)
            e.own_k[own, lanes] = e.dka[at_quarter(quarters[i]), :]
            e.own_v[own, lanes] = e.dva[at_quarter(quarters[i]), :]
            e.sk[own, lanes] = e.dka[at_quarter(theirs[i]), :].astype(BF)
            e.sv[own, lanes] = e.dva[at_quarter(theirs[i]), :].astype(BF)
        for k in range(pairs // 2):
            @pl.when(p == 2 * k + 1)
            def _(k=k):
                cut = slice(2 * k * 128, (2 * k + 2) * 128)
                for src, dst, s in ((e.sk, e.rk, 2), (e.sv, e.rv, 4)):
                    rcopy(
                        src.at[:, cut], dst.at[:, cut], e.msem.at[s], e.msem.at[s + 1], dev(z, y, 1 - c, x)
                    ).start()
        return carry

    lax.fori_loop(0, pairs, pair_body, 0)

    loads["xr"].wait()

    def norm_one(k, carry):
        at_rows = pl.ds(mult(k * lrows, lrows), lrows)
        n1, _ = norm_parts(e.xr[at_rows, :].astype(F32))
        e.a1[at_rows, :] = (n1 * e.vec[G1:G1 + 1, :] + e.vec[C1:C1 + 1, :]).astype(BF)
        return carry

    lax.fori_loop(0, rows // lrows, norm_one, 0)
    after("norm1")

    def qkv_grad(n, carry):
        cut = pl.ds(mult(n * tile, tile), tile)
        e.gq[cut, :] = dot_tn(e.dm[:, cut], e.a1[...]).astype(BF)
        return carry

    lax.fori_loop(0, 3, qkv_grad, 0)
    after("qa")
    wait_bytes(e.rk, e.msem.at[3])
    wait_bytes(e.rv, e.msem.at[5])
    for part, (mine, got) in enumerate(((e.own_k, e.rk), (e.own_v, e.rv))):
        def merge(k, carry, part=part, mine=mine, got=got):
            at_rows = pl.ds(mult(k * lrows, lrows), lrows)
            e.dm[at_rows, (part + 1) * width:(part + 2) * width] = (
                mine[at_rows, :] + got[at_rows, :].astype(F32)
            ).astype(BF)
            return carry

        lax.fori_loop(0, rows // lrows, merge, 0)
    after("merge")
    for name, first, stop in (("qb", 3, 5), ("qc", 5, 7), ("qd", 7, 9)):
        lax.fori_loop(first, stop, qkv_grad, 0)
        after(name)
    loads["wq"].wait()

    def input_back(n, carry):
        cut = pl.ds(mult(n * tile, tile), tile)
        e.d2[:, cut] = dot_nn(e.dm[...], e.wq[:, cut])
        return carry

    lax.fori_loop(0, steps, input_back, 0)
    after("da")

    def norm_one_back(k, sums):
        at_rows = pl.ds(mult(k * lrows, lrows), lrows)
        n1, rstd = norm_parts(e.xr[at_rows, :].astype(F32))
        da = e.d2[at_rows, :]
        ee = da * e.vec[G1:G1 + 1, :]
        m1 = jnp.mean(ee, axis=-1, keepdims=True)
        m2 = jnp.mean(ee * n1, axis=-1, keepdims=True)
        e.dx[at_rows, :] = (e.dr[at_rows, :] + (ee - m1 - n1 * m2) * rstd).astype(BF)
        return sums[0] + jnp.sum(da * n1, axis=0, keepdims=True), sums[1] + jnp.sum(da, axis=0, keepdims=True)

    sum_g1, sum_c1 = lax.fori_loop(0, rows // lrows, norm_one_back, (blank, blank))

    e.vs[0] = jnp.zeros_like(e.vs[0])
    for row, value in ((G1, sum_g1), (C1, sum_c1), (BP, sum_bp), (G2, sum_g2), (C2, sum_c2), (BD, total_bd)):
        e.vs[0, row:row + 1, :] = value
    per = width // tile
    for k in range(ff_tiles):
        e.vs[0, BU + k // per:BU + k // per + 1, (k % per) * tile:(k % per + 1) * tile] = e.bub[k]
    hops = (
        dev(z, y, 1 - c, x), dev(z, y, c, 1 - x), dev(z, 1 - y, c, x),
        dev(z + 1 - 2 * (z % 2), y, c, x), dev((z + 2) % 4, y, c, x),
    )

    def hop(k):
        rcopy(e.vs.at[k], e.vr.at[k], e.vsem.at[0, k], e.vsem.at[1, k], hops[k]).start()

    def land(k):
        wait_bytes(e.vr.at[k], e.vsem.at[1, k])
        e.vs[k + 1] = e.vs[k] + e.vr[k]

    hop(0)

    small = e.ret.shape[1]
    per_quarter = qrows // small
    slot = (z * Y + y) * C + x

    def give_back(k, carry):
        i = (k + x) % 2
        e8 = (k // 2 + d) % per_quarter
        td = ((i + c) % 2) * per_quarter + e8
        src = e.dx.at[pl.ds(mult(i * qrows + e8 * small, small), small)]
        mine = jnp.logical_and(td == d, x == i)

        @pl.when(mine)
        def _():
            lcopy(src, e.ret.at[slot], e.msem.at[7]).start()

        @pl.when(jnp.logical_not(mine))
        def _():
            rcopy(src, e.ret.at[slot], e.msem.at[6], e.msem.at[7], {"dp": td, "cp": i}).start()

        return carry

    share = per_quarter // 2

    def give(k):
        lax.fori_loop(k * share, (k + 1) * share, give_back, 0)

    after("ln")
    own = width // (Z * Y * C)
    e.osum[0:6, :] = pltpu.roll(e.vs[5, 0:6, :], (width - d * own) % width, 1)[:, :tile]
    long = ff // (Z * Y * C)
    per_row = width // long
    e.osum[6:7, :] = pltpu.roll(
        e.vs[5, pl.ds(BU + d // per_row, 1), :], (width - (d % per_row) * long) % width, 1
    )[:, :tile]
    e.osum[7:8, :] = jnp.zeros((1, tile), F32)
    wait_bytes(e.dx, e.msem.at[7])

    for ch in chunks:
        ch.drain()
    for k in range(5):
        wait_bytes(e.vr.at[k], e.vsem.at[0, k])
    wait_bytes(e.rk, e.msem.at[2])
    wait_bytes(e.rv, e.msem.at[4])

    @pl.when((x + c) % 2 == d // per_quarter)
    def _():
        wait_bytes(e.dx.at[pl.ds(0, rows - small)], e.msem.at[6])

    @pl.when((x + c) % 2 != d // per_quarter)
    def _():
        wait_bytes(e.dx, e.msem.at[6])

    @pl.when(c == x)
    def _():
        wait_bytes(e.dx.at[pl.ds(0, qrows)], e.msem.at[0])

    @pl.when(c != x)
    def _():
        wait_bytes(e.dx, e.msem.at[0])

    wait_bytes(e.dx, e.msem.at[1])


def backward(lengths, dealing, saved, shards):
    wq, wp, wu, wd, xr, gw, qs, ka, va, at, lse, r, a2, hd, gp, vec, outw = saved
    rows, width = xr.shape
    ff = hd.shape[1]
    n = Z * Y * C
    keys = ka.shape[0]
    small = rows // n
    pairs = width // 128

    def arr(shape, dtype=BF):
        return jax.ShapeDtypeStruct(shape, dtype)

    outs = [arr(s.shape, F32) for s in shards] + [
        arr((8, 256), F32), arr((n, small, width)), arr((rows, width)),
    ]
    vm = pltpu.VMEM
    acts = vm((rows, width), BF)
    acts32 = vm((rows, width), F32)
    scratch = [
        vm(wq.shape, BF), vm(wp.shape, BF), acts, acts, acts, vm(ka.shape, BF), vm(va.shape, BF), acts,
        vm(lse.shape, F32), acts32, acts, vm(vec.shape, F32), vm((width, rows), BF), acts32, acts32, acts, acts,
        vm(wq.shape, BF), vm(wp.shape, BF), vm(wu.shape, BF), vm(wd.shape, BF),
        vm((2, width, 256), BF), vm((2, 256, width), BF), vm((2, rows, 256), BF), vm((2, rows, 256), BF),
        vm((keys, 128), F32), vm((keys, 128), F32),
        acts32, acts, acts, acts, vm((rows, 3 * width), BF),
        vm((6, 16, width), F32), vm((5, 16, width), F32), vm((ff // 256, 1, 256), F32),
        pltpu.SemaphoreType.DMA((12,)), pltpu.SemaphoreType.DMA((4, 2)), pltpu.SemaphoreType.DMA((13, 10)),
        pltpu.SemaphoreType.DMA((8,)), pltpu.SemaphoreType.DMA((2, 5)),
    ]
    for kind, (_, R, _, _, cn, zlist, _) in zip(KINDS_BACK, reduce_shapes(width, ff)):
        k = len(zlist)
        last = (1, 4, 2) if kind == 2 else (k, 2, 1)
        scratch += [vm((2 * k, 2, R, cn), BF)] + [vm((m, R, cn), BF) for m in (2 * k,) + last]
    anyspec = pl.BlockSpec(memory_space=pl.ANY)
    smem = pl.BlockSpec(memory_space=pltpu.SMEM)
    vmem = pl.BlockSpec(memory_space=pltpu.VMEM)
    return pl.pallas_call(
        backward_kernel,
        out_shape=outs,
        in_specs=[smem, smem] + [anyspec] * len(saved),
        out_specs=[vmem] * 5 + [anyspec] * 2,
        scratch_shapes=scratch,
        compiler_params=pltpu.CompilerParams(
            collective_id=1, has_side_effects=True, vmem_limit_bytes=67043328
        ),
        name="backward",
    )(lengths, dealing, *saved)


def finish_kernel(deal_ref, gq, gp, gu, gd, sums, ret, out, grad_o, out_o, gq_o, gp_o, gu_o, gd_o, *rows_o):
    for s in range(ret.shape[0]):
        grad_o[s] = ret[deal_ref[s]]
    for src, dst in ((out, out_o), (gq, gq_o), (gp, gp_o), (gu, gu_o), (gd, gd_o)):
        dst[...] = src[...]
    for k, row in enumerate(rows_o):
        row[...] = sums[k:k + 1, :row.shape[1]]


def finish(dealing, grads, sums, ret, out, own, long):
    def like(a):
        return jax.ShapeDtypeStruct(a.shape, a.dtype)

    outs = [like(ret), like(out)] + [like(g) for g in grads]
    outs += [jax.ShapeDtypeStruct((1, own), F32)] * 6 + [jax.ShapeDtypeStruct((1, long), F32)]
    vmem = pl.BlockSpec(memory_space=pltpu.VMEM)
    return pl.pallas_call(
        finish_kernel,
        out_shape=outs,
        in_specs=[pl.BlockSpec(memory_space=pltpu.SMEM)] + [vmem] * 7,
        out_specs=[vmem] * len(outs),
        name="finish",
    )(dealing, *grads, sums, ret, out)


def slice_plan(
    x_source, cotangent, lengths, dealing, qkv_weight, proj_weight, up_weight, down_weight,
    first_gain, first_shift, proj_bias, second_gain, second_shift, up_bias, down_bias,
):
    shards = [w.T for w in (qkv_weight, proj_weight, up_weight, down_weight)]
    vectors = [
        v[None] for v in (first_gain, first_shift, proj_bias, second_gain, second_shift, down_bias, up_bias)
    ]
    saved = forward(lengths, dealing, cotangent[0], x_source, shards, vectors)
    gq, gp, gu, gd, sums, ret, out = backward(lengths, dealing, saved, shards)
    done = finish(dealing, (gq, gp, gu, gd), sums, ret, out, first_gain.shape[0], up_bias.shape[0])
    input_grad, output, gq, gp, gu, gd = done[:6]
    by_row = [v.reshape(-1) for v in done[6:]]
    return (
        output[None], input_grad, gq.T, gp.T, gu.T, gd.T,
        by_row[G1], by_row[C1], by_row[BP], by_row[G2], by_row[C2], by_row[6], by_row[BD],
    )


def layer_norm(values, scaling, offset):
    centered = values - jnp.mean(values, axis=-1, keepdims=True)
    spread = jnp.mean(centered * centered, axis=-1, keepdims=True)
    return centered * lax.rsqrt(spread + EPSILON) * scaling + offset


def gelu_tanh(values):
    return (
        0.5
        * values
        * (1.0 + jnp.tanh(TANH_SCALE * (values + CUBIC_TERM * values * values * values)))
    )


def grouped(array, block_seqs):
    return array.reshape(
        (array.shape[0] // block_seqs, block_seqs, array.shape[1], HEADS, array.shape[2] // HEADS)
    )


def grouped_stats(array, block_seqs):
    return array.reshape((array.shape[0] // block_seqs, block_seqs) + array.shape[1:])


def joined(array):
    return array.reshape(
        (array.shape[0] * array.shape[1], array.shape[2], array.shape[3] * array.shape[4])
    )


def masked_scores(queries, key_rows, query_start, score_scale):
    scores = (
        jnp.einsum("bqhd,bkhd->bhqk", queries, key_rows, preferred_element_type=jnp.float32)
        * score_scale
    )
    query_pos = query_start + jnp.arange(queries.shape[1])
    key_pos = jnp.arange(key_rows.shape[1])
    return jnp.where(key_pos[None, :] <= query_pos[:, None], scores, NEG_BIG)


def attend(inputs, query_start, score_scale):
    queries, key_rows, val_rows = inputs
    scores = masked_scores(queries, key_rows, query_start, score_scale)
    row_top = jnp.max(scores, axis=-1, keepdims=True)
    exponent = jnp.exp(scores - row_top)
    totals = jnp.sum(exponent, axis=-1, keepdims=True)
    weights = (exponent / totals).astype(jnp.bfloat16)
    attended = jnp.einsum("bhqk,bkhd->bqhd", weights, val_rows, preferred_element_type=jnp.float32)
    return (attended.astype(jnp.bfloat16), (row_top + jnp.log(totals))[..., 0])


def rows_back(inputs, query_start, score_scale):
    queries, key_rows, val_rows, grad_rows, log_total = inputs
    scores = masked_scores(queries, key_rows, query_start, score_scale)
    weights = jnp.exp(scores - log_total[..., None])
    grad_weights = jnp.einsum(
        "bqhd,bkhd->bhqk", grad_rows, val_rows, preferred_element_type=jnp.float32
    )
    delta_rows = jnp.sum(weights * grad_weights, axis=-1)
    grad_scores = (weights * (grad_weights - delta_rows[..., None])).astype(jnp.bfloat16)
    grad_query = (
        jnp.einsum("bhqk,bkhd->bqhd", grad_scores, key_rows, preferred_element_type=jnp.float32)
        * score_scale
    )
    grad_keys = (
        jnp.einsum("bhqk,bqhd->bkhd", grad_scores, queries, preferred_element_type=jnp.float32)
        * score_scale
    )
    grad_vals = jnp.einsum(
        "bhqk,bqhd->bkhd",
        weights.astype(jnp.bfloat16),
        grad_rows,
        preferred_element_type=jnp.float32,
    )
    return (grad_query, grad_keys, grad_vals)


def fetch_weights(
    qkv_weight,
    proj_weight,
    up_weight,
    down_weight,
    first_gain,
    first_shift,
    proj_bias,
    second_gain,
    second_shift,
    up_bias,
    down_bias,
):
    qkv_part, proj_part, up_part, down_part = (
        lax.all_gather(qkv_weight.astype(jnp.bfloat16), "cp", axis=0, tiled=True),
        lax.all_gather(proj_weight.astype(jnp.bfloat16), "cp", axis=0, tiled=True),
        lax.all_gather(up_weight.astype(jnp.bfloat16), "cp", axis=0, tiled=True),
        lax.all_gather(down_weight.astype(jnp.bfloat16), "cp", axis=0, tiled=True),
    )
    return (
        lax.all_gather(qkv_part, "dp", axis=1, tiled=True),
        lax.all_gather(proj_part, "dp", axis=1, tiled=True),
        lax.all_gather(up_part, "dp", axis=1, tiled=True),
        lax.all_gather(down_part, "dp", axis=1, tiled=True),
        lax.all_gather(first_gain.astype(jnp.bfloat16), "dp", axis=0, tiled=True),
        lax.all_gather(first_shift.astype(jnp.bfloat16), "dp", axis=0, tiled=True),
        lax.all_gather(proj_bias.astype(jnp.bfloat16), "dp", axis=0, tiled=True),
        lax.all_gather(second_gain.astype(jnp.bfloat16), "dp", axis=0, tiled=True),
        lax.all_gather(second_shift.astype(jnp.bfloat16), "dp", axis=0, tiled=True),
        lax.all_gather(up_bias.astype(jnp.bfloat16), "dp", axis=0, tiled=True),
        lax.all_gather(down_bias.astype(jnp.bfloat16), "dp", axis=0, tiled=True),
    )


def mat_rows(left, right):
    return jnp.einsum("sqd,de->sqe", left, right, preferred_element_type=jnp.float32)


def mat_back(left, right):
    return jnp.einsum("sqe,de->sqd", left, right, preferred_element_type=jnp.float32)


def mat_grad(left, right):
    return jnp.einsum("sqd,sqe->de", left, right, preferred_element_type=jnp.float32)


def general(
    x_source,
    cotangent,
    lengths,
    dealing,
    qkv_weight,
    proj_weight,
    up_weight,
    down_weight,
    first_gain,
    first_shift,
    proj_bias,
    second_gain,
    second_shift,
    up_bias,
    down_bias,
):
    groups = lax.axis_size("dp")
    seqs_all, piece_rows, features = x_source.shape
    seq_group = seqs_all // groups
    span_rows = groups * piece_rows
    score_scale = HEAD_DIM ** (-0.5)
    block_seqs = math.gcd(seq_group, max(1, 512 // span_rows))
    owners = jnp.argsort(dealing)
    send_order = owners.reshape(groups, seq_group).T.reshape(-1)
    outgoing = x_source[send_order].reshape(seq_group, span_rows, features)
    arrived = lax.all_to_all(outgoing, "dp", split_axis=1, concat_axis=1, tiled=True)
    first_slot = lax.axis_index("dp") * seq_group
    my_lengths = lax.dynamic_slice_in_dim(lengths[owners], first_slot, seq_group)
    query_start = lax.axis_index("cp") * span_rows
    positions = query_start + jnp.arange(span_rows)
    live_rows = positions[None, :] < my_lengths[:, None]
    fetched = fetch_weights(
        qkv_weight,
        proj_weight,
        up_weight,
        down_weight,
        first_gain,
        first_shift,
        proj_bias,
        second_gain,
        second_shift,
        up_bias,
        down_bias,
    )
    qkv_full, proj_full, up_full, down_full = (fetched[0], fetched[1], fetched[2], fetched[3])
    gain_one, shift_one, bias_proj, gain_two, shift_two, bias_up, bias_down = [
        vector.astype(jnp.float32) for vector in fetched[4:]
    ]
    inputs_f = arrived.astype(jnp.float32)
    norm_one, back_one = jax.vjp(layer_norm, inputs_f, gain_one, shift_one)
    act_one = norm_one.astype(jnp.bfloat16)
    mixed_rows = mat_rows(act_one, qkv_full).astype(jnp.bfloat16)
    queries = mixed_rows[..., :features]
    kv_local = mixed_rows[..., features:]
    kv_all = lax.all_gather(kv_local, "cp", axis=1, tiled=True)
    attended, log_total = lax.map(
        lambda inputs: attend(inputs, query_start, score_scale),
        (
            grouped(queries, block_seqs),
            grouped(kv_all[..., :features], block_seqs),
            grouped(kv_all[..., features:], block_seqs),
        ),
    )
    attended = joined(attended)
    log_total = log_total.reshape((seq_group,) + log_total.shape[2:])
    residual = inputs_f + mat_rows(attended, proj_full) + bias_proj
    norm_two, back_two = jax.vjp(layer_norm, residual, gain_two, shift_two)
    act_two = norm_two.astype(jnp.bfloat16)
    up_raw = mat_rows(act_two, up_full) + bias_up
    hidden, back_gelu = jax.vjp(gelu_tanh, up_raw)
    hid_low = hidden.astype(jnp.bfloat16)
    result = residual + mat_rows(hid_low, down_full) + bias_down
    output = jnp.where(live_rows[..., None], result, 0.0).astype(jnp.bfloat16)
    fetched = fetch_weights(
        qkv_weight,
        proj_weight,
        up_weight,
        down_weight,
        first_gain,
        first_shift,
        proj_bias,
        second_gain,
        second_shift,
        up_bias,
        down_bias,
    )
    qkv_full, proj_full, up_full, down_full = (fetched[0], fetched[1], fetched[2], fetched[3])
    gain_one, gain_two = (fetched[4].astype(jnp.float32), fetched[7].astype(jnp.float32))
    grad_out = jnp.where(live_rows[..., None], cotangent.astype(jnp.float32), 0.0)
    grad_low = grad_out.astype(jnp.bfloat16)
    grad_down = mat_grad(hid_low, grad_low)
    grad_bias_down = jnp.sum(grad_out, axis=(0, 1))
    grad_hidden = mat_back(grad_low, down_full)
    grad_up_raw = back_gelu(grad_hidden)[0].astype(jnp.bfloat16)
    grad_up = mat_grad(act_two, grad_up_raw)
    grad_bias_up = jnp.sum(grad_up_raw.astype(jnp.float32), axis=(0, 1))
    grad_act_two = mat_back(grad_up_raw, up_full)
    grad_resid, grad_gain_two, grad_shift_two = back_two(grad_act_two)
    grad_resid = grad_resid + grad_out
    grad_bias_proj = jnp.sum(grad_resid, axis=(0, 1))
    resid_low = grad_resid.astype(jnp.bfloat16)
    grad_proj = mat_grad(attended, resid_low)
    grad_attended = mat_back(resid_low, proj_full).astype(jnp.bfloat16)
    kv_back = lax.all_gather(kv_local, "cp", axis=1, tiled=True)
    key_rows = kv_back[..., :features]
    val_rows = kv_back[..., features:]
    grad_query, grad_keys, grad_vals = lax.map(
        lambda inputs: rows_back(inputs, query_start, score_scale),
        (
            grouped(queries, block_seqs),
            grouped(key_rows, block_seqs),
            grouped(val_rows, block_seqs),
            grouped(grad_attended, block_seqs),
            grouped_stats(log_total, block_seqs),
        ),
    )
    grad_keys, grad_vals = (
        lax.psum_scatter(
            joined(grad_keys).astype(jnp.bfloat16), "cp", scatter_dimension=1, tiled=True
        ).astype(jnp.float32),
        lax.psum_scatter(
            joined(grad_vals).astype(jnp.bfloat16), "cp", scatter_dimension=1, tiled=True
        ).astype(jnp.float32),
    )
    grad_mixed = jnp.concatenate([joined(grad_query), grad_keys, grad_vals], axis=-1).astype(
        jnp.bfloat16
    )
    grad_qkv = mat_grad(act_one, grad_mixed)
    grad_act_one = mat_back(grad_mixed, qkv_full)
    grad_input, grad_gain_one, grad_shift_one = back_one(grad_act_one)
    grad_input = (grad_input + grad_resid).astype(jnp.bfloat16)
    returned = lax.all_to_all(grad_input, "dp", split_axis=1, concat_axis=0, tiled=True)
    input_grad = returned[dealing]
    (
        grad_qkv,
        grad_proj,
        grad_up,
        grad_down,
        grad_gain_one,
        grad_shift_one,
        grad_bias_proj,
        grad_gain_two,
        grad_shift_two,
        grad_bias_up,
        grad_bias_down,
    ) = (
        lax.psum_scatter(
            grad_qkv.astype(jnp.bfloat16), "dp", scatter_dimension=1, tiled=True
        ).astype(jnp.float32),
        lax.psum_scatter(
            grad_proj.astype(jnp.bfloat16), "dp", scatter_dimension=1, tiled=True
        ).astype(jnp.float32),
        lax.psum_scatter(
            grad_up.astype(jnp.bfloat16), "dp", scatter_dimension=1, tiled=True
        ).astype(jnp.float32),
        lax.psum_scatter(
            grad_down.astype(jnp.bfloat16), "dp", scatter_dimension=1, tiled=True
        ).astype(jnp.float32),
        lax.psum_scatter(
            grad_gain_one.astype(jnp.bfloat16), "dp", scatter_dimension=0, tiled=True
        ).astype(jnp.float32),
        lax.psum_scatter(
            grad_shift_one.astype(jnp.bfloat16), "dp", scatter_dimension=0, tiled=True
        ).astype(jnp.float32),
        lax.psum_scatter(
            grad_bias_proj.astype(jnp.bfloat16), "dp", scatter_dimension=0, tiled=True
        ).astype(jnp.float32),
        lax.psum_scatter(
            grad_gain_two.astype(jnp.bfloat16), "dp", scatter_dimension=0, tiled=True
        ).astype(jnp.float32),
        lax.psum_scatter(
            grad_shift_two.astype(jnp.bfloat16), "dp", scatter_dimension=0, tiled=True
        ).astype(jnp.float32),
        lax.psum_scatter(
            grad_bias_up.astype(jnp.bfloat16), "dp", scatter_dimension=0, tiled=True
        ).astype(jnp.float32),
        lax.psum_scatter(
            grad_bias_down.astype(jnp.bfloat16), "dp", scatter_dimension=0, tiled=True
        ).astype(jnp.float32),
    )
    grad_qkv, grad_proj, grad_up, grad_down = (
        lax.psum_scatter(
            grad_qkv.astype(jnp.bfloat16), "cp", scatter_dimension=0, tiled=True
        ).astype(jnp.float32),
        lax.psum_scatter(
            grad_proj.astype(jnp.bfloat16), "cp", scatter_dimension=0, tiled=True
        ).astype(jnp.float32),
        lax.psum_scatter(
            grad_up.astype(jnp.bfloat16), "cp", scatter_dimension=0, tiled=True
        ).astype(jnp.float32),
        lax.psum_scatter(
            grad_down.astype(jnp.bfloat16), "cp", scatter_dimension=0, tiled=True
        ).astype(jnp.float32),
    )
    (
        grad_gain_one,
        grad_shift_one,
        grad_bias_proj,
        grad_gain_two,
        grad_shift_two,
        grad_bias_up,
        grad_bias_down,
    ) = lax.psum(
        (
            grad_gain_one,
            grad_shift_one,
            grad_bias_proj,
            grad_gain_two,
            grad_shift_two,
            grad_bias_up,
            grad_bias_down,
        ),
        "cp",
    )
    return (
        output,
        input_grad,
        grad_qkv,
        grad_proj,
        grad_up,
        grad_down,
        grad_gain_one,
        grad_shift_one,
        grad_bias_proj,
        grad_gain_two,
        grad_shift_two,
        grad_bias_up,
        grad_bias_down,
    )


def solution(mesh):
    in_specs = (
        P(None, ("cp", "dp"), None),
        P("dp", "cp", None),
        P(),
        P(),
        P("cp", "dp"),
        P("cp", "dp"),
        P("cp", "dp"),
        P("cp", "dp"),
        P("dp"),
        P("dp"),
        P("dp"),
        P("dp"),
        P("dp"),
        P("dp"),
        P("dp"),
    )
    out_specs = (
        P("dp", "cp", None),
        P(None, ("cp", "dp"), None),
        P("cp", "dp"),
        P("cp", "dp"),
        P("cp", "dp"),
        P("cp", "dp"),
        P("dp"),
        P("dp"),
        P("dp"),
        P("dp"),
        P("dp"),
        P("dp"),
        P("dp"),
    )
    planned = tuple(mesh.shape.items()) == (("dp", Z * Y * C), ("cp", X))
    local = slice_plan if planned else general
    return jax.shard_map(local, mesh=mesh, in_specs=in_specs, out_specs=out_specs, check_vma=False)
```

```python
import functools
import math

import jax
import jax.numpy as jnp
from jax import lax
from jax.experimental import pallas as pl
from jax.experimental.pallas import tpu as pltpu
from jax.sharding import PartitionSpec as P

HEADS = 12
HEAD_DIM = 64


EPSILON = 1e-05
NEG_BIG = -1e30
TANH_SCALE = 0.7978845608028654
CUBIC_TERM = 0.044715
MESH_IDS = pl.DeviceIdType.MESH
BF = jnp.bfloat16
F32 = jnp.float32

Z, Y, C, X = 4, 2, 2, 2


def mult(value, n):
    return value if isinstance(value, int) else pl.multiple_of(value, n)


def coords():
    d = lax.axis_index("dp")
    x = lax.axis_index("cp")
    return d // (Y * C), (d // C) % Y, d % C, x, d


def dev(z, y, c, x):
    return {"dp": (z * Y + y) * C + c, "cp": x}


def rcopy(src, dst, ssem, rsem, where):
    return pltpu.make_async_remote_copy(
        src_ref=src, dst_ref=dst, send_sem=ssem, recv_sem=rsem, device_id=where, device_id_type=MESH_IDS
    )


def lcopy(src, dst, sem):
    return pltpu.make_async_copy(src, dst, sem)


def wait_bytes(ref, sem):
    pltpu.make_async_copy(ref, ref, sem).wait()


def enter(everyone):
    d = lax.axis_index("dp")
    x = lax.axis_index("cp")
    barrier = pltpu.get_barrier_semaphore()

    def greet(k, carry):
        kd = k // X
        kx = k % X

        @pl.when(jnp.logical_or(kd != d, kx != x))
        def _():
            pl.semaphore_signal(barrier, inc=1, device_id={"dp": kd, "cp": kx}, device_id_type=MESH_IDS)

        return carry

    lax.fori_loop(0, everyone, greet, 0)

    def entered():
        pl.semaphore_wait(barrier, everyone - 1)

    return entered


def dot_nn(a, b):
    return lax.dot_general(a, b, (((1,), (0,)), ((), ())), preferred_element_type=F32)


def dot_nt(a, b):
    return lax.dot_general(a, b, (((1,), (1,)), ((), ())), preferred_element_type=F32)


def dot_tn(a, b):
    return lax.dot_general(a, b, (((0,), (0,)), ((), ())), preferred_element_type=F32)


def norm_parts(v):
    mean = jnp.mean(v, axis=-1, keepdims=True)
    cen = v - mean
    var = jnp.mean(cen * cen, axis=-1, keepdims=True)
    rstd = lax.rsqrt(var + EPSILON)
    return cen * rstd, rstd


def live_length(len_ref, deal_ref, slot):
    total = jnp.int32(0)
    for s in range(len_ref.shape[0]):
        total = total + jnp.where(deal_ref[s] == slot, len_ref[s], 0)
    return total


class Piece:
    def __init__(self, full, R, r0, rn, step, c0, cn):
        self.full = full
        self.R, self.r0, self.rn, self.step, self.c0, self.cn = R, r0, rn, step, c0, cn

    def at(self, z, y, c, x):
        d = (z * Y + y) * C + c
        return self.full.at[
            pl.ds(mult(d * self.R + self.r0, 16), self.rn), pl.ds(mult(x * self.step + self.c0, 128), self.cn)
        ]


class Gather:
    FAR, MATE, A, B, CORE = range(5)

    def __init__(self, piece, sems, k, dummy, where, kind, turned):
        self.p, self.sems, self.k, self.dummy, self.kind = piece, sems, k, dummy, kind
        z, y, c, x, _ = where
        self.z, self.y, self.c, self.x = z, y, c, x
        o = 1 if turned else c
        self.far, self.mate = 3 - z, z + 1 - 2 * (z % 2)
        self.ya, self.xa = (y + 1 - o) % 2, (x + o) % 2
        self.yb, self.xb = (y + o) % 2, (x + 1 - o) % 2
        self.to = {
            self.FAR: dev(self.far, y, c, x), self.MATE: dev(self.mate, y, c, x), self.A: dev(z, self.ya, c, self.xa),
            self.B: dev(z, self.yb, c, self.xb), self.CORE: dev(z, y, 1 - c, x),
        }
        self.counts = {self.FAR: 1, self.MATE: 2, self.A: 4} if kind == 1 else {self.FAR: 2, self.MATE: 4, self.A: 1}
        self.counts.update({self.B: 8, self.CORE: 16})

    def send(self, pieces, *ways):
        for way in ways:
            for z, y, x in pieces:
                q = self.p.at(z, y, self.c, x)
                rcopy(q, q, self.sems.at[self.k, 0, way], self.sems.at[self.k, 1, way], self.to[way]).start()

    def wait(self, way, side=1):
        p = self.p
        wait_bytes(self.dummy.at[pl.ds(0, self.counts[way] * p.rn), pl.ds(0, p.cn)], self.sems.at[self.k, side, way])

    def start(self):
        own = [(self.z, self.y, self.x)]
        if self.kind == 1:
            self.send(own, self.FAR, self.MATE, self.A, self.B, self.CORE)
        else:
            self.send(own, self.A, self.FAR, self.MATE, self.B, self.CORE)

    def tick1(self):
        if self.kind == 1:
            self.wait(self.FAR)
            self.send([(self.far, self.y, self.x)], self.MATE, self.A, self.B, self.CORE)
        else:
            self.wait(self.A)
            self.send([(self.z, self.ya, self.xa)], self.FAR, self.MATE, self.B, self.CORE)

    def tick2(self):
        if self.kind == 1:
            self.wait(self.MATE)
            self.send([(self.mate, self.y, self.x), (3 - self.mate, self.y, self.x)], self.A, self.B, self.CORE)
        else:
            self.wait(self.FAR)
            self.send([(self.far, self.y, self.x), (self.far, self.ya, self.xa)], self.MATE, self.B, self.CORE)

    def tick3(self):
        if self.kind == 1:
            self.wait(self.A)
            self.send([(k, self.ya, self.xa) for k in range(Z)], self.B, self.CORE)
        else:
            self.wait(self.MATE)
            self.send(
                [(k, y, x) for k in (self.mate, 3 - self.mate) for y, x in ((self.y, self.x), (self.ya, self.xa))],
                self.B, self.CORE,
            )

    def tick4(self):
        self.wait(self.B)
        self.send(
            [(k, y, x) for k in range(Z) for y, x in ((self.yb, self.xb), (1 - self.y, 1 - self.x))], self.CORE
        )

    def tick5(self):
        self.wait(self.CORE)

    def drain(self):
        for way in range(5):
            self.wait(way, 0)


class Vectors:
    FAR, MATE, A, CORE = range(4)

    def __init__(self, full, sems, where):
        self.full, self.sems = full, sems
        z, y, c, x, _ = where
        self.z, self.y, self.c = z, y, c
        self.far, self.mate = 3 - z, z + 1 - 2 * (z % 2)
        self.to = (dev(self.far, y, c, x), dev(self.mate, y, c, x), dev(z, 1 - y, c, x), dev(z, y, 1 - c, x))
        self.counts = (1, 2, 4, 8)

    def send(self, pieces, *ways):
        for way in ways:
            for z, y in pieces:
                q = self.full.at[(z * Y + y) * C + self.c]
                rcopy(q, q, self.sems.at[0, way], self.sems.at[1, way], self.to[way]).start()

    def wait(self, way, side=1):
        wait_bytes(self.full.at[pl.ds(0, self.counts[way])], self.sems.at[side, way])

    def start(self):
        self.send([(self.z, self.y)], self.FAR, self.MATE, self.A, self.CORE)

    def tick1(self):
        self.wait(self.FAR)
        self.send([(self.far, self.y)], self.MATE, self.A, self.CORE)

    def tick2(self):
        self.wait(self.MATE)
        self.send([(self.mate, self.y), (3 - self.mate, self.y)], self.A, self.CORE)

    def tick3(self):
        self.wait(self.A)
        self.send([(k, 1 - self.y) for k in range(Z)], self.CORE)

    def tick4(self):
        self.wait(self.CORE)

    def drain(self):
        for way in range(4):
            self.wait(way, 0)


G1, C1, BP, G2, C2, BD, BU = range(7)


def gather_chunks(wq, wp, wu, wd):
    rq, rp, ru, rd = (w.shape[0] // (Z * Y * C) for w in (wq, wp, wu, wd))
    half, wide = wq.shape[1] // X, wd.shape[1] // X
    out = []
    for k in range(3):
        out.append(Piece(wq, rq, k * (rq // 3), rq // 3, half, 0, half))
    out.append(Piece(wp, rp, 0, rp, half, 0, half))
    for k in range(4):
        out.append(Piece(wu, ru, k * (ru // 4), ru // 4, half, 0, half))
    for k in range(4):
        out.append(Piece(wd, rd, 0, rd, wide, k * (wide // 4), wide // 4))
    return out


def one_hot(count, width, first):
    at_row = lax.broadcasted_iota(jnp.int32, (count, width), 0)
    at_col = lax.broadcasted_iota(jnp.int32, (count, width), 1)
    return (at_col == at_row + first).astype(BF)


N_GATHER = 12
TICKS = ("tick1", "tick2", "tick3", "tick4")
KINDS = (1, 1, 1, 1, 2, 2, 1, 2, 2, 1, 2, 2)
TURNED = (7,)
COT_STEPS = (6, 6, 6, 6, 8, 8, 8, 8)
LAGS = ((0, 1, 2, 3),) * 4 + ((0, 1, 2, 4),) * 8


def forward_kernel(
    len_ref, deal_ref, cot, x_any, sq_any, sp_any, su_any, sd_any, g1_any, c1_any, bp_any, g2_any, c2_any, bd_any, bu_any,
    wq_o, wp_o, wu_o, wd_o, xr_o, gw_o, qs_o, ka_o, va_o, at_o, lse_o, r_o, a2_o, hd_o, gp_o, vec_o, out_o,
    wq, wp, wu, wd, xr, a1, qs, ka, va, at, lse, r, a2, hd, gp, vg, vec, bu3, sc0, sc1, outw, xg, acc,
    x_in, sq, sp, su, sd, v_g1, v_c1, v_bp, v_g2, v_c2, v_bd, v_bu,
    gsem, vsem, msem, osem, isem,
):
    where = coords()
    z, y, c, x, d = where
    width = xr.shape[1]
    rows = xr.shape[0]
    qrows = rows // 2
    small = x_in.shape[1]
    sources = (sq_any, sp_any, su_any, sd_any, g1_any, c1_any, bp_any, g2_any, c2_any, bd_any, bu_any, x_any)
    places = (sq, sp, su, sd, v_g1, v_c1, v_bp, v_g2, v_c2, v_bd, v_bu, x_in)
    loads = [pltpu.make_async_copy(s, t, isem.at[k]) for k, (s, t) in enumerate(zip(sources, places))]
    for load in loads:
        load.start()
    pairs = width // 128
    tile = 256

    entered = enter(Z * Y * C * X)

    n = Z * Y * C
    for load, shard, full in zip(loads, (sq, sp, su, sd), (wq, wp, wu, wd)):
        load.wait()
        own, long = shard.shape
        full[pl.ds(mult(d * own, 16), own), pl.ds(mult(x * long, 128), long)] = shard[...].astype(BF)
    for load in loads[4:]:
        load.wait()
    vg[d] = jnp.zeros(vg.shape[1:], BF)
    own = v_g1.shape[1]
    seven = jnp.concatenate([v[...] for v in (v_g1, v_c1, v_bp, v_g2, v_c2, v_bd)], axis=0).astype(BF)
    placed = dot_nn(seven, one_hot(own, width, d * own))
    long = v_bu.shape[1]
    per_row = width // long
    placed_long = dot_nn(v_bu[...].astype(BF), one_hot(long, width, (d % per_row) * long))
    rows_long = [jnp.where(d // per_row == k, placed_long, 0.0) for k in range(n // per_row)]
    rest = jnp.zeros((16 - 6 - n // per_row, width), F32)
    vg[d] = jnp.concatenate([placed] + rows_long + [rest], axis=0).astype(BF)
    slots = x_in.shape[0]
    for t in range(slots):
        owner = jnp.int32(0)
        for s in range(slots):
            owner = jnp.where(deal_ref[s] == t, s, owner)
        xg[t] = x_in[owner]

    entered()

    vectors = Vectors(vg, vsem, where)
    vectors.start()
    chunks = [
        Gather(p, gsem, k, wu, where, KINDS[k], k in TURNED) for k, p in enumerate(gather_chunks(wq, wp, wu, wd))
    ]

    def send_cot(k):
        b, part = k // 4, k % 4
        some = qrows // 4
        core_b = (x + b) % 2
        src_b = cot.at[pl.ds(b * qrows + part * some, some)]
        dst_b = gw_o.at[pl.ds(mult(x * qrows + part * some, some), some)]
        same = jnp.logical_and(core_b == c, c == x)

        @pl.when(same)
        def _():
            lcopy(src_b, dst_b, msem.at[3]).start()

        @pl.when(jnp.logical_not(same))
        def _():
            rcopy(src_b, dst_b, msem.at[2], msem.at[3], dev(z, y, core_b, c)).start()

    per_quarter = qrows // small
    place = mult(x * qrows + (d % per_quarter) * small, 16)
    core_to = (x + d // per_quarter) % 2
    dst = xr.at[pl.ds(place, small)]

    def deal_out(k, carry):
        t = (d + k + x * (slots // 2)) % slots
        td = (t // 2) * 2 + core_to
        tx = t % 2
        mine = jnp.logical_and(td == d, tx == x)

        @pl.when(mine)
        def _():
            lcopy(xg.at[t], dst, msem.at[1]).start()

        @pl.when(jnp.logical_not(mine))
        def _():
            rcopy(xg.at[t], dst, msem.at[0], msem.at[1], {"dp": td, "cp": tx}).start()

        return carry

    ahead = 2
    for ch in chunks[:ahead]:
        ch.start()

    def step(s):
        if s + ahead < len(chunks):
            chunks[s + ahead].start()
        if s < 4:
            lax.fori_loop(s * slots // 4, (s + 1) * slots // 4, deal_out, 0)
        for k, at_step in enumerate(COT_STEPS):
            if at_step == s:
                send_cot(k)
        for n in range(4):
            for k in range(len(chunks)):
                if k + LAGS[k][n] == s:
                    getattr(chunks[k], TICKS[n])()

    step(0)
    vectors.tick1()
    step(1)
    vectors.tick2()
    step(2)
    vectors.tick3()
    step(3)
    vectors.tick4()

    def add_table(k, acc):
        return acc + vg[k].astype(F32)

    vec[...] = lax.fori_loop(1, Z * Y * C, add_table, vg[0].astype(F32))
    for k in range(bu3.shape[0]):
        per = width // tile
        bu3[k] = vec[BU + k // per:BU + k // per + 1, (k % per) * tile:(k % per + 1) * tile]

    wait_bytes(xr, msem.at[1])
    lrows = 128

    def first_norm(k, carry):
        at_rows = pl.ds(mult(k * lrows, lrows), lrows)
        n1, _ = norm_parts(xr[at_rows, :].astype(F32))
        a1[at_rows, :] = (n1 * vec[G1:G1 + 1, :] + vec[C1:C1 + 1, :]).astype(BF)
        return carry

    lax.fori_loop(0, rows // lrows, first_norm, 0)

    step(4)
    step(5)
    for k in range(3):
        chunks[k].tick5()
    keep = [pltpu.make_async_copy(wq, wq_o, osem.at[0])]
    keep[-1].start()

    quarters = (c, 3 - c)

    def q_at(i):
        return pl.ds(mult(quarters[i] * qrows, qrows), qrows)

    steps = width // tile
    for part in range(3):
        def project(n, carry, part=part):
            lanes = pl.ds(mult(n * tile, tile), tile)
            res = dot_nt(a1[...], wq[pl.ds(mult(part * width + n * tile, tile), tile), :]).astype(BF)
            if part == 0:
                qs[:, lanes] = res * jnp.asarray(HEAD_DIM ** -0.5, BF)
            else:
                to = ka if part == 1 else va
                for i in range(2):
                    to[q_at(i), lanes] = res[i * qrows:(i + 1) * qrows]
            return carry

        lax.fori_loop(0, steps, project, 0)
        if part > 0:
            to = ka if part == 1 else va
            for i in range(2):
                rcopy(to.at[q_at(i)], to.at[q_at(i)], msem.at[4 + 2 * (part - 1)], msem.at[5 + 2 * (part - 1)], dev(z, y, 1 - c, x)).start()
    step(6)
    wait_bytes(ka.at[pl.ds(0, rows)], msem.at[5])
    wait_bytes(va.at[pl.ds(0, rows)], msem.at[7])
    for src, out, s in ((qs, qs_o, 1), (ka, ka_o, 2), (va, va_o, 3), (xr, xr_o, 4), (vec, vec_o, 5)):
        keep.append(pltpu.make_async_copy(src, out, osem.at[s]))
        keep[-1].start()

    lane = lax.broadcasted_iota(jnp.int32, (qrows, 128), 1)
    kpos = lax.broadcasted_iota(jnp.int32, (qrows, qrows), 0)
    qpos = lax.broadcasted_iota(jnp.int32, (qrows, qrows), 1)
    groups = qrows // 8

    def pair_body(p, carry):
        lanes = pl.ds(mult(p * 128, 128), 128)
        for i in range(2):
            quarter = quarters[i]
            qp = qs[i * qrows:(i + 1) * qrows, lanes]
            zero = jnp.zeros_like(qp)
            qh = (jnp.where(lane < HEAD_DIM, qp, zero), jnp.where(lane >= HEAD_DIM, qp, zero))

            def scores(j, tops, diagonal=False):
                at_keys = pl.ds(mult(j * qrows, qrows), qrows)
                kj = ka[at_keys, lanes]
                new = []
                for h, sc in enumerate((sc0, sc1)):
                    s = dot_nt(kj, qh[h])
                    if diagonal:
                        s = jnp.where(kpos <= qpos, s, NEG_BIG)
                    sc[at_keys, :] = s
                    new.append(jnp.maximum(tops[h], jnp.max(s.reshape(groups, 8, qrows), axis=0)))
                return tuple(new)

            low = jnp.full((8, qrows), NEG_BIG, F32)
            tops = scores(quarter, lax.fori_loop(0, quarter, scores, (low, low)), True)
            tops = tuple(jnp.max(t, axis=0, keepdims=True) for t in tops)

            def values(j, state):
                at_keys = pl.ds(mult(j * qrows, qrows), qrows)
                vt = va[at_keys, lanes].T
                new = []
                for h, sc in enumerate((sc0, sc1)):
                    total, acc = state[h]
                    e = jnp.exp(sc[at_keys, :] - tops[h])
                    total = total + jnp.sum(e.reshape(groups, 8, qrows), axis=0)
                    acc = acc + dot_nn(vt[h * HEAD_DIM:(h + 1) * HEAD_DIM], e.astype(BF))
                    new.append((total, acc))
                return tuple(new)

            blank = (jnp.zeros((8, qrows), F32), jnp.zeros((HEAD_DIM, qrows), F32))
            state = lax.fori_loop(0, quarter + 1, values, (blank, blank))
            parts = []
            for h in range(2):
                total = jnp.sum(state[h][0], axis=0, keepdims=True)
                parts.append(state[h][1] / total)
                lse[p, i * 2 + h:i * 2 + h + 1, :] = tops[h] + jnp.log(total)
            at[i * qrows:(i + 1) * qrows, lanes] = jnp.concatenate(parts, axis=0).T.astype(BF)
        return carry

    per = 2
    for k in range(0, pairs, per):
        lax.fori_loop(k, k + per, pair_body, 0)
        step(7 + k // per)

    chunks[3].tick5()
    for src, out, s in ((wp, wp_o, 6), (at, at_o, 7), (lse, lse_o, 8)):
        keep.append(pltpu.make_async_copy(src, out, osem.at[s]))
        keep[-1].start()

    def attend_out(n, carry):
        lanes = pl.ds(mult(n * tile, tile), tile)
        res = dot_nt(at[...], wp[pl.ds(mult(n * tile, tile), tile), :])
        r[:, lanes] = xr[:, lanes].astype(F32) + res + vec[BP:BP + 1, lanes]
        return carry

    lax.fori_loop(0, steps, attend_out, 0)

    def second_norm(k, carry):
        at_rows = pl.ds(mult(k * lrows, lrows), lrows)
        n2, _ = norm_parts(r[at_rows, :])
        a2[at_rows, :] = (n2 * vec[G2:G2 + 1, :] + vec[C2:C2 + 1, :]).astype(BF)
        return carry

    lax.fori_loop(0, rows // lrows, second_norm, 0)
    step(10)
    step(11)
    for k in range(4, 8):
        chunks[k].tick5()
    for src, out, s in ((wu, wu_o, 9), (r, r_o, 10), (a2, a2_o, 11)):
        keep.append(pltpu.make_async_copy(src, out, osem.at[s]))
        keep[-1].start()

    def up(n, carry):
        lanes = pl.ds(mult(n * tile, tile), tile)
        u = dot_nt(a2[...], wu[lanes, :]) + bu3[n]
        sq_u = u * u
        t = jnp.tanh(TANH_SCALE * (u + CUBIC_TERM * sq_u * u))
        half_up = 0.5 * (1.0 + t)
        hd[:, lanes] = (u * half_up).astype(BF)
        slope = TANH_SCALE * (1.0 + 3.0 * CUBIC_TERM * sq_u)
        gp[:, lanes] = (half_up + 0.5 * u * (1.0 - t * t) * slope).astype(BF)
        return carry

    blocks = hd.shape[1] // tile
    for k in range(0, blocks, 4):
        lax.fori_loop(k, k + 4, up, 0)
        step(12 + k // 4)
    for src, out, s in ((hd, hd_o, 12), (gp, gp_o, 13)):
        keep.append(pltpu.make_async_copy(src, out, osem.at[s]))
        keep[-1].start()
    my_len = live_length(len_ref, deal_ref, (z * Y + y) * C + x)
    rowpos = lax.broadcasted_iota(jnp.int32, (qrows, 1), 0)
    parts = len(chunks) - 8
    wide = wd.shape[1] // X
    for k in range(parts):
        if k == 1:
            step(15)
        chunks[8 + k].tick5()
        cuts = [slice(h * wide + k * (wide // parts), h * wide + (k + 1) * (wide // parts)) for h in range(X)]
        for h, cut in enumerate(cuts):
            keep.append(pltpu.make_async_copy(wd.at[:, cut], wd_o.at[:, cut], osem.at[16 + X * k + h]))
            keep[-1].start()

        def down(n, carry, k=k, cuts=cuts):
            lanes = pl.ds(mult(n * tile, tile), tile)
            res = dot_nt(hd[:, cuts[0]], wd[lanes, cuts[0]])
            for cut in cuts[1:]:
                res = res + dot_nt(hd[:, cut], wd[lanes, cut])
            res = res + (r[:, lanes] + vec[BD:BD + 1, lanes] if k == 0 else acc[:, lanes])
            if k < parts - 1:
                acc[:, lanes] = res
            else:
                for i in range(2):
                    live = quarters[i] * qrows + rowpos < my_len
                    outw[i * qrows:(i + 1) * qrows, lanes] = jnp.where(live, res[i * qrows:(i + 1) * qrows], 0.0).astype(BF)
            return carry

        lax.fori_loop(0, steps, down, 0)
    keep.append(pltpu.make_async_copy(outw, out_o, osem.at[15]))
    keep[-1].start()

    for ch in chunks:
        ch.drain()
    vectors.drain()

    @pl.when(core_to == c)
    def _():
        wait_bytes(xr.at[pl.ds(0, rows - small)], msem.at[0])

    @pl.when(core_to != c)
    def _():
        wait_bytes(xr, msem.at[0])

    @pl.when(c == x)
    def _():
        wait_bytes(xr.at[pl.ds(0, qrows)], msem.at[2])

    @pl.when(c != x)
    def _():
        wait_bytes(xr, msem.at[2])

    wait_bytes(xr, msem.at[3])
    wait_bytes(ka.at[pl.ds(0, rows)], msem.at[4])
    wait_bytes(va.at[pl.ds(0, rows)], msem.at[6])
    for cp in keep:
        cp.wait()


def forward(lengths, dealing, cot, x_source, shards, vectors):
    slots, small, width = x_source.shape
    rows = cot.shape[0]
    ff = shards[2].shape[0] * Z * Y * C
    keys = rows * 2
    pairs = width // 128

    def arr(shape, dtype=BF):
        return jax.ShapeDtypeStruct(shape, dtype)

    outs = [
        arr((3 * width, width)), arr((width, width)), arr((ff, width)), arr((width, ff)),
        arr((rows, width)), arr((rows, width)), arr((rows, width)), arr((keys, width)), arr((keys, width)),
        arr((rows, width)), arr((pairs, 8, rows // 2), F32), arr((rows, width), F32), arr((rows, width)),
        arr((rows, ff)), arr((rows, ff)), arr((16, width), F32), arr((rows, width)),
    ]
    vm = pltpu.VMEM
    scratch = [
        vm((3 * width, width), BF), vm((width, width), BF), vm((ff, width), BF), vm((width, ff), BF),
        vm((rows, width), BF), vm((rows, width), BF), vm((rows, width), BF), vm((keys, width), BF),
        vm((keys, width), BF), vm((rows, width), BF), vm((pairs, 8, rows // 2), F32), vm((rows, width), F32),
        vm((rows, width), BF), vm((rows, ff), BF), vm((rows, ff), BF), vm((Z * Y * C, 16, width), BF),
        vm((16, width), F32), vm((ff // 256, 1, 256), F32), vm((keys, rows // 2), F32), vm((keys, rows // 2), F32),
        vm((rows, width), BF), vm(x_source.shape, BF), vm((rows, width), F32),
        vm(x_source.shape, BF), *[vm(a.shape, F32) for a in (*shards, *vectors)],
        pltpu.SemaphoreType.DMA((N_GATHER, 2, 5)), pltpu.SemaphoreType.DMA((2, 4)), pltpu.SemaphoreType.DMA((8,)),
        pltpu.SemaphoreType.DMA((24,)), pltpu.SemaphoreType.DMA((12,)),
    ]
    anyspec = pl.BlockSpec(memory_space=pl.ANY)
    smem = pl.BlockSpec(memory_space=pltpu.SMEM)
    return pl.pallas_call(
        forward_kernel,
        out_shape=outs,
        in_specs=[smem, smem] + [anyspec] * 13,
        out_specs=[anyspec] * len(outs),
        scratch_shapes=scratch,
        compiler_params=pltpu.CompilerParams(
            collective_id=0, has_side_effects=True, vmem_limit_bytes=60 * 1024 * 1024
        ),
        name="forward",
    )(lengths, dealing, cot, x_source, *shards, *vectors)


def when(cond):
    if isinstance(cond, bool):
        return (lambda f: f()) if cond else (lambda f: None)
    return pl.when(cond)


class Reduce:
    S1, R1, S2, R2, S3, R3, S4, R4, S5, R5 = range(10)

    def __init__(self, grad, R, step, c0, C, zlist, bufs, out, out_c0, sems, k, where, kind, turned):
        self.kind = kind
        self.grad, self.R, self.step, self.c0, self.cn, self.zlist = grad, R, step, c0, C, zlist
        self.r1, self.r2, self.r3, self.r4, self.r5 = bufs
        self.out, self.out_c0, self.sems, self.k = out, out_c0, sems, k
        self.z, self.y, self.c, self.x, _ = where
        y, x = self.y, self.x
        self.o = o = 1 if turned else self.c
        self.y2, self.x2 = (y + o) % 2, (x + 1 - o) % 2
        self.y3, self.x3 = (y + 1 - o) % 2, (x + o) % 2
        self.every = len(zlist) == Z

    def sem(self, which):
        return self.sems.at[self.k, which]

    def rows(self, z, y, c):
        return pl.ds(mult(((z * Y + y) * C + c) * self.R, 16), self.R)

    def cols(self, x):
        return pl.ds(mult(x * self.step + self.c0, 128), self.cn)

    def at(self, z, y, c, x):
        return self.grad.at[self.rows(z, y, c), self.cols(x)]

    def add(self, rows, cols, got):
        self.grad[rows, cols] = (self.grad[rows, cols].astype(F32) + got.astype(F32)).astype(BF)

    def zidx(self, zi):
        return zi if self.every else self.zlist[0]

    def start(self):
        z, y, c, x = self.z, self.y, self.c, self.x
        to = dev(z, y, 1 - c, x)
        for zi, zz in enumerate(self.zlist):
            for yy in range(Y):
                for xx in range(X):
                    rcopy(
                        self.at(zz, yy, 1 - c, xx), self.r1.at[zi * Y + yy, xx],
                        self.sem(self.S1), self.sem(self.R1), to,
                    ).start()

    def tick2(self):
        z, y, c, x, o = self.z, self.y, self.c, self.x, self.o
        wait_bytes(self.r1, self.sem(self.R1))

        def body(e, carry):
            rows = self.rows(self.zidx(e // Y), e % Y, c)
            for xx in range(X):
                self.add(rows, self.cols(xx), self.r1[e, xx])
            return carry

        lax.fori_loop(0, len(self.zlist) * Y, body, 0)
        to = dev(z, self.y2, c, self.x2)
        for zi, zz in enumerate(self.zlist):
            for w in range(2):
                yy = w * (1 - o) + (1 - y) * o
                xx = (1 - x) * (1 - o) + w * o
                rcopy(self.at(zz, yy, c, xx), self.r2.at[zi * 2 + w], self.sem(self.S2), self.sem(self.R2), to).start()

    def tick3(self):
        z, y, c, x, o = self.z, self.y, self.c, self.x, self.o
        wait_bytes(self.r2, self.sem(self.R2))

        def body(e, carry):
            w = e % 2
            yy = w * (1 - o) + y * o
            xx = x * (1 - o) + w * o
            self.add(self.rows(self.zidx(e // 2), yy, c), self.cols(xx), self.r2[e])
            return carry

        lax.fori_loop(0, len(self.zlist) * 2, body, 0)
        if self.kind == 2:
            mate = z + 1 - 2 * (z % 2)
            for slot, zz in enumerate((mate, 3 - mate)):
                for w in range(2):
                    rcopy(
                        self.left(zz, w), self.r4.at[slot * 2 + w], self.sem(self.S4), self.sem(self.R4),
                        dev(mate, y, c, x),
                    ).start()
            return
        to = dev(z, self.y3, c, self.x3)
        for zi, zz in enumerate(self.zlist):
            rcopy(self.at(zz, self.y3, c, self.x3), self.r3.at[zi], self.sem(self.S3), self.sem(self.R3), to).start()

    def left_cut(self, zz, w):
        o = self.o
        return self.rows(zz, w * (1 - o) + self.y * o, self.c), self.cols(self.x * (1 - o) + w * o)

    def left(self, zz, w):
        return self.grad.at[self.left_cut(zz, w)]

    def first_hop(self, k):
        return [(k ^ 1, k, 0), ((3 - k) ^ 1, 3 - k, 1)]

    def tick4(self):
        z, y, c, x = self.z, self.y, self.c, self.x
        if self.kind == 2:
            wait_bytes(self.r4, self.sem(self.R4))
            for w in range(2):
                self.add(*self.left_cut(3 - z, w), self.r4[2 + w])
                rcopy(
                    self.left(3 - z, w), self.r5.at[w], self.sem(self.S5), self.sem(self.R5), dev(3 - z, y, c, x)
                ).start()
            for w in range(2):
                self.add(*self.left_cut(z, w), self.r4[w])
            return
        wait_bytes(self.r3, self.sem(self.R3))

        def body(zi, carry):
            self.add(self.rows(self.zidx(zi), y, c), self.cols(x), self.r3[zi])
            return carry

        lax.fori_loop(0, len(self.zlist), body, 0)
        if self.every:
            mate = z + 1 - 2 * (z % 2)
            for slot, zz in enumerate((mate, 3 - mate)):
                rcopy(
                    self.at(zz, y, c, x), self.r4.at[slot], self.sem(self.S4), self.sem(self.R4), dev(mate, y, c, x)
                ).start()
        else:
            k = self.zlist[0]
            for sender, taker, slot in self.first_hop(k):
                @pl.when(z == sender)
                def _(taker=taker, slot=slot):
                    rcopy(
                        self.at(k, y, c, x), self.r4.at[slot], self.sem(self.S4), self.sem(self.R4),
                        dev(taker, y, c, x),
                    ).start()

    def tick5(self):
        z, y, c, x = self.z, self.y, self.c, self.x
        if self.kind == 2:
            wait_bytes(self.r5, self.sem(self.R5))
            for w in range(2):
                self.add(*self.left_cut(z, w), self.r5[w])
            rcopy(
                self.at(z, self.y3, c, self.x3), self.r3.at[0], self.sem(self.S3), self.sem(self.R3),
                dev(z, self.y3, c, self.x3),
            ).start()
            return
        k = self.zlist[0]

        def take(zz, slot):
            self.add(self.rows(zz, y, c), self.cols(x), self.r4[slot])

        def pass_on(zz):
            rcopy(self.at(zz, y, c, x), self.r5.at[0], self.sem(self.S5), self.sem(self.R5), dev(zz, y, c, x)).start()

        if self.every:
            wait_bytes(self.r4, self.sem(self.R4))
            take(3 - z, 1)
            pass_on(3 - z)
            take(z, 0)
        else:
            @pl.when(z == 3 - k)
            def _():
                wait_bytes(self.r4.at[1], self.sem(self.R4))
                take(k, 1)
                pass_on(k)

            @pl.when(z == k)
            def _():
                wait_bytes(self.r4.at[0], self.sem(self.R4))
                take(k, 0)

    def tick6(self):
        z, y, c, x = self.z, self.y, self.c, self.x

        @when(True if self.every else z == self.zlist[0])
        def _():
            last, sem = (self.r3, self.R3) if self.kind == 2 else (self.r5, self.R5)
            wait_bytes(last, self.sem(sem))
            own = self.grad[self.rows(z, y, c), self.cols(x)].astype(F32)
            self.out[:, self.out_c0:self.out_c0 + self.cn] = own + last[0].astype(F32)

    def drain(self):
        z = self.z
        wait_bytes(self.r1, self.sem(self.S1))
        wait_bytes(self.r2, self.sem(self.S2))
        wait_bytes(self.r3, self.sem(self.S3))
        if self.every:
            wait_bytes(self.r4, self.sem(self.S4))
            wait_bytes(self.r5, self.sem(self.S5))
        else:
            k = self.zlist[0]
            for sender, _, slot in self.first_hop(k):
                @pl.when(z == sender)
                def _():
                    wait_bytes(self.r4.at[0], self.sem(self.S4))

            @pl.when(z == 3 - k)
            def _():
                wait_bytes(self.r5, self.sem(self.S5))


TURNED_BACK = ()
KINDS_BACK = (2,) * 4 + (1,) * 9


def reduce_shapes(width, ff):
    n = Z * Y * C
    every = list(range(Z))
    half = width // X
    wide = ff // X
    shapes = [("d", width // n, wide, k * (wide // 4), wide // 4, every, k * (wide // 4)) for k in range(4)]
    shapes += [("u", ff // n, half, 0, half, [k], 0) for k in range(Z)]
    shapes += [("p", width // n, half, 0, half, every, 0)]
    shapes += [("q", 3 * width // n, half, 0, half, [k], 0) for k in range(Z)]
    return shapes


(
    D0, D1, D2, D3, U0, U1, U2, U3, PJ, Q0, Q1, Q2, Q3, GIVE, OUT, HOP,
) = range(16)
(
    F2, F3, F4, F5, F6, F7, F8, F9, F10, F11, NORM_TWO, PROJ, A00, A01, A10, A11, A20, A21, A30, A31, A40, A41, A50,
    A51, NORM_ONE, QA, MERGE, QB, QC, QD, DA, LN,
) = range(100, 132)

PLAN = (
    F2, (U0, 1), F4, (U0, 2), F5, (U2, 1), (D0, 1), (D1, 1), F7, (U2, 2), F8, (U1, 1), (D0, 2), F9, (D1, 2), F10,
    (U1, 2), (U0, 3), F11, (U3, 1), (D2, 1), (D3, 1), NORM_TWO, (U2, 3), PROJ, (PJ, 1), (U3, 2), (D2, 2), (D0, 3),
    (D3, 2), A00, (PJ, 2), (D1, 3), (OUT, 0), A01, (OUT, 1), A10, (U1, 3), (D0, 4), (OUT, 2), A11, (U0, 4), (D1, 4),
    (U2, 4), (OUT, 3), A20, (OUT, 4), A21, (U3, 3), (D0, 5), (U0, 5), (OUT, 5), A30, (OUT, 6), A31, (D2, 3), (D1, 5),
    (U2, 5), (OUT, 7), A40, (D3, 3), A50, (PJ, 3), (D2, 4), (U1, 4), A51, (U3, 4), NORM_ONE, (D3, 4), QA, (Q0, 1),
    (PJ, 4), MERGE, (D2, 5), QB, (Q1, 1), (U1, 5), (Q0, 2), QC, (Q2, 1), (U3, 5), QD, (Q3, 1), (Q1, 2), (D3, 5), DA,
    (Q3, 2), (Q0, 3), (PJ, 5), LN, (U2, 6), (Q2, 2), (GIVE, 0), (U0, 6), (D0, 6), (D1, 6), (GIVE, 1), (HOP, 0),
    (Q1, 3), (D2, 6), (U1, 6), (U3, 6), (GIVE, 2), (HOP, 1), (Q2, 3), (D3, 6), (GIVE, 3), (Q3, 3), (Q0, 4), (HOP, 2),
    (PJ, 6), (Q1, 4), (Q0, 5), (HOP, 3), (Q2, 4), (Q1, 5), (Q3, 4), (Q2, 5), (HOP, 4), (Q3, 5), (Q0, 6), (Q1, 6),
    (Q2, 6), (Q3, 6),
)


def part_actions(plan):
    parts, now = {}, None
    for item in plan:
        if isinstance(item, int):
            now = parts.setdefault(item, [])
        else:
            now.append(item)
    return parts


def backward_kernel(*refs):
    names = (
        "len_ref", "deal_ref", "wq_i", "wp_i", "wu_i", "wd_i", "xr_i", "gw_i", "qs_i", "ka_i", "va_i", "at_i",
        "lse_i", "r_i", "a2_i", "hd_i", "gp_i", "vec_i", "out_i", "og_q", "og_p", "og_u", "og_d", "osum", "ret",
        "out_n", "wq", "wp", "xr", "g", "qs", "ka", "va", "at", "lse", "r", "a2", "vec", "gt", "d2", "dr", "drl",
        "do", "gq", "gp_", "gu", "gd", "wd_t", "wu_t", "hd_t", "gp_t", "dka", "dva", "own_v", "sv", "rk", "rv", "dm",
        "vs", "vr", "bub", "lsem", "tsem", "rsem", "msem", "vsem",
    )
    env = dict(zip(names, refs[: len(names)]))
    env.update(a1=env["a2"], own_k=env["d2"], sk=env["drl"], dx=env["do"])
    bufs = refs[len(names):]
    e = type("Refs", (), env)
    where = coords()
    z, y, c, x, d = where
    rows, width = e.g.shape
    ff = e.hd_i.shape[1]
    qrows = rows // 2
    pairs = width // 128
    tile = 256
    lrows = 128
    steps = width // tile
    quarters = (c, 3 - c)
    theirs = (1 - c, 2 + c)

    def at_quarter(k):
        return pl.ds(mult(k * qrows, qrows), qrows)

    entered = enter(Z * Y * C * X)

    loads = {}
    for k, (src, dst) in enumerate(
        (
            ("gw_i", "g"), ("a2_i", "a2"), ("r_i", "r"), ("vec_i", "vec"), ("wp_i", "wp"), ("at_i", "at"),
            ("qs_i", "qs"), ("ka_i", "ka"), ("va_i", "va"), ("lse_i", "lse"), ("xr_i", "xr"), ("wq_i", "wq"),
        )
    ):
        loads[dst] = pltpu.make_async_copy(env[src], env[dst], e.lsem.at[k])

    def tile_of(idx):
        block = idx // 3
        return (block % 2) * 2 * 3 + (block // 2) * 3 + idx % 3

    def tile_copies(idx):
        n = tile_of(idx)
        slot = idx % 2
        cut = pl.ds(mult(n * tile, tile), tile)
        return (
            pltpu.make_async_copy(e.wd_i.at[:, cut], e.wd_t.at[slot], e.tsem.at[0, slot]),
            pltpu.make_async_copy(e.gp_i.at[:, cut], e.gp_t.at[slot], e.tsem.at[1, slot]),
            pltpu.make_async_copy(e.hd_i.at[:, cut], e.hd_t.at[slot], e.tsem.at[2, slot]),
            pltpu.make_async_copy(e.wu_i.at[cut, :], e.wu_t.at[slot], e.tsem.at[3, slot]),
        )

    loads["g"].start()
    for cp in tile_copies(0):
        cp.start()
    loads["a2"].start()
    for name in ("r", "vec", "wp", "at", "qs", "ka", "va", "lse", "xr", "wq"):
        loads[name].start()

    def send_out(k):
        i, part = k // 4, k % 4
        some = qrows // 4
        same = jnp.logical_and(x == c, x == i)
        src = e.out_i.at[pl.ds(i * qrows + part * some, some)]
        dst = e.out_n.at[pl.ds(mult(((i + c) % 2) * qrows + part * some, some), some)]

        @pl.when(same)
        def _():
            lcopy(src, dst, e.msem.at[1]).start()

        @pl.when(jnp.logical_not(same))
        def _():
            rcopy(src, dst, e.msem.at[0], e.msem.at[1], dev(z, y, x, i)).start()

    grads = {"q": (e.gq, e.og_q), "p": (e.gp_, e.og_p), "u": (e.gu, e.og_u), "d": (e.gd, e.og_d)}
    chunks = []
    for k, (name, R, step, c0, cn, zlist, oc) in enumerate(reduce_shapes(width, ff)):
        grad, out = grads[name]
        chunks.append(Reduce(grad, R, step, c0, cn, zlist, bufs[5 * k:5 * k + 5], out, oc, e.rsem, k, where, KINDS_BACK[k], k in TURNED_BACK))
    parts = part_actions(PLAN)

    def after(part):
        for name, k in parts.get(part, ()):
            if name < len(chunks):
                ch = chunks[name]
                (ch.start, ch.tick2, ch.tick3, ch.tick4, ch.tick5, ch.tick6)[k - 1]()
            elif name == GIVE:
                give(k)
            elif name == OUT:
                send_out(k)
            else:
                land(k)
                if k < 4:
                    hop(k + 1)


    my_len = live_length(e.len_ref, e.deal_ref, (z * Y + y) * C + x)
    rowpos = lax.broadcasted_iota(jnp.int32, (lrows, 1), 0)
    loads["g"].wait()
    blank = jnp.zeros((1, width), F32)
    total_bd = blank
    for k in range(rows // lrows):
        base = quarters[k * lrows // qrows] * qrows + (k * lrows) % qrows
        live = base + rowpos < my_len
        part = jnp.where(live, e.g[k * lrows:(k + 1) * lrows, :], jnp.zeros((), BF))
        e.g[k * lrows:(k + 1) * lrows, :] = part
        e.gt[:, k * lrows:(k + 1) * lrows] = part.T
        total_bd = total_bd + jnp.sum(part.astype(F32), axis=0, keepdims=True)
    e.d2[...] = jnp.zeros_like(e.d2)
    loads["a2"].wait()

    ff_tiles = ff // tile
    def ffn(idx, carry, acting=True):
        slot = idx % 2
        n = tile_of(idx)
        cut = pl.ds(mult(n * tile, tile), tile)

        @pl.when(idx + 1 < ff_tiles)
        def _():
            for cp in tile_copies(idx + 1):
                cp.start()

        for cp in tile_copies(idx):
            cp.wait()
        du = (e.gp_t[slot].astype(F32) * dot_nn(e.g[...], e.wd_t[slot])).astype(BF)
        e.bub[n] = jnp.sum(du.astype(F32), axis=0, keepdims=True)
        e.gd[:, cut] = dot_nn(e.gt[...], e.hd_t[slot]).astype(BF)
        e.gu[cut, :] = dot_tn(du, e.a2[...]).astype(BF)
        e.d2[...] += dot_nn(du, e.wu_t[slot])
        for k in range(2, ff_tiles) if acting else ():
            if F2 + k - 2 in parts:
                @pl.when(idx == k)
                def _(k=k):
                    after(F2 + k - 2)

        return carry

    def ffn_first(idx, carry):
        return ffn(idx, carry, False)

    lax.fori_loop(0, 2, ffn_first, 0)

    entered()

    lax.fori_loop(2, ff_tiles, ffn, 0)

    loads["r"].wait()
    loads["vec"].wait()

    def norm_two(k, sums):
        at_rows = pl.ds(mult(k * lrows, lrows), lrows)
        n2, rstd = norm_parts(e.r[at_rows, :])
        da = e.d2[at_rows, :]
        ee = da * e.vec[G2:G2 + 1, :]
        gg = e.g[at_rows, :].astype(F32)
        m1 = jnp.mean(ee, axis=-1, keepdims=True)
        m2 = jnp.mean(ee * n2, axis=-1, keepdims=True)
        dr = gg + (ee - m1 - n2 * m2) * rstd
        e.dr[at_rows, :] = dr
        e.drl[at_rows, :] = dr.astype(BF)
        return (
            sums[0] + jnp.sum(da * n2, axis=0, keepdims=True),
            sums[1] + jnp.sum(da, axis=0, keepdims=True),
            sums[2] + jnp.sum(dr, axis=0, keepdims=True),
        )

    sum_g2, sum_c2, sum_bp = lax.fori_loop(0, rows // lrows, norm_two, (blank, blank, blank))

    after(NORM_TWO)

    loads["wp"].wait()
    loads["at"].wait()

    def proj_back(n, carry):
        cut = pl.ds(mult(n * tile, tile), tile)
        e.do[:, cut] = dot_nn(e.drl[...], e.wp[:, cut]).astype(BF)
        e.gp_[cut, :] = dot_tn(e.drl[:, cut], e.at[...]).astype(BF)
        return carry

    lax.fori_loop(0, steps, proj_back, 0)
    after(PROJ)

    for name in ("qs", "ka", "va", "lse"):
        loads[name].wait()
    lane = lax.broadcasted_iota(jnp.int32, (qrows, 128), 1)
    kpos = lax.broadcasted_iota(jnp.int32, (qrows, qrows), 0)
    qpos = lax.broadcasted_iota(jnp.int32, (qrows, qrows), 1)

    def split(v):
        zero = jnp.zeros_like(v)
        return jnp.where(lane < HEAD_DIM, v, zero), jnp.where(lane >= HEAD_DIM, v, zero)

    def pair_body(p, carry):
        lanes = pl.ds(mult(p * 128, 128), 128)
        e.dka[...] = jnp.zeros_like(e.dka)
        e.dva[...] = jnp.zeros_like(e.dva)
        for i in range(2):
            quarter = quarters[i]
            own = slice(i * qrows, (i + 1) * qrows)
            qp, dop = e.qs[own, lanes], e.do[own, lanes]
            qh, doh = split(qp), split(dop)
            qq, dd = jnp.concatenate(qh, axis=0), jnp.concatenate(doh, axis=0)
            prod = (dop.astype(F32) * e.at[own, lanes].astype(F32)).T
            delta = [jnp.sum(prod[h * HEAD_DIM:(h + 1) * HEAD_DIM], axis=0, keepdims=True) for h in range(2)]
            logs = [e.lse[p, i * 2 + h:i * 2 + h + 1, :] for h in range(2)]

            def keys(j, dq, diagonal=False):
                at_keys = pl.ds(mult(j * qrows, qrows), qrows)
                kj, vj = e.ka[at_keys, lanes], e.va[at_keys, lanes]
                kt = kj.T
                probs, grads_s, new = [], [], []
                for h in range(2):
                    s = dot_nt(kj, qh[h])
                    if diagonal:
                        s = jnp.where(kpos <= qpos, s, NEG_BIG)
                    pt = jnp.exp(s - logs[h])
                    ds = (pt * (dot_nt(vj, doh[h]) - delta[h])).astype(BF)
                    probs.append(pt.astype(BF))
                    grads_s.append(ds)
                    new.append(dq[h] + dot_nn(kt[h * HEAD_DIM:(h + 1) * HEAD_DIM], ds))
                e.dva[at_keys, :] += dot_nn(jnp.concatenate(probs, axis=1), dd)
                e.dka[at_keys, :] += dot_nn(jnp.concatenate(grads_s, axis=1), qq)
                return tuple(new)

            none = jnp.zeros((HEAD_DIM, qrows), F32)
            dq = lax.fori_loop(0, quarter, keys, (none, none))
            dq = keys(quarter, dq, True)
            e.dm[own, lanes] = (jnp.concatenate(dq, axis=0).T * HEAD_DIM ** -0.5).astype(BF)
            for k in range(pairs):
                if A00 + 2 * k + i in parts:
                    @pl.when(p == k)
                    def _(k=k, i=i):
                        after(A00 + 2 * k + i)

        for i in range(2):
            own = slice(i * qrows, (i + 1) * qrows)
            e.own_k[own, lanes] = e.dka[at_quarter(quarters[i]), :]
            e.own_v[own, lanes] = e.dva[at_quarter(quarters[i]), :]
            e.sk[own, lanes] = e.dka[at_quarter(theirs[i]), :].astype(BF)
            e.sv[own, lanes] = e.dva[at_quarter(theirs[i]), :].astype(BF)
        for k in range(pairs // 2):
            @pl.when(p == 2 * k + 1)
            def _(k=k):
                cut = slice(2 * k * 128, (2 * k + 2) * 128)
                for src, dst, s in ((e.sk, e.rk, 2), (e.sv, e.rv, 4)):
                    rcopy(
                        src.at[:, cut], dst.at[:, cut], e.msem.at[s], e.msem.at[s + 1], dev(z, y, 1 - c, x)
                    ).start()
        return carry

    lax.fori_loop(0, pairs, pair_body, 0)

    loads["xr"].wait()

    def norm_one(k, carry):
        at_rows = pl.ds(mult(k * lrows, lrows), lrows)
        n1, _ = norm_parts(e.xr[at_rows, :].astype(F32))
        e.a1[at_rows, :] = (n1 * e.vec[G1:G1 + 1, :] + e.vec[C1:C1 + 1, :]).astype(BF)
        return carry

    lax.fori_loop(0, rows // lrows, norm_one, 0)
    after(NORM_ONE)

    def qkv_grad(n, carry):
        cut = pl.ds(mult(n * tile, tile), tile)
        e.gq[cut, :] = dot_tn(e.dm[:, cut], e.a1[...]).astype(BF)
        return carry

    lax.fori_loop(0, 3, qkv_grad, 0)
    after(QA)
    wait_bytes(e.rk, e.msem.at[3])
    wait_bytes(e.rv, e.msem.at[5])
    for part, (mine, got) in enumerate(((e.own_k, e.rk), (e.own_v, e.rv))):
        def merge(k, carry, part=part, mine=mine, got=got):
            at_rows = pl.ds(mult(k * lrows, lrows), lrows)
            e.dm[at_rows, (part + 1) * width:(part + 2) * width] = (
                mine[at_rows, :] + got[at_rows, :].astype(F32)
            ).astype(BF)
            return carry

        lax.fori_loop(0, rows // lrows, merge, 0)
    after(MERGE)
    for name, first, stop in ((QB, 3, 5), (QC, 5, 7), (QD, 7, 9)):
        lax.fori_loop(first, stop, qkv_grad, 0)
        after(name)
    loads["wq"].wait()

    def input_back(n, carry):
        cut = pl.ds(mult(n * tile, tile), tile)
        e.d2[:, cut] = dot_nn(e.dm[...], e.wq[:, cut])
        return carry

    lax.fori_loop(0, steps, input_back, 0)
    after(DA)

    def norm_one_back(k, sums):
        at_rows = pl.ds(mult(k * lrows, lrows), lrows)
        n1, rstd = norm_parts(e.xr[at_rows, :].astype(F32))
        da = e.d2[at_rows, :]
        ee = da * e.vec[G1:G1 + 1, :]
        m1 = jnp.mean(ee, axis=-1, keepdims=True)
        m2 = jnp.mean(ee * n1, axis=-1, keepdims=True)
        e.dx[at_rows, :] = (e.dr[at_rows, :] + (ee - m1 - n1 * m2) * rstd).astype(BF)
        return sums[0] + jnp.sum(da * n1, axis=0, keepdims=True), sums[1] + jnp.sum(da, axis=0, keepdims=True)

    sum_g1, sum_c1 = lax.fori_loop(0, rows // lrows, norm_one_back, (blank, blank))

    e.vs[0] = jnp.zeros_like(e.vs[0])
    for row, value in ((G1, sum_g1), (C1, sum_c1), (BP, sum_bp), (G2, sum_g2), (C2, sum_c2), (BD, total_bd)):
        e.vs[0, row:row + 1, :] = value
    per = width // tile
    for k in range(ff_tiles):
        e.vs[0, BU + k // per:BU + k // per + 1, (k % per) * tile:(k % per + 1) * tile] = e.bub[k]
    hops = (
        dev(z, y, 1 - c, x), dev(z, y, c, 1 - x), dev(z, 1 - y, c, x),
        dev(z + 1 - 2 * (z % 2), y, c, x), dev((z + 2) % 4, y, c, x),
    )

    def hop(k):
        rcopy(e.vs.at[k], e.vr.at[k], e.vsem.at[0, k], e.vsem.at[1, k], hops[k]).start()

    def land(k):
        wait_bytes(e.vr.at[k], e.vsem.at[1, k])
        e.vs[k + 1] = e.vs[k] + e.vr[k]

    hop(0)

    small = e.ret.shape[1]
    per_quarter = qrows // small
    slot = (z * Y + y) * C + x

    def give_back(k, carry):
        i = (k + x) % 2
        e8 = (k // 2 + d) % per_quarter
        td = ((i + c) % 2) * per_quarter + e8
        src = e.dx.at[pl.ds(mult(i * qrows + e8 * small, small), small)]
        mine = jnp.logical_and(td == d, x == i)

        @pl.when(mine)
        def _():
            lcopy(src, e.ret.at[slot], e.msem.at[7]).start()

        @pl.when(jnp.logical_not(mine))
        def _():
            rcopy(src, e.ret.at[slot], e.msem.at[6], e.msem.at[7], {"dp": td, "cp": i}).start()

        return carry

    share = per_quarter // 2

    def give(k):
        lax.fori_loop(k * share, (k + 1) * share, give_back, 0)

    after(LN)
    own = width // (Z * Y * C)
    e.osum[0:6, :] = pltpu.roll(e.vs[5, 0:6, :], (width - d * own) % width, 1)[:, :tile]
    long = ff // (Z * Y * C)
    per_row = width // long
    e.osum[6:7, :] = pltpu.roll(
        e.vs[5, pl.ds(BU + d // per_row, 1), :], (width - (d % per_row) * long) % width, 1
    )[:, :tile]
    e.osum[7:8, :] = jnp.zeros((1, tile), F32)
    wait_bytes(e.dx, e.msem.at[7])

    for ch in chunks:
        ch.drain()
    for k in range(5):
        wait_bytes(e.vr.at[k], e.vsem.at[0, k])
    wait_bytes(e.rk, e.msem.at[2])
    wait_bytes(e.rv, e.msem.at[4])

    @pl.when((x + c) % 2 == d // per_quarter)
    def _():
        wait_bytes(e.dx.at[pl.ds(0, rows - small)], e.msem.at[6])

    @pl.when((x + c) % 2 != d // per_quarter)
    def _():
        wait_bytes(e.dx, e.msem.at[6])

    @pl.when(c == x)
    def _():
        wait_bytes(e.dx.at[pl.ds(0, qrows)], e.msem.at[0])

    @pl.when(c != x)
    def _():
        wait_bytes(e.dx, e.msem.at[0])

    wait_bytes(e.dx, e.msem.at[1])


def backward(lengths, dealing, saved, shards):
    wq, wp, wu, wd, xr, gw, qs, ka, va, at, lse, r, a2, hd, gp, vec, outw = saved
    rows, width = xr.shape
    ff = hd.shape[1]
    n = Z * Y * C
    keys = ka.shape[0]
    small = rows // n
    pairs = width // 128

    def arr(shape, dtype=BF):
        return jax.ShapeDtypeStruct(shape, dtype)

    outs = [arr(s.shape, F32) for s in shards] + [
        arr((8, 256), F32), arr((n, small, width)), arr((rows, width)),
    ]
    vm = pltpu.VMEM
    acts = vm((rows, width), BF)
    acts32 = vm((rows, width), F32)
    scratch = [
        vm(wq.shape, BF), vm(wp.shape, BF), acts, acts, acts, vm(ka.shape, BF), vm(va.shape, BF), acts,
        vm(lse.shape, F32), acts32, acts, vm(vec.shape, F32), vm((width, rows), BF), acts32, acts32, acts, acts,
        vm(wq.shape, BF), vm(wp.shape, BF), vm(wu.shape, BF), vm(wd.shape, BF),
        vm((2, width, 256), BF), vm((2, 256, width), BF), vm((2, rows, 256), BF), vm((2, rows, 256), BF),
        vm((keys, 128), F32), vm((keys, 128), F32),
        acts32, acts, acts, acts, vm((rows, 3 * width), BF),
        vm((6, 16, width), F32), vm((5, 16, width), F32), vm((ff // 256, 1, 256), F32),
        pltpu.SemaphoreType.DMA((12,)), pltpu.SemaphoreType.DMA((4, 2)), pltpu.SemaphoreType.DMA((13, 10)),
        pltpu.SemaphoreType.DMA((8,)), pltpu.SemaphoreType.DMA((2, 5)),
    ]
    for kind, (_, R, _, _, cn, zlist, _) in zip(KINDS_BACK, reduce_shapes(width, ff)):
        k = len(zlist)
        last = (1, 4, 2) if kind == 2 else (k, 2, 1)
        scratch += [vm((2 * k, 2, R, cn), BF)] + [vm((m, R, cn), BF) for m in (2 * k,) + last]
    anyspec = pl.BlockSpec(memory_space=pl.ANY)
    smem = pl.BlockSpec(memory_space=pltpu.SMEM)
    vmem = pl.BlockSpec(memory_space=pltpu.VMEM)
    return pl.pallas_call(
        backward_kernel,
        out_shape=outs,
        in_specs=[smem, smem] + [anyspec] * len(saved),
        out_specs=[vmem] * 5 + [anyspec] * 2,
        scratch_shapes=scratch,
        compiler_params=pltpu.CompilerParams(
            collective_id=1, has_side_effects=True, vmem_limit_bytes=67043328
        ),
        name="backward",
    )(lengths, dealing, *saved)


def finish_kernel(deal_ref, gq, gp, gu, gd, sums, ret, out, grad_o, out_o, gq_o, gp_o, gu_o, gd_o, *rows_o):
    for s in range(ret.shape[0]):
        grad_o[s] = ret[deal_ref[s]]
    for src, dst in ((out, out_o), (gq, gq_o), (gp, gp_o), (gu, gu_o), (gd, gd_o)):
        dst[...] = src[...]
    for k, row in enumerate(rows_o):
        row[...] = sums[k:k + 1, :row.shape[1]]


def finish(dealing, grads, sums, ret, out, own, long):
    def like(a):
        return jax.ShapeDtypeStruct(a.shape, a.dtype)

    outs = [like(ret), like(out)] + [like(g) for g in grads]
    outs += [jax.ShapeDtypeStruct((1, own), F32)] * 6 + [jax.ShapeDtypeStruct((1, long), F32)]
    vmem = pl.BlockSpec(memory_space=pltpu.VMEM)
    return pl.pallas_call(
        finish_kernel,
        out_shape=outs,
        in_specs=[pl.BlockSpec(memory_space=pltpu.SMEM)] + [vmem] * 7,
        out_specs=[vmem] * len(outs),
        name="finish",
    )(dealing, *grads, sums, ret, out)


def slice_plan(
    x_source, cotangent, lengths, dealing, qkv_weight, proj_weight, up_weight, down_weight,
    first_gain, first_shift, proj_bias, second_gain, second_shift, up_bias, down_bias,
):
    shards = [w.T for w in (qkv_weight, proj_weight, up_weight, down_weight)]
    vectors = [
        v[None] for v in (first_gain, first_shift, proj_bias, second_gain, second_shift, down_bias, up_bias)
    ]
    saved = forward(lengths, dealing, cotangent[0], x_source, shards, vectors)
    gq, gp, gu, gd, sums, ret, out = backward(lengths, dealing, saved, shards)
    done = finish(dealing, (gq, gp, gu, gd), sums, ret, out, first_gain.shape[0], up_bias.shape[0])
    input_grad, output, gq, gp, gu, gd = done[:6]
    by_row = [v.reshape(-1) for v in done[6:]]
    return (
        output[None], input_grad, gq.T, gp.T, gu.T, gd.T,
        by_row[G1], by_row[C1], by_row[BP], by_row[G2], by_row[C2], by_row[6], by_row[BD],
    )


def layer_norm(values, scaling, offset):
    centered = values - jnp.mean(values, axis=-1, keepdims=True)
    spread = jnp.mean(centered * centered, axis=-1, keepdims=True)
    return centered * lax.rsqrt(spread + EPSILON) * scaling + offset


def gelu_tanh(values):
    return (
        0.5
        * values
        * (1.0 + jnp.tanh(TANH_SCALE * (values + CUBIC_TERM * values * values * values)))
    )


def grouped(array, block_seqs):
    return array.reshape(
        (array.shape[0] // block_seqs, block_seqs, array.shape[1], HEADS, array.shape[2] // HEADS)
    )


def grouped_stats(array, block_seqs):
    return array.reshape((array.shape[0] // block_seqs, block_seqs) + array.shape[1:])


def joined(array):
    return array.reshape(
        (array.shape[0] * array.shape[1], array.shape[2], array.shape[3] * array.shape[4])
    )


def masked_scores(queries, key_rows, query_start, score_scale):
    scores = (
        jnp.einsum("bqhd,bkhd->bhqk", queries, key_rows, preferred_element_type=jnp.float32)
        * score_scale
    )
    query_pos = query_start + jnp.arange(queries.shape[1])
    key_pos = jnp.arange(key_rows.shape[1])
    return jnp.where(key_pos[None, :] <= query_pos[:, None], scores, NEG_BIG)


def attend(inputs, query_start, score_scale):
    queries, key_rows, val_rows = inputs
    scores = masked_scores(queries, key_rows, query_start, score_scale)
    row_top = jnp.max(scores, axis=-1, keepdims=True)
    exponent = jnp.exp(scores - row_top)
    totals = jnp.sum(exponent, axis=-1, keepdims=True)
    weights = (exponent / totals).astype(jnp.bfloat16)
    attended = jnp.einsum("bhqk,bkhd->bqhd", weights, val_rows, preferred_element_type=jnp.float32)
    return (attended.astype(jnp.bfloat16), (row_top + jnp.log(totals))[..., 0])


def rows_back(inputs, query_start, score_scale):
    queries, key_rows, val_rows, grad_rows, log_total = inputs
    scores = masked_scores(queries, key_rows, query_start, score_scale)
    weights = jnp.exp(scores - log_total[..., None])
    grad_weights = jnp.einsum(
        "bqhd,bkhd->bhqk", grad_rows, val_rows, preferred_element_type=jnp.float32
    )
    delta_rows = jnp.sum(weights * grad_weights, axis=-1)
    grad_scores = (weights * (grad_weights - delta_rows[..., None])).astype(jnp.bfloat16)
    grad_query = (
        jnp.einsum("bhqk,bkhd->bqhd", grad_scores, key_rows, preferred_element_type=jnp.float32)
        * score_scale
    )
    grad_keys = (
        jnp.einsum("bhqk,bqhd->bkhd", grad_scores, queries, preferred_element_type=jnp.float32)
        * score_scale
    )
    grad_vals = jnp.einsum(
        "bhqk,bqhd->bkhd",
        weights.astype(jnp.bfloat16),
        grad_rows,
        preferred_element_type=jnp.float32,
    )
    return (grad_query, grad_keys, grad_vals)


def fetch_weights(
    qkv_weight,
    proj_weight,
    up_weight,
    down_weight,
    first_gain,
    first_shift,
    proj_bias,
    second_gain,
    second_shift,
    up_bias,
    down_bias,
):
    qkv_part, proj_part, up_part, down_part = (
        lax.all_gather(qkv_weight.astype(jnp.bfloat16), "cp", axis=0, tiled=True),
        lax.all_gather(proj_weight.astype(jnp.bfloat16), "cp", axis=0, tiled=True),
        lax.all_gather(up_weight.astype(jnp.bfloat16), "cp", axis=0, tiled=True),
        lax.all_gather(down_weight.astype(jnp.bfloat16), "cp", axis=0, tiled=True),
    )
    return (
        lax.all_gather(qkv_part, "dp", axis=1, tiled=True),
        lax.all_gather(proj_part, "dp", axis=1, tiled=True),
        lax.all_gather(up_part, "dp", axis=1, tiled=True),
        lax.all_gather(down_part, "dp", axis=1, tiled=True),
        lax.all_gather(first_gain.astype(jnp.bfloat16), "dp", axis=0, tiled=True),
        lax.all_gather(first_shift.astype(jnp.bfloat16), "dp", axis=0, tiled=True),
        lax.all_gather(proj_bias.astype(jnp.bfloat16), "dp", axis=0, tiled=True),
        lax.all_gather(second_gain.astype(jnp.bfloat16), "dp", axis=0, tiled=True),
        lax.all_gather(second_shift.astype(jnp.bfloat16), "dp", axis=0, tiled=True),
        lax.all_gather(up_bias.astype(jnp.bfloat16), "dp", axis=0, tiled=True),
        lax.all_gather(down_bias.astype(jnp.bfloat16), "dp", axis=0, tiled=True),
    )


def mat_rows(left, right):
    return jnp.einsum("sqd,de->sqe", left, right, preferred_element_type=jnp.float32)


def mat_back(left, right):
    return jnp.einsum("sqe,de->sqd", left, right, preferred_element_type=jnp.float32)


def mat_grad(left, right):
    return jnp.einsum("sqd,sqe->de", left, right, preferred_element_type=jnp.float32)


def general(
    x_source,
    cotangent,
    lengths,
    dealing,
    qkv_weight,
    proj_weight,
    up_weight,
    down_weight,
    first_gain,
    first_shift,
    proj_bias,
    second_gain,
    second_shift,
    up_bias,
    down_bias,
):
    groups = lax.axis_size("dp")
    seqs_all, piece_rows, features = x_source.shape
    seq_group = seqs_all // groups
    span_rows = groups * piece_rows
    score_scale = HEAD_DIM ** (-0.5)
    block_seqs = math.gcd(seq_group, max(1, 512 // span_rows))
    owners = jnp.argsort(dealing)
    send_order = owners.reshape(groups, seq_group).T.reshape(-1)
    outgoing = x_source[send_order].reshape(seq_group, span_rows, features)
    arrived = lax.all_to_all(outgoing, "dp", split_axis=1, concat_axis=1, tiled=True)
    first_slot = lax.axis_index("dp") * seq_group
    my_lengths = lax.dynamic_slice_in_dim(lengths[owners], first_slot, seq_group)
    query_start = lax.axis_index("cp") * span_rows
    positions = query_start + jnp.arange(span_rows)
    live_rows = positions[None, :] < my_lengths[:, None]
    fetched = fetch_weights(
        qkv_weight,
        proj_weight,
        up_weight,
        down_weight,
        first_gain,
        first_shift,
        proj_bias,
        second_gain,
        second_shift,
        up_bias,
        down_bias,
    )
    qkv_full, proj_full, up_full, down_full = (fetched[0], fetched[1], fetched[2], fetched[3])
    gain_one, shift_one, bias_proj, gain_two, shift_two, bias_up, bias_down = [
        vector.astype(jnp.float32) for vector in fetched[4:]
    ]
    inputs_f = arrived.astype(jnp.float32)
    norm_one, back_one = jax.vjp(layer_norm, inputs_f, gain_one, shift_one)
    act_one = norm_one.astype(jnp.bfloat16)
    mixed_rows = mat_rows(act_one, qkv_full).astype(jnp.bfloat16)
    queries = mixed_rows[..., :features]
    kv_local = mixed_rows[..., features:]
    kv_all = lax.all_gather(kv_local, "cp", axis=1, tiled=True)
    attended, log_total = lax.map(
        lambda inputs: attend(inputs, query_start, score_scale),
        (
            grouped(queries, block_seqs),
            grouped(kv_all[..., :features], block_seqs),
            grouped(kv_all[..., features:], block_seqs),
        ),
    )
    attended = joined(attended)
    log_total = log_total.reshape((seq_group,) + log_total.shape[2:])
    residual = inputs_f + mat_rows(attended, proj_full) + bias_proj
    norm_two, back_two = jax.vjp(layer_norm, residual, gain_two, shift_two)
    act_two = norm_two.astype(jnp.bfloat16)
    up_raw = mat_rows(act_two, up_full) + bias_up
    hidden, back_gelu = jax.vjp(gelu_tanh, up_raw)
    hid_low = hidden.astype(jnp.bfloat16)
    result = residual + mat_rows(hid_low, down_full) + bias_down
    output = jnp.where(live_rows[..., None], result, 0.0).astype(jnp.bfloat16)
    fetched = fetch_weights(
        qkv_weight,
        proj_weight,
        up_weight,
        down_weight,
        first_gain,
        first_shift,
        proj_bias,
        second_gain,
        second_shift,
        up_bias,
        down_bias,
    )
    qkv_full, proj_full, up_full, down_full = (fetched[0], fetched[1], fetched[2], fetched[3])
    gain_one, gain_two = (fetched[4].astype(jnp.float32), fetched[7].astype(jnp.float32))
    grad_out = jnp.where(live_rows[..., None], cotangent.astype(jnp.float32), 0.0)
    grad_low = grad_out.astype(jnp.bfloat16)
    grad_down = mat_grad(hid_low, grad_low)
    grad_bias_down = jnp.sum(grad_out, axis=(0, 1))
    grad_hidden = mat_back(grad_low, down_full)
    grad_up_raw = back_gelu(grad_hidden)[0].astype(jnp.bfloat16)
    grad_up = mat_grad(act_two, grad_up_raw)
    grad_bias_up = jnp.sum(grad_up_raw.astype(jnp.float32), axis=(0, 1))
    grad_act_two = mat_back(grad_up_raw, up_full)
    grad_resid, grad_gain_two, grad_shift_two = back_two(grad_act_two)
    grad_resid = grad_resid + grad_out
    grad_bias_proj = jnp.sum(grad_resid, axis=(0, 1))
    resid_low = grad_resid.astype(jnp.bfloat16)
    grad_proj = mat_grad(attended, resid_low)
    grad_attended = mat_back(resid_low, proj_full).astype(jnp.bfloat16)
    kv_back = lax.all_gather(kv_local, "cp", axis=1, tiled=True)
    key_rows = kv_back[..., :features]
    val_rows = kv_back[..., features:]
    grad_query, grad_keys, grad_vals = lax.map(
        lambda inputs: rows_back(inputs, query_start, score_scale),
        (
            grouped(queries, block_seqs),
            grouped(key_rows, block_seqs),
            grouped(val_rows, block_seqs),
            grouped(grad_attended, block_seqs),
            grouped_stats(log_total, block_seqs),
        ),
    )
    grad_keys, grad_vals = (
        lax.psum_scatter(
            joined(grad_keys).astype(jnp.bfloat16), "cp", scatter_dimension=1, tiled=True
        ).astype(jnp.float32),
        lax.psum_scatter(
            joined(grad_vals).astype(jnp.bfloat16), "cp", scatter_dimension=1, tiled=True
        ).astype(jnp.float32),
    )
    grad_mixed = jnp.concatenate([joined(grad_query), grad_keys, grad_vals], axis=-1).astype(
        jnp.bfloat16
    )
    grad_qkv = mat_grad(act_one, grad_mixed)
    grad_act_one = mat_back(grad_mixed, qkv_full)
    grad_input, grad_gain_one, grad_shift_one = back_one(grad_act_one)
    grad_input = (grad_input + grad_resid).astype(jnp.bfloat16)
    returned = lax.all_to_all(grad_input, "dp", split_axis=1, concat_axis=0, tiled=True)
    input_grad = returned[dealing]
    (
        grad_qkv,
        grad_proj,
        grad_up,
        grad_down,
        grad_gain_one,
        grad_shift_one,
        grad_bias_proj,
        grad_gain_two,
        grad_shift_two,
        grad_bias_up,
        grad_bias_down,
    ) = (
        lax.psum_scatter(
            grad_qkv.astype(jnp.bfloat16), "dp", scatter_dimension=1, tiled=True
        ).astype(jnp.float32),
        lax.psum_scatter(
            grad_proj.astype(jnp.bfloat16), "dp", scatter_dimension=1, tiled=True
        ).astype(jnp.float32),
        lax.psum_scatter(
            grad_up.astype(jnp.bfloat16), "dp", scatter_dimension=1, tiled=True
        ).astype(jnp.float32),
        lax.psum_scatter(
            grad_down.astype(jnp.bfloat16), "dp", scatter_dimension=1, tiled=True
        ).astype(jnp.float32),
        lax.psum_scatter(
            grad_gain_one.astype(jnp.bfloat16), "dp", scatter_dimension=0, tiled=True
        ).astype(jnp.float32),
        lax.psum_scatter(
            grad_shift_one.astype(jnp.bfloat16), "dp", scatter_dimension=0, tiled=True
        ).astype(jnp.float32),
        lax.psum_scatter(
            grad_bias_proj.astype(jnp.bfloat16), "dp", scatter_dimension=0, tiled=True
        ).astype(jnp.float32),
        lax.psum_scatter(
            grad_gain_two.astype(jnp.bfloat16), "dp", scatter_dimension=0, tiled=True
        ).astype(jnp.float32),
        lax.psum_scatter(
            grad_shift_two.astype(jnp.bfloat16), "dp", scatter_dimension=0, tiled=True
        ).astype(jnp.float32),
        lax.psum_scatter(
            grad_bias_up.astype(jnp.bfloat16), "dp", scatter_dimension=0, tiled=True
        ).astype(jnp.float32),
        lax.psum_scatter(
            grad_bias_down.astype(jnp.bfloat16), "dp", scatter_dimension=0, tiled=True
        ).astype(jnp.float32),
    )
    grad_qkv, grad_proj, grad_up, grad_down = (
        lax.psum_scatter(
            grad_qkv.astype(jnp.bfloat16), "cp", scatter_dimension=0, tiled=True
        ).astype(jnp.float32),
        lax.psum_scatter(
            grad_proj.astype(jnp.bfloat16), "cp", scatter_dimension=0, tiled=True
        ).astype(jnp.float32),
        lax.psum_scatter(
            grad_up.astype(jnp.bfloat16), "cp", scatter_dimension=0, tiled=True
        ).astype(jnp.float32),
        lax.psum_scatter(
            grad_down.astype(jnp.bfloat16), "cp", scatter_dimension=0, tiled=True
        ).astype(jnp.float32),
    )
    (
        grad_gain_one,
        grad_shift_one,
        grad_bias_proj,
        grad_gain_two,
        grad_shift_two,
        grad_bias_up,
        grad_bias_down,
    ) = lax.psum(
        (
            grad_gain_one,
            grad_shift_one,
            grad_bias_proj,
            grad_gain_two,
            grad_shift_two,
            grad_bias_up,
            grad_bias_down,
        ),
        "cp",
    )
    return (
        output,
        input_grad,
        grad_qkv,
        grad_proj,
        grad_up,
        grad_down,
        grad_gain_one,
        grad_shift_one,
        grad_bias_proj,
        grad_gain_two,
        grad_shift_two,
        grad_bias_up,
        grad_bias_down,
    )


def solution(mesh):
    in_specs = (
        P(None, ("cp", "dp"), None),
        P("dp", "cp", None),
        P(),
        P(),
        P("cp", "dp"),
        P("cp", "dp"),
        P("cp", "dp"),
        P("cp", "dp"),
        P("dp"),
        P("dp"),
        P("dp"),
        P("dp"),
        P("dp"),
        P("dp"),
        P("dp"),
    )
    out_specs = (
        P("dp", "cp", None),
        P(None, ("cp", "dp"), None),
        P("cp", "dp"),
        P("cp", "dp"),
        P("cp", "dp"),
        P("cp", "dp"),
        P("dp"),
        P("dp"),
        P("dp"),
        P("dp"),
        P("dp"),
        P("dp"),
        P("dp"),
    )
    planned = tuple(mesh.shape.items()) == (("dp", Z * Y * C), ("cp", X))
    local = slice_plan if planned else general
    return jax.shard_map(local, mesh=mesh, in_specs=in_specs, out_specs=out_specs, check_vma=False)
```

```python
import functools
import math

import jax
import jax.numpy as jnp
from jax import lax
from jax.experimental import pallas as pl
from jax.experimental.pallas import tpu as pltpu
from jax.sharding import PartitionSpec as P

HEADS = 12
HEAD_DIM = 64


EPSILON = 1e-05
NEG_BIG = -1e30
TANH_SCALE = 0.7978845608028654
CUBIC_TERM = 0.044715
MESH_IDS = pl.DeviceIdType.MESH
BF = jnp.bfloat16
F32 = jnp.float32

Z, Y, C, X = 4, 2, 2, 2


def mult(value, n):
    return value if isinstance(value, int) else pl.multiple_of(value, n)


def coords():
    d = lax.axis_index("dp")
    x = lax.axis_index("cp")
    return d // (Y * C), (d // C) % Y, d % C, x, d


def dev(z, y, c, x):
    return {"dp": (z * Y + y) * C + c, "cp": x}


def rcopy(src, dst, ssem, rsem, where):
    return pltpu.make_async_remote_copy(
        src_ref=src, dst_ref=dst, send_sem=ssem, recv_sem=rsem, device_id=where, device_id_type=MESH_IDS
    )


def lcopy(src, dst, sem):
    return pltpu.make_async_copy(src, dst, sem)


def wait_bytes(ref, sem):
    pltpu.make_async_copy(ref, ref, sem).wait()


def enter(everyone):
    d = lax.axis_index("dp")
    x = lax.axis_index("cp")
    barrier = pltpu.get_barrier_semaphore()

    def greet(k, carry):
        kd = k // X
        kx = k % X

        @pl.when(jnp.logical_or(kd != d, kx != x))
        def _():
            pl.semaphore_signal(barrier, inc=1, device_id={"dp": kd, "cp": kx}, device_id_type=MESH_IDS)

        return carry

    lax.fori_loop(0, everyone, greet, 0)

    def entered():
        pl.semaphore_wait(barrier, everyone - 1)

    return entered


def dot_nn(a, b):
    return lax.dot_general(a, b, (((1,), (0,)), ((), ())), preferred_element_type=F32)


def dot_nt(a, b):
    return lax.dot_general(a, b, (((1,), (1,)), ((), ())), preferred_element_type=F32)


def dot_tn(a, b):
    return lax.dot_general(a, b, (((0,), (0,)), ((), ())), preferred_element_type=F32)


def norm_parts(v):
    mean = jnp.mean(v, axis=-1, keepdims=True)
    cen = v - mean
    var = jnp.mean(cen * cen, axis=-1, keepdims=True)
    rstd = lax.rsqrt(var + EPSILON)
    return cen * rstd, rstd


def live_length(len_ref, deal_ref, slot):
    total = jnp.int32(0)
    for s in range(len_ref.shape[0]):
        total = total + jnp.where(deal_ref[s] == slot, len_ref[s], 0)
    return total


class Piece:
    def __init__(self, full, R, r0, rn, step, c0, cn):
        self.full = full
        self.R, self.r0, self.rn, self.step, self.c0, self.cn = R, r0, rn, step, c0, cn

    def at(self, z, y, c, x):
        d = (z * Y + y) * C + c
        return self.full.at[
            pl.ds(mult(d * self.R + self.r0, 16), self.rn), pl.ds(mult(x * self.step + self.c0, 128), self.cn)
        ]


class Gather:
    FAR, MATE, A, B, CORE = range(5)

    def __init__(self, piece, sems, k, dummy, where, kind, turned):
        self.p, self.sems, self.k, self.dummy, self.kind = piece, sems, k, dummy, kind
        z, y, c, x, _ = where
        self.z, self.y, self.c, self.x = z, y, c, x
        o = 1 if turned else c
        self.far, self.mate = 3 - z, z + 1 - 2 * (z % 2)
        self.ya, self.xa = (y + 1 - o) % 2, (x + o) % 2
        self.yb, self.xb = (y + o) % 2, (x + 1 - o) % 2
        self.to = {
            self.FAR: dev(self.far, y, c, x), self.MATE: dev(self.mate, y, c, x), self.A: dev(z, self.ya, c, self.xa),
            self.B: dev(z, self.yb, c, self.xb), self.CORE: dev(z, y, 1 - c, x),
        }
        self.counts = {self.FAR: 1, self.MATE: 2, self.A: 4} if kind == 1 else {self.FAR: 2, self.MATE: 4, self.A: 1}
        self.counts.update({self.B: 8, self.CORE: 16})

    def send(self, pieces, *ways):
        for way in ways:
            for z, y, x in pieces:
                q = self.p.at(z, y, self.c, x)
                rcopy(q, q, self.sems.at[self.k, 0, way], self.sems.at[self.k, 1, way], self.to[way]).start()

    def wait(self, way, side=1):
        p = self.p
        wait_bytes(self.dummy.at[pl.ds(0, self.counts[way] * p.rn), pl.ds(0, p.cn)], self.sems.at[self.k, side, way])

    def start(self):
        own = [(self.z, self.y, self.x)]
        if self.kind == 1:
            self.send(own, self.FAR, self.MATE, self.A, self.B, self.CORE)
        else:
            self.send(own, self.A, self.FAR, self.MATE, self.B, self.CORE)

    def tick1(self):
        if self.kind == 1:
            self.wait(self.FAR)
            self.send([(self.far, self.y, self.x)], self.MATE, self.A, self.B, self.CORE)
        else:
            self.wait(self.A)
            self.send([(self.z, self.ya, self.xa)], self.FAR, self.MATE, self.B, self.CORE)

    def tick2(self):
        if self.kind == 1:
            self.wait(self.MATE)
            self.send([(self.mate, self.y, self.x), (3 - self.mate, self.y, self.x)], self.A, self.B, self.CORE)
        else:
            self.wait(self.FAR)
            self.send([(self.far, self.y, self.x), (self.far, self.ya, self.xa)], self.MATE, self.B, self.CORE)

    def tick3(self):
        if self.kind == 1:
            self.wait(self.A)
            self.send([(k, self.ya, self.xa) for k in range(Z)], self.B, self.CORE)
        else:
            self.wait(self.MATE)
            self.send(
                [(k, y, x) for k in (self.mate, 3 - self.mate) for y, x in ((self.y, self.x), (self.ya, self.xa))],
                self.B, self.CORE,
            )

    def tick4(self):
        self.wait(self.B)
        self.send(
            [(k, y, x) for k in range(Z) for y, x in ((self.yb, self.xb), (1 - self.y, 1 - self.x))], self.CORE
        )

    def tick5(self):
        self.wait(self.CORE)

    def drain(self):
        for way in range(5):
            self.wait(way, 0)


class Vectors:
    FAR, MATE, A, CORE = range(4)

    def __init__(self, full, sems, where):
        self.full, self.sems = full, sems
        z, y, c, x, _ = where
        self.z, self.y, self.c = z, y, c
        self.far, self.mate = 3 - z, z + 1 - 2 * (z % 2)
        self.to = (dev(self.far, y, c, x), dev(self.mate, y, c, x), dev(z, 1 - y, c, x), dev(z, y, 1 - c, x))
        self.counts = (1, 2, 4, 8)

    def send(self, pieces, *ways):
        for way in ways:
            for z, y in pieces:
                q = self.full.at[(z * Y + y) * C + self.c]
                rcopy(q, q, self.sems.at[0, way], self.sems.at[1, way], self.to[way]).start()

    def wait(self, way, side=1):
        wait_bytes(self.full.at[pl.ds(0, self.counts[way])], self.sems.at[side, way])

    def start(self):
        self.send([(self.z, self.y)], self.FAR, self.MATE, self.A, self.CORE)

    def tick1(self):
        self.wait(self.FAR)
        self.send([(self.far, self.y)], self.MATE, self.A, self.CORE)

    def tick2(self):
        self.wait(self.MATE)
        self.send([(self.mate, self.y), (3 - self.mate, self.y)], self.A, self.CORE)

    def tick3(self):
        self.wait(self.A)
        self.send([(k, 1 - self.y) for k in range(Z)], self.CORE)

    def tick4(self):
        self.wait(self.CORE)

    def drain(self):
        for way in range(4):
            self.wait(way, 0)


G1, C1, BP, G2, C2, BD, BU = range(7)


def gather_chunks(wq, wp, wu, wd):
    rq, rp, ru, rd = (w.shape[0] // (Z * Y * C) for w in (wq, wp, wu, wd))
    half, wide = wq.shape[1] // X, wd.shape[1] // X
    out = []
    for k in range(3):
        out.append(Piece(wq, rq, k * (rq // 3), rq // 3, half, 0, half))
    out.append(Piece(wp, rp, 0, rp, half, 0, half))
    for k in range(4):
        out.append(Piece(wu, ru, k * (ru // 4), ru // 4, half, 0, half))
    for k in range(4):
        out.append(Piece(wd, rd, 0, rd, wide, k * (wide // 4), wide // 4))
    return out


def one_hot(count, width, first):
    at_row = lax.broadcasted_iota(jnp.int32, (count, width), 0)
    at_col = lax.broadcasted_iota(jnp.int32, (count, width), 1)
    return (at_col == at_row + first).astype(BF)


N_GATHER = 12
TICKS = ("tick1", "tick2", "tick3", "tick4")
KINDS = (1, 1, 1, 1, 2, 2, 1, 2, 2, 1, 2, 2)
TURNED = (7,)
COT_STEPS = (6, 6, 6, 6, 8, 8, 8, 8)
LAGS = ((0, 1, 2, 3),) * 4 + ((0, 1, 2, 4),) * 8


def forward_kernel(
    len_ref, deal_ref, cot, x_any, sq_any, sp_any, su_any, sd_any, g1_any, c1_any, bp_any, g2_any, c2_any, bd_any, bu_any,
    wq_o, wp_o, wu_o, wd_o, xr_o, gw_o, qs_o, ka_o, va_o, at_o, lse_o, r_o, a2_o, hd_o, gp_o, vec_o, out_o,
    wq, wp, wu, wd, xr, a1, qs, ka, va, at, lse, r, a2, hd, gp, vg, vec, bu3, sc0, sc1, outw, xg, acc,
    x_in, sq, sp, su, sd, v_g1, v_c1, v_bp, v_g2, v_c2, v_bd, v_bu,
    gsem, vsem, msem, osem, isem,
):
    where = coords()
    z, y, c, x, d = where
    width = xr.shape[1]
    rows = xr.shape[0]
    qrows = rows // 2
    small = x_in.shape[1]
    sources = (sq_any, sp_any, su_any, sd_any, g1_any, c1_any, bp_any, g2_any, c2_any, bd_any, bu_any, x_any)
    places = (sq, sp, su, sd, v_g1, v_c1, v_bp, v_g2, v_c2, v_bd, v_bu, x_in)
    loads = [pltpu.make_async_copy(s, t, isem.at[k]) for k, (s, t) in enumerate(zip(sources, places))]
    for load in loads:
        load.start()
    pairs = width // 128
    tile = 256

    entered = enter(Z * Y * C * X)

    n = Z * Y * C
    for load, shard, full in zip(loads, (sq, sp, su, sd), (wq, wp, wu, wd)):
        load.wait()
        own, long = shard.shape
        full[pl.ds(mult(d * own, 16), own), pl.ds(mult(x * long, 128), long)] = shard[...].astype(BF)
    for load in loads[4:]:
        load.wait()
    vg[d] = jnp.zeros(vg.shape[1:], BF)
    own = v_g1.shape[1]
    seven = jnp.concatenate([v[...] for v in (v_g1, v_c1, v_bp, v_g2, v_c2, v_bd)], axis=0).astype(BF)
    placed = dot_nn(seven, one_hot(own, width, d * own))
    long = v_bu.shape[1]
    per_row = width // long
    placed_long = dot_nn(v_bu[...].astype(BF), one_hot(long, width, (d % per_row) * long))
    rows_long = [jnp.where(d // per_row == k, placed_long, 0.0) for k in range(n // per_row)]
    rest = jnp.zeros((16 - 6 - n // per_row, width), F32)
    vg[d] = jnp.concatenate([placed] + rows_long + [rest], axis=0).astype(BF)
    slots = x_in.shape[0]
    for t in range(slots):
        owner = jnp.int32(0)
        for s in range(slots):
            owner = jnp.where(deal_ref[s] == t, s, owner)
        xg[t] = x_in[owner]

    entered()

    vectors = Vectors(vg, vsem, where)
    vectors.start()
    chunks = [
        Gather(p, gsem, k, wu, where, KINDS[k], k in TURNED) for k, p in enumerate(gather_chunks(wq, wp, wu, wd))
    ]

    def send_cot(k):
        b, part = k // 4, k % 4
        some = qrows // 4
        core_b = (x + b) % 2
        src_b = cot.at[pl.ds(b * qrows + part * some, some)]
        dst_b = gw_o.at[pl.ds(mult(x * qrows + part * some, some), some)]
        same = jnp.logical_and(core_b == c, c == x)

        @pl.when(same)
        def _():
            lcopy(src_b, dst_b, msem.at[3]).start()

        @pl.when(jnp.logical_not(same))
        def _():
            rcopy(src_b, dst_b, msem.at[2], msem.at[3], dev(z, y, core_b, c)).start()

    per_quarter = qrows // small
    place = mult(x * qrows + (d % per_quarter) * small, 16)
    core_to = (x + d // per_quarter) % 2
    dst = xr.at[pl.ds(place, small)]

    def deal_out(k, carry):
        t = (d + k + x * (slots // 2)) % slots
        td = (t // 2) * 2 + core_to
        tx = t % 2
        mine = jnp.logical_and(td == d, tx == x)

        @pl.when(mine)
        def _():
            lcopy(xg.at[t], dst, msem.at[1]).start()

        @pl.when(jnp.logical_not(mine))
        def _():
            rcopy(xg.at[t], dst, msem.at[0], msem.at[1], {"dp": td, "cp": tx}).start()

        return carry

    ahead = 2
    for ch in chunks[:ahead]:
        ch.start()

    def step(s):
        if s + ahead < len(chunks):
            chunks[s + ahead].start()
        if s < 4:
            lax.fori_loop(s * slots // 4, (s + 1) * slots // 4, deal_out, 0)
        for k, at_step in enumerate(COT_STEPS):
            if at_step == s:
                send_cot(k)
        for n in range(4):
            for k in range(len(chunks)):
                if k + LAGS[k][n] == s:
                    getattr(chunks[k], TICKS[n])()

    step(0)
    vectors.tick1()
    step(1)
    vectors.tick2()
    step(2)
    vectors.tick3()
    step(3)
    vectors.tick4()

    def add_table(k, acc):
        return acc + vg[k].astype(F32)

    vec[...] = lax.fori_loop(1, Z * Y * C, add_table, vg[0].astype(F32))
    for k in range(bu3.shape[0]):
        per = width // tile
        bu3[k] = vec[BU + k // per:BU + k // per + 1, (k % per) * tile:(k % per + 1) * tile]

    wait_bytes(xr, msem.at[1])
    lrows = 128

    def first_norm(k, carry):
        at_rows = pl.ds(mult(k * lrows, lrows), lrows)
        n1, _ = norm_parts(xr[at_rows, :].astype(F32))
        a1[at_rows, :] = (n1 * vec[G1:G1 + 1, :] + vec[C1:C1 + 1, :]).astype(BF)
        return carry

    lax.fori_loop(0, rows // lrows, first_norm, 0)

    step(4)
    step(5)
    for k in range(3):
        chunks[k].tick5()
    keep = [pltpu.make_async_copy(wq, wq_o, osem.at[0])]
    keep[-1].start()

    quarters = (c, 3 - c)

    def q_at(i):
        return pl.ds(mult(quarters[i] * qrows, qrows), qrows)

    steps = width // tile
    for part in range(3):
        def project(n, carry, part=part):
            lanes = pl.ds(mult(n * tile, tile), tile)
            res = dot_nt(a1[...], wq[pl.ds(mult(part * width + n * tile, tile), tile), :]).astype(BF)
            if part == 0:
                qs[:, lanes] = res * jnp.asarray(HEAD_DIM ** -0.5, BF)
            else:
                to = ka if part == 1 else va
                for i in range(2):
                    to[q_at(i), lanes] = res[i * qrows:(i + 1) * qrows]
            return carry

        lax.fori_loop(0, steps, project, 0)
        if part > 0:
            to = ka if part == 1 else va
            for i in range(2):
                rcopy(to.at[q_at(i)], to.at[q_at(i)], msem.at[4 + 2 * (part - 1)], msem.at[5 + 2 * (part - 1)], dev(z, y, 1 - c, x)).start()
    step(6)
    wait_bytes(ka.at[pl.ds(0, rows)], msem.at[5])
    wait_bytes(va.at[pl.ds(0, rows)], msem.at[7])
    for src, out, s in ((qs, qs_o, 1), (ka, ka_o, 2), (va, va_o, 3), (xr, xr_o, 4), (vec, vec_o, 5)):
        keep.append(pltpu.make_async_copy(src, out, osem.at[s]))
        keep[-1].start()

    lane = lax.broadcasted_iota(jnp.int32, (qrows, 128), 1)
    kpos = lax.broadcasted_iota(jnp.int32, (qrows, qrows), 0)
    qpos = lax.broadcasted_iota(jnp.int32, (qrows, qrows), 1)
    groups = qrows // 8

    def pair_body(p, carry):
        lanes = pl.ds(mult(p * 128, 128), 128)
        for i in range(2):
            quarter = quarters[i]
            qp = qs[i * qrows:(i + 1) * qrows, lanes]
            zero = jnp.zeros_like(qp)
            qh = (jnp.where(lane < HEAD_DIM, qp, zero), jnp.where(lane >= HEAD_DIM, qp, zero))

            def scores(j, tops, diagonal=False):
                at_keys = pl.ds(mult(j * qrows, qrows), qrows)
                kj = ka[at_keys, lanes]
                new = []
                for h, sc in enumerate((sc0, sc1)):
                    s = dot_nt(kj, qh[h])
                    if diagonal:
                        s = jnp.where(kpos <= qpos, s, NEG_BIG)
                    sc[at_keys, :] = s
                    new.append(jnp.maximum(tops[h], jnp.max(s.reshape(groups, 8, qrows), axis=0)))
                return tuple(new)

            low = jnp.full((8, qrows), NEG_BIG, F32)
            tops = scores(quarter, lax.fori_loop(0, quarter, scores, (low, low)), True)
            tops = tuple(jnp.max(t, axis=0, keepdims=True) for t in tops)

            def values(j, state):
                at_keys = pl.ds(mult(j * qrows, qrows), qrows)
                vt = va[at_keys, lanes].T
                new = []
                for h, sc in enumerate((sc0, sc1)):
                    total, acc = state[h]
                    e = jnp.exp(sc[at_keys, :] - tops[h])
                    total = total + jnp.sum(e.reshape(groups, 8, qrows), axis=0)
                    acc = acc + dot_nn(vt[h * HEAD_DIM:(h + 1) * HEAD_DIM], e.astype(BF))
                    new.append((total, acc))
                return tuple(new)

            blank = (jnp.zeros((8, qrows), F32), jnp.zeros((HEAD_DIM, qrows), F32))
            state = lax.fori_loop(0, quarter + 1, values, (blank, blank))
            parts = []
            for h in range(2):
                total = jnp.sum(state[h][0], axis=0, keepdims=True)
                parts.append(state[h][1] / total)
                lse[p, i * 2 + h:i * 2 + h + 1, :] = tops[h] + jnp.log(total)
            at[i * qrows:(i + 1) * qrows, lanes] = jnp.concatenate(parts, axis=0).T.astype(BF)
        return carry

    per = 2
    for k in range(0, pairs, per):
        lax.fori_loop(k, k + per, pair_body, 0)
        step(7 + k // per)

    chunks[3].tick5()
    for src, out, s in ((wp, wp_o, 6), (at, at_o, 7), (lse, lse_o, 8)):
        keep.append(pltpu.make_async_copy(src, out, osem.at[s]))
        keep[-1].start()

    def attend_out(n, carry):
        lanes = pl.ds(mult(n * tile, tile), tile)
        res = dot_nt(at[...], wp[pl.ds(mult(n * tile, tile), tile), :])
        r[:, lanes] = xr[:, lanes].astype(F32) + res + vec[BP:BP + 1, lanes]
        return carry

    lax.fori_loop(0, steps, attend_out, 0)

    def second_norm(k, carry):
        at_rows = pl.ds(mult(k * lrows, lrows), lrows)
        n2, _ = norm_parts(r[at_rows, :])
        a2[at_rows, :] = (n2 * vec[G2:G2 + 1, :] + vec[C2:C2 + 1, :]).astype(BF)
        return carry

    lax.fori_loop(0, rows // lrows, second_norm, 0)
    step(10)
    step(11)
    for k in range(4, 8):
        chunks[k].tick5()
    for src, out, s in ((wu, wu_o, 9), (r, r_o, 10), (a2, a2_o, 11)):
        keep.append(pltpu.make_async_copy(src, out, osem.at[s]))
        keep[-1].start()

    def up(n, carry):
        lanes = pl.ds(mult(n * tile, tile), tile)
        u = dot_nt(a2[...], wu[lanes, :]) + bu3[n]
        sq_u = u * u
        t = jnp.tanh(TANH_SCALE * (u + CUBIC_TERM * sq_u * u))
        half_up = 0.5 * (1.0 + t)
        hd[:, lanes] = (u * half_up).astype(BF)
        slope = TANH_SCALE * (1.0 + 3.0 * CUBIC_TERM * sq_u)
        gp[:, lanes] = (half_up + 0.5 * u * (1.0 - t * t) * slope).astype(BF)
        return carry

    blocks = hd.shape[1] // tile
    for k in range(0, blocks, 4):
        lax.fori_loop(k, k + 4, up, 0)
        step(12 + k // 4)
    for src, out, s in ((hd, hd_o, 12), (gp, gp_o, 13)):
        keep.append(pltpu.make_async_copy(src, out, osem.at[s]))
        keep[-1].start()
    my_len = live_length(len_ref, deal_ref, (z * Y + y) * C + x)
    rowpos = lax.broadcasted_iota(jnp.int32, (qrows, 1), 0)
    parts = len(chunks) - 8
    wide = wd.shape[1] // X
    for k in range(parts):
        if k == 1:
            step(15)
        chunks[8 + k].tick5()
        cuts = [slice(h * wide + k * (wide // parts), h * wide + (k + 1) * (wide // parts)) for h in range(X)]
        for h, cut in enumerate(cuts):
            keep.append(pltpu.make_async_copy(wd.at[:, cut], wd_o.at[:, cut], osem.at[16 + X * k + h]))
            keep[-1].start()

        def down(n, carry, k=k, cuts=cuts):
            lanes = pl.ds(mult(n * tile, tile), tile)
            res = dot_nt(hd[:, cuts[0]], wd[lanes, cuts[0]])
            for cut in cuts[1:]:
                res = res + dot_nt(hd[:, cut], wd[lanes, cut])
            res = res + (r[:, lanes] + vec[BD:BD + 1, lanes] if k == 0 else acc[:, lanes])
            if k < parts - 1:
                acc[:, lanes] = res
            else:
                for i in range(2):
                    live = quarters[i] * qrows + rowpos < my_len
                    outw[i * qrows:(i + 1) * qrows, lanes] = jnp.where(live, res[i * qrows:(i + 1) * qrows], 0.0).astype(BF)
            return carry

        lax.fori_loop(0, steps, down, 0)
    keep.append(pltpu.make_async_copy(outw, out_o, osem.at[15]))
    keep[-1].start()

    for ch in chunks:
        ch.drain()
    vectors.drain()

    @pl.when(core_to == c)
    def _():
        wait_bytes(xr.at[pl.ds(0, rows - small)], msem.at[0])

    @pl.when(core_to != c)
    def _():
        wait_bytes(xr, msem.at[0])

    @pl.when(c == x)
    def _():
        wait_bytes(xr.at[pl.ds(0, qrows)], msem.at[2])

    @pl.when(c != x)
    def _():
        wait_bytes(xr, msem.at[2])

    wait_bytes(xr, msem.at[3])
    wait_bytes(ka.at[pl.ds(0, rows)], msem.at[4])
    wait_bytes(va.at[pl.ds(0, rows)], msem.at[6])
    for cp in keep:
        cp.wait()


def forward(lengths, dealing, cot, x_source, shards, vectors):
    slots, small, width = x_source.shape
    rows = cot.shape[0]
    ff = shards[2].shape[0] * Z * Y * C
    keys = rows * 2
    pairs = width // 128

    def arr(shape, dtype=BF):
        return jax.ShapeDtypeStruct(shape, dtype)

    outs = [
        arr((3 * width, width)), arr((width, width)), arr((ff, width)), arr((width, ff)),
        arr((rows, width)), arr((rows, width)), arr((rows, width)), arr((keys, width)), arr((keys, width)),
        arr((rows, width)), arr((pairs, 8, rows // 2), F32), arr((rows, width), F32), arr((rows, width)),
        arr((rows, ff)), arr((rows, ff)), arr((16, width), F32), arr((rows, width)),
    ]
    vm = pltpu.VMEM
    scratch = [
        vm((3 * width, width), BF), vm((width, width), BF), vm((ff, width), BF), vm((width, ff), BF),
        vm((rows, width), BF), vm((rows, width), BF), vm((rows, width), BF), vm((keys, width), BF),
        vm((keys, width), BF), vm((rows, width), BF), vm((pairs, 8, rows // 2), F32), vm((rows, width), F32),
        vm((rows, width), BF), vm((rows, ff), BF), vm((rows, ff), BF), vm((Z * Y * C, 16, width), BF),
        vm((16, width), F32), vm((ff // 256, 1, 256), F32), vm((keys, rows // 2), F32), vm((keys, rows // 2), F32),
        vm((rows, width), BF), vm(x_source.shape, BF), vm((rows, width), F32),
        vm(x_source.shape, BF), *[vm(a.shape, F32) for a in (*shards, *vectors)],
        pltpu.SemaphoreType.DMA((N_GATHER, 2, 5)), pltpu.SemaphoreType.DMA((2, 4)), pltpu.SemaphoreType.DMA((8,)),
        pltpu.SemaphoreType.DMA((24,)), pltpu.SemaphoreType.DMA((12,)),
    ]
    anyspec = pl.BlockSpec(memory_space=pl.ANY)
    smem = pl.BlockSpec(memory_space=pltpu.SMEM)
    return pl.pallas_call(
        forward_kernel,
        out_shape=outs,
        in_specs=[smem, smem] + [anyspec] * 13,
        out_specs=[anyspec] * len(outs),
        scratch_shapes=scratch,
        compiler_params=pltpu.CompilerParams(
            collective_id=0, has_side_effects=True, vmem_limit_bytes=60 * 1024 * 1024
        ),
        name="forward",
    )(lengths, dealing, cot, x_source, *shards, *vectors)


def when(cond):
    if isinstance(cond, bool):
        return (lambda f: f()) if cond else (lambda f: None)
    return pl.when(cond)


class Reduce:
    S1, R1, S2, R2, S3, R3, S4, R4, S5, R5 = range(10)

    def __init__(self, grad, R, step, c0, C, zlist, bufs, out, out_c0, sems, k, where, kind, turned):
        self.kind = kind
        self.grad, self.R, self.step, self.c0, self.cn, self.zlist = grad, R, step, c0, C, zlist
        self.r1, self.r2, self.r3, self.r4, self.r5 = bufs
        self.out, self.out_c0, self.sems, self.k = out, out_c0, sems, k
        self.z, self.y, self.c, self.x, _ = where
        y, x = self.y, self.x
        self.o = o = 1 if turned else self.c
        self.y2, self.x2 = (y + o) % 2, (x + 1 - o) % 2
        self.y3, self.x3 = (y + 1 - o) % 2, (x + o) % 2
        self.every = len(zlist) == Z

    def sem(self, which):
        return self.sems.at[self.k, which]

    def rows(self, z, y, c):
        return pl.ds(mult(((z * Y + y) * C + c) * self.R, 16), self.R)

    def cols(self, x):
        return pl.ds(mult(x * self.step + self.c0, 128), self.cn)

    def at(self, z, y, c, x):
        return self.grad.at[self.rows(z, y, c), self.cols(x)]

    def add(self, rows, cols, got):
        self.grad[rows, cols] = (self.grad[rows, cols].astype(F32) + got.astype(F32)).astype(BF)

    def zidx(self, zi):
        return zi if self.every else self.zlist[0]

    def start(self):
        z, y, c, x = self.z, self.y, self.c, self.x
        to = dev(z, y, 1 - c, x)
        for zi, zz in enumerate(self.zlist):
            for yy in range(Y):
                for xx in range(X):
                    rcopy(
                        self.at(zz, yy, 1 - c, xx), self.r1.at[zi * Y + yy, xx],
                        self.sem(self.S1), self.sem(self.R1), to,
                    ).start()

    def tick2(self):
        z, y, c, x, o = self.z, self.y, self.c, self.x, self.o
        wait_bytes(self.r1, self.sem(self.R1))

        def body(e, carry):
            rows = self.rows(self.zidx(e // Y), e % Y, c)
            for xx in range(X):
                self.add(rows, self.cols(xx), self.r1[e, xx])
            return carry

        lax.fori_loop(0, len(self.zlist) * Y, body, 0)
        to = dev(z, self.y2, c, self.x2)
        for zi, zz in enumerate(self.zlist):
            for w in range(2):
                yy = w * (1 - o) + (1 - y) * o
                xx = (1 - x) * (1 - o) + w * o
                rcopy(self.at(zz, yy, c, xx), self.r2.at[zi * 2 + w], self.sem(self.S2), self.sem(self.R2), to).start()

    def tick3(self):
        z, y, c, x, o = self.z, self.y, self.c, self.x, self.o
        wait_bytes(self.r2, self.sem(self.R2))

        def body(e, carry):
            w = e % 2
            yy = w * (1 - o) + y * o
            xx = x * (1 - o) + w * o
            self.add(self.rows(self.zidx(e // 2), yy, c), self.cols(xx), self.r2[e])
            return carry

        lax.fori_loop(0, len(self.zlist) * 2, body, 0)
        if self.kind == 2:
            mate = z + 1 - 2 * (z % 2)
            for slot, zz in enumerate((mate, 3 - mate)):
                for w in range(2):
                    rcopy(
                        self.left(zz, w), self.r4.at[slot * 2 + w], self.sem(self.S4), self.sem(self.R4),
                        dev(mate, y, c, x),
                    ).start()
            return
        to = dev(z, self.y3, c, self.x3)
        for zi, zz in enumerate(self.zlist):
            rcopy(self.at(zz, self.y3, c, self.x3), self.r3.at[zi], self.sem(self.S3), self.sem(self.R3), to).start()

    def left_cut(self, zz, w):
        o = self.o
        return self.rows(zz, w * (1 - o) + self.y * o, self.c), self.cols(self.x * (1 - o) + w * o)

    def left(self, zz, w):
        return self.grad.at[self.left_cut(zz, w)]

    def first_hop(self, k):
        return [(k ^ 1, k, 0), ((3 - k) ^ 1, 3 - k, 1)]

    def tick4(self):
        z, y, c, x = self.z, self.y, self.c, self.x
        if self.kind == 2:
            wait_bytes(self.r4, self.sem(self.R4))
            for w in range(2):
                self.add(*self.left_cut(3 - z, w), self.r4[2 + w])
                rcopy(
                    self.left(3 - z, w), self.r5.at[w], self.sem(self.S5), self.sem(self.R5), dev(3 - z, y, c, x)
                ).start()
            for w in range(2):
                self.add(*self.left_cut(z, w), self.r4[w])
            return
        wait_bytes(self.r3, self.sem(self.R3))

        def body(zi, carry):
            self.add(self.rows(self.zidx(zi), y, c), self.cols(x), self.r3[zi])
            return carry

        lax.fori_loop(0, len(self.zlist), body, 0)
        if self.every:
            mate = z + 1 - 2 * (z % 2)
            for slot, zz in enumerate((mate, 3 - mate)):
                rcopy(
                    self.at(zz, y, c, x), self.r4.at[slot], self.sem(self.S4), self.sem(self.R4), dev(mate, y, c, x)
                ).start()
        else:
            k = self.zlist[0]
            for sender, taker, slot in self.first_hop(k):
                @pl.when(z == sender)
                def _(taker=taker, slot=slot):
                    rcopy(
                        self.at(k, y, c, x), self.r4.at[slot], self.sem(self.S4), self.sem(self.R4),
                        dev(taker, y, c, x),
                    ).start()

    def tick5(self):
        z, y, c, x = self.z, self.y, self.c, self.x
        if self.kind == 2:
            wait_bytes(self.r5, self.sem(self.R5))
            for w in range(2):
                self.add(*self.left_cut(z, w), self.r5[w])
            rcopy(
                self.at(z, self.y3, c, self.x3), self.r3.at[0], self.sem(self.S3), self.sem(self.R3),
                dev(z, self.y3, c, self.x3),
            ).start()
            return
        k = self.zlist[0]

        def take(zz, slot):
            self.add(self.rows(zz, y, c), self.cols(x), self.r4[slot])

        def pass_on(zz):
            rcopy(self.at(zz, y, c, x), self.r5.at[0], self.sem(self.S5), self.sem(self.R5), dev(zz, y, c, x)).start()

        if self.every:
            wait_bytes(self.r4, self.sem(self.R4))
            take(3 - z, 1)
            pass_on(3 - z)
            take(z, 0)
        else:
            @pl.when(z == 3 - k)
            def _():
                wait_bytes(self.r4.at[1], self.sem(self.R4))
                take(k, 1)
                pass_on(k)

            @pl.when(z == k)
            def _():
                wait_bytes(self.r4.at[0], self.sem(self.R4))
                take(k, 0)

    def tick6(self):
        z, y, c, x = self.z, self.y, self.c, self.x

        @when(True if self.every else z == self.zlist[0])
        def _():
            last, sem = (self.r3, self.R3) if self.kind == 2 else (self.r5, self.R5)
            wait_bytes(last, self.sem(sem))
            own = self.grad[self.rows(z, y, c), self.cols(x)].astype(F32)
            self.out[:, self.out_c0:self.out_c0 + self.cn] = own + last[0].astype(F32)

    def drain(self):
        z = self.z
        wait_bytes(self.r1, self.sem(self.S1))
        wait_bytes(self.r2, self.sem(self.S2))
        wait_bytes(self.r3, self.sem(self.S3))
        if self.every:
            wait_bytes(self.r4, self.sem(self.S4))
            wait_bytes(self.r5, self.sem(self.S5))
        else:
            k = self.zlist[0]
            for sender, _, slot in self.first_hop(k):
                @pl.when(z == sender)
                def _():
                    wait_bytes(self.r4.at[0], self.sem(self.S4))

            @pl.when(z == 3 - k)
            def _():
                wait_bytes(self.r5, self.sem(self.S5))


TURNED_BACK = ()
KINDS_BACK = (2, 2, 2, 1) + (1,) * 9


def reduce_shapes(width, ff):
    n = Z * Y * C
    every = list(range(Z))
    half = width // X
    wide = ff // X
    shapes = [("d", width // n, wide, k * (wide // 4), wide // 4, every, k * (wide // 4)) for k in range(4)]
    shapes += [("u", ff // n, half, 0, half, [k], 0) for k in range(Z)]
    shapes += [("p", width // n, half, 0, half, every, 0)]
    shapes += [("q", 3 * width // n, half, 0, half, [k], 0) for k in range(Z)]
    return shapes


(
    D0, D1, D2, D3, U0, U1, U2, U3, PJ, Q0, Q1, Q2, Q3, GIVE, OUT, HOP,
) = range(16)
(
    F2, F3, F4, F5, F6, F7, F8, F9, F10, F11, NORM_TWO, PROJ, A00, A01, A10, A11, A20, A21, A30, A31, A40, A41, A50,
    A51, NORM_ONE, QA, MERGE, QB, QC, QD, DA, LN,
) = range(100, 132)

PLAN = (
    F2, (U0, 1), F4, (U0, 2), F5, (U2, 1), (D0, 1), (D1, 1), F7, (U2, 2), F8, (U1, 1), (D0, 2), F9, (D1, 2), F10,
    (U1, 2), (U0, 3), F11, (U3, 1), (D2, 1), (D3, 1), NORM_TWO, (U2, 3), PROJ, (PJ, 1), (U3, 2), (D2, 2), (D0, 3),
    (D3, 2), A00, (PJ, 2), (D1, 3), (OUT, 0), A01, (OUT, 1), A10, (U1, 3), (D0, 4), (OUT, 2), A11, (U0, 4), (D1, 4),
    (U2, 4), (OUT, 3), A20, (OUT, 4), A21, (U3, 3), (D0, 5), (U0, 5), (OUT, 5), A30, (OUT, 6), A31, (D2, 3), (D1, 5),
    (U2, 5), (OUT, 7), A40, (D3, 3), A50, (PJ, 3), (D2, 4), (U1, 4), A51, (U3, 4), NORM_ONE, (D3, 4), QA, (Q0, 1),
    (PJ, 4), MERGE, (D2, 5), QB, (Q1, 1), (U1, 5), (Q0, 2), QC, (Q2, 1), (U3, 5), QD, (Q3, 1), (Q1, 2), (D3, 5), DA,
    (Q3, 2), (Q0, 3), (PJ, 5), LN, (U2, 6), (Q2, 2), (GIVE, 0), (U0, 6), (D0, 6), (D1, 6), (GIVE, 1), (HOP, 0),
    (Q1, 3), (D2, 6), (U1, 6), (U3, 6), (GIVE, 2), (HOP, 1), (Q2, 3), (D3, 6), (GIVE, 3), (Q3, 3), (Q0, 4), (HOP, 2),
    (PJ, 6), (Q1, 4), (Q0, 5), (HOP, 3), (Q2, 4), (Q1, 5), (Q3, 4), (Q2, 5), (HOP, 4), (Q3, 5), (Q0, 6), (Q1, 6),
    (Q2, 6), (Q3, 6),
)


def part_actions(plan):
    parts, now = {}, None
    for item in plan:
        if isinstance(item, int):
            now = parts.setdefault(item, [])
        else:
            now.append(item)
    return parts


def backward_kernel(*refs):
    names = (
        "len_ref", "deal_ref", "wq_i", "wp_i", "wu_i", "wd_i", "xr_i", "gw_i", "qs_i", "ka_i", "va_i", "at_i",
        "lse_i", "r_i", "a2_i", "hd_i", "gp_i", "vec_i", "out_i", "og_q", "og_p", "og_u", "og_d", "osum", "ret",
        "out_n", "wq", "wp", "xr", "g", "qs", "ka", "va", "at", "lse", "r", "a2", "vec", "gt", "d2", "dr", "drl",
        "do", "gq", "gp_", "gu", "gd", "wd_t", "wu_t", "hd_t", "gp_t", "dka", "dva", "own_v", "sv", "rk", "rv", "dm",
        "vs", "vr", "bub", "lsem", "tsem", "rsem", "msem", "vsem",
    )
    env = dict(zip(names, refs[: len(names)]))
    env.update(a1=env["a2"], own_k=env["d2"], sk=env["drl"], dx=env["do"])
    bufs = refs[len(names):]
    e = type("Refs", (), env)
    where = coords()
    z, y, c, x, d = where
    rows, width = e.g.shape
    ff = e.hd_i.shape[1]
    qrows = rows // 2
    pairs = width // 128
    tile = 256
    lrows = 128
    steps = width // tile
    quarters = (c, 3 - c)
    theirs = (1 - c, 2 + c)

    def at_quarter(k):
        return pl.ds(mult(k * qrows, qrows), qrows)

    entered = enter(Z * Y * C * X)

    loads = {}
    for k, (src, dst) in enumerate(
        (
            ("gw_i", "g"), ("a2_i", "a2"), ("r_i", "r"), ("vec_i", "vec"), ("wp_i", "wp"), ("at_i", "at"),
            ("qs_i", "qs"), ("ka_i", "ka"), ("va_i", "va"), ("lse_i", "lse"), ("xr_i", "xr"), ("wq_i", "wq"),
        )
    ):
        loads[dst] = pltpu.make_async_copy(env[src], env[dst], e.lsem.at[k])

    def tile_of(idx):
        block = idx // 3
        return (block % 2) * 2 * 3 + (block // 2) * 3 + idx % 3

    def tile_copies(idx):
        n = tile_of(idx)
        slot = idx % 2
        cut = pl.ds(mult(n * tile, tile), tile)
        return (
            pltpu.make_async_copy(e.wd_i.at[:, cut], e.wd_t.at[slot], e.tsem.at[0, slot]),
            pltpu.make_async_copy(e.gp_i.at[:, cut], e.gp_t.at[slot], e.tsem.at[1, slot]),
            pltpu.make_async_copy(e.hd_i.at[:, cut], e.hd_t.at[slot], e.tsem.at[2, slot]),
            pltpu.make_async_copy(e.wu_i.at[cut, :], e.wu_t.at[slot], e.tsem.at[3, slot]),
        )

    loads["g"].start()
    for cp in tile_copies(0):
        cp.start()
    loads["a2"].start()
    for name in ("r", "vec", "wp", "at", "qs", "ka", "va", "lse", "xr", "wq"):
        loads[name].start()

    def send_out(k):
        i, part = k // 4, k % 4
        some = qrows // 4
        same = jnp.logical_and(x == c, x == i)
        src = e.out_i.at[pl.ds(i * qrows + part * some, some)]
        dst = e.out_n.at[pl.ds(mult(((i + c) % 2) * qrows + part * some, some), some)]

        @pl.when(same)
        def _():
            lcopy(src, dst, e.msem.at[1]).start()

        @pl.when(jnp.logical_not(same))
        def _():
            rcopy(src, dst, e.msem.at[0], e.msem.at[1], dev(z, y, x, i)).start()

    grads = {"q": (e.gq, e.og_q), "p": (e.gp_, e.og_p), "u": (e.gu, e.og_u), "d": (e.gd, e.og_d)}
    chunks = []
    for k, (name, R, step, c0, cn, zlist, oc) in enumerate(reduce_shapes(width, ff)):
        grad, out = grads[name]
        chunks.append(Reduce(grad, R, step, c0, cn, zlist, bufs[5 * k:5 * k + 5], out, oc, e.rsem, k, where, KINDS_BACK[k], k in TURNED_BACK))
    parts = part_actions(PLAN)

    def after(part):
        for name, k in parts.get(part, ()):
            if name < len(chunks):
                ch = chunks[name]
                (ch.start, ch.tick2, ch.tick3, ch.tick4, ch.tick5, ch.tick6)[k - 1]()
            elif name == GIVE:
                give(k)
            elif name == OUT:
                send_out(k)
            else:
                land(k)
                if k < 4:
                    hop(k + 1)


    my_len = live_length(e.len_ref, e.deal_ref, (z * Y + y) * C + x)
    rowpos = lax.broadcasted_iota(jnp.int32, (lrows, 1), 0)
    loads["g"].wait()
    blank = jnp.zeros((1, width), F32)
    total_bd = blank
    for k in range(rows // lrows):
        base = quarters[k * lrows // qrows] * qrows + (k * lrows) % qrows
        live = base + rowpos < my_len
        part = jnp.where(live, e.g[k * lrows:(k + 1) * lrows, :], jnp.zeros((), BF))
        e.g[k * lrows:(k + 1) * lrows, :] = part
        e.gt[:, k * lrows:(k + 1) * lrows] = part.T
        total_bd = total_bd + jnp.sum(part.astype(F32), axis=0, keepdims=True)
    e.d2[...] = jnp.zeros_like(e.d2)
    loads["a2"].wait()

    ff_tiles = ff // tile
    def ffn(idx, carry, acting=True):
        slot = idx % 2
        n = tile_of(idx)
        cut = pl.ds(mult(n * tile, tile), tile)

        @pl.when(idx + 1 < ff_tiles)
        def _():
            for cp in tile_copies(idx + 1):
                cp.start()

        for cp in tile_copies(idx):
            cp.wait()
        du = (e.gp_t[slot].astype(F32) * dot_nn(e.g[...], e.wd_t[slot])).astype(BF)
        e.bub[n] = jnp.sum(du.astype(F32), axis=0, keepdims=True)
        e.gd[:, cut] = dot_nn(e.gt[...], e.hd_t[slot]).astype(BF)
        e.gu[cut, :] = dot_tn(du, e.a2[...]).astype(BF)
        e.d2[...] += dot_nn(du, e.wu_t[slot])
        for k in range(2, ff_tiles) if acting else ():
            if F2 + k - 2 in parts:
                @pl.when(idx == k)
                def _(k=k):
                    after(F2 + k - 2)

        return carry

    def ffn_first(idx, carry):
        return ffn(idx, carry, False)

    lax.fori_loop(0, 2, ffn_first, 0)

    entered()

    lax.fori_loop(2, ff_tiles, ffn, 0)

    loads["r"].wait()
    loads["vec"].wait()

    def norm_two(k, sums):
        at_rows = pl.ds(mult(k * lrows, lrows), lrows)
        n2, rstd = norm_parts(e.r[at_rows, :])
        da = e.d2[at_rows, :]
        ee = da * e.vec[G2:G2 + 1, :]
        gg = e.g[at_rows, :].astype(F32)
        m1 = jnp.mean(ee, axis=-1, keepdims=True)
        m2 = jnp.mean(ee * n2, axis=-1, keepdims=True)
        dr = gg + (ee - m1 - n2 * m2) * rstd
        e.dr[at_rows, :] = dr
        e.drl[at_rows, :] = dr.astype(BF)
        return (
            sums[0] + jnp.sum(da * n2, axis=0, keepdims=True),
            sums[1] + jnp.sum(da, axis=0, keepdims=True),
            sums[2] + jnp.sum(dr, axis=0, keepdims=True),
        )

    sum_g2, sum_c2, sum_bp = lax.fori_loop(0, rows // lrows, norm_two, (blank, blank, blank))

    after(NORM_TWO)

    loads["wp"].wait()
    loads["at"].wait()

    def proj_back(n, carry):
        cut = pl.ds(mult(n * tile, tile), tile)
        e.do[:, cut] = dot_nn(e.drl[...], e.wp[:, cut]).astype(BF)
        e.gp_[cut, :] = dot_tn(e.drl[:, cut], e.at[...]).astype(BF)
        return carry

    lax.fori_loop(0, steps, proj_back, 0)
    after(PROJ)

    for name in ("qs", "ka", "va", "lse"):
        loads[name].wait()
    lane = lax.broadcasted_iota(jnp.int32, (qrows, 128), 1)
    kpos = lax.broadcasted_iota(jnp.int32, (qrows, qrows), 0)
    qpos = lax.broadcasted_iota(jnp.int32, (qrows, qrows), 1)

    def split(v):
        zero = jnp.zeros_like(v)
        return jnp.where(lane < HEAD_DIM, v, zero), jnp.where(lane >= HEAD_DIM, v, zero)

    def pair_body(p, carry):
        lanes = pl.ds(mult(p * 128, 128), 128)
        e.dka[...] = jnp.zeros_like(e.dka)
        e.dva[...] = jnp.zeros_like(e.dva)
        for i in range(2):
            quarter = quarters[i]
            own = slice(i * qrows, (i + 1) * qrows)
            qp, dop = e.qs[own, lanes], e.do[own, lanes]
            qh, doh = split(qp), split(dop)
            qq, dd = jnp.concatenate(qh, axis=0), jnp.concatenate(doh, axis=0)
            prod = (dop.astype(F32) * e.at[own, lanes].astype(F32)).T
            delta = [jnp.sum(prod[h * HEAD_DIM:(h + 1) * HEAD_DIM], axis=0, keepdims=True) for h in range(2)]
            logs = [e.lse[p, i * 2 + h:i * 2 + h + 1, :] for h in range(2)]

            def keys(j, dq, diagonal=False):
                at_keys = pl.ds(mult(j * qrows, qrows), qrows)
                kj, vj = e.ka[at_keys, lanes], e.va[at_keys, lanes]
                kt = kj.T
                probs, grads_s, new = [], [], []
                for h in range(2):
                    s = dot_nt(kj, qh[h])
                    if diagonal:
                        s = jnp.where(kpos <= qpos, s, NEG_BIG)
                    pt = jnp.exp(s - logs[h])
                    ds = (pt * (dot_nt(vj, doh[h]) - delta[h])).astype(BF)
                    probs.append(pt.astype(BF))
                    grads_s.append(ds)
                    new.append(dq[h] + dot_nn(kt[h * HEAD_DIM:(h + 1) * HEAD_DIM], ds))
                e.dva[at_keys, :] += dot_nn(jnp.concatenate(probs, axis=1), dd)
                e.dka[at_keys, :] += dot_nn(jnp.concatenate(grads_s, axis=1), qq)
                return tuple(new)

            none = jnp.zeros((HEAD_DIM, qrows), F32)
            dq = lax.fori_loop(0, quarter, keys, (none, none))
            dq = keys(quarter, dq, True)
            e.dm[own, lanes] = (jnp.concatenate(dq, axis=0).T * HEAD_DIM ** -0.5).astype(BF)
            for k in range(pairs):
                if A00 + 2 * k + i in parts:
                    @pl.when(p == k)
                    def _(k=k, i=i):
                        after(A00 + 2 * k + i)

        for i in range(2):
            own = slice(i * qrows, (i + 1) * qrows)
            e.own_k[own, lanes] = e.dka[at_quarter(quarters[i]), :]
            e.own_v[own, lanes] = e.dva[at_quarter(quarters[i]), :]
            e.sk[own, lanes] = e.dka[at_quarter(theirs[i]), :].astype(BF)
            e.sv[own, lanes] = e.dva[at_quarter(theirs[i]), :].astype(BF)
        for k in range(pairs // 2):
            @pl.when(p == 2 * k + 1)
            def _(k=k):
                cut = slice(2 * k * 128, (2 * k + 2) * 128)
                for src, dst, s in ((e.sk, e.rk, 2), (e.sv, e.rv, 4)):
                    rcopy(
                        src.at[:, cut], dst.at[:, cut], e.msem.at[s], e.msem.at[s + 1], dev(z, y, 1 - c, x)
                    ).start()
        return carry

    lax.fori_loop(0, pairs, pair_body, 0)

    loads["xr"].wait()

    def norm_one(k, carry):
        at_rows = pl.ds(mult(k * lrows, lrows), lrows)
        n1, _ = norm_parts(e.xr[at_rows, :].astype(F32))
        e.a1[at_rows, :] = (n1 * e.vec[G1:G1 + 1, :] + e.vec[C1:C1 + 1, :]).astype(BF)
        return carry

    lax.fori_loop(0, rows // lrows, norm_one, 0)
    after(NORM_ONE)

    def qkv_grad(n, carry):
        cut = pl.ds(mult(n * tile, tile), tile)
        e.gq[cut, :] = dot_tn(e.dm[:, cut], e.a1[...]).astype(BF)
        return carry

    lax.fori_loop(0, 3, qkv_grad, 0)
    after(QA)
    wait_bytes(e.rk, e.msem.at[3])
    wait_bytes(e.rv, e.msem.at[5])
    for part, (mine, got) in enumerate(((e.own_k, e.rk), (e.own_v, e.rv))):
        def merge(k, carry, part=part, mine=mine, got=got):
            at_rows = pl.ds(mult(k * lrows, lrows), lrows)
            e.dm[at_rows, (part + 1) * width:(part + 2) * width] = (
                mine[at_rows, :] + got[at_rows, :].astype(F32)
            ).astype(BF)
            return carry

        lax.fori_loop(0, rows // lrows, merge, 0)
    after(MERGE)
    for name, first, stop in ((QB, 3, 5), (QC, 5, 7), (QD, 7, 9)):
        lax.fori_loop(first, stop, qkv_grad, 0)
        after(name)
    loads["wq"].wait()

    def input_back(n, carry):
        cut = pl.ds(mult(n * tile, tile), tile)
        e.d2[:, cut] = dot_nn(e.dm[...], e.wq[:, cut])
        return carry

    lax.fori_loop(0, steps, input_back, 0)
    after(DA)

    def norm_one_back(k, sums):
        at_rows = pl.ds(mult(k * lrows, lrows), lrows)
        n1, rstd = norm_parts(e.xr[at_rows, :].astype(F32))
        da = e.d2[at_rows, :]
        ee = da * e.vec[G1:G1 + 1, :]
        m1 = jnp.mean(ee, axis=-1, keepdims=True)
        m2 = jnp.mean(ee * n1, axis=-1, keepdims=True)
        e.dx[at_rows, :] = (e.dr[at_rows, :] + (ee - m1 - n1 * m2) * rstd).astype(BF)
        return sums[0] + jnp.sum(da * n1, axis=0, keepdims=True), sums[1] + jnp.sum(da, axis=0, keepdims=True)

    sum_g1, sum_c1 = lax.fori_loop(0, rows // lrows, norm_one_back, (blank, blank))

    e.vs[0] = jnp.zeros_like(e.vs[0])
    for row, value in ((G1, sum_g1), (C1, sum_c1), (BP, sum_bp), (G2, sum_g2), (C2, sum_c2), (BD, total_bd)):
        e.vs[0, row:row + 1, :] = value
    per = width // tile
    for k in range(ff_tiles):
        e.vs[0, BU + k // per:BU + k // per + 1, (k % per) * tile:(k % per + 1) * tile] = e.bub[k]
    hops = (
        dev(z, y, 1 - c, x), dev(z, y, c, 1 - x), dev(z, 1 - y, c, x),
        dev(z + 1 - 2 * (z % 2), y, c, x), dev((z + 2) % 4, y, c, x),
    )

    def hop(k):
        rcopy(e.vs.at[k], e.vr.at[k], e.vsem.at[0, k], e.vsem.at[1, k], hops[k]).start()

    def land(k):
        wait_bytes(e.vr.at[k], e.vsem.at[1, k])
        e.vs[k + 1] = e.vs[k] + e.vr[k]

    hop(0)

    small = e.ret.shape[1]
    per_quarter = qrows // small
    slot = (z * Y + y) * C + x

    def give_back(k, carry):
        i = (k + x) % 2
        e8 = (k // 2 + d) % per_quarter
        td = ((i + c) % 2) * per_quarter + e8
        src = e.dx.at[pl.ds(mult(i * qrows + e8 * small, small), small)]
        mine = jnp.logical_and(td == d, x == i)

        @pl.when(mine)
        def _():
            lcopy(src, e.ret.at[slot], e.msem.at[7]).start()

        @pl.when(jnp.logical_not(mine))
        def _():
            rcopy(src, e.ret.at[slot], e.msem.at[6], e.msem.at[7], {"dp": td, "cp": i}).start()

        return carry

    share = per_quarter // 2

    def give(k):
        lax.fori_loop(k * share, (k + 1) * share, give_back, 0)

    after(LN)
    own = width // (Z * Y * C)
    e.osum[0:6, :] = pltpu.roll(e.vs[5, 0:6, :], (width - d * own) % width, 1)[:, :tile]
    long = ff // (Z * Y * C)
    per_row = width // long
    e.osum[6:7, :] = pltpu.roll(
        e.vs[5, pl.ds(BU + d // per_row, 1), :], (width - (d % per_row) * long) % width, 1
    )[:, :tile]
    e.osum[7:8, :] = jnp.zeros((1, tile), F32)
    wait_bytes(e.dx, e.msem.at[7])

    for ch in chunks:
        ch.drain()
    for k in range(5):
        wait_bytes(e.vr.at[k], e.vsem.at[0, k])
    wait_bytes(e.rk, e.msem.at[2])
    wait_bytes(e.rv, e.msem.at[4])

    @pl.when((x + c) % 2 == d // per_quarter)
    def _():
        wait_bytes(e.dx.at[pl.ds(0, rows - small)], e.msem.at[6])

    @pl.when((x + c) % 2 != d // per_quarter)
    def _():
        wait_bytes(e.dx, e.msem.at[6])

    @pl.when(c == x)
    def _():
        wait_bytes(e.dx.at[pl.ds(0, qrows)], e.msem.at[0])

    @pl.when(c != x)
    def _():
        wait_bytes(e.dx, e.msem.at[0])

    wait_bytes(e.dx, e.msem.at[1])


def backward(lengths, dealing, saved, shards):
    wq, wp, wu, wd, xr, gw, qs, ka, va, at, lse, r, a2, hd, gp, vec, outw = saved
    rows, width = xr.shape
    ff = hd.shape[1]
    n = Z * Y * C
    keys = ka.shape[0]
    small = rows // n
    pairs = width // 128

    def arr(shape, dtype=BF):
        return jax.ShapeDtypeStruct(shape, dtype)

    outs = [arr(s.shape, F32) for s in shards] + [
        arr((8, 256), F32), arr((n, small, width)), arr((rows, width)),
    ]
    vm = pltpu.VMEM
    acts = vm((rows, width), BF)
    acts32 = vm((rows, width), F32)
    scratch = [
        vm(wq.shape, BF), vm(wp.shape, BF), acts, acts, acts, vm(ka.shape, BF), vm(va.shape, BF), acts,
        vm(lse.shape, F32), acts32, acts, vm(vec.shape, F32), vm((width, rows), BF), acts32, acts32, acts, acts,
        vm(wq.shape, BF), vm(wp.shape, BF), vm(wu.shape, BF), vm(wd.shape, BF),
        vm((2, width, 256), BF), vm((2, 256, width), BF), vm((2, rows, 256), BF), vm((2, rows, 256), BF),
        vm((keys, 128), F32), vm((keys, 128), F32),
        acts32, acts, acts, acts, vm((rows, 3 * width), BF),
        vm((6, 16, width), F32), vm((5, 16, width), F32), vm((ff // 256, 1, 256), F32),
        pltpu.SemaphoreType.DMA((12,)), pltpu.SemaphoreType.DMA((4, 2)), pltpu.SemaphoreType.DMA((13, 10)),
        pltpu.SemaphoreType.DMA((8,)), pltpu.SemaphoreType.DMA((2, 5)),
    ]
    for kind, (_, R, _, _, cn, zlist, _) in zip(KINDS_BACK, reduce_shapes(width, ff)):
        k = len(zlist)
        last = (1, 4, 2) if kind == 2 else (k, 2, 1)
        scratch += [vm((2 * k, 2, R, cn), BF)] + [vm((m, R, cn), BF) for m in (2 * k,) + last]
    anyspec = pl.BlockSpec(memory_space=pl.ANY)
    smem = pl.BlockSpec(memory_space=pltpu.SMEM)
    vmem = pl.BlockSpec(memory_space=pltpu.VMEM)
    return pl.pallas_call(
        backward_kernel,
        out_shape=outs,
        in_specs=[smem, smem] + [anyspec] * len(saved),
        out_specs=[vmem] * 5 + [anyspec] * 2,
        scratch_shapes=scratch,
        compiler_params=pltpu.CompilerParams(
            collective_id=1, has_side_effects=True, vmem_limit_bytes=67043328
        ),
        name="backward",
    )(lengths, dealing, *saved)


def finish_kernel(deal_ref, gq, gp, gu, gd, sums, ret, out, grad_o, out_o, gq_o, gp_o, gu_o, gd_o, *rows_o):
    for s in range(ret.shape[0]):
        grad_o[s] = ret[deal_ref[s]]
    for src, dst in ((out, out_o), (gq, gq_o), (gp, gp_o), (gu, gu_o), (gd, gd_o)):
        dst[...] = src[...]
    for k, row in enumerate(rows_o):
        row[...] = sums[k:k + 1, :row.shape[1]]


def finish(dealing, grads, sums, ret, out, own, long):
    def like(a):
        return jax.ShapeDtypeStruct(a.shape, a.dtype)

    outs = [like(ret), like(out)] + [like(g) for g in grads]
    outs += [jax.ShapeDtypeStruct((1, own), F32)] * 6 + [jax.ShapeDtypeStruct((1, long), F32)]
    vmem = pl.BlockSpec(memory_space=pltpu.VMEM)
    return pl.pallas_call(
        finish_kernel,
        out_shape=outs,
        in_specs=[pl.BlockSpec(memory_space=pltpu.SMEM)] + [vmem] * 7,
        out_specs=[vmem] * len(outs),
        name="finish",
    )(dealing, *grads, sums, ret, out)


def slice_plan(
    x_source, cotangent, lengths, dealing, qkv_weight, proj_weight, up_weight, down_weight,
    first_gain, first_shift, proj_bias, second_gain, second_shift, up_bias, down_bias,
):
    shards = [w.T for w in (qkv_weight, proj_weight, up_weight, down_weight)]
    vectors = [
        v[None] for v in (first_gain, first_shift, proj_bias, second_gain, second_shift, down_bias, up_bias)
    ]
    saved = forward(lengths, dealing, cotangent[0], x_source, shards, vectors)
    gq, gp, gu, gd, sums, ret, out = backward(lengths, dealing, saved, shards)
    done = finish(dealing, (gq, gp, gu, gd), sums, ret, out, first_gain.shape[0], up_bias.shape[0])
    input_grad, output, gq, gp, gu, gd = done[:6]
    by_row = [v.reshape(-1) for v in done[6:]]
    return (
        output[None], input_grad, gq.T, gp.T, gu.T, gd.T,
        by_row[G1], by_row[C1], by_row[BP], by_row[G2], by_row[C2], by_row[6], by_row[BD],
    )


def layer_norm(values, scaling, offset):
    centered = values - jnp.mean(values, axis=-1, keepdims=True)
    spread = jnp.mean(centered * centered, axis=-1, keepdims=True)
    return centered * lax.rsqrt(spread + EPSILON) * scaling + offset


def gelu_tanh(values):
    return (
        0.5
        * values
        * (1.0 + jnp.tanh(TANH_SCALE * (values + CUBIC_TERM * values * values * values)))
    )


def grouped(array, block_seqs):
    return array.reshape(
        (array.shape[0] // block_seqs, block_seqs, array.shape[1], HEADS, array.shape[2] // HEADS)
    )


def grouped_stats(array, block_seqs):
    return array.reshape((array.shape[0] // block_seqs, block_seqs) + array.shape[1:])


def joined(array):
    return array.reshape(
        (array.shape[0] * array.shape[1], array.shape[2], array.shape[3] * array.shape[4])
    )


def masked_scores(queries, key_rows, query_start, score_scale):
    scores = (
        jnp.einsum("bqhd,bkhd->bhqk", queries, key_rows, preferred_element_type=jnp.float32)
        * score_scale
    )
    query_pos = query_start + jnp.arange(queries.shape[1])
    key_pos = jnp.arange(key_rows.shape[1])
    return jnp.where(key_pos[None, :] <= query_pos[:, None], scores, NEG_BIG)


def attend(inputs, query_start, score_scale):
    queries, key_rows, val_rows = inputs
    scores = masked_scores(queries, key_rows, query_start, score_scale)
    row_top = jnp.max(scores, axis=-1, keepdims=True)
    exponent = jnp.exp(scores - row_top)
    totals = jnp.sum(exponent, axis=-1, keepdims=True)
    weights = (exponent / totals).astype(jnp.bfloat16)
    attended = jnp.einsum("bhqk,bkhd->bqhd", weights, val_rows, preferred_element_type=jnp.float32)
    return (attended.astype(jnp.bfloat16), (row_top + jnp.log(totals))[..., 0])


def rows_back(inputs, query_start, score_scale):
    queries, key_rows, val_rows, grad_rows, log_total = inputs
    scores = masked_scores(queries, key_rows, query_start, score_scale)
    weights = jnp.exp(scores - log_total[..., None])
    grad_weights = jnp.einsum(
        "bqhd,bkhd->bhqk", grad_rows, val_rows, preferred_element_type=jnp.float32
    )
    delta_rows = jnp.sum(weights * grad_weights, axis=-1)
    grad_scores = (weights * (grad_weights - delta_rows[..., None])).astype(jnp.bfloat16)
    grad_query = (
        jnp.einsum("bhqk,bkhd->bqhd", grad_scores, key_rows, preferred_element_type=jnp.float32)
        * score_scale
    )
    grad_keys = (
        jnp.einsum("bhqk,bqhd->bkhd", grad_scores, queries, preferred_element_type=jnp.float32)
        * score_scale
    )
    grad_vals = jnp.einsum(
        "bhqk,bqhd->bkhd",
        weights.astype(jnp.bfloat16),
        grad_rows,
        preferred_element_type=jnp.float32,
    )
    return (grad_query, grad_keys, grad_vals)


def fetch_weights(
    qkv_weight,
    proj_weight,
    up_weight,
    down_weight,
    first_gain,
    first_shift,
    proj_bias,
    second_gain,
    second_shift,
    up_bias,
    down_bias,
):
    qkv_part, proj_part, up_part, down_part = (
        lax.all_gather(qkv_weight.astype(jnp.bfloat16), "cp", axis=0, tiled=True),
        lax.all_gather(proj_weight.astype(jnp.bfloat16), "cp", axis=0, tiled=True),
        lax.all_gather(up_weight.astype(jnp.bfloat16), "cp", axis=0, tiled=True),
        lax.all_gather(down_weight.astype(jnp.bfloat16), "cp", axis=0, tiled=True),
    )
    return (
        lax.all_gather(qkv_part, "dp", axis=1, tiled=True),
        lax.all_gather(proj_part, "dp", axis=1, tiled=True),
        lax.all_gather(up_part, "dp", axis=1, tiled=True),
        lax.all_gather(down_part, "dp", axis=1, tiled=True),
        lax.all_gather(first_gain.astype(jnp.bfloat16), "dp", axis=0, tiled=True),
        lax.all_gather(first_shift.astype(jnp.bfloat16), "dp", axis=0, tiled=True),
        lax.all_gather(proj_bias.astype(jnp.bfloat16), "dp", axis=0, tiled=True),
        lax.all_gather(second_gain.astype(jnp.bfloat16), "dp", axis=0, tiled=True),
        lax.all_gather(second_shift.astype(jnp.bfloat16), "dp", axis=0, tiled=True),
        lax.all_gather(up_bias.astype(jnp.bfloat16), "dp", axis=0, tiled=True),
        lax.all_gather(down_bias.astype(jnp.bfloat16), "dp", axis=0, tiled=True),
    )


def mat_rows(left, right):
    return jnp.einsum("sqd,de->sqe", left, right, preferred_element_type=jnp.float32)


def mat_back(left, right):
    return jnp.einsum("sqe,de->sqd", left, right, preferred_element_type=jnp.float32)


def mat_grad(left, right):
    return jnp.einsum("sqd,sqe->de", left, right, preferred_element_type=jnp.float32)


def general(
    x_source,
    cotangent,
    lengths,
    dealing,
    qkv_weight,
    proj_weight,
    up_weight,
    down_weight,
    first_gain,
    first_shift,
    proj_bias,
    second_gain,
    second_shift,
    up_bias,
    down_bias,
):
    groups = lax.axis_size("dp")
    seqs_all, piece_rows, features = x_source.shape
    seq_group = seqs_all // groups
    span_rows = groups * piece_rows
    score_scale = HEAD_DIM ** (-0.5)
    block_seqs = math.gcd(seq_group, max(1, 512 // span_rows))
    owners = jnp.argsort(dealing)
    send_order = owners.reshape(groups, seq_group).T.reshape(-1)
    outgoing = x_source[send_order].reshape(seq_group, span_rows, features)
    arrived = lax.all_to_all(outgoing, "dp", split_axis=1, concat_axis=1, tiled=True)
    first_slot = lax.axis_index("dp") * seq_group
    my_lengths = lax.dynamic_slice_in_dim(lengths[owners], first_slot, seq_group)
    query_start = lax.axis_index("cp") * span_rows
    positions = query_start + jnp.arange(span_rows)
    live_rows = positions[None, :] < my_lengths[:, None]
    fetched = fetch_weights(
        qkv_weight,
        proj_weight,
        up_weight,
        down_weight,
        first_gain,
        first_shift,
        proj_bias,
        second_gain,
        second_shift,
        up_bias,
        down_bias,
    )
    qkv_full, proj_full, up_full, down_full = (fetched[0], fetched[1], fetched[2], fetched[3])
    gain_one, shift_one, bias_proj, gain_two, shift_two, bias_up, bias_down = [
        vector.astype(jnp.float32) for vector in fetched[4:]
    ]
    inputs_f = arrived.astype(jnp.float32)
    norm_one, back_one = jax.vjp(layer_norm, inputs_f, gain_one, shift_one)
    act_one = norm_one.astype(jnp.bfloat16)
    mixed_rows = mat_rows(act_one, qkv_full).astype(jnp.bfloat16)
    queries = mixed_rows[..., :features]
    kv_local = mixed_rows[..., features:]
    kv_all = lax.all_gather(kv_local, "cp", axis=1, tiled=True)
    attended, log_total = lax.map(
        lambda inputs: attend(inputs, query_start, score_scale),
        (
            grouped(queries, block_seqs),
            grouped(kv_all[..., :features], block_seqs),
            grouped(kv_all[..., features:], block_seqs),
        ),
    )
    attended = joined(attended)
    log_total = log_total.reshape((seq_group,) + log_total.shape[2:])
    residual = inputs_f + mat_rows(attended, proj_full) + bias_proj
    norm_two, back_two = jax.vjp(layer_norm, residual, gain_two, shift_two)
    act_two = norm_two.astype(jnp.bfloat16)
    up_raw = mat_rows(act_two, up_full) + bias_up
    hidden, back_gelu = jax.vjp(gelu_tanh, up_raw)
    hid_low = hidden.astype(jnp.bfloat16)
    result = residual + mat_rows(hid_low, down_full) + bias_down
    output = jnp.where(live_rows[..., None], result, 0.0).astype(jnp.bfloat16)
    fetched = fetch_weights(
        qkv_weight,
        proj_weight,
        up_weight,
        down_weight,
        first_gain,
        first_shift,
        proj_bias,
        second_gain,
        second_shift,
        up_bias,
        down_bias,
    )
    qkv_full, proj_full, up_full, down_full = (fetched[0], fetched[1], fetched[2], fetched[3])
    gain_one, gain_two = (fetched[4].astype(jnp.float32), fetched[7].astype(jnp.float32))
    grad_out = jnp.where(live_rows[..., None], cotangent.astype(jnp.float32), 0.0)
    grad_low = grad_out.astype(jnp.bfloat16)
    grad_down = mat_grad(hid_low, grad_low)
    grad_bias_down = jnp.sum(grad_out, axis=(0, 1))
    grad_hidden = mat_back(grad_low, down_full)
    grad_up_raw = back_gelu(grad_hidden)[0].astype(jnp.bfloat16)
    grad_up = mat_grad(act_two, grad_up_raw)
    grad_bias_up = jnp.sum(grad_up_raw.astype(jnp.float32), axis=(0, 1))
    grad_act_two = mat_back(grad_up_raw, up_full)
    grad_resid, grad_gain_two, grad_shift_two = back_two(grad_act_two)
    grad_resid = grad_resid + grad_out
    grad_bias_proj = jnp.sum(grad_resid, axis=(0, 1))
    resid_low = grad_resid.astype(jnp.bfloat16)
    grad_proj = mat_grad(attended, resid_low)
    grad_attended = mat_back(resid_low, proj_full).astype(jnp.bfloat16)
    kv_back = lax.all_gather(kv_local, "cp", axis=1, tiled=True)
    key_rows = kv_back[..., :features]
    val_rows = kv_back[..., features:]
    grad_query, grad_keys, grad_vals = lax.map(
        lambda inputs: rows_back(inputs, query_start, score_scale),
        (
            grouped(queries, block_seqs),
            grouped(key_rows, block_seqs),
            grouped(val_rows, block_seqs),
            grouped(grad_attended, block_seqs),
            grouped_stats(log_total, block_seqs),
        ),
    )
    grad_keys, grad_vals = (
        lax.psum_scatter(
            joined(grad_keys).astype(jnp.bfloat16), "cp", scatter_dimension=1, tiled=True
        ).astype(jnp.float32),
        lax.psum_scatter(
            joined(grad_vals).astype(jnp.bfloat16), "cp", scatter_dimension=1, tiled=True
        ).astype(jnp.float32),
    )
    grad_mixed = jnp.concatenate([joined(grad_query), grad_keys, grad_vals], axis=-1).astype(
        jnp.bfloat16
    )
    grad_qkv = mat_grad(act_one, grad_mixed)
    grad_act_one = mat_back(grad_mixed, qkv_full)
    grad_input, grad_gain_one, grad_shift_one = back_one(grad_act_one)
    grad_input = (grad_input + grad_resid).astype(jnp.bfloat16)
    returned = lax.all_to_all(grad_input, "dp", split_axis=1, concat_axis=0, tiled=True)
    input_grad = returned[dealing]
    (
        grad_qkv,
        grad_proj,
        grad_up,
        grad_down,
        grad_gain_one,
        grad_shift_one,
        grad_bias_proj,
        grad_gain_two,
        grad_shift_two,
        grad_bias_up,
        grad_bias_down,
    ) = (
        lax.psum_scatter(
            grad_qkv.astype(jnp.bfloat16), "dp", scatter_dimension=1, tiled=True
        ).astype(jnp.float32),
        lax.psum_scatter(
            grad_proj.astype(jnp.bfloat16), "dp", scatter_dimension=1, tiled=True
        ).astype(jnp.float32),
        lax.psum_scatter(
            grad_up.astype(jnp.bfloat16), "dp", scatter_dimension=1, tiled=True
        ).astype(jnp.float32),
        lax.psum_scatter(
            grad_down.astype(jnp.bfloat16), "dp", scatter_dimension=1, tiled=True
        ).astype(jnp.float32),
        lax.psum_scatter(
            grad_gain_one.astype(jnp.bfloat16), "dp", scatter_dimension=0, tiled=True
        ).astype(jnp.float32),
        lax.psum_scatter(
            grad_shift_one.astype(jnp.bfloat16), "dp", scatter_dimension=0, tiled=True
        ).astype(jnp.float32),
        lax.psum_scatter(
            grad_bias_proj.astype(jnp.bfloat16), "dp", scatter_dimension=0, tiled=True
        ).astype(jnp.float32),
        lax.psum_scatter(
            grad_gain_two.astype(jnp.bfloat16), "dp", scatter_dimension=0, tiled=True
        ).astype(jnp.float32),
        lax.psum_scatter(
            grad_shift_two.astype(jnp.bfloat16), "dp", scatter_dimension=0, tiled=True
        ).astype(jnp.float32),
        lax.psum_scatter(
            grad_bias_up.astype(jnp.bfloat16), "dp", scatter_dimension=0, tiled=True
        ).astype(jnp.float32),
        lax.psum_scatter(
            grad_bias_down.astype(jnp.bfloat16), "dp", scatter_dimension=0, tiled=True
        ).astype(jnp.float32),
    )
    grad_qkv, grad_proj, grad_up, grad_down = (
        lax.psum_scatter(
            grad_qkv.astype(jnp.bfloat16), "cp", scatter_dimension=0, tiled=True
        ).astype(jnp.float32),
        lax.psum_scatter(
            grad_proj.astype(jnp.bfloat16), "cp", scatter_dimension=0, tiled=True
        ).astype(jnp.float32),
        lax.psum_scatter(
            grad_up.astype(jnp.bfloat16), "cp", scatter_dimension=0, tiled=True
        ).astype(jnp.float32),
        lax.psum_scatter(
            grad_down.astype(jnp.bfloat16), "cp", scatter_dimension=0, tiled=True
        ).astype(jnp.float32),
    )
    (
        grad_gain_one,
        grad_shift_one,
        grad_bias_proj,
        grad_gain_two,
        grad_shift_two,
        grad_bias_up,
        grad_bias_down,
    ) = lax.psum(
        (
            grad_gain_one,
            grad_shift_one,
            grad_bias_proj,
            grad_gain_two,
            grad_shift_two,
            grad_bias_up,
            grad_bias_down,
        ),
        "cp",
    )
    return (
        output,
        input_grad,
        grad_qkv,
        grad_proj,
        grad_up,
        grad_down,
        grad_gain_one,
        grad_shift_one,
        grad_bias_proj,
        grad_gain_two,
        grad_shift_two,
        grad_bias_up,
        grad_bias_down,
    )


def solution(mesh):
    in_specs = (
        P(None, ("cp", "dp"), None),
        P("dp", "cp", None),
        P(),
        P(),
        P("cp", "dp"),
        P("cp", "dp"),
        P("cp", "dp"),
        P("cp", "dp"),
        P("dp"),
        P("dp"),
        P("dp"),
        P("dp"),
        P("dp"),
        P("dp"),
        P("dp"),
    )
    out_specs = (
        P("dp", "cp", None),
        P(None, ("cp", "dp"), None),
        P("cp", "dp"),
        P("cp", "dp"),
        P("cp", "dp"),
        P("cp", "dp"),
        P("dp"),
        P("dp"),
        P("dp"),
        P("dp"),
        P("dp"),
        P("dp"),
        P("dp"),
    )
    planned = tuple(mesh.shape.items()) == (("dp", Z * Y * C), ("cp", X))
    local = slice_plan if planned else general
    return jax.shard_map(local, mesh=mesh, in_specs=in_specs, out_specs=out_specs, check_vma=False)
```
